128 devices in a mesh: gx: 2 (over core), gy: 4 (over x), gz: 16 (over z, y).
Axes of the slice: x: 4, y: 4, z: 4, core: 2. Of those that a mesh axis runs over, the one named last changes fastest.
Arguments:
- right_side: float32 [96, 192, 768], P('gx', 'gy', 'gz'), may hold values from -6 to 6
- start_guess: float32 [96, 192, 768], P('gx', 'gy', 'gz'), may hold values from -3 to 3
- reaction: float32 [96, 192, 768], P('gx', 'gy', 'gz'), may hold values from 0.0005 to 0.005
Outputs:
- solution_field: float32 [96, 192, 768], P('gx', 'gy', 'gz')
- residual: float32 [96, 192, 768], P('gx', 'gy', 'gz')
The draws below stay inside these ranges and needn't reach their ends.
All inputs are finite; a program needn't handle non-finite values.
Results may differ from the reference program's by a relative error of at most 0.0003.
Values sent between devices are 32-bit elements.
No kernel may reach another device: no remote copies, remote signals or barrier semaphores. Data moves between devices by JAX's collectives and lax.ppermute only.
A program may use at most 128 MiB of HBM per device.

```python
import math
import jax
import jax.numpy as jnp

LEVELS = 5
BOTTOM_ITERS = 6
NX = 96
NY = 192
NZ = 768


def block_scale(rng, shape, cuts, low, largest):
    def one(axis_at, parts):
        heights = jax.random.uniform(jax.random.fold_in(jax.random.fold_in(rng, 6), axis_at), (parts,), jnp.float32, low / len(cuts), largest / len(cuts))
        return jnp.repeat(jnp.exp(heights), shape[axis_at] // parts).reshape((-1,) + (1,) * (len(shape) - axis_at - 1))

    gain = one(*cuts[0])
    for cut in cuts[1:]:
        gain = gain * one(*cut)
    return gain


def scatter_about(own_key, extent, scale, bound, shards=(), dtype=jnp.bfloat16):
    values = jax.random.normal(own_key, extent, jnp.float32) * scale
    if len(shards) > 0:
        values = block_scale(own_key, extent, shards, -0.22, 0.18) * values
    return jnp.clip(values, min=-bound, max=bound).astype(dtype)


def setup_inputs(seed: int = 0) -> dict:
    key_list = jax.random.split(jax.random.key(seed), 4)
    right_side = scatter_about(key_list[0], (NX, NY, NZ), 1.0, 6.0, ((0, 2), (1, 4), (2, 16)), jnp.float32)
    start_guess = scatter_about(key_list[1], (NX, NY, NZ), 0.2, 3.0, ((0, 2), (1, 4), (2, 16)), jnp.float32)
    reaction = jnp.clip(jnp.exp(math.log(0.005) - 2.30258502 * jax.random.uniform(key_list[2], (NX, NY, NZ), jnp.float32) ** block_scale(key_list[2], (NX, NY, NZ), ((0, 2), (1, 4), (2, 16)), -0.2, 0.2)), 0.0005, 0.005)
    return {"right_side": right_side, "start_guess": start_guess, "reaction": reaction}


damping = 6.0 / 7.0


def operate(values, shifted, factor):
    padded = jnp.pad(values, 1)
    beside = padded[2:, 1:-1, 1:-1] + padded[:-2, 1:-1, 1:-1]
    beside = beside + padded[1:-1, 2:, 1:-1] + padded[1:-1, :-2, 1:-1]
    beside = beside + padded[1:-1, 1:-1, 2:] + padded[1:-1, 1:-1, :-2]
    return factor * (6.0 * values - beside) + shifted * values


def coarsen(values):
    size_x, size_y, size_z = values.shape
    blocks = values.reshape(size_x // 2, 2, size_y // 2, 2, size_z // 2, 2)
    return jnp.mean(blocks, axis=(1, 3, 5))


def refine(values):
    size_x, size_y, size_z = values.shape
    spread = jnp.broadcast_to(values[:, None, :, None, :, None], (size_x, 2, size_y, 2, size_z, 2))
    return spread.reshape(2 * size_x, 2 * size_y, 2 * size_z)


def smooth_once(estimate, source, shifted, factor):
    return estimate + damping * (source - operate(estimate, shifted, factor)) / (6.0 * factor + shifted)


def bottom(source, shifted, factor):
    estimate = jnp.zeros_like(source)
    leftover = source
    direction = source
    norm_now = jnp.sum(leftover * leftover)
    for repeat_index in range(BOTTOM_ITERS):
        applied = operate(direction, shifted, factor)
        step_length = norm_now / jnp.sum(direction * applied)
        estimate = estimate + step_length * direction
        leftover = leftover - step_length * applied
        norm_next = jnp.sum(leftover * leftover)
        direction = leftover + (norm_next / norm_now) * direction
        norm_now = norm_next
    return estimate


def vcycle_level(source, shifts, depth_index):
    factor = 0.25 ** depth_index
    shifted = shifts[depth_index]
    if depth_index == LEVELS - 1:
        return bottom(source, shifted, factor)
    estimate = damping * source / (6.0 * factor + shifted)
    estimate = smooth_once(estimate, source, shifted, factor)
    leftover = source - operate(estimate, shifted, factor)
    estimate = estimate + refine(vcycle_level(coarsen(leftover), shifts, depth_index + 1))
    estimate = smooth_once(estimate, source, shifted, factor)
    estimate = smooth_once(estimate, source, shifted, factor)
    return estimate


def reference(right_side, start_guess, reaction):
    shifts = [reaction]
    for depth_index in range(LEVELS - 1):
        shifts.append(coarsen(shifts[-1]))
    start_residual = right_side - operate(start_guess, reaction, 1.0)
    precond = vcycle_level(start_residual, shifts, 0)
    upper = jnp.sum(start_residual * precond)
    applied = operate(precond, reaction, 1.0)
    step_length = upper / jnp.sum(precond * applied)
    solution_field = start_guess + step_length * precond
    residual = start_residual - step_length * applied
    return solution_field, residual
```

```python
import functools
import jax
import jax.numpy as jnp
from jax import lax
from jax.experimental import pallas as pl
from jax.experimental.pallas import tpu as pltpu
from jax.sharding import PartitionSpec as P

W = 6.0 / 7.0
BOTTOM_ITERS = 6
N0 = 48
F32 = jnp.float32
HI = lax.Precision.HIGHEST
LIMIT = 56 * 1024 * 1024


class Spec:
    def __init__(self, n, h, na, gp, r0, R, hx):
        self.n, self.h, self.na, self.gp, self.r0, self.R, self.hx = n, h, na, gp, r0, R, hx
        self.lw = 128 // gp
        self.zshape = (n // gp, n, 128)
        self.yrows = -(-na * h // 8) * 8
        self.yshape = (n // 2, self.yrows, 128)
        self.xshape = (hx, na, R, 128)
        self.nx = n + hx


L0 = Spec(48, 5, 3, 8, 8, 64, 6)
L1 = Spec(24, 12, 2, 4, 16, 56, 12)


def sds(*shape):
    return jax.ShapeDtypeStruct(shape, F32)


def run(kernel, outs, args, scratch=()):
    smem = pl.BlockSpec(memory_space=pltpu.SMEM)
    vmem = pl.BlockSpec(memory_space=pltpu.VMEM)
    specs = [smem if a.dtype == jnp.int32 else vmem for a in args]
    return pl.pallas_call(
        kernel,
        out_shape=outs,
        in_specs=specs,
        out_specs=jax.tree.map(lambda _: vmem, outs),
        scratch_shapes=[pltpu.VMEM(s, F32) for s in scratch],
        compiler_params=pltpu.CompilerParams(vmem_limit_bytes=LIMIT),
    )(*args)


def lanes(rows):
    return lax.broadcasted_iota(jnp.int32, (rows, 128), 1)


def roll(v, shift, axis):
    if isinstance(shift, int):
        shift = shift % v.shape[axis]
        if shift == 0:
            return v
    return pltpu.roll(v, shift, axis)


def loop(n, f):
    lax.fori_loop(0, n, lambda i, c: (f(i), c)[1], 0)


def widen(dst, src, rows=N0):
    def one(x):
        dst[x, :, :] = jnp.zeros(dst.shape[1:], F32)
        dst[x, :, 0:rows] = src[x]

    loop(src.shape[0], one)


def zpack(sp, get, hi_ref, lo_ref):
    ln = lanes(sp.n)

    def group(g):
        hi = jnp.zeros((sp.n, 128), F32)
        lo = hi
        for j in range(sp.gp):
            for a in range(sp.na):
                v = get(g * sp.gp + j, a, 0, sp.n)
                at = sp.lw * j + sp.h * a
                here = (ln >= at) & (ln < at + sp.h)
                hi = jnp.where(here, roll(v, at - (sp.n - sp.h), 1), hi)
                lo = jnp.where(here, roll(v, at, 1), lo)
        hi_ref[g] = hi
        lo_ref[g] = lo

    loop(sp.n // sp.gp, group)


def ypack(sp, get, zl, zh, up_ref, dn_ref):
    n, h = sp.n, sp.h
    up0 = (n - h) // 8 * 8
    dn1 = -(-h // 8) * 8

    def fold(x, g, j, a, b, e):
        o = 64 * (j % 2)
        ln = lanes(e - b)
        at = sp.lw * j + h * a
        own = roll(get(x, a, b, e), o, 1)
        high = roll(zh[g, b:e, :], o + n - at, 1)
        low = roll(zl[g, b:e, :], o + 64 - h - at, 1)
        return jnp.where(ln < o + n, own, jnp.where(ln < o + n + h, high, low))

    def group(g):
        for q in range(sp.gp // 2):
            p = g * (sp.gp // 2) + q
            for a in range(sp.na):
                for ref, b, e, s, t in ((up_ref, up0, n, n - h - up0, n - up0), (dn_ref, 0, dn1, 0, h)):
                    even = fold(g * sp.gp + 2 * q, g, 2 * q, a, b, e)
                    odd = fold(g * sp.gp + 2 * q + 1, g, 2 * q + 1, a, b, e)
                    both = jnp.where(lanes(e - b) < 64, even, odd)
                    ref[p, a * h : (a + 1) * h, :] = both[s:t]
            if sp.yrows > sp.na * h:
                pad = jnp.zeros((sp.yrows - sp.na * h, 128), F32)
                up_ref[p, sp.na * h :, :] = pad
                dn_ref[p, sp.na * h :, :] = pad

    loop(n // sp.gp, group)


def plane(sp, get, zl, zh, yl, yh, x, g, j, a, dst, xw):
    n, h, r0 = sp.n, sp.h, sp.r0
    at = sp.lw * j + h * a
    ln = lanes(n)
    static = isinstance(j, int)

    def amount(k):
        return k - at if static else lax.rem(k + 128 - at, 128)

    high = roll(zh[g], amount(n), 1)
    low = roll(zl[g], amount(128 - h), 1)
    v = jnp.where(ln < n, get(x, a, 0, n), jnp.where(ln < n + h, high, jnp.where(ln >= 128 - h, low, 0.0)))
    dst[xw, r0 : r0 + n, :] = v
    lh = lanes(h)
    half = g * (sp.gp // 2) + j // 2
    for ref, r in ((yl, r0 - h), (yh, r0 + n)):
        u = ref[half, a * h : (a + 1) * h, :]
        if static:
            near, far = (u, roll(u, 64, 1)) if j % 2 == 0 else (roll(u, 64, 1), u)
        else:
            s = 64 * lax.rem(j, 2)
            near, far = roll(u, s, 1), roll(u, 64 - s, 1)
        dst[xw, r : r + h, :] = jnp.where(lh < n + h, near, jnp.where(lh >= 128 - h, far, 0.0))
    dst[xw, 0 : r0 - h, :] = jnp.zeros((r0 - h, 128), F32)
    dst[xw, r0 + n + h :, :] = jnp.zeros((sp.R - r0 - n - h, 128), F32)


def domain(sp, n, h, r0, R, ids):
    row = lax.broadcasted_iota(jnp.int32, (R, 128), 0) - r0
    ln = lanes(R)
    z = jnp.where(ln < 64, ln, ln - 128)
    gy, gz, ny, nz = ids[1], ids[2], ids[3], ids[4]
    y_at, z_at = row + gy * n, z + gz * n
    ok = (row >= -h) & (row < n + h) & (z >= -h) & (z < n + h)
    return ok & (y_at >= 0) & (y_at < ny * n) & (z_at >= 0) & (z_at < nz * n)


def neighbours(ref, x):
    c = ref[x + 1]
    R = c.shape[0]
    s = ref[x] + ref[x + 2]
    s = s + (roll(c, 1, 0) + roll(c, R - 1, 0))
    return s + (roll(c, 1, 1) + roll(c, 127, 1))


def zero_ends(ref, n):
    ref[0] = jnp.zeros(ref.shape[1:], F32)
    ref[n + 1] = jnp.zeros(ref.shape[1:], F32)


def relax(src, dst, f, c, n, factor):
    def one(x):
        dst[x + 1] = (1.0 - W) * src[x + 1] + c[x] * (f[x] + factor * neighbours(src, x))

    loop(n, one)


def lane_map(signed, value):
    l = lax.broadcasted_iota(jnp.int32, (128, 128), 0)
    m = lax.broadcasted_iota(jnp.int32, (128, 128), 1)
    c = l // 2
    if signed:
        c = jnp.where(l < 64, c, c + 64)
    return jnp.where(c == m, value, 0.0).astype(F32)


def spread_map(signed):
    m = lax.broadcasted_iota(jnp.int32, (128, 128), 0)
    l = lax.broadcasted_iota(jnp.int32, (128, 128), 1)
    c = l // 2
    if signed:
        c = jnp.where(l < 64, c, c + 64)
    return jnp.where(c == m, 1.0, 0.0).astype(F32)


def coarsen_planes(pair, n, tmp, acc, signed):
    half = tmp.shape[0] // 2

    def one(x):
        tmp[...] = pair(x)
        acc[x] = tmp[pl.ds(0, half, stride=2), :] + tmp[pl.ds(1, half, stride=2), :]

    loop(n, one)
    m = lane_map(signed, 0.125)

    def two(x):
        acc[x] = jnp.dot(acc[x], m, precision=HI, preferred_element_type=F32)

    loop(n, two)


def add_refined(coarse, r, n, dst, tmp, m):
    rows = tmp.shape[0] // 2

    def one(i):
        v = jnp.dot(coarse(i)[r : r + rows], m, precision=HI, preferred_element_type=F32)
        tmp[pl.ds(0, rows, stride=2), :] = v
        tmp[pl.ds(1, rows, stride=2), :] = v
        t = tmp[...]
        dst[2 * i + 1] = dst[2 * i + 1] + t
        dst[2 * i + 2] = dst[2 * i + 2] + t

    loop(n, one)


def wide_get(s):
    return lambda x, a, b, e: s[a, x, b:e, :]


def k_zpack0(x0, b, rea, hi, lo, s):
    for a, ref in enumerate((x0, b, rea)):
        widen(s.at[a], ref)
    zpack(L0, wide_get(s), hi, lo)


def k_ypack0(x0, b, rea, zl, zh, up, dn, s):
    for a, ref in enumerate((x0, b, rea)):
        widen(s.at[a], ref)
    ypack(L0, wide_get(s), zl, zh, up, dn)


def k_xpack(sp, ids, get, zl, zh, yl, yh, out):
    start = (1 - ids[0]) * (sp.n - sp.hx)

    def one(i):
        x = start + i
        g, j = lax.div(x, sp.gp), lax.rem(x, sp.gp)
        for a in range(sp.na):
            plane(sp, get, zl, zh, yl, yh, x, g, j, a, out.at[i], a)

    loop(sp.hx, one)


def k_xpack0(ids, x0, b, rea, zl, zh, yl, yh, out, s):
    for a, ref in enumerate((x0, b, rea)):
        widen(s.at[a], ref)
    k_xpack(L0, ids, wide_get(s), zl, zh, yl, yh, out)


def assemble(sp, ids, get, zl, zh, yl, yh, xr, dsts):
    shift = ids[0] * sp.hx

    def group(g):
        for j in range(sp.gp):
            x = g * sp.gp + j
            for a, (dst, off) in enumerate(dsts):
                plane(sp, get, zl, zh, yl, yh, x, g, j, a, dst, x + shift + off)

    loop(sp.n // sp.gp, group)
    other = (1 - ids[0]) * sp.n

    def take(i):
        for a, (dst, off) in enumerate(dsts):
            dst[other + i + off] = xr[i, a]

    loop(sp.hx, take)


def k_down0(ids, x0, b, rea, zl, zh, yl, yh, xr, f_out, c_out, e_out, f1, r1, z1h, z1l, s, xw, bw, rw, ew, tmp):
    for a, ref in enumerate((x0, b, rea)):
        widen(s.at[a], ref)
    assemble(L0, ids, wide_get(s), zl, zh, yl, yh, xr, ((xw, 1), (bw, 0), (rw, 0)))
    n = L0.nx
    ok = domain(L0, 48, 5, 8, 64, ids)
    zero_ends(xw, n)
    zero_ends(ew, n)
    zero_ends(e_out, n)

    def mask(x):
        xw[x + 1] = jnp.where(ok, xw[x + 1], 0.0)

    loop(n, mask)

    def first(x):
        d = 6.0 + rw[x]
        c = jnp.where(ok, W / d, 0.0)
        f = bw[x] - d * xw[x + 1] + neighbours(xw, x)
        f_out[x] = f
        c_out[x] = c
        ew[x + 1] = c * f

    loop(n, first)
    relax(ew, e_out, f_out, c_out, n, 1.0)
    shift = ids[0] * L0.hx

    def left(x):
        r = f_out[x] - (6.0 + rw[x]) * e_out[x + 1] + neighbours(e_out, x)
        return r[8:56]

    inner = lanes(48) < 48
    coarsen_planes(lambda x: jnp.where(inner, left(2 * x + shift) + left(2 * x + shift + 1), 0.0), 24, tmp, f1, True)
    coarsen_planes(lambda x: s[2, 2 * x] + s[2, 2 * x + 1], 24, tmp, r1, True)
    both = (f1, r1)
    zpack(L1, lambda x, a, p, q: both[a][x, p:q, :], z1h, z1l)


def k_ypack1(f1, r1, zl, zh, up, dn):
    both = (f1, r1)
    ypack(L1, lambda x, a, p, q: both[a][x, p:q, :], zl, zh, up, dn)


def k_xpack1(ids, f1, r1, zl, zh, yl, yh, out):
    both = (f1, r1)

    def get(x, a, p, q):
        return both[a][x, p:q, :]

    k_xpack(L1, ids, get, zl, zh, yl, yh, out)


def k_down1(ids, f1, r1, zl, zh, yl, yh, xr, fw, cw, e_out, f2, c2, e2, out3, rw, ew, tmp, r2, ew2, tmp2, t3):
    both = (f1, r1)
    assemble(L1, ids, lambda x, a, p, q: both[a][x, p:q, :], zl, zh, yl, yh, xr, ((fw, 0), (rw, 0)))
    n = L1.nx
    ok = domain(L1, 24, 12, 16, 56, ids)
    zero_ends(ew, n)
    zero_ends(e_out, n)

    def first(x):
        c = jnp.where(ok, W / (1.5 + rw[x]), 0.0)
        cw[x] = c
        ew[x + 1] = c * fw[x]

    loop(n, first)
    relax(ew, e_out, fw, cw, n, 0.25)

    def left(x):
        return fw[x] - (1.5 + rw[x]) * e_out[x + 1] + 0.25 * neighbours(e_out, x)

    def keep(ref):
        def one(x):
            ref[x, 28:32, :] = jnp.zeros((4, 128), F32)

        loop(18, one)

    keep(f2)
    keep(r2)
    coarsen_planes(lambda x: left(2 * x) + left(2 * x + 1), 18, tmp, f2.at[:, 0:28, :], True)
    coarsen_planes(lambda x: rw[2 * x] + rw[2 * x + 1], 18, tmp, r2.at[:, 0:28, :], True)
    ok2 = domain(None, 12, 6, 8, 32, ids)
    zero_ends(ew2, 18)
    zero_ends(e2, 18)

    def second(x):
        c = jnp.where(ok2, W / (0.375 + r2[x]), 0.0)
        c2[x] = c
        ew2[x + 1] = c * f2[x]

    loop(18, second)
    relax(ew2, e2, f2, c2, 18, 0.0625)

    def left2(x):
        return f2[x] - (0.375 + r2[x]) * e2[x + 1] + 0.0625 * neighbours(e2, x)

    coarsen_planes(lambda x: left2(2 * x) + left2(2 * x + 1), 9, tmp2, t3.at[0], True)
    coarsen_planes(lambda x: r2[2 * x] + r2[2 * x + 1], 9, tmp2, t3.at[1], True)
    shift = ids[0] * 3

    def give(x):
        for a in range(2):
            out3[a, x] = t3[a, x + shift, 4:10, 0:6]

    loop(6, give)


def sum_all(v):
    s = jnp.sum(v, axis=0)
    return jnp.sum(jnp.sum(s, axis=1, keepdims=True), axis=0, keepdims=True)


def coarse_solve(g3, e3, s3, f3, c3, r3, tmp, f4, r4):
    nx, ny, nz = g3.shape[1:]
    R = f3.shape[1]
    for ref in (f3, r3):
        ref[...] = jnp.zeros(ref.shape, F32)
    f3[:, 0:ny, 0:nz] = g3[0]
    r3[:, 0:ny, 0:nz] = g3[1]
    factor = 0.25**3
    ok = (lax.broadcasted_iota(jnp.int32, (R, 128), 0) < ny) & (lanes(R) < nz)
    for ref in (e3, s3):
        zero_ends(ref, nx)

    def first(x):
        c = jnp.where(ok, W / (6.0 * factor + r3[x]), 0.0)
        c3[x] = c
        s3[x + 1] = c * f3[x]

    loop(nx, first)
    relax(s3, e3, f3, c3, nx, factor)

    def left(x):
        v = f3[x] - (6.0 * factor + r3[x]) * e3[x + 1] + factor * neighbours(e3, x)
        return jnp.where(ok, v, 0.0)

    coarsen_planes(lambda x: left(2 * x) + left(2 * x + 1), nx // 2, tmp, f4, False)
    coarsen_planes(lambda x: r3[2 * x] + r3[2 * x + 1], nx // 2, tmp, r4, False)
    f4k = 0.25**4
    H = R // 2
    row = lax.broadcasted_iota(jnp.int32, (nx // 2, H, 128), 1)
    lane = lax.broadcasted_iota(jnp.int32, (nx // 2, H, 128), 2)
    inside = (row < ny // 2) & (lane < nz // 2)
    diag = 6.0 * f4k + r4[...]
    zero = jnp.zeros((1, H, 128), F32)

    def apply(p):
        s = jnp.concatenate([zero, p[:-1]], axis=0) + jnp.concatenate([p[1:], zero], axis=0)
        s = s + roll(p, 1, 1) + roll(p, H - 1, 1) + roll(p, 1, 2) + roll(p, 127, 2)
        return jnp.where(inside, diag * p - f4k * s, 0.0)

    r = jnp.where(inside, f4[...], 0.0)
    p = r
    e = jnp.zeros_like(r)
    rr = sum_all(r * r)
    for i in range(BOTTOM_ITERS):
        q = apply(p)
        a = rr / sum_all(p * q)
        e = e + a * p
        if i + 1 < BOTTOM_ITERS:
            r = r - a * q
            new = sum_all(r * r)
            p = r + (new / rr) * p
            rr = new
    f4[...] = e
    add_refined(lambda i: f4[i], 0, nx // 2, e3, tmp, spread_map(False))
    relax(e3, s3, f3, c3, nx, factor)
    relax(s3, e3, f3, c3, nx, factor)


def k_up(ids, g3, f2, c2, e2i, f1, c1, e1i, f0, c0, e0i, rea, z_out, az_out, f_own, sums,
         e3, s3, f3, c3, r3, tmp3, f4, r4, w3, e2, s2, tmp2, e1, s1, tmp1, e0, s0, tmp0):
    coarse_solve(g3, e3, s3, f3, c3, r3, tmp3, f4, r4)
    gx, gy, gz = ids[0], ids[1], ids[2]
    for dst, src in ((e2, e2i), (e1, e1i), (e0, e0i)):
        def copy(x, dst=dst, src=src):
            dst[x] = src[x]
        loop(src.shape[0], copy)
    for ref, n in ((s2, 18), (s1, 36), (s0, 54)):
        zero_ends(ref, n)
    R3 = e3.shape[1]
    pick = lax.broadcasted_iota(jnp.int32, (16, R3), 1) == lax.broadcasted_iota(jnp.int32, (16, R3), 0) + (gy * 6 - 4)
    pick = pick.astype(F32)
    c = lax.broadcasted_iota(jnp.int32, (128, 128), 0)
    l = lanes(128)
    half = l // 2
    spread = (c == gz * 6 + jnp.where(l < 64, half, half - 64)).astype(F32)
    ok2 = domain(None, 12, 6, 8, 32, ids)

    def window(i):
        w3[i] = jnp.dot(pick, e3[i + 1 + gx * 3], precision=HI, preferred_element_type=F32)

    loop(9, window)
    add_refined(lambda i: w3[i], 0, 9, e2, tmp2, spread)
    relax(e2, s2, f2, c2, 18, 0.0625)
    relax(s2, e2, f2, c2, 18, 0.0625)
    m = spread_map(True)
    add_refined(lambda i: e2[i + 1], 0, 18, e1, tmp1, m)
    relax(e1, s1, f1, c1, 36, 0.25)
    relax(s1, e1, f1, c1, 36, 0.25)
    ok0 = domain(L0, 48, 5, 8, 64, ids)
    m0 = m
    add_refined(lambda i: e1[i + 1 + gx * 9], 12, 27, e0, tmp0, m0)

    def mask(x):
        e0[x + 1] = jnp.where(ok0, e0[x + 1], 0.0)

    loop(54, mask)
    relax(e0, s0, f0, c0, 54, 1.0)
    relax(s0, e0, f0, c0, 54, 1.0)
    shift = gx * 6

    def last(x, carry):
        u, v = carry
        z = e0[x + shift + 1][8:56, 0:48]
        nb = neighbours(e0, x + shift)[8:56, 0:48]
        az = (6.0 + rea[x]) * z - nb
        f = f0[x + shift][8:56, 0:48]
        z_out[x] = z
        az_out[x] = az
        f_own[x] = f
        return u + f * z, v + z * az

    zero = jnp.zeros((48, 48), F32)
    u, v = lax.fori_loop(0, 48, last, (zero, zero))

    def total(t):
        return jnp.sum(jnp.sum(t, axis=1, keepdims=True), axis=0, keepdims=True)

    ln = lanes(8)
    sums[...] = jnp.where(ln == 0, total(u), jnp.where(ln == 1, total(v), 0.0))


def k_last(sums, x0, z, az, f, sol, res):
    s = jnp.sum(sums[...], axis=0, keepdims=True)
    ln = lanes(1)
    upper = jnp.sum(jnp.where(ln == 0, s, 0.0), axis=1, keepdims=True)
    lower = jnp.sum(jnp.where(ln == 1, s, 0.0), axis=1, keepdims=True)
    step = upper / lower

    def one(x):
        sol[x] = x0[x] + step * z[x]
        res[x] = f[x] - step * az[x]

    loop(48, one)


def ring(up, dn, axis):
    n = lax.axis_size(axis)
    low = lax.ppermute(up, axis, [(i, (i + 1) % n) for i in range(n)])
    high = lax.ppermute(dn, axis, [(i, (i - 1) % n) for i in range(n)])
    return low, high


def swap(v):
    return lax.ppermute(v, "gx", [(0, 1), (1, 0)])


def body(b, x0, rea):
    ALL = ("gx", "gy", "gz")
    sizes = [lax.axis_size(a) for a in ALL]
    count = sizes[0] * sizes[1] * sizes[2]
    ids = jnp.stack([lax.axis_index(a) for a in ALL] + [jnp.int32(sizes[1]), jnp.int32(sizes[2])]).astype(jnp.int32)
    wide = (3, 48, 48, 128)
    hi, lo = run(k_zpack0, (sds(*L0.zshape),) * 2, (x0, b, rea), [wide])
    zl, zh = ring(hi, lo, "gz")
    up, dn = run(k_ypack0, (sds(*L0.yshape),) * 2, (x0, b, rea, zl, zh), [wide])
    yl, yh = ring(up, dn, "gy")
    xs = run(k_xpack0, sds(*L0.xshape), (ids, x0, b, rea, zl, zh, yl, yh), [wide])
    xr = swap(xs)
    p0 = (54, 64, 128)
    q0 = (56, 64, 128)
    f0, c0, e0, f1, r1, z1h, z1l = run(
        k_down0,
        (sds(*p0), sds(*p0), sds(*q0), sds(24, 24, 128), sds(24, 24, 128), sds(*L1.zshape), sds(*L1.zshape)),
        (ids, x0, b, rea, zl, zh, yl, yh, xr),
        [wide, q0, p0, p0, q0, (48, 128)],
    )
    zl, zh = ring(z1h, z1l, "gz")
    up, dn = run(k_ypack1, (sds(*L1.yshape),) * 2, (f1, r1, zl, zh))
    yl, yh = ring(up, dn, "gy")
    xs = run(k_xpack1, sds(*L1.xshape), (ids, f1, r1, zl, zh, yl, yh))
    xr = swap(xs)
    p1, q1, p2, q2 = (36, 56, 128), (38, 56, 128), (18, 32, 128), (20, 32, 128)
    f1w, c1w, e1w, f2w, c2w, e2w, g = run(
        k_down1,
        (sds(*p1), sds(*p1), sds(*q1), sds(*p2), sds(*p2), sds(*q2), sds(2, 6, 6, 6)),
        (ids, f1, r1, zl, zh, yl, yh, xr),
        [p1, q1, (56, 128), p2, q2, (32, 128), (2, 9, 16, 128)],
    )
    g = jnp.broadcast_to(g.reshape(1, 432), (count, 432))
    g = lax.all_to_all(g, ALL, 0, 0)
    g = g.reshape(sizes[0], sizes[1], sizes[2], 2, 6, 6, 6).transpose(3, 0, 4, 1, 5, 2, 6)
    n3 = [6 * s for s in sizes]
    g = g.reshape(2, *n3)
    R3 = (n3[1] + 8) // 8 * 8
    if R3 % 16:
        R3 += 8
    p3, q3, p4 = (n3[0], R3, 128), (n3[0] + 2, R3, 128), (n3[0] // 2, R3 // 2, 128)
    z, az, f, sums = run(
        k_up,
        (sds(48, 48, 48), sds(48, 48, 48), sds(48, 48, 48), sds(8, 128)),
        (ids, g, f2w, c2w, e2w, f1w, c1w, e1w, f0, c0, e0, rea),
        [q3, q3, p3, p3, p3, (R3, 128), p4, p4, (9, 16, 128), q2, q2, (32, 128), q1, q1, (56, 128), q0, q0, (64, 128)],
    )
    sums = lax.all_to_all(jnp.broadcast_to(sums[:1], (count, 128)), ALL, 0, 0)
    return run(k_last, (sds(48, 48, 48), sds(48, 48, 48)), (sums, x0, z, az, f))


def solution(mesh):
    spec = P("gx", "gy", "gz")
    return jax.shard_map(body, mesh=mesh, in_specs=(spec, spec, spec), out_specs=(spec, spec), check_vma=False)
```

```python
import functools
import jax
import jax.numpy as jnp
from jax import lax
from jax.experimental import pallas as pl
from jax.experimental.pallas import tpu as pltpu
from jax.sharding import PartitionSpec as P

W = 6.0 / 7.0
BOTTOM_ITERS = 6
N0 = 48
F32 = jnp.float32
HI = lax.Precision.HIGHEST
M0, M1, M2 = 20, 12, 20


class Spec:
    def __init__(self, n, h, na, gp, r0, R, hx):
        self.n, self.h, self.na, self.gp, self.r0, self.R, self.hx = n, h, na, gp, r0, R, hx
        self.lw = 128 // gp
        self.zshape = (n // gp, n, 128)
        self.yrows = -(-na * h // 8) * 8
        self.yshape = (n // 2, self.yrows, 128)
        self.xshape = (hx, na, R, 128)
        self.nx = n + hx


L0 = Spec(48, 5, 3, 8, 8, 64, 6)
L1 = Spec(24, 12, 2, 4, 16, 56, 12)


def sds(*shape):
    return jax.ShapeDtypeStruct(shape, F32)


def run(kernel, outs, args, scratch=(), mib=12):
    vmem = pl.BlockSpec(memory_space=pltpu.VMEM)
    return pl.pallas_call(
        kernel,
        out_shape=outs,
        in_specs=[vmem] * len(args),
        out_specs=jax.tree.map(lambda _: vmem, outs),
        scratch_shapes=[pltpu.VMEM(s, F32) for s in scratch],
        compiler_params=pltpu.CompilerParams(vmem_limit_bytes=mib * 1024 * 1024),
    )(*args)


def place():
    return [lax.axis_index(a) for a in ("gx", "gy", "gz")] + [lax.axis_size(a) for a in ("gy", "gz")]


def lanes(rows):
    return lax.broadcasted_iota(jnp.int32, (rows, 128), 1)


def roll(v, shift, axis):
    if isinstance(shift, int):
        shift = shift % v.shape[axis]
        if shift == 0:
            return v
    return pltpu.roll(v, shift, axis)


def loop(n, f, u=1):
    u = max(d for d in range(1, u + 1) if n % d == 0)

    def some(i, c):
        for k in range(u):
            f(i * u + k)
        return c

    lax.fori_loop(0, n // u, some, 0)


def edge(sp, ids):
    _, gy, gz, ny, nz = ids
    high = jnp.where(gz < nz - 1, sp.n + sp.h, sp.n)
    low = jnp.where(gz > 0, 128 - sp.h, 128)
    return high, low, jnp.where(gy > 0, 1.0, 0.0), jnp.where(gy < ny - 1, 1.0, 0.0)


def zpack(sp, get, hi_ref, lo_ref):
    ln = lanes(sp.n)

    def group(g):
        hi = jnp.zeros((sp.n, 128), F32)
        lo = hi
        for j in range(sp.gp):
            for a in range(sp.na):
                v = get(g * sp.gp + j, a, 0, sp.n)
                at = sp.lw * j + sp.h * a
                here = (ln >= at) & (ln < at + sp.h)
                hi = jnp.where(here, roll(v, at - (sp.n - sp.h), 1), hi)
                lo = jnp.where(here, roll(v, at, 1), lo)
        hi_ref[g] = hi
        lo_ref[g] = lo

    loop(sp.n // sp.gp, group)


def ypack(sp, get, zl, zh, up_ref, dn_ref):
    n, h = sp.n, sp.h
    up0 = (n - h) // 8 * 8
    dn1 = -(-h // 8) * 8

    def fold(x, g, j, a, b, e):
        o = 64 * (j % 2)
        ln = lanes(e - b)
        at = sp.lw * j + h * a
        own = roll(get(x, a, b, e), o, 1)
        high = roll(zh[g, b:e, :], o + n - at, 1)
        low = roll(zl[g, b:e, :], o + 64 - h - at, 1)
        return jnp.where(ln < o + n, own, jnp.where(ln < o + n + h, high, low))

    def group(g):
        for q in range(sp.gp // 2):
            p = g * (sp.gp // 2) + q
            for a in range(sp.na):
                for ref, b, e, s, t in ((up_ref, up0, n, n - h - up0, n - up0), (dn_ref, 0, dn1, 0, h)):
                    even = fold(g * sp.gp + 2 * q, g, 2 * q, a, b, e)
                    odd = fold(g * sp.gp + 2 * q + 1, g, 2 * q + 1, a, b, e)
                    both = jnp.where(lanes(e - b) < 64, even, odd)
                    ref[p, a * h : (a + 1) * h, :] = both[s:t]
            if sp.yrows > sp.na * h:
                pad = jnp.zeros((sp.yrows - sp.na * h, 128), F32)
                up_ref[p, sp.na * h :, :] = pad
                dn_ref[p, sp.na * h :, :] = pad

    loop(n // sp.gp, group)


def plane(sp, own, zl, zh, yl, yh, x, g, j, a, dst, xw, ends):
    n, h, r0 = sp.n, sp.h, sp.r0
    at = sp.lw * j + h * a
    ln = lanes(n)
    top, bottom, below, above = ends
    static = isinstance(j, int)

    def amount(k):
        return k - at if static else lax.rem(k + 128 - at, 128)

    high = roll(zh[g], amount(n), 1)
    low = roll(zl[g], amount(128 - h), 1)
    dst[xw, r0 : r0 + n, :] = jnp.where(ln < top, high, jnp.where(ln >= bottom, low, 0.0))
    dst[xw, r0 : r0 + n, 0:n] = own(x, a)
    lh = lanes(h)
    half = g * (sp.gp // 2) + j // 2
    dst[xw, 0:r0, :] = jnp.zeros((r0, 128), F32)
    dst[xw, r0 + n :, :] = jnp.zeros((sp.R - r0 - n, 128), F32)
    for ref, r, weight in ((yl, r0 - h, below), (yh, r0 + n, above)):
        u = ref[half, a * h : (a + 1) * h, :] * weight
        if static:
            near, far = (u, roll(u, 64, 1)) if j % 2 == 0 else (roll(u, 64, 1), u)
        else:
            t = 64 * lax.rem(j, 2)
            near, far = roll(u, t, 1), roll(u, 64 - t, 1)
        dst[xw, r : r + h, :] = jnp.where(lh < top, near, jnp.where(lh >= bottom, far, 0.0))


def domain(sp, n, h, r0, R, ids):
    row = lax.broadcasted_iota(jnp.int32, (R, 128), 0) - r0
    ln = lanes(R)
    z = jnp.where(ln < 64, ln, ln - 128)
    gy, gz, ny, nz = ids[1], ids[2], ids[3], ids[4]
    y_at, z_at = row + gy * n, z + gz * n
    ok = (row >= -h) & (row < n + h) & (z >= -h) & (z < n + h)
    return ok & (y_at >= 0) & (y_at < ny * n) & (z_at >= 0) & (z_at < nz * n)


def neighbours(ref, x):
    c = ref[x + 1]
    R = c.shape[0]
    s = ref[x] + ref[x + 2]
    s = s + (roll(c, 1, 0) + roll(c, R - 1, 0))
    return s + (roll(c, 1, 1) + roll(c, 127, 1))


def zero_ends(ref, n):
    ref[0] = jnp.zeros(ref.shape[1:], F32)
    ref[n + 1] = jnp.zeros(ref.shape[1:], F32)


def relax(src, dst, f, c, n, factor, u=3):
    def one(x):
        dst[x + 1] = (1.0 - W) * src[x + 1] + c[x] * (f[x] + factor * neighbours(src, x))

    loop(n, one, u)


def coarse_lane(l, signed):
    c = l // 2
    return jnp.where(l < 64, c, c + 64) if signed else c


def lane_map(signed, value):
    l = lax.broadcasted_iota(jnp.int32, (256, 128), 0) % 128
    m = lax.broadcasted_iota(jnp.int32, (256, 128), 1)
    return jnp.where(coarse_lane(l, signed) == m, value, 0.0).astype(jnp.bfloat16)


def spread_map(pick):
    m = lax.broadcasted_iota(jnp.int32, (256, 128), 0) % 128
    l = lax.broadcasted_iota(jnp.int32, (256, 128), 1)
    return jnp.where(pick(l) == m, 1.0, 0.0).astype(jnp.bfloat16)


def times(v, m):
    big = v.astype(jnp.bfloat16)
    rest = (v - big.astype(F32)).astype(jnp.bfloat16)
    return jnp.dot(jnp.concatenate([big, rest], axis=1), m, preferred_element_type=F32)


def coarsen_planes(pair, n, tmp, acc, signed, rows=None, u=2):
    half = acc.shape[1]
    rows = rows or 2 * half

    def one(x):
        tmp[x, 0:rows, :] = pair(x)
        acc[x] = tmp[x, pl.ds(0, half, stride=2), :] + tmp[x, pl.ds(1, half, stride=2), :]

    loop(n, one, u)
    v = acc[...].reshape(n * half, 128)
    acc[...] = times(v, lane_map(signed, 0.125)).reshape(n, half, 128)


def add_refined(coarse, n, src, dst, wide, m, u=3):
    rows = coarse.shape[1]
    wide[0:n, 0:rows, :] = times(coarse[...].reshape(n * rows, 128), m).reshape(n, rows, 128)
    R = dst.shape[1]

    def one(i):
        v = wide[i, 0 : R // 2, :]
        for k in range(2):
            dst[2 * i + 1, pl.ds(k, R // 2, stride=2), :] = v
        t = dst[2 * i + 1]
        dst[2 * i + 1] = src[2 * i + 1] + t
        dst[2 * i + 2] = src[2 * i + 2] + t

    loop(n, one, u)


def k_zpack0(x0, b, rea, hi, lo, s):
    for a, ref in enumerate((x0, b, rea)):
        def one(x, a=a, ref=ref):
            s[a, x, :, 0:48] = ref[x]
        loop(48, one, 4)
    zpack(L0, lambda x, a, p, q: s[a, x, p:q, :], hi, lo)


def k_ypack0(x0, b, rea, zl, zh, up, dn, s):
    for a, ref in enumerate((x0, b, rea)):
        def one(x, a=a, ref=ref):
            s[a, x, 0:8, 0:48] = ref[x, 0:8]
            s[a, x, 8:16, 0:48] = ref[x, 40:48]
        loop(48, one, 8)
    ypack(L0, lambda x, a, p, q: s[a, x, 0:8, :] if p == 0 else s[a, x, 8:16, :], zl, zh, up, dn)


def k_xpack(sp, own, zl, zh, yl, yh, out):
    ids = place()
    ends = edge(sp, ids)
    start = (1 - ids[0]) * (sp.n - sp.hx)

    def one(i):
        x = start + i
        g, j = lax.div(x, sp.gp), lax.rem(x, sp.gp)
        for a in range(sp.na):
            plane(sp, own, zl, zh, yl, yh, x, g, j, a, out.at[i], a, ends)

    loop(sp.hx, one, 2)


def k_xpack0(x0, b, rea, zl, zh, yl, yh, out):
    refs = (x0, b, rea)
    k_xpack(L0, lambda x, a: refs[a][x], zl, zh, yl, yh, out)


def assemble(sp, ids, own, zl, zh, yl, yh, xr, dsts):
    shift = ids[0] * sp.hx
    ends = edge(sp, ids)

    def group(g):
        for j in range(sp.gp):
            x = g * sp.gp + j
            for a, (dst, off) in enumerate(dsts):
                plane(sp, own, zl, zh, yl, yh, x, g, j, a, dst, x + shift + off, ends)

    loop(sp.n // sp.gp, group)
    other = (1 - ids[0]) * sp.n

    def take(i):
        for a, (dst, off) in enumerate(dsts):
            dst[other + i + off] = xr[i, a]

    loop(sp.hx, take, 2)


def k_down0(x0, b, rea, zl, zh, yl, yh, xr, f_out, c_out, e_out, f1, r1, z1h, z1l, xw, bw, rw, ew, tmp):
    ids = place()
    refs = (x0, b, rea)
    assemble(L0, ids, lambda x, a: refs[a][x], zl, zh, yl, yh, xr, ((xw, 1), (bw, 0), (rw, 0)))
    n = L0.nx
    ok = domain(L0, 48, 5, 8, 64, ids)
    zero_ends(xw, n)
    zero_ends(ew, n)
    zero_ends(e_out, n)

    def first(x):
        d = 6.0 + rw[x]
        c = jnp.where(ok, W / d, 0.0)
        f = bw[x] - d * xw[x + 1] + neighbours(xw, x)
        f_out[x] = f
        c_out[x] = c
        ew[x + 1] = c * f

    loop(n, first, 3)
    relax(ew, e_out, f_out, c_out, n, 1.0)
    shift = ids[0] * L0.hx

    def left(x):
        r = f_out[x] - (6.0 + rw[x]) * e_out[x + 1] + neighbours(e_out, x)
        return r[8:56]

    inner = lanes(48) < 48
    coarsen_planes(lambda x: jnp.where(inner, left(2 * x + shift) + left(2 * x + shift + 1), 0.0), 24, tmp, f1, True)

    def react(x):
        return jnp.where(inner, rw[2 * x + shift, 8:56, :] + rw[2 * x + shift + 1, 8:56, :], 0.0)

    coarsen_planes(react, 24, tmp, r1, True)
    both = (f1, r1)
    zpack(L1, lambda x, a, p, q: both[a][x, p:q, :], z1h, z1l)


def k_ypack1(f1, r1, zl, zh, up, dn):
    both = (f1, r1)
    ypack(L1, lambda x, a, p, q: both[a][x, p:q, :], zl, zh, up, dn)


def k_xpack1(f1, r1, zl, zh, yl, yh, out):
    both = (f1, r1)
    k_xpack(L1, lambda x, a: both[a][x, :, 0:24], zl, zh, yl, yh, out)


def k_down1(f1, r1, zl, zh, yl, yh, xr, fw, cw, e_out, f2, c2, e2, out3, rw, ew, tmp, r2, ew2, tmp2, t3, sq):
    ids = place()
    both = (f1, r1)
    assemble(L1, ids, lambda x, a: both[a][x, :, 0:24], zl, zh, yl, yh, xr, ((fw, 0), (rw, 0)))
    n = L1.nx
    ok = domain(L1, 24, 12, 16, 56, ids)
    zero_ends(ew, n)
    zero_ends(e_out, n)

    def first(x):
        c = jnp.where(ok, W / (1.5 + rw[x]), 0.0)
        cw[x] = c
        ew[x + 1] = c * fw[x]

    loop(n, first, 4)
    relax(ew, e_out, fw, cw, n, 0.25)

    def left(x):
        return fw[x] - (1.5 + rw[x]) * e_out[x + 1] + 0.25 * neighbours(e_out, x)

    def pad(x):
        tmp[x, 56:64, :] = jnp.zeros((8, 128), F32)

    loop(18, pad, 3)
    coarsen_planes(lambda x: left(2 * x) + left(2 * x + 1), 18, tmp, f2, True, 56)
    coarsen_planes(lambda x: rw[2 * x] + rw[2 * x + 1], 18, tmp, r2, True, 56)
    ok2 = domain(None, 12, 6, 8, 32, ids)
    zero_ends(ew2, 18)
    zero_ends(e2, 18)

    def second(x):
        c = jnp.where(ok2, W / (0.375 + r2[x]), 0.0)
        c2[x] = c
        ew2[x + 1] = c * f2[x]

    loop(18, second, 6)
    relax(ew2, e2, f2, c2, 18, 0.0625, 6)

    def left2(x):
        return f2[x] - (0.375 + r2[x]) * e2[x + 1] + 0.0625 * neighbours(e2, x)

    coarsen_planes(lambda x: left2(2 * x) + left2(2 * x + 1), 9, tmp2, t3.at[0], True, u=3)
    coarsen_planes(lambda x: r2[2 * x] + r2[2 * x + 1], 9, tmp2, t3.at[1], True, u=3)
    shift = ids[0] * 3
    sq[...] = jnp.zeros((128, 128), F32)
    for a in range(2):
        for x in range(6):
            at = a * 36 + x * 6
            sq[at : at + 6, :] = t3[a, x + shift, 4:10, :]
    t = sq[...].T[0:8]
    out3[...] = jnp.broadcast_to(t[None], out3.shape)


def sum_all(v):
    s = jnp.sum(v, axis=0)
    return jnp.sum(jnp.sum(s, axis=1, keepdims=True), axis=0, keepdims=True)


def coarse_solve(g3, nx, ny, nz, e3, s3, f3, c3, r3, tmp, f4, r4, wide, sq):
    R = f3.shape[1]
    for ref in (f3, r3):
        ref[...] = jnp.zeros(ref.shape, F32)
    kx, ky, kz = nx // 6, ny // 6, nz // 6
    for bx in range(kx):
        for by in range(ky):
            k = bx * ky + by
            if kz * 6 < 128:
                sq[k, kz * 6 :, :] = jnp.zeros((128 - kz * 6, 128), F32)
            for bz in range(kz):
                sq[k, bz * 6 : bz * 6 + 6, :] = g3[k * kz + bz, 0:6, :]
            t = sq[k].T
            for x in range(6):
                f3[bx * 6 + x, by * 6 : by * 6 + 6, :] = t[x * 6 : x * 6 + 6]
                r3[bx * 6 + x, by * 6 : by * 6 + 6, :] = t[36 + x * 6 : 42 + x * 6]
    factor = 0.25**3
    ok = (lax.broadcasted_iota(jnp.int32, (R, 128), 0) < ny) & (lanes(R) < nz)
    for ref in (e3, s3):
        zero_ends(ref, nx)

    def first(x):
        c = jnp.where(ok, W / (6.0 * factor + r3[x]), 0.0)
        c3[x] = c
        s3[x + 1] = c * f3[x]

    loop(nx, first, 6)
    relax(s3, e3, f3, c3, nx, factor, 6)

    def left(x):
        v = f3[x] - (6.0 * factor + r3[x]) * e3[x + 1] + factor * neighbours(e3, x)
        return jnp.where(ok, v, 0.0)

    coarsen_planes(lambda x: left(2 * x) + left(2 * x + 1), nx // 2, tmp, f4, False, u=3)
    coarsen_planes(lambda x: r3[2 * x] + r3[2 * x + 1], nx // 2, tmp, r4, False, u=3)
    f4k = 0.25**4
    H = R // 2
    row = lax.broadcasted_iota(jnp.int32, (nx // 2, H, 128), 1)
    lane = lax.broadcasted_iota(jnp.int32, (nx // 2, H, 128), 2)
    inside = (row < ny // 2) & (lane < nz // 2)
    diag = 6.0 * f4k + r4[...]
    zero = jnp.zeros((1, H, 128), F32)

    def apply(p):
        s = jnp.concatenate([zero, p[:-1]], axis=0) + jnp.concatenate([p[1:], zero], axis=0)
        s = s + roll(p, 1, 1) + roll(p, H - 1, 1) + roll(p, 1, 2) + roll(p, 127, 2)
        return jnp.where(inside, diag * p - f4k * s, 0.0)

    r = jnp.where(inside, f4[...], 0.0)
    p = r
    e = jnp.zeros_like(r)
    rr = sum_all(r * r)
    for i in range(BOTTOM_ITERS):
        q = apply(p)
        a = rr / sum_all(p * q)
        e = e + a * p
        if i + 1 < BOTTOM_ITERS:
            r = r - a * q
            new = sum_all(r * r)
            p = r + (new / rr) * p
            rr = new
    f4[...] = e
    add_refined(f4, nx // 2, e3, s3, wide, spread_map(lambda l: coarse_lane(l, False)))
    relax(s3, e3, f3, c3, nx, factor, 6)
    relax(e3, s3, f3, c3, nx, factor, 6)


def k_up(g3, f2, c2, e2i, f1, c1, e1i, f0, c0, e0i, rea, z_out, az_out, f_own, sums,
         e3, s3, f3, c3, r3, tmp3, f4, r4, sq, w3, w2, n1, w1, e2, s2, e1, s1, e0, s0):
    gx, gy, gz, sy, sz = place()
    nx, ny, nz = f3.shape[0], sy * 6, sz * 6
    coarse_solve(g3, nx, ny, nz, e3, s3, f3, c3, r3, tmp3, f4, r4, w3, sq)
    for ref, n in ((s2, 18), (s1, 36), (s0, 54), (e2, 18), (e1, 36), (e0, 54)):
        zero_ends(ref, n)
    R3 = s3.shape[1]
    pick = lax.broadcasted_iota(jnp.int32, (16, R3), 1) == lax.broadcasted_iota(jnp.int32, (16, R3), 0) + (gy * 6 - 4)
    pick = pick.astype(F32)
    for i in range(9):
        w3[i, 0:16, :] = jnp.dot(pick, s3[i + 1 + gx * 3], precision=HI, preferred_element_type=F32)
    spread = spread_map(lambda l: gz * 6 + jnp.where(l < 64, l // 2, l // 2 - 64))
    add_refined(w3.at[:, 0:16, :], 9, e2i, e2, w2, spread)
    relax(e2, s2, f2, c2, 18, 0.0625, 6)
    relax(s2, e2, f2, c2, 18, 0.0625, 6)
    m = spread_map(lambda l: coarse_lane(l, True))
    add_refined(e2.at[1:19], 18, e1i, e1, w2, m)
    relax(e1, s1, f1, c1, 36, 0.25)
    relax(s1, e1, f1, c1, 36, 0.25)

    def near(i):
        n1[i] = e1[i + 1 + gx * 9, 12:44, :]

    loop(27, near, 3)
    add_refined(n1, 27, e0i, e0, w1, m)
    ok0 = domain(L0, 48, 5, 8, 64, (gx, gy, gz, sy, sz))

    def mask(x):
        e0[x + 1] = jnp.where(ok0, e0[x + 1], 0.0)

    loop(54, mask, 3)
    relax(e0, s0, f0, c0, 54, 1.0)
    relax(s0, e0, f0, c0, 54, 1.0)
    shift = gx * 6

    def last(x, carry):
        u, v = carry
        z = e0[x + shift + 1][8:56, 0:48]
        nb = neighbours(e0, x + shift)[8:56, 0:48]
        az = (6.0 + rea[x]) * z - nb
        f = f0[x + shift][8:56, 0:48]
        z_out[x] = z
        az_out[x] = az
        f_own[x] = f
        return u + f * z, v + z * az

    zero = jnp.zeros((48, 48), F32)
    u, v = lax.fori_loop(0, 24, lambda i, c: last(2 * i + 1, last(2 * i, c)), (zero, zero))

    def total(t):
        return jnp.sum(jnp.sum(t, axis=1, keepdims=True), axis=0, keepdims=True)

    ln = lanes(sums.shape[0])
    sums[...] = jnp.where(ln == 0, total(u), jnp.where(ln == 1, total(v), 0.0))


def k_last(sums, x0, z, az, f, sol, res):
    s = jnp.sum(sums[...], axis=0, keepdims=True)
    ln = lanes(1)
    upper = jnp.sum(jnp.where(ln == 0, s, 0.0), axis=1, keepdims=True)
    lower = jnp.sum(jnp.where(ln == 1, s, 0.0), axis=1, keepdims=True)
    step = upper / lower

    def one(x):
        sol[x] = x0[x] + step * z[x]
        res[x] = f[x] - step * az[x]

    loop(48, one, 4)


def ring(up, dn, axis):
    n = lax.axis_size(axis)
    low = lax.ppermute(up, axis, [(i, (i + 1) % n) for i in range(n)])
    high = lax.ppermute(dn, axis, [(i, (i - 1) % n) for i in range(n)])
    return low, high


def swap(v):
    return lax.ppermute(v, "gx", [(0, 1), (1, 0)])


def body(b, x0, rea):
    ALL = ("gx", "gy", "gz")
    sizes = [lax.axis_size(a) for a in ALL]
    count = sizes[0] * sizes[1] * sizes[2]
    hi, lo = run(k_zpack0, (sds(*L0.zshape),) * 2, (x0, b, rea), [(3, 48, 48, 128)])
    zl, zh = ring(hi, lo, "gz")
    up, dn = run(k_ypack0, (sds(*L0.yshape),) * 2, (x0, b, rea, zl, zh), [(3, 48, 16, 128)])
    yl, yh = ring(up, dn, "gy")
    xs = run(k_xpack0, sds(*L0.xshape), (x0, b, rea, zl, zh, yl, yh))
    xr = swap(xs)
    p0 = (54, 64, 128)
    q0 = (56, 64, 128)
    f0, c0, e0, f1, r1, z1h, z1l = run(
        k_down0,
        (sds(*p0), sds(*p0), sds(*q0), sds(24, 24, 128), sds(24, 24, 128), sds(*L1.zshape), sds(*L1.zshape)),
        (x0, b, rea, zl, zh, yl, yh, xr),
        [q0, p0, p0, q0, (24, 48, 128)],
        mib=M0,
    )
    zl, zh = ring(z1h, z1l, "gz")
    up, dn = run(k_ypack1, (sds(*L1.yshape),) * 2, (f1, r1, zl, zh))
    yl, yh = ring(up, dn, "gy")
    xs = run(k_xpack1, sds(*L1.xshape), (f1, r1, zl, zh, yl, yh))
    xr = swap(xs)
    p1, q1, p2, q2 = (36, 56, 128), (38, 56, 128), (18, 32, 128), (20, 32, 128)
    f1w, c1w, e1w, f2w, c2w, e2w, g = run(
        k_down1,
        (sds(*p1), sds(*p1), sds(*q1), sds(*p2), sds(*p2), sds(*q2), sds(count, 8, 128)),
        (f1, r1, zl, zh, yl, yh, xr),
        [p1, q1, (18, 64, 128), p2, q2, (9, 32, 128), (2, 9, 16, 128), (128, 128)],
        mib=M1,
    )
    g = lax.all_to_all(g, ALL, 0, 0, tiled=True)
    n3 = [6 * s for s in sizes]
    R3 = (n3[1] + 8) // 8 * 8
    if R3 % 16:
        R3 += 8
    p3, q3, p4 = (n3[0], R3, 128), (n3[0] + 2, R3, 128), (n3[0] // 2, R3 // 2, 128)
    z, az, f, sums = run(
        k_up,
        (sds(48, 48, 48), sds(48, 48, 48), sds(48, 48, 48), sds(count, 128)),
        (g, f2w, c2w, e2w, f1w, c1w, e1w, f0, c0, e0, rea),
        [q3, q3, p3, p3, p3, (n3[0] // 2, R3, 128), p4, p4, (sizes[0] * sizes[1], 128, 128), (9, 16, 128), (18, 32, 128),
         (27, 32, 128), (27, 32, 128), q2, q2, q1, q1, q0, q0],
        mib=M2,
    )
    sums = lax.all_to_all(sums.reshape(count, 1, 128), ALL, 0, 0, tiled=True).reshape(count, 128)
    return run(k_last, (sds(48, 48, 48), sds(48, 48, 48)), (sums, x0, z, az, f))


def solution(mesh):
    spec = P("gx", "gy", "gz")
    return jax.shard_map(body, mesh=mesh, in_specs=(spec, spec, spec), out_specs=(spec, spec), check_vma=False)
```

```python
import functools
import jax
import jax.numpy as jnp
from jax import lax
from jax.experimental import pallas as pl
from jax.experimental.pallas import tpu as pltpu
from jax.sharding import PartitionSpec as P

W = 6.0 / 7.0
BOTTOM_ITERS = 6
N0 = 48
F32 = jnp.float32
HI = lax.Precision.HIGHEST
M0, M1, M2 = 20, 12, 20


class Spec:
    def __init__(self, n, h, na, gp, r0, R, hx):
        self.n, self.h, self.na, self.gp, self.r0, self.R, self.hx = n, h, na, gp, r0, R, hx
        self.lw = 128 // gp
        self.zshape = (n // gp, n, 128)
        self.yrows = -(-na * h // 8) * 8
        self.yshape = (n // 2, self.yrows, 128)
        self.xshape = (hx, na, R, 128)
        self.nx = n + hx


L0 = Spec(48, 5, 3, 8, 8, 64, 6)
L1 = Spec(24, 12, 2, 4, 16, 56, 12)


def sds(*shape):
    return jax.ShapeDtypeStruct(shape, F32)


def run(kernel, outs, args, scratch=(), mib=12):
    vmem = pl.BlockSpec(memory_space=pltpu.VMEM)
    return pl.pallas_call(
        kernel,
        out_shape=outs,
        in_specs=[vmem] * len(args),
        out_specs=jax.tree.map(lambda _: vmem, outs),
        scratch_shapes=[pltpu.VMEM(s, F32) for s in scratch],
        compiler_params=pltpu.CompilerParams(vmem_limit_bytes=mib * 1024 * 1024),
    )(*args)


def place():
    return [lax.axis_index(a) for a in ("gx", "gy", "gz")] + [lax.axis_size(a) for a in ("gy", "gz")]


def lanes(rows):
    return lax.broadcasted_iota(jnp.int32, (rows, 128), 1)


def roll(v, shift, axis):
    if isinstance(shift, int):
        shift = shift % v.shape[axis]
        if shift == 0:
            return v
    return pltpu.roll(v, shift, axis)


def loop(n, f, u=1):
    u = max(d for d in range(1, u + 1) if n % d == 0)

    def some(i, c):
        for k in range(u):
            f(i * u + k)
        return c

    lax.fori_loop(0, n // u, some, 0)


def edge(sp, ids):
    _, gy, gz, ny, nz = ids
    high = jnp.where(gz < nz - 1, sp.n + sp.h, sp.n)
    low = jnp.where(gz > 0, 128 - sp.h, 128)
    return high, low, jnp.where(gy > 0, 1.0, 0.0), jnp.where(gy < ny - 1, 1.0, 0.0)


def zpack(sp, get, hi_ref, lo_ref):
    ln = lanes(sp.n)

    def group(g):
        hi = jnp.zeros((sp.n, 128), F32)
        lo = hi
        for j in range(sp.gp):
            for a in range(sp.na):
                v = get(g * sp.gp + j, a, 0, sp.n)
                at = sp.lw * j + sp.h * a
                here = (ln >= at) & (ln < at + sp.h)
                hi = jnp.where(here, roll(v, at - (sp.n - sp.h), 1), hi)
                lo = jnp.where(here, roll(v, at, 1), lo)
        hi_ref[g] = hi
        lo_ref[g] = lo

    loop(sp.n // sp.gp, group)


def ypack(sp, get, zl, zh, up_ref, dn_ref):
    n, h = sp.n, sp.h
    up0 = (n - h) // 8 * 8
    dn1 = -(-h // 8) * 8

    def fold(x, g, j, a, b, e):
        o = 64 * (j % 2)
        ln = lanes(e - b)
        at = sp.lw * j + h * a
        own = roll(get(x, a, b, e), o, 1)
        high = roll(zh[g, b:e, :], o + n - at, 1)
        low = roll(zl[g, b:e, :], o + 64 - h - at, 1)
        return jnp.where(ln < o + n, own, jnp.where(ln < o + n + h, high, low))

    def group(g):
        for q in range(sp.gp // 2):
            p = g * (sp.gp // 2) + q
            for a in range(sp.na):
                for ref, b, e, s, t in ((up_ref, up0, n, n - h - up0, n - up0), (dn_ref, 0, dn1, 0, h)):
                    even = fold(g * sp.gp + 2 * q, g, 2 * q, a, b, e)
                    odd = fold(g * sp.gp + 2 * q + 1, g, 2 * q + 1, a, b, e)
                    both = jnp.where(lanes(e - b) < 64, even, odd)
                    ref[p, a * h : (a + 1) * h, :] = both[s:t]
            if sp.yrows > sp.na * h:
                pad = jnp.zeros((sp.yrows - sp.na * h, 128), F32)
                up_ref[p, sp.na * h :, :] = pad
                dn_ref[p, sp.na * h :, :] = pad

    loop(n // sp.gp, group)


def plane(sp, own, zl, zh, yl, yh, x, g, j, a, dst, xw, ends):
    n, h, r0 = sp.n, sp.h, sp.r0
    at = sp.lw * j + h * a
    ln = lanes(n)
    top, bottom, below, above = ends
    static = isinstance(j, int)

    def amount(k):
        return k - at if static else lax.rem(k + 128 - at, 128)

    high = roll(zh[g], amount(n), 1)
    low = roll(zl[g], amount(128 - h), 1)
    dst[xw, r0 : r0 + n, :] = jnp.where(ln < top, high, jnp.where(ln >= bottom, low, 0.0))
    dst[xw, r0 : r0 + n, 0:n] = own(x, a)
    lh = lanes(h)
    half = g * (sp.gp // 2) + j // 2
    dst[xw, 0:r0, :] = jnp.zeros((r0, 128), F32)
    dst[xw, r0 + n :, :] = jnp.zeros((sp.R - r0 - n, 128), F32)
    for ref, r, weight in ((yl, r0 - h, below), (yh, r0 + n, above)):
        u = ref[half, a * h : (a + 1) * h, :] * weight
        if static:
            near, far = (u, roll(u, 64, 1)) if j % 2 == 0 else (roll(u, 64, 1), u)
        else:
            t = 64 * lax.rem(j, 2)
            near, far = roll(u, t, 1), roll(u, 64 - t, 1)
        dst[xw, r : r + h, :] = jnp.where(lh < top, near, jnp.where(lh >= bottom, far, 0.0))


def domain(sp, n, h, r0, R, ids):
    row = lax.broadcasted_iota(jnp.int32, (R, 128), 0) - r0
    ln = lanes(R)
    z = jnp.where(ln < 64, ln, ln - 128)
    gy, gz, ny, nz = ids[1], ids[2], ids[3], ids[4]
    y_at, z_at = row + gy * n, z + gz * n
    ok = (row >= -h) & (row < n + h) & (z >= -h) & (z < n + h)
    return ok & (y_at >= 0) & (y_at < ny * n) & (z_at >= 0) & (z_at < nz * n)


def neighbours(ref, x):
    c = ref[x + 1]
    R = c.shape[0]
    s = ref[x] + ref[x + 2]
    s = s + (roll(c, 1, 0) + roll(c, R - 1, 0))
    return s + (roll(c, 1, 1) + roll(c, 127, 1))


def zero_ends(ref, n):
    ref[0] = jnp.zeros(ref.shape[1:], F32)
    ref[n + 1] = jnp.zeros(ref.shape[1:], F32)


def relax(src, dst, f, c, n, factor, u=9):
    def one(x):
        dst[x + 1] = (1.0 - W) * src[x + 1] + c[x] * (f[x] + factor * neighbours(src, x))

    loop(n, one, u)


def coarse_lane(l, signed):
    c = l // 2
    return jnp.where(l < 64, c, c + 64) if signed else c


def lane_map(signed, value):
    l = lax.broadcasted_iota(jnp.int32, (256, 128), 0) % 128
    m = lax.broadcasted_iota(jnp.int32, (256, 128), 1)
    return jnp.where(coarse_lane(l, signed) == m, value, 0.0).astype(jnp.bfloat16)


def spread_map(pick):
    m = lax.broadcasted_iota(jnp.int32, (256, 128), 0) % 128
    l = lax.broadcasted_iota(jnp.int32, (256, 128), 1)
    return jnp.where(pick(l) == m, 1.0, 0.0).astype(jnp.bfloat16)


def times(v, m):
    big = v.astype(jnp.bfloat16)
    rest = (v - big.astype(F32)).astype(jnp.bfloat16)
    return jnp.dot(jnp.concatenate([big, rest], axis=1), m, preferred_element_type=F32)


def coarsen_planes(pair, n, tmp, acc, signed, rows=None, u=2):
    half = acc.shape[1]
    rows = rows or 2 * half

    def one(x):
        tmp[x, 0:rows, :] = pair(x)
        acc[x] = tmp[x, pl.ds(0, half, stride=2), :] + tmp[x, pl.ds(1, half, stride=2), :]

    loop(n, one, u)
    v = acc[...].reshape(n * half, 128)
    acc[...] = times(v, lane_map(signed, 0.125)).reshape(n, half, 128)


def add_refined(coarse, n, src, dst, wide, m, u=3):
    rows = coarse.shape[1]
    wide[0:n, 0:rows, :] = times(coarse[...].reshape(n * rows, 128), m).reshape(n, rows, 128)
    R = dst.shape[1]

    def one(i):
        v = wide[i, 0 : R // 2, :]
        for k in range(2):
            dst[2 * i + 1, pl.ds(k, R // 2, stride=2), :] = v
        t = dst[2 * i + 1]
        dst[2 * i + 1] = src[2 * i + 1] + t
        dst[2 * i + 2] = src[2 * i + 2] + t

    loop(n, one, u)


def k_zpack0(x0, b, rea, hi, lo, s):
    for a, ref in enumerate((x0, b, rea)):
        def one(x, a=a, ref=ref):
            s[a, x, :, 0:48] = ref[x]
        loop(48, one, 4)
    zpack(L0, lambda x, a, p, q: s[a, x, p:q, :], hi, lo)


def k_ypack0(x0, b, rea, zl, zh, up, dn, s):
    for a, ref in enumerate((x0, b, rea)):
        def one(x, a=a, ref=ref):
            s[a, x, 0:8, 0:48] = ref[x, 0:8]
            s[a, x, 8:16, 0:48] = ref[x, 40:48]
        loop(48, one, 8)
    ypack(L0, lambda x, a, p, q: s[a, x, 0:8, :] if p == 0 else s[a, x, 8:16, :], zl, zh, up, dn)


def k_xpack(sp, own, zl, zh, yl, yh, out):
    ids = place()
    ends = edge(sp, ids)
    start = (1 - ids[0]) * (sp.n - sp.hx)

    def one(i):
        x = start + i
        g, j = lax.div(x, sp.gp), lax.rem(x, sp.gp)
        for a in range(sp.na):
            plane(sp, own, zl, zh, yl, yh, x, g, j, a, out.at[i], a, ends)

    loop(sp.hx, one, 2)


def k_xpack0(x0, b, rea, zl, zh, yl, yh, out):
    refs = (x0, b, rea)
    k_xpack(L0, lambda x, a: refs[a][x], zl, zh, yl, yh, out)


def assemble(sp, ids, own, zl, zh, yl, yh, xr, dsts):
    shift = ids[0] * sp.hx
    ends = edge(sp, ids)

    def group(g):
        for j in range(sp.gp):
            x = g * sp.gp + j
            for a, (dst, off) in enumerate(dsts):
                plane(sp, own, zl, zh, yl, yh, x, g, j, a, dst, x + shift + off, ends)

    loop(sp.n // sp.gp, group)
    other = (1 - ids[0]) * sp.n

    def take(i):
        for a, (dst, off) in enumerate(dsts):
            dst[other + i + off] = xr[i, a]

    loop(sp.hx, take, 2)


def k_down0(x0, b, rea, zl, zh, yl, yh, xr, f_out, c_out, e_out, f1, r1, z1h, z1l, xw, bw, rw, ew, tmp):
    ids = place()
    refs = (x0, b, rea)
    assemble(L0, ids, lambda x, a: refs[a][x], zl, zh, yl, yh, xr, ((xw, 1), (bw, 0), (rw, 0)))
    n = L0.nx
    ok = domain(L0, 48, 5, 8, 64, ids)
    zero_ends(xw, n)
    zero_ends(ew, n)
    zero_ends(e_out, n)

    def first(x):
        d = 6.0 + rw[x]
        c = jnp.where(ok, W / d, 0.0)
        f = bw[x] - d * xw[x + 1] + neighbours(xw, x)
        f_out[x] = f
        c_out[x] = c
        ew[x + 1] = c * f

    loop(n, first, 3)
    relax(ew, e_out, f_out, c_out, n, 1.0)
    shift = ids[0] * L0.hx

    def left(x):
        r = f_out[x] - (6.0 + rw[x]) * e_out[x + 1] + neighbours(e_out, x)
        return r[8:56]

    inner = lanes(48) < 48
    coarsen_planes(lambda x: jnp.where(inner, left(2 * x + shift) + left(2 * x + shift + 1), 0.0), 24, tmp, f1, True)

    def react(x):
        return jnp.where(inner, rw[2 * x + shift, 8:56, :] + rw[2 * x + shift + 1, 8:56, :], 0.0)

    coarsen_planes(react, 24, tmp, r1, True)
    both = (f1, r1)
    zpack(L1, lambda x, a, p, q: both[a][x, p:q, :], z1h, z1l)


def k_ypack1(f1, r1, zl, zh, up, dn):
    both = (f1, r1)
    ypack(L1, lambda x, a, p, q: both[a][x, p:q, :], zl, zh, up, dn)


def k_xpack1(f1, r1, zl, zh, yl, yh, out):
    both = (f1, r1)
    k_xpack(L1, lambda x, a: both[a][x, :, 0:24], zl, zh, yl, yh, out)


def k_down1(f1, r1, zl, zh, yl, yh, xr, fw, cw, e_out, f2, c2, e2, out3, rw, ew, tmp, r2, ew2, tmp2, t3, sq):
    ids = place()
    both = (f1, r1)
    assemble(L1, ids, lambda x, a: both[a][x, :, 0:24], zl, zh, yl, yh, xr, ((fw, 0), (rw, 0)))
    n = L1.nx
    ok = domain(L1, 24, 12, 16, 56, ids)
    zero_ends(ew, n)
    zero_ends(e_out, n)

    def first(x):
        c = jnp.where(ok, W / (1.5 + rw[x]), 0.0)
        cw[x] = c
        ew[x + 1] = c * fw[x]

    loop(n, first, 4)
    relax(ew, e_out, fw, cw, n, 0.25)

    def left(x):
        return fw[x] - (1.5 + rw[x]) * e_out[x + 1] + 0.25 * neighbours(e_out, x)

    def pad(x):
        tmp[x, 56:64, :] = jnp.zeros((8, 128), F32)

    loop(18, pad, 3)
    coarsen_planes(lambda x: left(2 * x) + left(2 * x + 1), 18, tmp, f2, True, 56)
    coarsen_planes(lambda x: rw[2 * x] + rw[2 * x + 1], 18, tmp, r2, True, 56)
    ok2 = domain(None, 12, 6, 8, 32, ids)
    zero_ends(ew2, 18)
    zero_ends(e2, 18)

    def second(x):
        c = jnp.where(ok2, W / (0.375 + r2[x]), 0.0)
        c2[x] = c
        ew2[x + 1] = c * f2[x]

    loop(18, second, 6)
    relax(ew2, e2, f2, c2, 18, 0.0625, 18)

    def left2(x):
        return f2[x] - (0.375 + r2[x]) * e2[x + 1] + 0.0625 * neighbours(e2, x)

    coarsen_planes(lambda x: left2(2 * x) + left2(2 * x + 1), 9, tmp2, t3.at[0], True, u=3)
    coarsen_planes(lambda x: r2[2 * x] + r2[2 * x + 1], 9, tmp2, t3.at[1], True, u=3)
    shift = ids[0] * 3
    sq[...] = jnp.zeros((128, 128), F32)
    for a in range(2):
        for x in range(6):
            at = a * 36 + x * 6
            sq[at : at + 6, :] = t3[a, x + shift, 4:10, :]
    t = sq[...].T[0:8]
    ln = lanes(1)
    rows = []
    for u in range(2):
        for a in range(2):
            parts = [roll(t, 36 * (w - a), 1)[3 * u + w : 3 * u + w + 1] for w in range(3)]
            rows.append(jnp.where(ln < 36, parts[0], jnp.where(ln < 72, parts[1], parts[2])))
    tile = jnp.concatenate(rows + rows, axis=0)
    n8 = out3.shape[0] // 8
    out3[...] = jnp.broadcast_to(tile[None], (n8, 8, 128)).reshape(n8 * 8, 128)


def sum_all(v):
    s = jnp.sum(v, axis=0)
    return jnp.sum(jnp.sum(s, axis=1, keepdims=True), axis=0, keepdims=True)


def coarse_solve(g3, nx, ny, nz, e3, s3, f3, c3, r3, tmp, f4, r4, wide, sq):
    R = f3.shape[1]
    for ref in (f3, r3):
        ref[...] = jnp.zeros(ref.shape, F32)
    kx, ky, kz = nx // 6, ny // 6, nz // 6
    for bx in range(kx):
        for by in range(ky):
            k = bx * ky + by
            if kz * 6 < 128:
                sq[k, kz * 6 :, :] = jnp.zeros((128 - kz * 6, 128), F32)
            got = [g3[pl.ds(k * kz * 4 + r, kz, stride=4), :] for r in range(4)]
            ln = lanes(kz)
            for u in range(2):
                for w in range(3):
                    f, r = roll(got[2 * u], -36 * w, 1), roll(got[2 * u + 1], 36 - 36 * w, 1)
                    sq[k, pl.ds(3 * u + w, kz, stride=6), :] = jnp.where(ln < 36, f, r)
            t = sq[k].T
            for x in range(6):
                f3[bx * 6 + x, by * 6 : by * 6 + 6, :] = t[x * 6 : x * 6 + 6]
                r3[bx * 6 + x, by * 6 : by * 6 + 6, :] = t[36 + x * 6 : 42 + x * 6]
    factor = 0.25**3
    ok = (lax.broadcasted_iota(jnp.int32, (R, 128), 0) < ny) & (lanes(R) < nz)
    for ref in (e3, s3):
        zero_ends(ref, nx)

    def first(x):
        c = jnp.where(ok, W / (6.0 * factor + r3[x]), 0.0)
        c3[x] = c
        s3[x + 1] = c * f3[x]

    loop(nx, first, 6)
    relax(s3, e3, f3, c3, nx, factor, 6)

    def left(x):
        v = f3[x] - (6.0 * factor + r3[x]) * e3[x + 1] + factor * neighbours(e3, x)
        return jnp.where(ok, v, 0.0)

    coarsen_planes(lambda x: left(2 * x) + left(2 * x + 1), nx // 2, tmp, f4, False, u=3)
    coarsen_planes(lambda x: r3[2 * x] + r3[2 * x + 1], nx // 2, tmp, r4, False, u=3)
    f4k = 0.25**4
    H = R // 2
    row = lax.broadcasted_iota(jnp.int32, (nx // 2, H, 128), 1)
    lane = lax.broadcasted_iota(jnp.int32, (nx // 2, H, 128), 2)
    inside = (row < ny // 2) & (lane < nz // 2)
    diag = 6.0 * f4k + r4[...]
    zero = jnp.zeros((1, H, 128), F32)

    def apply(p):
        s = jnp.concatenate([zero, p[:-1]], axis=0) + jnp.concatenate([p[1:], zero], axis=0)
        s = s + roll(p, 1, 1) + roll(p, H - 1, 1) + roll(p, 1, 2) + roll(p, 127, 2)
        return jnp.where(inside, diag * p - f4k * s, 0.0)

    r = jnp.where(inside, f4[...], 0.0)
    p = r
    e = jnp.zeros_like(r)
    rr = sum_all(r * r)
    for i in range(BOTTOM_ITERS):
        q = apply(p)
        a = rr / sum_all(p * q)
        e = e + a * p
        if i + 1 < BOTTOM_ITERS:
            r = r - a * q
            new = sum_all(r * r)
            p = r + (new / rr) * p
            rr = new
    f4[...] = e
    add_refined(f4, nx // 2, e3, s3, wide, spread_map(lambda l: coarse_lane(l, False)))
    relax(s3, e3, f3, c3, nx, factor, 6)
    relax(e3, s3, f3, c3, nx, factor, 6)


def k_up(g3, f2, c2, e2i, f1, c1, e1i, f0, c0, e0i, rea, z_out, az_out, f_own, sums,
         e3, s3, f3, c3, r3, tmp3, f4, r4, sq, w3, w2, n1, w1, e2, s2, e1, s1, e0, s0):
    gx, gy, gz, sy, sz = place()
    nx, ny, nz = f3.shape[0], sy * 6, sz * 6
    coarse_solve(g3, nx, ny, nz, e3, s3, f3, c3, r3, tmp3, f4, r4, w3, sq)
    for ref, n in ((s2, 18), (s1, 36), (s0, 54), (e2, 18), (e1, 36), (e0, 54)):
        zero_ends(ref, n)
    R3 = s3.shape[1]
    pick = lax.broadcasted_iota(jnp.int32, (16, R3), 1) == lax.broadcasted_iota(jnp.int32, (16, R3), 0) + (gy * 6 - 4)
    pick = pick.astype(F32)
    for i in range(9):
        w3[i, 0:16, :] = jnp.dot(pick, s3[i + 1 + gx * 3], precision=HI, preferred_element_type=F32)
    spread = spread_map(lambda l: gz * 6 + jnp.where(l < 64, l // 2, l // 2 - 64))
    add_refined(w3.at[:, 0:16, :], 9, e2i, e2, w2, spread)
    relax(e2, s2, f2, c2, 18, 0.0625, 18)
    relax(s2, e2, f2, c2, 18, 0.0625, 18)
    m = spread_map(lambda l: coarse_lane(l, True))
    add_refined(e2.at[1:19], 18, e1i, e1, w2, m)
    relax(e1, s1, f1, c1, 36, 0.25)
    relax(s1, e1, f1, c1, 36, 0.25)

    def near(i):
        n1[i] = e1[i + 1 + gx * 9, 12:44, :]

    loop(27, near, 3)
    add_refined(n1, 27, e0i, e0, w1, m)
    ok0 = domain(L0, 48, 5, 8, 64, (gx, gy, gz, sy, sz))

    def mask(x):
        e0[x + 1] = jnp.where(ok0, e0[x + 1], 0.0)

    loop(54, mask, 3)
    relax(e0, s0, f0, c0, 54, 1.0)
    relax(s0, e0, f0, c0, 54, 1.0)
    shift = gx * 6

    def last(x, carry):
        u, v = carry
        z = e0[x + shift + 1][8:56, 0:48]
        nb = neighbours(e0, x + shift)[8:56, 0:48]
        az = (6.0 + rea[x]) * z - nb
        f = f0[x + shift][8:56, 0:48]
        z_out[x] = z
        az_out[x] = az
        f_own[x] = f
        return u + f * z, v + z * az

    zero = jnp.zeros((48, 48), F32)
    u, v = lax.fori_loop(0, 24, lambda i, c: last(2 * i + 1, last(2 * i, c)), (zero, zero))

    def total(t):
        return jnp.sum(jnp.sum(t, axis=1, keepdims=True), axis=0, keepdims=True)

    ln = lanes(sums.shape[0])
    sums[...] = jnp.where(ln == 0, total(u), jnp.where(ln == 1, total(v), 0.0))


def k_last(sums, x0, z, az, f, sol, res):
    s = jnp.sum(sums[...], axis=0, keepdims=True)
    ln = lanes(1)
    upper = jnp.sum(jnp.where(ln == 0, s, 0.0), axis=1, keepdims=True)
    lower = jnp.sum(jnp.where(ln == 1, s, 0.0), axis=1, keepdims=True)
    step = upper / lower

    def one(x):
        sol[x] = x0[x] + step * z[x]
        res[x] = f[x] - step * az[x]

    loop(48, one, 4)


def ring(up, dn, axis):
    n = lax.axis_size(axis)
    low = lax.ppermute(up, axis, [(i, (i + 1) % n) for i in range(n)])
    high = lax.ppermute(dn, axis, [(i, (i - 1) % n) for i in range(n)])
    return low, high


def swap(v):
    return lax.ppermute(v, "gx", [(0, 1), (1, 0)])


def body(b, x0, rea):
    ALL = ("gx", "gy", "gz")
    sizes = [lax.axis_size(a) for a in ALL]
    count = sizes[0] * sizes[1] * sizes[2]
    hi, lo = run(k_zpack0, (sds(*L0.zshape),) * 2, (x0, b, rea), [(3, 48, 48, 128)])
    zl, zh = ring(hi, lo, "gz")
    up, dn = run(k_ypack0, (sds(*L0.yshape),) * 2, (x0, b, rea, zl, zh), [(3, 48, 16, 128)])
    yl, yh = ring(up, dn, "gy")
    xs = run(k_xpack0, sds(*L0.xshape), (x0, b, rea, zl, zh, yl, yh))
    xr = swap(xs)
    p0 = (54, 64, 128)
    q0 = (56, 64, 128)
    f0, c0, e0, f1, r1, z1h, z1l = run(
        k_down0,
        (sds(*p0), sds(*p0), sds(*q0), sds(24, 24, 128), sds(24, 24, 128), sds(*L1.zshape), sds(*L1.zshape)),
        (x0, b, rea, zl, zh, yl, yh, xr),
        [q0, p0, p0, q0, (24, 48, 128)],
        mib=M0,
    )
    zl, zh = ring(z1h, z1l, "gz")
    up, dn = run(k_ypack1, (sds(*L1.yshape),) * 2, (f1, r1, zl, zh))
    yl, yh = ring(up, dn, "gy")
    xs = run(k_xpack1, sds(*L1.xshape), (f1, r1, zl, zh, yl, yh))
    xr = swap(xs)
    p1, q1, p2, q2 = (36, 56, 128), (38, 56, 128), (18, 32, 128), (20, 32, 128)
    f1w, c1w, e1w, f2w, c2w, e2w, g = run(
        k_down1,
        (sds(*p1), sds(*p1), sds(*q1), sds(*p2), sds(*p2), sds(*q2), sds(count * 4, 128)),
        (f1, r1, zl, zh, yl, yh, xr),
        [p1, q1, (18, 64, 128), p2, q2, (9, 32, 128), (2, 9, 16, 128), (128, 128)],
        mib=M1,
    )
    g = lax.all_to_all(g, ALL, 0, 0, tiled=True)
    n3 = [6 * s for s in sizes]
    R3 = (n3[1] + 8) // 8 * 8
    if R3 % 16:
        R3 += 8
    p3, q3, p4 = (n3[0], R3, 128), (n3[0] + 2, R3, 128), (n3[0] // 2, R3 // 2, 128)
    z, az, f, sums = run(
        k_up,
        (sds(48, 48, 48), sds(48, 48, 48), sds(48, 48, 48), sds(count, 128)),
        (g, f2w, c2w, e2w, f1w, c1w, e1w, f0, c0, e0, rea),
        [q3, q3, p3, p3, p3, (n3[0] // 2, R3, 128), p4, p4, (sizes[0] * sizes[1], 128, 128), (9, 16, 128), (18, 32, 128),
         (27, 32, 128), (27, 32, 128), q2, q2, q1, q1, q0, q0],
        mib=M2,
    )
    sums = lax.all_to_all(sums.reshape(count, 1, 128), ALL, 0, 0, tiled=True).reshape(count, 128)
    return run(k_last, (sds(48, 48, 48), sds(48, 48, 48)), (sums, x0, z, az, f))


def solution(mesh):
    spec = P("gx", "gy", "gz")
    return jax.shard_map(body, mesh=mesh, in_specs=(spec, spec, spec), out_specs=(spec, spec), check_vma=False)
```

```python
import functools
import jax
import jax.numpy as jnp
from jax import lax
from jax.experimental import pallas as pl
from jax.experimental.pallas import tpu as pltpu
from jax.sharding import PartitionSpec as P

W = 6.0 / 7.0
BOTTOM_ITERS = 6
N0 = 48
F32 = jnp.float32
HI = lax.Precision.HIGHEST
M0, M1, M2 = 10, 8, 12


class Spec:
    def __init__(self, n, h, na, R, o, hx, cut, kp, st):
        self.n, self.h, self.na, self.R, self.o, self.hx, self.cut, self.kp, self.st = n, h, na, R, o, hx, cut, kp, st
        self.half = n // 2
        self.zshape = (n // (kp * st), self.half * st, 128)
        self.yrows = -(-na * h // 8) * 8
        self.yshape = (self.half, self.yrows, 128)
        self.xshape = (hx, na, R, 128)
        self.nx = n + hx


L0 = Spec(48, 5, 3, 32, 8, 6, 56, 4, 1)
L1 = Spec(24, 12, 2, 24, 12, 12, 44, 2, 2)


def sds(*shape):
    return jax.ShapeDtypeStruct(shape, F32)


def run(kernel, outs, args, scratch=(), mib=12):
    vmem = pl.BlockSpec(memory_space=pltpu.VMEM)
    return pl.pallas_call(
        kernel,
        out_shape=outs,
        in_specs=[vmem] * len(args),
        out_specs=jax.tree.map(lambda _: vmem, outs),
        scratch_shapes=[pltpu.VMEM(s, F32) for s in scratch],
        compiler_params=pltpu.CompilerParams(vmem_limit_bytes=mib * 1024 * 1024),
    )(*args)


def place():
    return [lax.axis_index(a) for a in ("gx", "gy", "gz")] + [lax.axis_size(a) for a in ("gy", "gz")]


def lanes(rows):
    return lax.broadcasted_iota(jnp.int32, (rows, 128), 1)


def roll(v, shift, axis):
    if isinstance(shift, int):
        shift = shift % v.shape[axis]
        if shift == 0:
            return v
    return pltpu.roll(v, shift, axis)


def loop(n, f, u=1):
    u = max(d for d in range(1, u + 1) if n % d == 0)

    def some(i, c):
        for k in range(u):
            f(i * u + k)
        return c

    lax.fori_loop(0, n // u, some, 0)


def upper(sp, rows):
    l = lanes(rows)
    return (l >= sp.cut) & (l < sp.cut + 64)


def edge(sp, ids):
    _, gy, gz, ny, nz = ids
    high = jnp.where(gz < nz - 1, sp.n + sp.h, sp.n)
    low = jnp.where(gz > 0, 64 - sp.h, 64)
    return high, low, jnp.where(gy > 0, 1.0, 0.0), jnp.where(gy < ny - 1, 1.0, 0.0)


def zpack(sp, own, hi_ref, lo_ref):
    q = lanes(sp.half) % 64

    def tile(g):
        for t in range(sp.st):
            hi = jnp.zeros((sp.half, 128), F32)
            lo = hi
            for k in range(sp.kp):
                for a in range(sp.na):
                    v = own(t * (sp.n // sp.st) + g * sp.kp + k, a)
                    at = sp.h * (k * sp.na + a)
                    here = (q >= at) & (q < at + sp.h)
                    hi = jnp.where(here, roll(v, at - (sp.n - sp.h), 1), hi)
                    lo = jnp.where(here, roll(v, at, 1), lo)
            hi_ref[g, t * sp.half : (t + 1) * sp.half, :] = hi
            lo_ref[g, t * sp.half : (t + 1) * sp.half, :] = lo

    loop(sp.zshape[0], tile, 2)


def merged(sp, own, zl, zh, x, a, b, e, top, bottom):
    per = sp.n // sp.st
    t, y = lax.div(x, per), lax.rem(x, per)
    g, k = lax.div(y, sp.kp), lax.rem(y, sp.kp)
    at = sp.h * (k * sp.na + a)
    if sp.st == 1:
        high, low = zh[g, b:e, :], zl[g, b:e, :]
    else:
        high = jnp.where(t == 0, zh[g, b:e, :], zh[g, sp.half + b : sp.half + e, :])
        low = jnp.where(t == 0, zl[g, b:e, :], zl[g, sp.half + b : sp.half + e, :])
    high = roll(high, lax.rem(sp.n + 128 - at, 128), 1)
    low = roll(low, lax.rem(256 - sp.h - at, 128), 1)
    q = lanes(e - b) % 64
    return jnp.where(q < sp.n, own(x, a)[b:e], jnp.where(q < top, high, jnp.where(q >= bottom, low, 0.0)))


def ypack(sp, own, zl, zh, up_ref, dn_ref):
    h, half = sp.h, sp.half
    up0 = (half - h) // 8 * 8
    dn1 = min(half, -(-h // 8) * 8)
    top, bottom, _, _ = edge(sp, place())

    def pair(p):
        for a in range(sp.na):
            for ref, b, e, s, t, swap in ((up_ref, up0, half, half - h - up0, half - up0, False), (dn_ref, 0, dn1, 0, h, True)):
                even = merged(sp, own, zl, zh, 2 * p, a, b, e, top, bottom)
                odd = roll(merged(sp, own, zl, zh, 2 * p + 1, a, b, e, top, bottom), 64, 1)
                first, second = (odd, even) if swap else (even, odd)
                ref[p, a * h : (a + 1) * h, :] = jnp.where(upper(sp, e - b), first, second)[s:t]
        if sp.yrows > sp.na * h:
            pad = jnp.zeros((sp.yrows - sp.na * h, 128), F32)
            up_ref[p, sp.na * h :, :] = pad
            dn_ref[p, sp.na * h :, :] = pad

    loop(half, pair, 3)


def plane(sp, own, zl, zh, yl, yh, x, a, dst, xw, ends, spare):
    top, bottom, below, above = ends
    h, half = sp.h, sp.half
    m = merged(sp, own, zl, zh, x, a, 0, half, top, bottom)
    p = lax.div(x, 2)
    turn = 64 * (1 - lax.rem(x, 2))
    if sp.o == 8:
        low = roll(roll(yl[p], 8 - h - a * h, 0)[0:8], turn, 1) * below
        high = roll(roll(yh[p], -a * h, 0)[0:8], turn, 1) * above
        lower = jnp.concatenate([low, m], axis=0)
        higher = jnp.concatenate([m, high], axis=0)
        dst[xw] = jnp.where(upper(sp, sp.R), higher, lower)
    else:
        spare[0, 0:h, :] = roll(yl[p, a * h : (a + 1) * h, :], turn, 1) * below
        spare[0, h:, :] = m
        spare[1, 0:half, :] = m
        spare[1, half:, :] = roll(yh[p, a * h : (a + 1) * h, :], turn, 1) * above
        dst[xw] = jnp.where(upper(sp, sp.R), spare[1], spare[0])


def lane_z(sp, l):
    return jnp.where(l < sp.cut, l, jnp.where(l < sp.cut + 64, l - 64, l - 128))


def inside(sp, ids):
    _, gy, gz, ny, nz = ids
    n, h = sp.n, sp.h
    y = lax.broadcasted_iota(jnp.int32, (sp.R, 128), 0) - sp.o + jnp.where(upper(sp, sp.R), sp.R, 0)
    z = lane_z(sp, lanes(sp.R))
    ok = (y >= -h) & (y < n + h) & (z >= -h) & (z < n + h)
    y, z = y + gy * n, z + gz * n
    return ok & (y >= 0) & (y < ny * n) & (z >= 0) & (z < nz * n)


def paired(ref, x):
    c = ref[x + 1]
    R = c.shape[0]
    s = ref[x] + ref[x + 2]
    sub = lax.broadcasted_iota(jnp.int32, (8, 128), 0)
    seam = roll(jnp.where(sub == 0, c[0:8], c[R - 8 : R]), 64, 1)
    up, down = roll(c, R - 1, 0), roll(c, 1, 0)
    up = jnp.concatenate([up[: R - 8], jnp.where(sub == 7, roll(seam, 7, 0), up[R - 8 :])], axis=0)
    down = jnp.concatenate([jnp.where(sub == 0, roll(seam, 1, 0), down[0:8]), down[8:]], axis=0)
    s = s + (up + down)
    return s + (roll(c, 1, 1) + roll(c, 127, 1))


def domain(sp, n, h, r0, R, ids):
    row = lax.broadcasted_iota(jnp.int32, (R, 128), 0) - r0
    ln = lanes(R)
    z = jnp.where(ln < 64, ln, ln - 128)
    gy, gz, ny, nz = ids[1], ids[2], ids[3], ids[4]
    y_at, z_at = row + gy * n, z + gz * n
    ok = (row >= -h) & (row < n + h) & (z >= -h) & (z < n + h)
    return ok & (y_at >= 0) & (y_at < ny * n) & (z_at >= 0) & (z_at < nz * n)


def neighbours(ref, x):
    c = ref[x + 1]
    R = c.shape[0]
    s = ref[x] + ref[x + 2]
    s = s + (roll(c, 1, 0) + roll(c, R - 1, 0))
    return s + (roll(c, 1, 1) + roll(c, 127, 1))


def zero_ends(ref, n):
    ref[0] = jnp.zeros(ref.shape[1:], F32)
    ref[n + 1] = jnp.zeros(ref.shape[1:], F32)


def relax(src, dst, f, c, n, factor, u=9, near=None):
    near = near or neighbours

    def one(x):
        dst[x + 1] = (1.0 - W) * src[x + 1] + c[x] * (f[x] + factor * near(src, x))

    loop(n, one, u)


def lane_map(pick, value, cols=128):
    l = lax.broadcasted_iota(jnp.int32, (256, cols), 0) % 128
    m = lax.broadcasted_iota(jnp.int32, (256, cols), 1)
    return jnp.where(pick(l, m) == m, value, 0.0).astype(jnp.bfloat16)


def spread_map(pick):
    m = lax.broadcasted_iota(jnp.int32, (256, 128), 0) % 128
    l = lax.broadcasted_iota(jnp.int32, (256, 128), 1)
    return jnp.where(pick(l) == m, 1.0, 0.0).astype(jnp.bfloat16)


def floor_half(z):
    return lax.shift_right_arithmetic(z, 1)


def times(v, m):
    big = v.astype(jnp.bfloat16)
    rest = (v - big.astype(F32)).astype(jnp.bfloat16)
    return jnp.dot(jnp.concatenate([big, rest], axis=1), m, preferred_element_type=F32)


def coarsen_planes(pair, n, tmp, acc, rows, u=2):
    half = rows // 2

    def one(x):
        tmp[x, 0:rows, :] = pair(x)
        acc[x, 0:half, :] = tmp[x, pl.ds(0, half, stride=2), :] + tmp[x, pl.ds(1, half, stride=2), :]

    loop(n, one, u)


def flat(ref):
    n, rows, _ = ref.shape
    return ref[...].reshape(n * rows, 128)


def add_refined(wide, n, src, dst, u=3):
    R = dst.shape[1]

    def one(i):
        v = wide[i, 0 : R // 2, :]
        for k in range(2):
            dst[2 * i + 1, pl.ds(k, R // 2, stride=2), :] = v
        t = dst[2 * i + 1]
        dst[2 * i + 1] = src[2 * i + 1] + t
        dst[2 * i + 2] = src[2 * i + 2] + t

    loop(n, one, u)


def k_zpack0(x0, b, rea, hi, lo, own):
    def one(x):
        for a, ref in enumerate((x0, b, rea)):
            own[a, x, :, 0:48] = ref[x, 0:24, :]
            own[a, x, :, 64:112] = ref[x, 24:48, :]

    loop(48, one, 4)
    zpack(L0, lambda x, a: own[a, x], hi, lo)


def k_ypack0(own, zl, zh, up, dn):
    ypack(L0, lambda x, a: own[a, x], zl, zh, up, dn)


def xpack(sp, own, zl, zh, yl, yh, out, spare):
    ids = place()
    ends = edge(sp, ids)
    start = (1 - ids[0]) * (sp.n - sp.hx)

    def one(i):
        for a in range(sp.na):
            plane(sp, own, zl, zh, yl, yh, start + i, a, out.at[i], a, ends, None if spare is None else spare.at[a])

    loop(sp.hx, one, 2)


def k_xpack0(own, zl, zh, yl, yh, out):
    xpack(L0, lambda x, a: own[a, x], zl, zh, yl, yh, out, None)


def assemble(sp, ids, own, zl, zh, yl, yh, xr, dsts, spare, u):
    shift = ids[0] * sp.hx
    ends = edge(sp, ids)

    def some(i):
        for k in range(u):
            x = i * u + k
            for a, (dst, off) in enumerate(dsts):
                plane(sp, own, zl, zh, yl, yh, x, a, dst, x + shift + off, ends, None if spare is None else spare.at[k * sp.na + a])

    loop(sp.n // u, some)
    other = (1 - ids[0]) * sp.n

    def take(i):
        for a, (dst, off) in enumerate(dsts):
            dst[other + i + off] = xr[i, a]

    loop(sp.hx, take, 2)


def own_rows(sp, v):
    return jnp.where(upper(sp, sp.half), v[0 : sp.half], v[sp.o :])


def k_down0(own, zl, zh, yl, yh, xr, f_out, c_out, d_out, e_out, f1, r1, z1h, z1l, xw, bw, rw, ew, tmp, acc):
    ids = place()
    assemble(L0, ids, lambda x, a: own[a, x], zl, zh, yl, yh, xr, ((xw, 1), (bw, 0), (rw, 0)), None, 4)
    n = L0.nx
    ok = inside(L0, ids)
    zero_ends(xw, n)
    zero_ends(ew, n)
    zero_ends(e_out, n)

    def first(x):
        d = 6.0 + rw[x]
        c = jnp.where(ok, W / d, 0.0)
        f = bw[x] - d * xw[x + 1] + paired(xw, x)
        d_out[x] = d
        f_out[x] = f
        c_out[x] = c
        ew[x + 1] = c * f

    loop(n, first, 6)
    relax(ew, e_out, f_out, c_out, n, 1.0, 9, paired)
    shift = ids[0] * L0.hx

    def left(x):
        return own_rows(L0, f_out[x] - d_out[x] * e_out[x + 1] + paired(e_out, x))

    mine = lanes(24) % 64 < 48
    m = lane_map(lambda l, m: jnp.where(l < 64, l // 2, 32 + l // 2), 0.125)
    for ref, pair in (
        (f1, lambda x: left(2 * x + shift) + left(2 * x + shift + 1)),
        (r1, lambda x: own_rows(L0, rw[2 * x + shift] + rw[2 * x + shift + 1])),
    ):
        coarsen_planes(lambda x, pair=pair: jnp.where(mine, pair(x), 0.0), 24, tmp, acc, 24, 4)
        acc[...] = times(flat(acc), m).reshape(24, 16, 128)

        def keep(x, ref=ref):
            ref[x] = acc[x, 0:12, :]

        loop(24, keep, 6)
    both = (f1, r1)
    zpack(L1, lambda x, a: both[a][x], z1h, z1l)


def k_ypack1(f1, r1, zl, zh, up, dn):
    both = (f1, r1)
    ypack(L1, lambda x, a: both[a][x], zl, zh, up, dn)


def k_xpack1(f1, r1, zl, zh, yl, yh, out, spare):
    both = (f1, r1)
    xpack(L1, lambda x, a: both[a][x], zl, zh, yl, yh, out, spare)


def k_down1(f1, r1, zl, zh, yl, yh, xr, fw, cw, e_out, f2, c2, e2, out3, rw, ew, tmp, acc, r2, ew2, tmp2, t3, sq, spare):
    ids = place()
    both = (f1, r1)
    assemble(L1, ids, lambda x, a: both[a][x], zl, zh, yl, yh, xr, ((fw, 0), (rw, 0)), spare, 4)
    n = L1.nx
    ok = inside(L1, ids)
    zero_ends(ew, n)
    zero_ends(e_out, n)

    def first(x):
        c = jnp.where(ok, W / (1.5 + rw[x]), 0.0)
        cw[x] = c
        ew[x + 1] = c * fw[x]

    loop(n, first, 6)
    relax(ew, e_out, fw, cw, n, 0.25, 12, paired)

    def left(x):
        return fw[x] - (1.5 + rw[x]) * e_out[x + 1] + 0.25 * paired(e_out, x)

    def pick(l, m):
        z = lane_z(L1, l)
        up = (l >= L1.cut) & (l < L1.cut + 64)
        good = (z >= -12) & (z < 36) & (up == (m >= 128))
        return jnp.where(good, floor_half(z) + jnp.where(z < 0, 128, 0) + jnp.where(up, 128, 0), -1)

    m = lane_map(pick, 0.125, 256)
    for ref, pair in ((f2, lambda x: left(2 * x) + left(2 * x + 1)), (r2, lambda x: rw[2 * x] + rw[2 * x + 1])):
        coarsen_planes(pair, 18, tmp, acc.at[0], 24, 6)
        v = times(flat(acc.at[0]), m)
        acc[0] = v[:, 0:128].reshape(18, 16, 128)
        acc[1] = v[:, 128:256].reshape(18, 16, 128)

        def keep(x, ref=ref):
            ref[x] = jnp.zeros((32, 128), F32)
            ref[x, 2:14, :] = acc[0, x, 0:12, :]
            ref[x, 14:26, :] = acc[1, x, 0:12, :]

        loop(18, keep, 6)
    ok2 = domain(None, 12, 6, 8, 32, ids)
    zero_ends(ew2, 18)
    zero_ends(e2, 18)

    def second(x):
        c = jnp.where(ok2, W / (0.375 + r2[x]), 0.0)
        c2[x] = c
        ew2[x + 1] = c * f2[x]

    loop(18, second, 6)
    relax(ew2, e2, f2, c2, 18, 0.0625, 18)

    def left2(x):
        return f2[x] - (0.375 + r2[x]) * e2[x + 1] + 0.0625 * neighbours(e2, x)

    m = lane_map(lambda l, m: jnp.where(l < 64, l // 2, l // 2 + 64), 0.125)
    for a, pair in enumerate((lambda x: left2(2 * x) + left2(2 * x + 1), lambda x: r2[2 * x] + r2[2 * x + 1])):
        coarsen_planes(pair, 9, tmp2, t3.at[a], 32, 9)
        t3[a] = times(flat(t3.at[a]), m).reshape(9, 16, 128)
    shift = ids[0] * 3
    sq[...] = jnp.zeros((128, 128), F32)
    for a in range(2):
        for x in range(6):
            at = a * 36 + x * 6
            sq[at : at + 6, :] = t3[a, x + shift, 4:10, :]
    t = sq[...].T[0:8]
    ln = lanes(1)
    rows = []
    for u in range(2):
        for a in range(2):
            parts = [roll(t, 36 * (w - a), 1)[3 * u + w : 3 * u + w + 1] for w in range(3)]
            rows.append(jnp.where(ln < 36, parts[0], jnp.where(ln < 72, parts[1], parts[2])))
    tile = jnp.concatenate(rows + rows, axis=0)
    n8 = out3.shape[0] // 8
    out3[...] = jnp.broadcast_to(tile[None], (n8, 8, 128)).reshape(n8 * 8, 128)


def sum_all(v):
    s = jnp.sum(v, axis=0)
    return jnp.sum(jnp.sum(s, axis=1, keepdims=True), axis=0, keepdims=True)


def coarse_solve(g3, nx, ny, nz, e3, s3, f3, c3, r3, tmp, f4, r4, sq):
    R = f3.shape[1]
    for ref in (f3, r3):
        ref[...] = jnp.zeros(ref.shape, F32)
    kx, ky, kz = nx // 6, ny // 6, nz // 6
    for bx in range(kx):
        for by in range(ky):
            k = bx * ky + by
            if kz * 6 < 128:
                sq[k, kz * 6 :, :] = jnp.zeros((128 - kz * 6, 128), F32)
            got = [g3[pl.ds(k * kz * 4 + r, kz, stride=4), :] for r in range(4)]
            ln = lanes(kz)
            for u in range(2):
                for w in range(3):
                    f, r = roll(got[2 * u], -36 * w, 1), roll(got[2 * u + 1], 36 - 36 * w, 1)
                    sq[k, pl.ds(3 * u + w, kz, stride=6), :] = jnp.where(ln < 36, f, r)
            t = sq[k].T
            for x in range(6):
                f3[bx * 6 + x, by * 6 : by * 6 + 6, :] = t[x * 6 : x * 6 + 6]
                r3[bx * 6 + x, by * 6 : by * 6 + 6, :] = t[36 + x * 6 : 42 + x * 6]
    factor = 0.25**3
    ok = (lax.broadcasted_iota(jnp.int32, (R, 128), 0) < ny) & (lanes(R) < nz)
    for ref in (e3, s3):
        zero_ends(ref, nx)

    def first(x):
        c = jnp.where(ok, W / (6.0 * factor + r3[x]), 0.0)
        c3[x] = c
        s3[x + 1] = c * f3[x]

    loop(nx, first, 6)
    relax(s3, e3, f3, c3, nx, factor, 6)

    def left(x):
        v = f3[x] - (6.0 * factor + r3[x]) * e3[x + 1] + factor * neighbours(e3, x)
        return jnp.where(ok, v, 0.0)

    m = lane_map(lambda l, m: l // 2, 0.125)
    for ref, pair in ((f4, lambda x: left(2 * x) + left(2 * x + 1)), (r4, lambda x: r3[2 * x] + r3[2 * x + 1])):
        coarsen_planes(pair, nx // 2, tmp, ref, R, 6)
        ref[...] = times(flat(ref), m).reshape(ref.shape)
    f4k = 0.25**4
    H = R // 2
    row = lax.broadcasted_iota(jnp.int32, (nx // 2, H, 128), 1)
    lane = lax.broadcasted_iota(jnp.int32, (nx // 2, H, 128), 2)
    within = (row < ny // 2) & (lane < nz // 2)
    diag = 6.0 * f4k + r4[...]
    zero = jnp.zeros((1, H, 128), F32)

    def apply(p):
        s = jnp.concatenate([zero, p[:-1]], axis=0) + jnp.concatenate([p[1:], zero], axis=0)
        s = s + roll(p, 1, 1) + roll(p, H - 1, 1) + roll(p, 1, 2) + roll(p, 127, 2)
        return jnp.where(within, diag * p - f4k * s, 0.0)

    r = jnp.where(within, f4[...], 0.0)
    p = r
    e = jnp.zeros_like(r)
    rr = sum_all(r * r)
    for i in range(BOTTOM_ITERS):
        q = apply(p)
        a = rr / sum_all(p * q)
        e = e + a * p
        if i + 1 < BOTTOM_ITERS:
            r = r - a * q
            new = sum_all(r * r)
            p = r + (new / rr) * p
            rr = new
    f4[...] = times(e.reshape(nx // 2 * H, 128), spread_map(lambda l: l // 2)).reshape(e.shape)
    add_refined(f4, nx // 2, e3, s3, 6)
    relax(s3, e3, f3, c3, nx, factor, 6)
    relax(e3, s3, f3, c3, nx, factor, 6)


def k_up(g3, f2, c2, e2i, f1, c1, e1i, f0, c0, d0, e0i, z_out, az_out, sums,
         e3, s3, f3, c3, r3, tmp3, f4, r4, sq, w3, w2, na, nb, n1, e2, s2, e1, s1, e0, s0):
    gx, gy, gz, sy, sz = place()
    nx, ny, nz = f3.shape[0], sy * 6, sz * 6
    coarse_solve(g3, nx, ny, nz, e3, s3, f3, c3, r3, tmp3, f4, r4, sq)
    for ref, n in ((s2, 18), (s1, 36), (s0, 54), (e2, 18), (e1, 36), (e0, 54)):
        zero_ends(ref, n)
    R3 = s3.shape[1]
    pick = lax.broadcasted_iota(jnp.int32, (16, R3), 1) == lax.broadcasted_iota(jnp.int32, (16, R3), 0) + (gy * 6 - 4)
    pick = pick.astype(F32)
    for i in range(9):
        w3[i] = jnp.dot(pick, s3[i + 1 + gx * 3], precision=HI, preferred_element_type=F32)
    spread = spread_map(lambda l: gz * 6 + jnp.where(l < 64, l // 2, l // 2 - 64))
    w3[...] = times(flat(w3), spread).reshape(9, 16, 128)
    add_refined(w3, 9, e2i, e2, 9)
    relax(e2, s2, f2, c2, 18, 0.0625, 18)
    relax(s2, e2, f2, c2, 18, 0.0625, 18)

    def halves(i):
        na[i] = e2[i + 1, 2:18, :]
        nb[i] = e2[i + 1, 14:30, :]

    loop(18, halves, 6)

    def down(sp, l, want):
        z = lane_z(sp, l)
        up = (l >= sp.cut) & (l < sp.cut + 64)
        good = (z >= -sp.h) & (z < sp.n + sp.h)
        good = good & (up if want else jnp.logical_not(up))
        return jnp.where(good, floor_half(z) + jnp.where(z < 0, 128, 0), -1)

    w2[...] = (
        times(flat(na), spread_map(lambda l: down(L1, l, False))) + times(flat(nb), spread_map(lambda l: down(L1, l, True)))
    ).reshape(18, 16, 128)
    add_refined(w2, 18, e1i, e1, 6)
    relax(e1, s1, f1, c1, 36, 0.25, 12, paired)
    relax(s1, e1, f1, c1, 36, 0.25, 12, paired)

    def near(i):
        v = e1[i + 1 + gx * 9]
        n1[i] = jnp.where(upper(L1, 16), v[0:16], v[8:24])

    loop(27, near, 9)

    def both(l):
        lower, higher = down(L0, l, False), down(L0, l, True)
        return jnp.where(lower >= 0, lower, jnp.where(higher >= 0, (higher + 64) % 128, -1))

    n1[...] = times(flat(n1), spread_map(both)).reshape(27, 16, 128)
    add_refined(n1, 27, e0i, e0, 9)
    relax(e0, s0, f0, c0, 54, 1.0, 9, paired)
    relax(s0, e0, f0, c0, 54, 1.0, 9, paired)
    shift = gx * 6
    mine = lanes(24) % 64 < 48

    def last(x, carry):
        u, v = carry
        w = x + shift
        z = e0[w + 1]
        az = own_rows(L0, d0[w] * z - paired(e0, w))
        z = own_rows(L0, z)
        f = own_rows(L0, f0[w])
        z_out[x] = z
        az_out[x] = az
        return u + jnp.where(mine, f * z, 0.0), v + jnp.where(mine, z * az, 0.0)

    def some(i, carry):
        for k in range(6):
            carry = last(6 * i + k, carry)
        return carry

    zero = jnp.zeros((24, 128), F32)
    u, v = lax.fori_loop(0, 8, some, (zero, zero))

    def total(t):
        return jnp.sum(jnp.sum(t, axis=1, keepdims=True), axis=0, keepdims=True)

    ln = lanes(sums.shape[0])
    sums[...] = jnp.where(ln == 0, total(u), jnp.where(ln == 1, total(v), 0.0))


def k_last(sums, own, z, az, f, sol, res):
    s = jnp.sum(sums[...], axis=0, keepdims=True)
    ln = lanes(1)
    over = jnp.sum(jnp.where(ln == 0, s, 0.0), axis=1, keepdims=True)
    under = jnp.sum(jnp.where(ln == 1, s, 0.0), axis=1, keepdims=True)
    step = over / under
    shift = lax.axis_index("gx") * 6

    def one(x):
        for ref, v in ((sol, own[0, x] + step * z[x]), (res, own_rows(L0, f[x + shift]) - step * az[x])):
            ref[x, 0:24, :] = v[:, 0:48]
            ref[x, 24:48, :] = roll(v, 64, 1)[:, 0:48]

    loop(48, one, 4)


def ring(up, dn, axis):
    n = lax.axis_size(axis)
    low = lax.ppermute(up, axis, [(i, (i + 1) % n) for i in range(n)])
    high = lax.ppermute(dn, axis, [(i, (i - 1) % n) for i in range(n)])
    return low, high


def swap(v):
    return lax.ppermute(v, "gx", [(0, 1), (1, 0)])


def body(b, x0, rea):
    ALL = ("gx", "gy", "gz")
    sizes = [lax.axis_size(a) for a in ALL]
    count = sizes[0] * sizes[1] * sizes[2]
    hi, lo, own = run(k_zpack0, (sds(*L0.zshape), sds(*L0.zshape), sds(3, 48, 24, 128)), (x0, b, rea))
    zl, zh = ring(hi, lo, "gz")
    up, dn = run(k_ypack0, (sds(*L0.yshape),) * 2, (own, zl, zh))
    yl, yh = ring(up, dn, "gy")
    xr = swap(run(k_xpack0, sds(*L0.xshape), (own, zl, zh, yl, yh)))
    p0, q0 = (54, 32, 128), (56, 32, 128)
    f0, c0, d0, e0, f1, r1, z1h, z1l = run(
        k_down0,
        (sds(*p0), sds(*p0), sds(*p0), sds(*q0), sds(24, 12, 128), sds(24, 12, 128), sds(*L1.zshape), sds(*L1.zshape)),
        (own, zl, zh, yl, yh, xr),
        [q0, p0, p0, q0, (24, 24, 128), (24, 16, 128)],
        mib=M0,
    )
    zl, zh = ring(z1h, z1l, "gz")
    up, dn = run(k_ypack1, (sds(*L1.yshape),) * 2, (f1, r1, zl, zh))
    yl, yh = ring(up, dn, "gy")
    xr = swap(run(k_xpack1, sds(*L1.xshape), (f1, r1, zl, zh, yl, yh), [(2, 2, 24, 128)]))
    p1, q1, p2, q2 = (36, 24, 128), (38, 24, 128), (18, 32, 128), (20, 32, 128)
    f1w, c1w, e1w, f2w, c2w, e2w, g = run(
        k_down1,
        (sds(*p1), sds(*p1), sds(*q1), sds(*p2), sds(*p2), sds(*q2), sds(count * 4, 128)),
        (f1, r1, zl, zh, yl, yh, xr),
        [p1, q1, (18, 24, 128), (2, 18, 16, 128), p2, q2, (9, 32, 128), (2, 9, 16, 128), (128, 128), (8, 2, 24, 128)],
        mib=M1,
    )
    g = lax.all_to_all(g, ALL, 0, 0, tiled=True)
    n3 = [6 * s for s in sizes]
    R3 = (n3[1] + 8) // 8 * 8
    if R3 % 16:
        R3 += 8
    p3, q3, p4 = (n3[0], R3, 128), (n3[0] + 2, R3, 128), (n3[0] // 2, R3 // 2, 128)
    z, az, sums = run(
        k_up,
        (sds(48, 24, 128), sds(48, 24, 128), sds(count, 128)),
        (g, f2w, c2w, e2w, f1w, c1w, e1w, f0, c0, d0, e0),
        [q3, q3, p3, p3, p3, (n3[0] // 2, R3, 128), p4, p4, (sizes[0] * sizes[1], 128, 128), (9, 16, 128), (18, 16, 128),
         (18, 16, 128), (18, 16, 128), (27, 16, 128), q2, q2, q1, q1, q0, q0],
        mib=M2,
    )
    sums = lax.all_to_all(sums.reshape(count, 1, 128), ALL, 0, 0, tiled=True).reshape(count, 128)
    return run(k_last, (sds(48, 48, 48), sds(48, 48, 48)), (sums, own, z, az, f0))


def solution(mesh):
    spec = P("gx", "gy", "gz")
    return jax.shard_map(body, mesh=mesh, in_specs=(spec, spec, spec), out_specs=(spec, spec), check_vma=False)
```

```python
import functools
import jax
import jax.numpy as jnp
from jax import lax
from jax.experimental import pallas as pl
from jax.experimental.pallas import tpu as pltpu
from jax.sharding import PartitionSpec as P

W = 6.0 / 7.0
BOTTOM_ITERS = 6
N0 = 48
F32 = jnp.float32
HI = lax.Precision.HIGHEST
M0, M1, M2 = 10, 8, 12


class Spec:
    def __init__(self, n, h, na, R, o, hx, cut, kp, st):
        self.n, self.h, self.na, self.R, self.o, self.hx, self.cut, self.kp, self.st = n, h, na, R, o, hx, cut, kp, st
        self.half = n // 2
        self.zshape = (n // (kp * st), self.half * st, 128)
        self.yrows = -(-na * h // 8) * 8
        self.yshape = (self.half, self.yrows, 128)
        self.xshape = (hx, na, R, 128)
        self.nx = n + hx


L0 = Spec(48, 5, 3, 32, 8, 6, 56, 4, 1)
L1 = Spec(24, 12, 2, 24, 12, 12, 44, 2, 2)


def sds(*shape):
    return jax.ShapeDtypeStruct(shape, F32)


def run(kernel, outs, args, scratch=(), mib=12, far_in=False, far_out=False):
    vmem = pl.BlockSpec(memory_space=pltpu.VMEM)
    hbm = pl.BlockSpec(memory_space=pltpu.HBM)
    return pl.pallas_call(
        kernel,
        out_shape=outs,
        in_specs=[hbm if far_in else vmem] * len(args),
        out_specs=jax.tree.map(lambda _: hbm if far_out else vmem, outs),
        scratch_shapes=[pltpu.VMEM(s, F32) if isinstance(s, tuple) else s for s in scratch],
        compiler_params=pltpu.CompilerParams(vmem_limit_bytes=mib * 1024 * 1024),
    )(*args)


def place():
    return [lax.axis_index(a) for a in ("gx", "gy", "gz")] + [lax.axis_size(a) for a in ("gy", "gz")]


def lanes(rows):
    return lax.broadcasted_iota(jnp.int32, (rows, 128), 1)


def roll(v, shift, axis):
    if isinstance(shift, int):
        shift = shift % v.shape[axis]
        if shift == 0:
            return v
    return pltpu.roll(v, shift, axis)


def loop(n, f, u=1):
    u = max(d for d in range(1, u + 1) if n % d == 0)

    def some(i, c):
        for k in range(u):
            f(i * u + k)
        return c

    lax.fori_loop(0, n // u, some, 0)


def upper(sp, rows):
    l = lanes(rows)
    return (l >= sp.cut) & (l < sp.cut + 64)


def edge(sp, ids):
    _, gy, gz, ny, nz = ids
    high = jnp.where(gz < nz - 1, sp.n + sp.h, sp.n)
    low = jnp.where(gz > 0, 64 - sp.h, 64)
    return high, low, jnp.where(gy > 0, 1.0, 0.0), jnp.where(gy < ny - 1, 1.0, 0.0)


def ztile(sp, own, hi_ref, lo_ref, g):
    q = lanes(sp.half) % 64
    for t in range(sp.st):
        hi = jnp.zeros((sp.half, 128), F32)
        lo = hi
        for k in range(sp.kp):
            for a in range(sp.na):
                v = own(t * (sp.n // sp.st) + g * sp.kp + k, a)
                at = sp.h * (k * sp.na + a)
                here = (q >= at) & (q < at + sp.h)
                hi = jnp.where(here, roll(v, at - (sp.n - sp.h), 1), hi)
                lo = jnp.where(here, roll(v, at, 1), lo)
        hi_ref[g, t * sp.half : (t + 1) * sp.half, :] = hi
        lo_ref[g, t * sp.half : (t + 1) * sp.half, :] = lo


def merged(sp, own, zl, zh, x, a, b, e, top, bottom):
    per = sp.n // sp.st
    t, y = lax.div(x, per), lax.rem(x, per)
    g, k = lax.div(y, sp.kp), lax.rem(y, sp.kp)
    at = sp.h * (k * sp.na + a)
    if sp.st == 1:
        high, low = zh[g, b:e, :], zl[g, b:e, :]
    else:
        high = jnp.where(t == 0, zh[g, b:e, :], zh[g, sp.half + b : sp.half + e, :])
        low = jnp.where(t == 0, zl[g, b:e, :], zl[g, sp.half + b : sp.half + e, :])
    high = roll(high, lax.rem(sp.n + 128 - at, 128), 1)
    low = roll(low, lax.rem(256 - sp.h - at, 128), 1)
    q = lanes(e - b) % 64
    return jnp.where(q < sp.n, own(x, a)[b:e], jnp.where(q < top, high, jnp.where(q >= bottom, low, 0.0)))


def ypack(sp, own, zl, zh, up_ref, dn_ref):
    h, half = sp.h, sp.half
    up0 = (half - h) // 8 * 8
    dn1 = min(half, -(-h // 8) * 8)
    top, bottom, _, _ = edge(sp, place())

    def pair(p):
        for a in range(sp.na):
            for ref, b, e, s, t, swap in ((up_ref, up0, half, half - h - up0, half - up0, False), (dn_ref, 0, dn1, 0, h, True)):
                even = merged(sp, own, zl, zh, 2 * p, a, b, e, top, bottom)
                odd = roll(merged(sp, own, zl, zh, 2 * p + 1, a, b, e, top, bottom), 64, 1)
                first, second = (odd, even) if swap else (even, odd)
                ref[p, a * h : (a + 1) * h, :] = jnp.where(upper(sp, e - b), first, second)[s:t]
        if sp.yrows > sp.na * h:
            pad = jnp.zeros((sp.yrows - sp.na * h, 128), F32)
            up_ref[p, sp.na * h :, :] = pad
            dn_ref[p, sp.na * h :, :] = pad

    loop(half, pair, 3)


def plane(sp, own, zl, zh, yl, yh, x, a, dst, xw, ends, spare):
    top, bottom, below, above = ends
    h, half = sp.h, sp.half
    m = merged(sp, own, zl, zh, x, a, 0, half, top, bottom)
    p = lax.div(x, 2)
    turn = 64 * (1 - lax.rem(x, 2))
    if sp.o == 8:
        low = roll(roll(yl[p], 8 - h - a * h, 0)[0:8], turn, 1) * below
        high = roll(roll(yh[p], -a * h, 0)[0:8], turn, 1) * above
        lower = jnp.concatenate([low, m], axis=0)
        higher = jnp.concatenate([m, high], axis=0)
        dst[xw] = jnp.where(upper(sp, sp.R), higher, lower)
    else:
        spare[0, 0:h, :] = roll(yl[p, a * h : (a + 1) * h, :], turn, 1) * below
        spare[0, h:, :] = m
        spare[1, 0:half, :] = m
        spare[1, half:, :] = roll(yh[p, a * h : (a + 1) * h, :], turn, 1) * above
        dst[xw] = jnp.where(upper(sp, sp.R), spare[1], spare[0])


def lane_z(sp, l):
    return jnp.where(l < sp.cut, l, jnp.where(l < sp.cut + 64, l - 64, l - 128))


def inside(sp, ids):
    _, gy, gz, ny, nz = ids
    n, h = sp.n, sp.h
    y = lax.broadcasted_iota(jnp.int32, (sp.R, 128), 0) - sp.o + jnp.where(upper(sp, sp.R), sp.R, 0)
    z = lane_z(sp, lanes(sp.R))
    ok = (y >= -h) & (y < n + h) & (z >= -h) & (z < n + h)
    y, z = y + gy * n, z + gz * n
    return ok & (y >= 0) & (y < ny * n) & (z >= 0) & (z < nz * n)


def paired(ref, x):
    c = ref[x + 1]
    R = c.shape[0]
    s = ref[x] + ref[x + 2]
    sub = lax.broadcasted_iota(jnp.int32, (8, 128), 0)
    seam = roll(jnp.where(sub == 0, c[0:8], c[R - 8 : R]), 64, 1)
    up, down = roll(c, R - 1, 0), roll(c, 1, 0)
    up = jnp.concatenate([up[: R - 8], jnp.where(sub == 7, roll(seam, 7, 0), up[R - 8 :])], axis=0)
    down = jnp.concatenate([jnp.where(sub == 0, roll(seam, 1, 0), down[0:8]), down[8:]], axis=0)
    s = s + (up + down)
    return s + (roll(c, 1, 1) + roll(c, 127, 1))


def domain(sp, n, h, r0, R, ids):
    row = lax.broadcasted_iota(jnp.int32, (R, 128), 0) - r0
    ln = lanes(R)
    z = jnp.where(ln < 64, ln, ln - 128)
    gy, gz, ny, nz = ids[1], ids[2], ids[3], ids[4]
    y_at, z_at = row + gy * n, z + gz * n
    ok = (row >= -h) & (row < n + h) & (z >= -h) & (z < n + h)
    return ok & (y_at >= 0) & (y_at < ny * n) & (z_at >= 0) & (z_at < nz * n)


def neighbours(ref, x):
    c = ref[x + 1]
    R = c.shape[0]
    s = ref[x] + ref[x + 2]
    s = s + (roll(c, 1, 0) + roll(c, R - 1, 0))
    return s + (roll(c, 1, 1) + roll(c, 127, 1))


def zero_ends(ref, n):
    ref[0] = jnp.zeros(ref.shape[1:], F32)
    ref[n + 1] = jnp.zeros(ref.shape[1:], F32)


def relax(src, dst, f, c, n, factor, u=9, near=None):
    near = near or neighbours

    def one(x):
        dst[x + 1] = (1.0 - W) * src[x + 1] + c[x] * (f[x] + factor * near(src, x))

    loop(n, one, u)


def lane_map(pick, value, cols=128):
    l = lax.broadcasted_iota(jnp.int32, (256, cols), 0) % 128
    m = lax.broadcasted_iota(jnp.int32, (256, cols), 1)
    return jnp.where(pick(l, m) == m, value, 0.0).astype(jnp.bfloat16)


def spread_map(pick):
    m = lax.broadcasted_iota(jnp.int32, (256, 128), 0) % 128
    l = lax.broadcasted_iota(jnp.int32, (256, 128), 1)
    return jnp.where(pick(l) == m, 1.0, 0.0).astype(jnp.bfloat16)


def floor_half(z):
    return lax.shift_right_arithmetic(z, 1)


def times(v, m):
    big = v.astype(jnp.bfloat16)
    rest = (v - big.astype(F32)).astype(jnp.bfloat16)
    return jnp.dot(jnp.concatenate([big, rest], axis=1), m, preferred_element_type=F32)


def coarsen_planes(pair, n, tmp, acc, rows, u=2):
    half = rows // 2

    def one(x):
        tmp[x, 0:rows, :] = pair(x)
        acc[x, 0:half, :] = tmp[x, pl.ds(0, half, stride=2), :] + tmp[x, pl.ds(1, half, stride=2), :]

    loop(n, one, u)


def flat(ref):
    n, rows, _ = ref.shape
    return ref[...].reshape(n * rows, 128)


def add_refined(wide, n, src, dst, u=3):
    R = dst.shape[1]

    def one(i):
        v = wide[i, 0 : R // 2, :]
        for k in range(2):
            dst[2 * i + 1, pl.ds(k, R // 2, stride=2), :] = v
        t = dst[2 * i + 1]
        dst[2 * i + 1] = src[2 * i + 1] + t
        dst[2 * i + 2] = src[2 * i + 2] + t

    loop(n, one, u)


def k_zpack0(x0, b, rea, hi, lo, own, raw, sems):
    def copy(a, ref, i):
        part = pl.ds(i * 8, 8)
        return pltpu.make_async_copy(ref.at[part], raw.at[a, part], sems.at[a, i])

    refs = (x0, b, rea)
    for i in range(6):
        for a, ref in enumerate(refs):
            copy(a, ref, i).start()

    def some(i):
        for a, ref in enumerate(refs):
            copy(a, ref, i).wait()
        for k in range(8):
            x = i * 8 + k
            for a in range(3):
                own[a, x, :, 0:48] = raw[a, x, 0:24, :]
                own[a, x, :, 64:112] = raw[a, x, 24:48, :]
        for k in range(2):
            ztile(L0, lambda x, a: own[a, x], hi, lo, i * 2 + k)

    loop(6, some)


def k_ypack0(own, zl, zh, up, dn):
    ypack(L0, lambda x, a: own[a, x], zl, zh, up, dn)


def xpack(sp, own, zl, zh, yl, yh, out, spare):
    ids = place()
    ends = edge(sp, ids)
    start = (1 - ids[0]) * (sp.n - sp.hx)

    def one(i):
        for a in range(sp.na):
            plane(sp, own, zl, zh, yl, yh, start + i, a, out.at[i], a, ends, None if spare is None else spare.at[a])

    loop(sp.hx, one, 2)


def k_xpack0(own, zl, zh, yl, yh, out):
    xpack(L0, lambda x, a: own[a, x], zl, zh, yl, yh, out, None)


def assemble(sp, ids, own, zl, zh, yl, yh, xr, dsts, spare, u):
    shift = ids[0] * sp.hx
    ends = edge(sp, ids)

    def some(i):
        for k in range(u):
            x = i * u + k
            for a, (dst, off) in enumerate(dsts):
                plane(sp, own, zl, zh, yl, yh, x, a, dst, x + shift + off, ends, None if spare is None else spare.at[k * sp.na + a])

    loop(sp.n // u, some)
    other = (1 - ids[0]) * sp.n

    def take(i):
        for a, (dst, off) in enumerate(dsts):
            dst[other + i + off] = xr[i, a]

    loop(sp.hx, take, 2)


def own_rows(sp, v):
    return jnp.where(upper(sp, sp.half), v[0 : sp.half], v[sp.o :])


def k_down0(own, zl, zh, yl, yh, xr, f_out, c_out, d_out, e_out, f1, r1, z1h, z1l, xw, bw, rw, ew, tmp, acc):
    ids = place()
    assemble(L0, ids, lambda x, a: own[a, x], zl, zh, yl, yh, xr, ((xw, 1), (bw, 0), (rw, 0)), None, 4)
    n = L0.nx
    ok = inside(L0, ids)
    zero_ends(xw, n)
    zero_ends(ew, n)
    zero_ends(e_out, n)

    def first(x):
        d = 6.0 + rw[x]
        c = jnp.where(ok, W / d, 0.0)
        f = bw[x] - d * xw[x + 1] + paired(xw, x)
        d_out[x] = d
        f_out[x] = f
        c_out[x] = c
        ew[x + 1] = c * f

    loop(n, first, 6)
    relax(ew, e_out, f_out, c_out, n, 1.0, 9, paired)
    shift = ids[0] * L0.hx

    def left(x):
        return own_rows(L0, f_out[x] - d_out[x] * e_out[x + 1] + paired(e_out, x))

    mine = lanes(24) % 64 < 48
    m = lane_map(lambda l, m: jnp.where(l < 64, l // 2, 32 + l // 2), 0.125)
    for ref, pair in (
        (f1, lambda x: left(2 * x + shift) + left(2 * x + shift + 1)),
        (r1, lambda x: own_rows(L0, rw[2 * x + shift] + rw[2 * x + shift + 1])),
    ):
        coarsen_planes(lambda x, pair=pair: jnp.where(mine, pair(x), 0.0), 24, tmp, acc, 24, 4)
        acc[...] = times(flat(acc), m).reshape(24, 16, 128)

        def keep(x, ref=ref):
            ref[x] = acc[x, 0:12, :]

        loop(24, keep, 6)
    both = (f1, r1)
    loop(6, lambda g: ztile(L1, lambda x, a: both[a][x], z1h, z1l, g), 3)


def k_ypack1(f1, r1, zl, zh, up, dn):
    both = (f1, r1)
    ypack(L1, lambda x, a: both[a][x], zl, zh, up, dn)


def k_xpack1(f1, r1, zl, zh, yl, yh, out, spare):
    both = (f1, r1)
    xpack(L1, lambda x, a: both[a][x], zl, zh, yl, yh, out, spare)


def k_down1(f1, r1, zl, zh, yl, yh, xr, fw, cw, e_out, f2, c2, e2, out3, rw, ew, tmp, acc, r2, ew2, tmp2, t3, sq, spare):
    ids = place()
    both = (f1, r1)
    assemble(L1, ids, lambda x, a: both[a][x], zl, zh, yl, yh, xr, ((fw, 0), (rw, 0)), spare, 4)
    n = L1.nx
    ok = inside(L1, ids)
    zero_ends(ew, n)
    zero_ends(e_out, n)

    def first(x):
        c = jnp.where(ok, W / (1.5 + rw[x]), 0.0)
        cw[x] = c
        ew[x + 1] = c * fw[x]

    loop(n, first, 6)
    relax(ew, e_out, fw, cw, n, 0.25, 12, paired)

    def left(x):
        return fw[x] - (1.5 + rw[x]) * e_out[x + 1] + 0.25 * paired(e_out, x)

    def pick(l, m):
        z = lane_z(L1, l)
        up = (l >= L1.cut) & (l < L1.cut + 64)
        good = (z >= -12) & (z < 36) & (up == (m >= 128))
        return jnp.where(good, floor_half(z) + jnp.where(z < 0, 128, 0) + jnp.where(up, 128, 0), -1)

    m = lane_map(pick, 0.125, 256)
    for ref, pair in ((f2, lambda x: left(2 * x) + left(2 * x + 1)), (r2, lambda x: rw[2 * x] + rw[2 * x + 1])):
        coarsen_planes(pair, 18, tmp, acc.at[0], 24, 6)
        v = times(flat(acc.at[0]), m)
        acc[0] = v[:, 0:128].reshape(18, 16, 128)
        acc[1] = v[:, 128:256].reshape(18, 16, 128)

        def keep(x, ref=ref):
            ref[x] = jnp.zeros((32, 128), F32)
            ref[x, 2:14, :] = acc[0, x, 0:12, :]
            ref[x, 14:26, :] = acc[1, x, 0:12, :]

        loop(18, keep, 6)
    ok2 = domain(None, 12, 6, 8, 32, ids)
    zero_ends(ew2, 18)
    zero_ends(e2, 18)

    def second(x):
        c = jnp.where(ok2, W / (0.375 + r2[x]), 0.0)
        c2[x] = c
        ew2[x + 1] = c * f2[x]

    loop(18, second, 6)
    relax(ew2, e2, f2, c2, 18, 0.0625, 18)

    def left2(x):
        return f2[x] - (0.375 + r2[x]) * e2[x + 1] + 0.0625 * neighbours(e2, x)

    m = lane_map(lambda l, m: jnp.where(l < 64, l // 2, l // 2 + 64), 0.125)
    for a, pair in enumerate((lambda x: left2(2 * x) + left2(2 * x + 1), lambda x: r2[2 * x] + r2[2 * x + 1])):
        coarsen_planes(pair, 9, tmp2, t3.at[a], 32, 9)
        t3[a] = times(flat(t3.at[a]), m).reshape(9, 16, 128)
    shift = ids[0] * 3
    sq[...] = jnp.zeros((128, 128), F32)
    for a in range(2):
        for x in range(6):
            at = a * 36 + x * 6
            sq[at : at + 6, :] = t3[a, x + shift, 4:10, :]
    t = sq[...].T[0:8]
    ln = lanes(1)
    rows = []
    for u in range(2):
        for a in range(2):
            parts = [roll(t, 36 * (w - a), 1)[3 * u + w : 3 * u + w + 1] for w in range(3)]
            rows.append(jnp.where(ln < 36, parts[0], jnp.where(ln < 72, parts[1], parts[2])))
    tile = jnp.concatenate(rows + rows, axis=0)
    n8 = out3.shape[0] // 8
    out3[...] = jnp.broadcast_to(tile[None], (n8, 8, 128)).reshape(n8 * 8, 128)


def sum_all(v):
    s = jnp.sum(v, axis=0)
    return jnp.sum(jnp.sum(s, axis=1, keepdims=True), axis=0, keepdims=True)


def coarse_solve(g3, nx, ny, nz, e3, s3, f3, c3, r3, tmp, f4, r4, sq):
    R = f3.shape[1]
    for ref in (f3, r3):
        ref[...] = jnp.zeros(ref.shape, F32)
    kx, ky, kz = nx // 6, ny // 6, nz // 6
    for bx in range(kx):
        for by in range(ky):
            k = bx * ky + by
            if kz * 6 < 128:
                sq[k, kz * 6 :, :] = jnp.zeros((128 - kz * 6, 128), F32)
            got = [g3[pl.ds(k * kz * 4 + r, kz, stride=4), :] for r in range(4)]
            ln = lanes(kz)
            for u in range(2):
                for w in range(3):
                    f, r = roll(got[2 * u], -36 * w, 1), roll(got[2 * u + 1], 36 - 36 * w, 1)
                    sq[k, pl.ds(3 * u + w, kz, stride=6), :] = jnp.where(ln < 36, f, r)
            t = sq[k].T
            for x in range(6):
                f3[bx * 6 + x, by * 6 : by * 6 + 6, :] = t[x * 6 : x * 6 + 6]
                r3[bx * 6 + x, by * 6 : by * 6 + 6, :] = t[36 + x * 6 : 42 + x * 6]
    factor = 0.25**3
    ok = (lax.broadcasted_iota(jnp.int32, (R, 128), 0) < ny) & (lanes(R) < nz)
    for ref in (e3, s3):
        zero_ends(ref, nx)

    def first(x):
        c = jnp.where(ok, W / (6.0 * factor + r3[x]), 0.0)
        c3[x] = c
        s3[x + 1] = c * f3[x]

    loop(nx, first, 6)
    relax(s3, e3, f3, c3, nx, factor, 6)

    def left(x):
        v = f3[x] - (6.0 * factor + r3[x]) * e3[x + 1] + factor * neighbours(e3, x)
        return jnp.where(ok, v, 0.0)

    m = lane_map(lambda l, m: l // 2, 0.125)
    for ref, pair in ((f4, lambda x: left(2 * x) + left(2 * x + 1)), (r4, lambda x: r3[2 * x] + r3[2 * x + 1])):
        coarsen_planes(pair, nx // 2, tmp, ref, R, 6)
        ref[...] = times(flat(ref), m).reshape(ref.shape)
    f4k = 0.25**4
    H = R // 2
    row = lax.broadcasted_iota(jnp.int32, (nx // 2, H, 128), 1)
    lane = lax.broadcasted_iota(jnp.int32, (nx // 2, H, 128), 2)
    within = (row < ny // 2) & (lane < nz // 2)
    diag = 6.0 * f4k + r4[...]
    zero = jnp.zeros((1, H, 128), F32)

    def apply(p):
        s = jnp.concatenate([zero, p[:-1]], axis=0) + jnp.concatenate([p[1:], zero], axis=0)
        s = s + roll(p, 1, 1) + roll(p, H - 1, 1) + roll(p, 1, 2) + roll(p, 127, 2)
        return jnp.where(within, diag * p - f4k * s, 0.0)

    r = jnp.where(within, f4[...], 0.0)
    p = r
    e = jnp.zeros_like(r)
    rr = sum_all(r * r)
    for i in range(BOTTOM_ITERS):
        q = apply(p)
        a = rr / sum_all(p * q)
        e = e + a * p
        if i + 1 < BOTTOM_ITERS:
            r = r - a * q
            new = sum_all(r * r)
            p = r + (new / rr) * p
            rr = new
    f4[...] = times(e.reshape(nx // 2 * H, 128), spread_map(lambda l: l // 2)).reshape(e.shape)
    add_refined(f4, nx // 2, e3, s3, 6)
    relax(s3, e3, f3, c3, nx, factor, 6)
    relax(e3, s3, f3, c3, nx, factor, 6)


def k_up(g3, f2, c2, e2i, f1, c1, e1i, f0, c0, d0, e0i, z_out, az_out, sums,
         e3, s3, f3, c3, r3, tmp3, f4, r4, sq, w3, w2, na, nb, n1, e2, s2, e1, s1, e0, s0):
    gx, gy, gz, sy, sz = place()
    nx, ny, nz = f3.shape[0], sy * 6, sz * 6
    coarse_solve(g3, nx, ny, nz, e3, s3, f3, c3, r3, tmp3, f4, r4, sq)
    for ref, n in ((s2, 18), (s1, 36), (s0, 54), (e2, 18), (e1, 36), (e0, 54)):
        zero_ends(ref, n)
    R3 = s3.shape[1]
    pick = lax.broadcasted_iota(jnp.int32, (16, R3), 1) == lax.broadcasted_iota(jnp.int32, (16, R3), 0) + (gy * 6 - 4)
    pick = pick.astype(F32)
    for i in range(9):
        w3[i] = jnp.dot(pick, s3[i + 1 + gx * 3], precision=HI, preferred_element_type=F32)
    spread = spread_map(lambda l: gz * 6 + jnp.where(l < 64, l // 2, l // 2 - 64))
    w3[...] = times(flat(w3), spread).reshape(9, 16, 128)
    add_refined(w3, 9, e2i, e2, 9)
    relax(e2, s2, f2, c2, 18, 0.0625, 18)
    relax(s2, e2, f2, c2, 18, 0.0625, 18)

    def halves(i):
        na[i] = e2[i + 1, 2:18, :]
        nb[i] = e2[i + 1, 14:30, :]

    loop(18, halves, 6)

    def down(sp, l, want):
        z = lane_z(sp, l)
        up = (l >= sp.cut) & (l < sp.cut + 64)
        good = (z >= -sp.h) & (z < sp.n + sp.h)
        good = good & (up if want else jnp.logical_not(up))
        return jnp.where(good, floor_half(z) + jnp.where(z < 0, 128, 0), -1)

    w2[...] = (
        times(flat(na), spread_map(lambda l: down(L1, l, False))) + times(flat(nb), spread_map(lambda l: down(L1, l, True)))
    ).reshape(18, 16, 128)
    add_refined(w2, 18, e1i, e1, 6)
    relax(e1, s1, f1, c1, 36, 0.25, 12, paired)
    relax(s1, e1, f1, c1, 36, 0.25, 12, paired)

    def near(i):
        v = e1[i + 1 + gx * 9]
        n1[i] = jnp.where(upper(L1, 16), v[0:16], v[8:24])

    loop(27, near, 9)

    def both(l):
        lower, higher = down(L0, l, False), down(L0, l, True)
        return jnp.where(lower >= 0, lower, jnp.where(higher >= 0, (higher + 64) % 128, -1))

    n1[...] = times(flat(n1), spread_map(both)).reshape(27, 16, 128)
    add_refined(n1, 27, e0i, e0, 9)
    relax(e0, s0, f0, c0, 54, 1.0, 9, paired)
    relax(s0, e0, f0, c0, 54, 1.0, 9, paired)
    shift = gx * 6
    mine = lanes(24) % 64 < 48

    def last(x, carry):
        u, v = carry
        w = x + shift
        z = e0[w + 1]
        az = own_rows(L0, d0[w] * z - paired(e0, w))
        z = own_rows(L0, z)
        f = own_rows(L0, f0[w])
        z_out[x] = z
        az_out[x] = az
        return u + jnp.where(mine, f * z, 0.0), v + jnp.where(mine, z * az, 0.0)

    def some(i, carry):
        for k in range(6):
            carry = last(6 * i + k, carry)
        return carry

    zero = jnp.zeros((24, 128), F32)
    u, v = lax.fori_loop(0, 8, some, (zero, zero))

    def total(t):
        return jnp.sum(jnp.sum(t, axis=1, keepdims=True), axis=0, keepdims=True)

    ln = lanes(sums.shape[0])
    sums[...] = jnp.where(ln == 0, total(u), jnp.where(ln == 1, total(v), 0.0))


def k_last(sums, own, z, az, f, sol, res, sv, rv, sems):
    s = jnp.sum(sums[...], axis=0, keepdims=True)
    ln = lanes(1)
    over = jnp.sum(jnp.where(ln == 0, s, 0.0), axis=1, keepdims=True)
    under = jnp.sum(jnp.where(ln == 1, s, 0.0), axis=1, keepdims=True)
    step = over / under
    shift = lax.axis_index("gx") * 6
    pairs = ((0, sv, sol), (1, rv, res))

    def copy(a, src, dst, i):
        part = pl.ds(i * 8, 8)
        return pltpu.make_async_copy(src.at[part], dst.at[part], sems.at[a, i])

    def some(i):
        for k in range(8):
            x = i * 8 + k
            for ref, v in ((sv, own[0, x] + step * z[x]), (rv, own_rows(L0, f[x + shift]) - step * az[x])):
                ref[x, 0:24, :] = v[:, 0:48]
                ref[x, 24:48, :] = roll(v, 64, 1)[:, 0:48]
        for a, src, dst in pairs:
            copy(a, src, dst, i).start()

    loop(6, some)
    for i in range(6):
        for a, src, dst in pairs:
            copy(a, src, dst, i).wait()


def ring(up, dn, axis):
    n = lax.axis_size(axis)
    low = lax.ppermute(up, axis, [(i, (i + 1) % n) for i in range(n)])
    high = lax.ppermute(dn, axis, [(i, (i - 1) % n) for i in range(n)])
    return low, high


def swap(v):
    return lax.ppermute(v, "gx", [(0, 1), (1, 0)])


def body(b, x0, rea):
    ALL = ("gx", "gy", "gz")
    sizes = [lax.axis_size(a) for a in ALL]
    count = sizes[0] * sizes[1] * sizes[2]
    hi, lo, own = run(
        k_zpack0,
        (sds(*L0.zshape), sds(*L0.zshape), sds(3, 48, 24, 128)),
        (x0, b, rea),
        [(3, 48, 48, 48), pltpu.SemaphoreType.DMA((3, 6))],
        far_in=True,
    )
    zl, zh = ring(hi, lo, "gz")
    up, dn = run(k_ypack0, (sds(*L0.yshape),) * 2, (own, zl, zh))
    yl, yh = ring(up, dn, "gy")
    xr = swap(run(k_xpack0, sds(*L0.xshape), (own, zl, zh, yl, yh)))
    p0, q0 = (54, 32, 128), (56, 32, 128)
    f0, c0, d0, e0, f1, r1, z1h, z1l = run(
        k_down0,
        (sds(*p0), sds(*p0), sds(*p0), sds(*q0), sds(24, 12, 128), sds(24, 12, 128), sds(*L1.zshape), sds(*L1.zshape)),
        (own, zl, zh, yl, yh, xr),
        [q0, p0, p0, q0, (24, 24, 128), (24, 16, 128)],
        mib=M0,
    )
    zl, zh = ring(z1h, z1l, "gz")
    up, dn = run(k_ypack1, (sds(*L1.yshape),) * 2, (f1, r1, zl, zh))
    yl, yh = ring(up, dn, "gy")
    xr = swap(run(k_xpack1, sds(*L1.xshape), (f1, r1, zl, zh, yl, yh), [(2, 2, 24, 128)]))
    p1, q1, p2, q2 = (36, 24, 128), (38, 24, 128), (18, 32, 128), (20, 32, 128)
    f1w, c1w, e1w, f2w, c2w, e2w, g = run(
        k_down1,
        (sds(*p1), sds(*p1), sds(*q1), sds(*p2), sds(*p2), sds(*q2), sds(count * 4, 128)),
        (f1, r1, zl, zh, yl, yh, xr),
        [p1, q1, (18, 24, 128), (2, 18, 16, 128), p2, q2, (9, 32, 128), (2, 9, 16, 128), (128, 128), (8, 2, 24, 128)],
        mib=M1,
    )
    g = lax.all_to_all(g, ALL, 0, 0, tiled=True)
    n3 = [6 * s for s in sizes]
    R3 = (n3[1] + 8) // 8 * 8
    if R3 % 16:
        R3 += 8
    p3, q3, p4 = (n3[0], R3, 128), (n3[0] + 2, R3, 128), (n3[0] // 2, R3 // 2, 128)
    z, az, sums = run(
        k_up,
        (sds(48, 24, 128), sds(48, 24, 128), sds(count, 128)),
        (g, f2w, c2w, e2w, f1w, c1w, e1w, f0, c0, d0, e0),
        [q3, q3, p3, p3, p3, (n3[0] // 2, R3, 128), p4, p4, (sizes[0] * sizes[1], 128, 128), (9, 16, 128), (18, 16, 128),
         (18, 16, 128), (18, 16, 128), (27, 16, 128), q2, q2, q1, q1, q0, q0],
        mib=M2,
    )
    sums = lax.all_to_all(sums.reshape(count, 1, 128), ALL, 0, 0, tiled=True).reshape(count, 128)
    return run(
        k_last,
        (sds(48, 48, 48), sds(48, 48, 48)),
        (sums, own, z, az, f0),
        [(48, 48, 48), (48, 48, 48), pltpu.SemaphoreType.DMA((2, 6))],
        far_out=True,
    )


def solution(mesh):
    spec = P("gx", "gy", "gz")
    return jax.shard_map(body, mesh=mesh, in_specs=(spec, spec, spec), out_specs=(spec, spec), check_vma=False)
```

```python
import functools
import jax
import jax.numpy as jnp
from jax import lax
from jax.experimental import pallas as pl
from jax.experimental.pallas import tpu as pltpu
from jax.sharding import PartitionSpec as P

W = 6.0 / 7.0
BOTTOM_ITERS = 6
N0 = 48
F32 = jnp.float32
HI = lax.Precision.HIGHEST
M0, M1, M2 = 10, 8, 12


class Spec:
    def __init__(self, n, h, na, R, o, hx, cut, kp, st):
        self.n, self.h, self.na, self.R, self.o, self.hx, self.cut, self.kp, self.st = n, h, na, R, o, hx, cut, kp, st
        self.half = n // 2
        self.zshape = (n // (kp * st), self.half * st, 128)
        self.yrows = -(-na * h // 8) * 8
        self.yshape = (self.half, self.yrows, 128)
        self.xshape = (hx, na, R, 128)
        self.nx = n + hx


L0 = Spec(48, 5, 3, 32, 8, 6, 56, 4, 1)
L1 = Spec(24, 12, 2, 24, 12, 12, 44, 2, 2)


def sds(*shape):
    return jax.ShapeDtypeStruct(shape, F32)


def run(kernel, outs, args, scratch=(), mib=12, far_in=False, far_out=False):
    vmem = pl.BlockSpec(memory_space=pltpu.VMEM)
    hbm = pl.BlockSpec(memory_space=pl.ANY)
    return pl.pallas_call(
        kernel,
        out_shape=outs,
        in_specs=[hbm if far_in else vmem] * len(args),
        out_specs=jax.tree.map(lambda _: hbm if far_out else vmem, outs),
        scratch_shapes=[pltpu.VMEM(s, F32) if isinstance(s, tuple) else s for s in scratch],
        compiler_params=pltpu.CompilerParams(vmem_limit_bytes=mib * 1024 * 1024),
    )(*args)


def place():
    return [lax.axis_index(a) for a in ("gx", "gy", "gz")] + [lax.axis_size(a) for a in ("gy", "gz")]


def lanes(rows):
    return lax.broadcasted_iota(jnp.int32, (rows, 128), 1)


def roll(v, shift, axis):
    if isinstance(shift, int):
        shift = shift % v.shape[axis]
        if shift == 0:
            return v
    return pltpu.roll(v, shift, axis)


def loop(n, f, u=1):
    u = max(d for d in range(1, u + 1) if n % d == 0)

    def some(i, c):
        for k in range(u):
            f(i * u + k)
        return c

    lax.fori_loop(0, n // u, some, 0)


def upper(sp, rows):
    l = lanes(rows)
    return (l >= sp.cut) & (l < sp.cut + 64)


def edge(sp, ids):
    _, gy, gz, ny, nz = ids
    high = jnp.where(gz < nz - 1, sp.n + sp.h, sp.n)
    low = jnp.where(gz > 0, 64 - sp.h, 64)
    return high, low, jnp.where(gy > 0, 1.0, 0.0), jnp.where(gy < ny - 1, 1.0, 0.0)


def ztile(sp, own, hi_ref, lo_ref, g):
    q = lanes(sp.half) % 64
    for t in range(sp.st):
        hi = jnp.zeros((sp.half, 128), F32)
        lo = hi
        for k in range(sp.kp):
            for a in range(sp.na):
                v = own(t * (sp.n // sp.st) + g * sp.kp + k, a)
                at = sp.h * (k * sp.na + a)
                here = (q >= at) & (q < at + sp.h)
                hi = jnp.where(here, roll(v, at - (sp.n - sp.h), 1), hi)
                lo = jnp.where(here, roll(v, at, 1), lo)
        hi_ref[g, t * sp.half : (t + 1) * sp.half, :] = hi
        lo_ref[g, t * sp.half : (t + 1) * sp.half, :] = lo


def merged(sp, own, zl, zh, x, a, b, e, top, bottom):
    per = sp.n // sp.st
    t, y = lax.div(x, per), lax.rem(x, per)
    g, k = lax.div(y, sp.kp), lax.rem(y, sp.kp)
    at = sp.h * (k * sp.na + a)
    if sp.st == 1:
        high, low = zh[g, b:e, :], zl[g, b:e, :]
    else:
        high = jnp.where(t == 0, zh[g, b:e, :], zh[g, sp.half + b : sp.half + e, :])
        low = jnp.where(t == 0, zl[g, b:e, :], zl[g, sp.half + b : sp.half + e, :])
    high = roll(high, lax.rem(sp.n + 128 - at, 128), 1)
    low = roll(low, lax.rem(256 - sp.h - at, 128), 1)
    q = lanes(e - b) % 64
    return jnp.where(q < sp.n, own(x, a)[b:e], jnp.where(q < top, high, jnp.where(q >= bottom, low, 0.0)))


def ypack(sp, own, zl, zh, up_ref, dn_ref):
    h, half = sp.h, sp.half
    up0 = (half - h) // 8 * 8
    dn1 = min(half, -(-h // 8) * 8)
    top, bottom, _, _ = edge(sp, place())

    def pair(p):
        for a in range(sp.na):
            for ref, b, e, s, t, swap in ((up_ref, up0, half, half - h - up0, half - up0, False), (dn_ref, 0, dn1, 0, h, True)):
                even = merged(sp, own, zl, zh, 2 * p, a, b, e, top, bottom)
                odd = roll(merged(sp, own, zl, zh, 2 * p + 1, a, b, e, top, bottom), 64, 1)
                first, second = (odd, even) if swap else (even, odd)
                ref[p, a * h : (a + 1) * h, :] = jnp.where(upper(sp, e - b), first, second)[s:t]
        if sp.yrows > sp.na * h:
            pad = jnp.zeros((sp.yrows - sp.na * h, 128), F32)
            up_ref[p, sp.na * h :, :] = pad
            dn_ref[p, sp.na * h :, :] = pad

    loop(half, pair, 3)


def plane(sp, own, zl, zh, yl, yh, x, a, dst, xw, ends, spare):
    top, bottom, below, above = ends
    h, half = sp.h, sp.half
    m = merged(sp, own, zl, zh, x, a, 0, half, top, bottom)
    p = lax.div(x, 2)
    turn = 64 * (1 - lax.rem(x, 2))
    if sp.o == 8:
        low = roll(roll(yl[p], 8 - h - a * h, 0)[0:8], turn, 1) * below
        high = roll(roll(yh[p], -a * h, 0)[0:8], turn, 1) * above
        lower = jnp.concatenate([low, m], axis=0)
        higher = jnp.concatenate([m, high], axis=0)
        dst[xw] = jnp.where(upper(sp, sp.R), higher, lower)
    else:
        spare[0, 0:h, :] = roll(yl[p, a * h : (a + 1) * h, :], turn, 1) * below
        spare[0, h:, :] = m
        spare[1, 0:half, :] = m
        spare[1, half:, :] = roll(yh[p, a * h : (a + 1) * h, :], turn, 1) * above
        dst[xw] = jnp.where(upper(sp, sp.R), spare[1], spare[0])


def lane_z(sp, l):
    return jnp.where(l < sp.cut, l, jnp.where(l < sp.cut + 64, l - 64, l - 128))


def inside(sp, ids):
    _, gy, gz, ny, nz = ids
    n, h = sp.n, sp.h
    y = lax.broadcasted_iota(jnp.int32, (sp.R, 128), 0) - sp.o + jnp.where(upper(sp, sp.R), sp.R, 0)
    z = lane_z(sp, lanes(sp.R))
    ok = (y >= -h) & (y < n + h) & (z >= -h) & (z < n + h)
    y, z = y + gy * n, z + gz * n
    return ok & (y >= 0) & (y < ny * n) & (z >= 0) & (z < nz * n)


def paired(ref, x):
    c = ref[x + 1]
    R = c.shape[0]
    s = ref[x] + ref[x + 2]
    sub = lax.broadcasted_iota(jnp.int32, (8, 128), 0)
    seam = roll(jnp.where(sub == 0, c[0:8], c[R - 8 : R]), 64, 1)
    up, down = roll(c, R - 1, 0), roll(c, 1, 0)
    up = jnp.concatenate([up[: R - 8], jnp.where(sub == 7, roll(seam, 7, 0), up[R - 8 :])], axis=0)
    down = jnp.concatenate([jnp.where(sub == 0, roll(seam, 1, 0), down[0:8]), down[8:]], axis=0)
    s = s + (up + down)
    return s + (roll(c, 1, 1) + roll(c, 127, 1))


def domain(sp, n, h, r0, R, ids):
    row = lax.broadcasted_iota(jnp.int32, (R, 128), 0) - r0
    ln = lanes(R)
    z = jnp.where(ln < 64, ln, ln - 128)
    gy, gz, ny, nz = ids[1], ids[2], ids[3], ids[4]
    y_at, z_at = row + gy * n, z + gz * n
    ok = (row >= -h) & (row < n + h) & (z >= -h) & (z < n + h)
    return ok & (y_at >= 0) & (y_at < ny * n) & (z_at >= 0) & (z_at < nz * n)


def neighbours(ref, x):
    c = ref[x + 1]
    R = c.shape[0]
    s = ref[x] + ref[x + 2]
    s = s + (roll(c, 1, 0) + roll(c, R - 1, 0))
    return s + (roll(c, 1, 1) + roll(c, 127, 1))


def zero_ends(ref, n):
    ref[0] = jnp.zeros(ref.shape[1:], F32)
    ref[n + 1] = jnp.zeros(ref.shape[1:], F32)


def relax(src, dst, f, c, n, factor, u=9, near=None):
    near = near or neighbours

    def one(x):
        dst[x + 1] = (1.0 - W) * src[x + 1] + c[x] * (f[x] + factor * near(src, x))

    loop(n, one, u)


def lane_map(pick, value, cols=128):
    l = lax.broadcasted_iota(jnp.int32, (256, cols), 0) % 128
    m = lax.broadcasted_iota(jnp.int32, (256, cols), 1)
    return jnp.where(pick(l, m) == m, value, 0.0).astype(jnp.bfloat16)


def spread_map(pick):
    m = lax.broadcasted_iota(jnp.int32, (256, 128), 0) % 128
    l = lax.broadcasted_iota(jnp.int32, (256, 128), 1)
    return jnp.where(pick(l) == m, 1.0, 0.0).astype(jnp.bfloat16)


def floor_half(z):
    return lax.shift_right_arithmetic(z, 1)


def times(v, m):
    big = v.astype(jnp.bfloat16)
    rest = (v - big.astype(F32)).astype(jnp.bfloat16)
    return jnp.dot(jnp.concatenate([big, rest], axis=1), m, preferred_element_type=F32)


def coarsen_planes(pair, n, tmp, acc, rows, u=2):
    half = rows // 2

    def one(x):
        tmp[x, 0:rows, :] = pair(x)
        acc[x, 0:half, :] = tmp[x, pl.ds(0, half, stride=2), :] + tmp[x, pl.ds(1, half, stride=2), :]

    loop(n, one, u)


def flat(ref):
    n, rows, _ = ref.shape
    return ref[...].reshape(n * rows, 128)


def add_refined(wide, n, src, dst, u=3):
    R = dst.shape[1]

    def one(i):
        v = wide[i, 0 : R // 2, :]
        for k in range(2):
            dst[2 * i + 1, pl.ds(k, R // 2, stride=2), :] = v
        t = dst[2 * i + 1]
        dst[2 * i + 1] = src[2 * i + 1] + t
        dst[2 * i + 2] = src[2 * i + 2] + t

    loop(n, one, u)


def k_zpack0(x0, b, rea, hi, lo, own, raw, sems):
    def copy(a, ref, i):
        part = pl.ds(i * 8, 8)
        return pltpu.make_async_copy(ref.at[part], raw.at[a, part], sems.at[a, i])

    refs = (x0, b, rea)
    for i in range(6):
        for a, ref in enumerate(refs):
            copy(a, ref, i).start()

    def some(i):
        for a, ref in enumerate(refs):
            copy(a, ref, i).wait()
        for k in range(8):
            x = i * 8 + k
            for a in range(3):
                own[a, x, :, 0:48] = raw[a, x, 0:24, :]
                own[a, x, :, 64:112] = raw[a, x, 24:48, :]
        for k in range(2):
            ztile(L0, lambda x, a: own[a, x], hi, lo, i * 2 + k)

    loop(6, some)


def k_ypack0(own, zl, zh, up, dn):
    ypack(L0, lambda x, a: own[a, x], zl, zh, up, dn)


def xpack(sp, own, zl, zh, yl, yh, out, spare):
    ids = place()
    ends = edge(sp, ids)
    start = (1 - ids[0]) * (sp.n - sp.hx)

    def one(i):
        for a in range(sp.na):
            plane(sp, own, zl, zh, yl, yh, start + i, a, out.at[i], a, ends, None if spare is None else spare.at[a])

    loop(sp.hx, one, 2)


def k_xpack0(own, zl, zh, yl, yh, out):
    xpack(L0, lambda x, a: own[a, x], zl, zh, yl, yh, out, None)


def assemble(sp, ids, own, zl, zh, yl, yh, xr, dsts, spare, u):
    shift = ids[0] * sp.hx
    ends = edge(sp, ids)

    def some(i):
        for k in range(u):
            x = i * u + k
            for a, (dst, off) in enumerate(dsts):
                plane(sp, own, zl, zh, yl, yh, x, a, dst, x + shift + off, ends, None if spare is None else spare.at[k * sp.na + a])

    loop(sp.n // u, some)
    other = (1 - ids[0]) * sp.n

    def take(i):
        for a, (dst, off) in enumerate(dsts):
            dst[other + i + off] = xr[i, a]

    loop(sp.hx, take, 2)


def own_rows(sp, v):
    return jnp.where(upper(sp, sp.half), v[0 : sp.half], v[sp.o :])


def k_down0(own, zl, zh, yl, yh, xr, f_out, c_out, d_out, e_out, f1, r1, z1h, z1l, xw, bw, rw, ew, tmp, acc):
    ids = place()
    assemble(L0, ids, lambda x, a: own[a, x], zl, zh, yl, yh, xr, ((xw, 1), (bw, 0), (rw, 0)), None, 4)
    n = L0.nx
    ok = inside(L0, ids)
    zero_ends(xw, n)
    zero_ends(ew, n)
    zero_ends(e_out, n)

    def first(x):
        d = 6.0 + rw[x]
        c = jnp.where(ok, W / d, 0.0)
        f = bw[x] - d * xw[x + 1] + paired(xw, x)
        d_out[x] = d
        f_out[x] = f
        c_out[x] = c
        ew[x + 1] = c * f

    loop(n, first, 6)
    relax(ew, e_out, f_out, c_out, n, 1.0, 9, paired)
    shift = ids[0] * L0.hx

    def left(x):
        return own_rows(L0, f_out[x] - d_out[x] * e_out[x + 1] + paired(e_out, x))

    mine = lanes(24) % 64 < 48
    m = lane_map(lambda l, m: jnp.where(l < 64, l // 2, 32 + l // 2), 0.125)
    for ref, pair in (
        (f1, lambda x: left(2 * x + shift) + left(2 * x + shift + 1)),
        (r1, lambda x: own_rows(L0, rw[2 * x + shift] + rw[2 * x + shift + 1])),
    ):
        coarsen_planes(lambda x, pair=pair: jnp.where(mine, pair(x), 0.0), 24, tmp, acc, 24, 4)
        acc[...] = times(flat(acc), m).reshape(24, 16, 128)

        def keep(x, ref=ref):
            ref[x] = acc[x, 0:12, :]

        loop(24, keep, 6)
    both = (f1, r1)
    loop(6, lambda g: ztile(L1, lambda x, a: both[a][x], z1h, z1l, g), 3)


def k_ypack1(f1, r1, zl, zh, up, dn):
    both = (f1, r1)
    ypack(L1, lambda x, a: both[a][x], zl, zh, up, dn)


def k_xpack1(f1, r1, zl, zh, yl, yh, out, spare):
    both = (f1, r1)
    xpack(L1, lambda x, a: both[a][x], zl, zh, yl, yh, out, spare)


def k_down1(f1, r1, zl, zh, yl, yh, xr, fw, cw, e_out, f2, c2, e2, out3, rw, ew, tmp, acc, r2, ew2, tmp2, t3, sq, spare):
    ids = place()
    both = (f1, r1)
    assemble(L1, ids, lambda x, a: both[a][x], zl, zh, yl, yh, xr, ((fw, 0), (rw, 0)), spare, 4)
    n = L1.nx
    ok = inside(L1, ids)
    zero_ends(ew, n)
    zero_ends(e_out, n)

    def first(x):
        c = jnp.where(ok, W / (1.5 + rw[x]), 0.0)
        cw[x] = c
        ew[x + 1] = c * fw[x]

    loop(n, first, 6)
    relax(ew, e_out, fw, cw, n, 0.25, 12, paired)

    def left(x):
        return fw[x] - (1.5 + rw[x]) * e_out[x + 1] + 0.25 * paired(e_out, x)

    def pick(l, m):
        z = lane_z(L1, l)
        up = (l >= L1.cut) & (l < L1.cut + 64)
        good = (z >= -12) & (z < 36) & (up == (m >= 128))
        return jnp.where(good, floor_half(z) + jnp.where(z < 0, 128, 0) + jnp.where(up, 128, 0), -1)

    m = lane_map(pick, 0.125, 256)
    for ref, pair in ((f2, lambda x: left(2 * x) + left(2 * x + 1)), (r2, lambda x: rw[2 * x] + rw[2 * x + 1])):
        coarsen_planes(pair, 18, tmp, acc.at[0], 24, 6)
        v = times(flat(acc.at[0]), m)
        acc[0] = v[:, 0:128].reshape(18, 16, 128)
        acc[1] = v[:, 128:256].reshape(18, 16, 128)

        def keep(x, ref=ref):
            ref[x] = jnp.zeros((32, 128), F32)
            ref[x, 2:14, :] = acc[0, x, 0:12, :]
            ref[x, 14:26, :] = acc[1, x, 0:12, :]

        loop(18, keep, 6)
    ok2 = domain(None, 12, 6, 8, 32, ids)
    zero_ends(ew2, 18)
    zero_ends(e2, 18)

    def second(x):
        c = jnp.where(ok2, W / (0.375 + r2[x]), 0.0)
        c2[x] = c
        ew2[x + 1] = c * f2[x]

    loop(18, second, 6)
    relax(ew2, e2, f2, c2, 18, 0.0625, 18)

    def left2(x):
        return f2[x] - (0.375 + r2[x]) * e2[x + 1] + 0.0625 * neighbours(e2, x)

    m = lane_map(lambda l, m: jnp.where(l < 64, l // 2, l // 2 + 64), 0.125)
    for a, pair in enumerate((lambda x: left2(2 * x) + left2(2 * x + 1), lambda x: r2[2 * x] + r2[2 * x + 1])):
        coarsen_planes(pair, 9, tmp2, t3.at[a], 32, 9)
        t3[a] = times(flat(t3.at[a]), m).reshape(9, 16, 128)
    shift = ids[0] * 3
    sq[...] = jnp.zeros((128, 128), F32)
    for a in range(2):
        for x in range(6):
            at = a * 36 + x * 6
            sq[at : at + 6, :] = t3[a, x + shift, 4:10, :]
    t = sq[...].T[0:8]
    ln = lanes(1)
    rows = []
    for u in range(2):
        for a in range(2):
            parts = [roll(t, 36 * (w - a), 1)[3 * u + w : 3 * u + w + 1] for w in range(3)]
            rows.append(jnp.where(ln < 36, parts[0], jnp.where(ln < 72, parts[1], parts[2])))
    tile = jnp.concatenate(rows + rows, axis=0)
    n8 = out3.shape[0] // 8
    out3[...] = jnp.broadcast_to(tile[None], (n8, 8, 128)).reshape(n8 * 8, 128)


def sum_all(v):
    s = jnp.sum(v, axis=0)
    return jnp.sum(jnp.sum(s, axis=1, keepdims=True), axis=0, keepdims=True)


def coarse_solve(g3, nx, ny, nz, e3, s3, f3, c3, r3, tmp, f4, r4, sq):
    R = f3.shape[1]
    for ref in (f3, r3):
        ref[...] = jnp.zeros(ref.shape, F32)
    kx, ky, kz = nx // 6, ny // 6, nz // 6
    for bx in range(kx):
        for by in range(ky):
            k = bx * ky + by
            if kz * 6 < 128:
                sq[k, kz * 6 :, :] = jnp.zeros((128 - kz * 6, 128), F32)
            got = [g3[pl.ds(k * kz * 4 + r, kz, stride=4), :] for r in range(4)]
            ln = lanes(kz)
            for u in range(2):
                for w in range(3):
                    f, r = roll(got[2 * u], -36 * w, 1), roll(got[2 * u + 1], 36 - 36 * w, 1)
                    sq[k, pl.ds(3 * u + w, kz, stride=6), :] = jnp.where(ln < 36, f, r)
            t = sq[k].T
            for x in range(6):
                f3[bx * 6 + x, by * 6 : by * 6 + 6, :] = t[x * 6 : x * 6 + 6]
                r3[bx * 6 + x, by * 6 : by * 6 + 6, :] = t[36 + x * 6 : 42 + x * 6]
    factor = 0.25**3
    ok = (lax.broadcasted_iota(jnp.int32, (R, 128), 0) < ny) & (lanes(R) < nz)
    for ref in (e3, s3):
        zero_ends(ref, nx)

    def first(x):
        c = jnp.where(ok, W / (6.0 * factor + r3[x]), 0.0)
        c3[x] = c
        s3[x + 1] = c * f3[x]

    loop(nx, first, 6)
    relax(s3, e3, f3, c3, nx, factor, 6)

    def left(x):
        v = f3[x] - (6.0 * factor + r3[x]) * e3[x + 1] + factor * neighbours(e3, x)
        return jnp.where(ok, v, 0.0)

    m = lane_map(lambda l, m: l // 2, 0.125)
    for ref, pair in ((f4, lambda x: left(2 * x) + left(2 * x + 1)), (r4, lambda x: r3[2 * x] + r3[2 * x + 1])):
        coarsen_planes(pair, nx // 2, tmp, ref, R, 6)
        ref[...] = times(flat(ref), m).reshape(ref.shape)
    f4k = 0.25**4
    H = R // 2
    row = lax.broadcasted_iota(jnp.int32, (nx // 2, H, 128), 1)
    lane = lax.broadcasted_iota(jnp.int32, (nx // 2, H, 128), 2)
    within = (row < ny // 2) & (lane < nz // 2)
    diag = 6.0 * f4k + r4[...]
    zero = jnp.zeros((1, H, 128), F32)

    def apply(p):
        s = jnp.concatenate([zero, p[:-1]], axis=0) + jnp.concatenate([p[1:], zero], axis=0)
        s = s + roll(p, 1, 1) + roll(p, H - 1, 1) + roll(p, 1, 2) + roll(p, 127, 2)
        return jnp.where(within, diag * p - f4k * s, 0.0)

    r = jnp.where(within, f4[...], 0.0)
    p = r
    e = jnp.zeros_like(r)
    rr = sum_all(r * r)
    for i in range(BOTTOM_ITERS):
        q = apply(p)
        a = rr / sum_all(p * q)
        e = e + a * p
        if i + 1 < BOTTOM_ITERS:
            r = r - a * q
            new = sum_all(r * r)
            p = r + (new / rr) * p
            rr = new
    f4[...] = times(e.reshape(nx // 2 * H, 128), spread_map(lambda l: l // 2)).reshape(e.shape)
    add_refined(f4, nx // 2, e3, s3, 6)
    relax(s3, e3, f3, c3, nx, factor, 6)
    relax(e3, s3, f3, c3, nx, factor, 6)


def k_up(g3, f2, c2, e2i, f1, c1, e1i, f0, c0, d0, e0i, z_out, az_out, sums,
         e3, s3, f3, c3, r3, tmp3, f4, r4, sq, w3, w2, na, nb, n1, e2, s2, e1, s1, e0, s0):
    gx, gy, gz, sy, sz = place()
    nx, ny, nz = f3.shape[0], sy * 6, sz * 6
    coarse_solve(g3, nx, ny, nz, e3, s3, f3, c3, r3, tmp3, f4, r4, sq)
    for ref, n in ((s2, 18), (s1, 36), (s0, 54), (e2, 18), (e1, 36), (e0, 54)):
        zero_ends(ref, n)
    R3 = s3.shape[1]
    pick = lax.broadcasted_iota(jnp.int32, (16, R3), 1) == lax.broadcasted_iota(jnp.int32, (16, R3), 0) + (gy * 6 - 4)
    pick = pick.astype(F32)
    for i in range(9):
        w3[i] = jnp.dot(pick, s3[i + 1 + gx * 3], precision=HI, preferred_element_type=F32)
    spread = spread_map(lambda l: gz * 6 + jnp.where(l < 64, l // 2, l // 2 - 64))
    w3[...] = times(flat(w3), spread).reshape(9, 16, 128)
    add_refined(w3, 9, e2i, e2, 9)
    relax(e2, s2, f2, c2, 18, 0.0625, 18)
    relax(s2, e2, f2, c2, 18, 0.0625, 18)

    def halves(i):
        na[i] = e2[i + 1, 2:18, :]
        nb[i] = e2[i + 1, 14:30, :]

    loop(18, halves, 6)

    def down(sp, l, want):
        z = lane_z(sp, l)
        up = (l >= sp.cut) & (l < sp.cut + 64)
        good = (z >= -sp.h) & (z < sp.n + sp.h)
        good = good & (up if want else jnp.logical_not(up))
        return jnp.where(good, floor_half(z) + jnp.where(z < 0, 128, 0), -1)

    w2[...] = (
        times(flat(na), spread_map(lambda l: down(L1, l, False))) + times(flat(nb), spread_map(lambda l: down(L1, l, True)))
    ).reshape(18, 16, 128)
    add_refined(w2, 18, e1i, e1, 6)
    relax(e1, s1, f1, c1, 36, 0.25, 12, paired)
    relax(s1, e1, f1, c1, 36, 0.25, 12, paired)

    def near(i):
        v = e1[i + 1 + gx * 9]
        n1[i] = jnp.where(upper(L1, 16), v[0:16], v[8:24])

    loop(27, near, 9)

    def both(l):
        lower, higher = down(L0, l, False), down(L0, l, True)
        return jnp.where(lower >= 0, lower, jnp.where(higher >= 0, (higher + 64) % 128, -1))

    n1[...] = times(flat(n1), spread_map(both)).reshape(27, 16, 128)
    add_refined(n1, 27, e0i, e0, 9)
    relax(e0, s0, f0, c0, 54, 1.0, 9, paired)
    relax(s0, e0, f0, c0, 54, 1.0, 9, paired)
    shift = gx * 6
    mine = lanes(24) % 64 < 48

    def last(x, carry):
        u, v = carry
        w = x + shift
        z = e0[w + 1]
        az = own_rows(L0, d0[w] * z - paired(e0, w))
        z = own_rows(L0, z)
        f = own_rows(L0, f0[w])
        z_out[x] = z
        az_out[x] = az
        return u + jnp.where(mine, f * z, 0.0), v + jnp.where(mine, z * az, 0.0)

    def some(i, carry):
        for k in range(6):
            carry = last(6 * i + k, carry)
        return carry

    zero = jnp.zeros((24, 128), F32)
    u, v = lax.fori_loop(0, 8, some, (zero, zero))

    def total(t):
        return jnp.sum(jnp.sum(t, axis=1, keepdims=True), axis=0, keepdims=True)

    ln = lanes(sums.shape[0])
    sums[...] = jnp.where(ln == 0, total(u), jnp.where(ln == 1, total(v), 0.0))


def k_last(sums, own, z, az, f, sol, res, sv, rv, sems):
    s = jnp.sum(sums[...], axis=0, keepdims=True)
    ln = lanes(1)
    over = jnp.sum(jnp.where(ln == 0, s, 0.0), axis=1, keepdims=True)
    under = jnp.sum(jnp.where(ln == 1, s, 0.0), axis=1, keepdims=True)
    step = over / under
    shift = lax.axis_index("gx") * 6
    pairs = ((0, sv, sol), (1, rv, res))

    def copy(a, src, dst, i):
        part = pl.ds(i * 8, 8)
        return pltpu.make_async_copy(src.at[part], dst.at[part], sems.at[a, i])

    def some(i):
        for k in range(8):
            x = i * 8 + k
            for ref, v in ((sv, own[0, x] + step * z[x]), (rv, own_rows(L0, f[x + shift]) - step * az[x])):
                ref[x, 0:24, :] = v[:, 0:48]
                ref[x, 24:48, :] = roll(v, 64, 1)[:, 0:48]
        for a, src, dst in pairs:
            copy(a, src, dst, i).start()

    loop(6, some)
    for i in range(6):
        for a, src, dst in pairs:
            copy(a, src, dst, i).wait()


def ring(up, dn, axis):
    n = lax.axis_size(axis)
    low = lax.ppermute(up, axis, [(i, (i + 1) % n) for i in range(n)])
    high = lax.ppermute(dn, axis, [(i, (i - 1) % n) for i in range(n)])
    return low, high


def swap(v):
    return lax.ppermute(v, "gx", [(0, 1), (1, 0)])


def body(b, x0, rea):
    ALL = ("gx", "gy", "gz")
    sizes = [lax.axis_size(a) for a in ALL]
    count = sizes[0] * sizes[1] * sizes[2]
    b, x0, rea = (pltpu.with_memory_space_constraint(v, pltpu.HBM) for v in (b, x0, rea))
    hi, lo, own = run(
        k_zpack0,
        (sds(*L0.zshape), sds(*L0.zshape), sds(3, 48, 24, 128)),
        (x0, b, rea),
        [(3, 48, 48, 48), pltpu.SemaphoreType.DMA((3, 6))],
        far_in=True,
    )
    zl, zh = ring(hi, lo, "gz")
    up, dn = run(k_ypack0, (sds(*L0.yshape),) * 2, (own, zl, zh))
    yl, yh = ring(up, dn, "gy")
    xr = swap(run(k_xpack0, sds(*L0.xshape), (own, zl, zh, yl, yh)))
    p0, q0 = (54, 32, 128), (56, 32, 128)
    f0, c0, d0, e0, f1, r1, z1h, z1l = run(
        k_down0,
        (sds(*p0), sds(*p0), sds(*p0), sds(*q0), sds(24, 12, 128), sds(24, 12, 128), sds(*L1.zshape), sds(*L1.zshape)),
        (own, zl, zh, yl, yh, xr),
        [q0, p0, p0, q0, (24, 24, 128), (24, 16, 128)],
        mib=M0,
    )
    zl, zh = ring(z1h, z1l, "gz")
    up, dn = run(k_ypack1, (sds(*L1.yshape),) * 2, (f1, r1, zl, zh))
    yl, yh = ring(up, dn, "gy")
    xr = swap(run(k_xpack1, sds(*L1.xshape), (f1, r1, zl, zh, yl, yh), [(2, 2, 24, 128)]))
    p1, q1, p2, q2 = (36, 24, 128), (38, 24, 128), (18, 32, 128), (20, 32, 128)
    f1w, c1w, e1w, f2w, c2w, e2w, g = run(
        k_down1,
        (sds(*p1), sds(*p1), sds(*q1), sds(*p2), sds(*p2), sds(*q2), sds(count * 4, 128)),
        (f1, r1, zl, zh, yl, yh, xr),
        [p1, q1, (18, 24, 128), (2, 18, 16, 128), p2, q2, (9, 32, 128), (2, 9, 16, 128), (128, 128), (8, 2, 24, 128)],
        mib=M1,
    )
    g = lax.all_to_all(g, ALL, 0, 0, tiled=True)
    n3 = [6 * s for s in sizes]
    R3 = (n3[1] + 8) // 8 * 8
    if R3 % 16:
        R3 += 8
    p3, q3, p4 = (n3[0], R3, 128), (n3[0] + 2, R3, 128), (n3[0] // 2, R3 // 2, 128)
    z, az, sums = run(
        k_up,
        (sds(48, 24, 128), sds(48, 24, 128), sds(count, 128)),
        (g, f2w, c2w, e2w, f1w, c1w, e1w, f0, c0, d0, e0),
        [q3, q3, p3, p3, p3, (n3[0] // 2, R3, 128), p4, p4, (sizes[0] * sizes[1], 128, 128), (9, 16, 128), (18, 16, 128),
         (18, 16, 128), (18, 16, 128), (27, 16, 128), q2, q2, q1, q1, q0, q0],
        mib=M2,
    )
    sums = lax.all_to_all(sums.reshape(count, 1, 128), ALL, 0, 0, tiled=True).reshape(count, 128)
    return run(
        k_last,
        (sds(48, 48, 48), sds(48, 48, 48)),
        (sums, own, z, az, f0),
        [(48, 48, 48), (48, 48, 48), pltpu.SemaphoreType.DMA((2, 6))],
        far_out=True,
    )


def solution(mesh):
    spec = P("gx", "gy", "gz")
    return jax.shard_map(body, mesh=mesh, in_specs=(spec, spec, spec), out_specs=(spec, spec), check_vma=False)
```

```python
import functools
import jax
import jax.numpy as jnp
from jax import lax
from jax.experimental import pallas as pl
from jax.experimental.pallas import tpu as pltpu
from jax.sharding import PartitionSpec as P

W = 6.0 / 7.0
BOTTOM_ITERS = 6
N0 = 48
F32 = jnp.float32
HI = lax.Precision.HIGHEST
M0, M1, M2 = 10, 8, 12
UA, UF, UR, UM, UZ, UY, UL = 8, 9, 18, 18, 12, 4, 6


class Spec:
    def __init__(self, n, h, na, R, o, hx, cut, kp, st):
        self.n, self.h, self.na, self.R, self.o, self.hx, self.cut, self.kp, self.st = n, h, na, R, o, hx, cut, kp, st
        self.half = n // 2
        self.zshape = (n // (kp * st), self.half * st, 128)
        self.yrows = -(-na * h // 8) * 8
        self.yshape = (self.half, self.yrows, 128)
        self.xshape = (hx, na, R, 128)
        self.nx = n + hx


L0 = Spec(48, 5, 3, 32, 8, 6, 56, 4, 1)
L1 = Spec(24, 12, 2, 24, 12, 12, 44, 2, 2)


def sds(*shape):
    return jax.ShapeDtypeStruct(shape, F32)


def run(kernel, outs, args, scratch=(), mib=12, far_in=False, far_out=False):
    vmem = pl.BlockSpec(memory_space=pltpu.VMEM)
    hbm = pl.BlockSpec(memory_space=pl.ANY)
    return pl.pallas_call(
        kernel,
        out_shape=outs,
        in_specs=[hbm if far_in else vmem] * len(args),
        out_specs=jax.tree.map(lambda _: hbm if far_out else vmem, outs),
        scratch_shapes=[pltpu.VMEM(s, F32) if isinstance(s, tuple) else s for s in scratch],
        compiler_params=pltpu.CompilerParams(vmem_limit_bytes=mib * 1024 * 1024),
    )(*args)


def place():
    return [lax.axis_index(a) for a in ("gx", "gy", "gz")] + [lax.axis_size(a) for a in ("gy", "gz")]


def lanes(rows):
    return lax.broadcasted_iota(jnp.int32, (rows, 128), 1)


def roll(v, shift, axis):
    if isinstance(shift, int):
        shift = shift % v.shape[axis]
        if shift == 0:
            return v
    return pltpu.roll(v, shift, axis)


def loop(n, f, u=1):
    u = max(d for d in range(1, u + 1) if n % d == 0)

    def some(i, c):
        for k in range(u):
            f(i * u + k)
        return c

    lax.fori_loop(0, n // u, some, 0)


def upper(sp, rows):
    l = lanes(rows)
    return (l >= sp.cut) & (l < sp.cut + 64)


def edge(sp, ids):
    _, gy, gz, ny, nz = ids
    high = jnp.where(gz < nz - 1, sp.n + sp.h, sp.n)
    low = jnp.where(gz > 0, 64 - sp.h, 64)
    return high, low, jnp.where(gy > 0, 1.0, 0.0), jnp.where(gy < ny - 1, 1.0, 0.0)


def ztile(sp, own, hi_ref, lo_ref, g):
    l = lanes(sp.half)
    for t in range(sp.st):
        hi = jnp.zeros((sp.half, 128), F32)
        lo = hi
        for k in range(sp.kp):
            for a in range(sp.na):
                v = own(t * (sp.n // sp.st) + g * sp.kp + k, a)
                at = sp.h * (k * sp.na + a)
                far = (at - sp.n - sp.h) % 64
                hi = jnp.where((l - far) % 64 < sp.h, roll(v, at - 2 * sp.n, 1), hi)
                lo = jnp.where((l - at) % 64 < sp.h, roll(v, at, 1), lo)
        hi_ref[g, t * sp.half : (t + 1) * sp.half, :] = hi
        lo_ref[g, t * sp.half : (t + 1) * sp.half, :] = lo


def merged(sp, own, zl, zh, x, a, b, e, top, bottom):
    per = sp.n // sp.st
    t, y = lax.div(x, per), lax.rem(x, per)
    g, k = lax.div(y, sp.kp), lax.rem(y, sp.kp)
    at = sp.h * (k * sp.na + a)
    if sp.st == 1:
        high, low = zh[g, b:e, :], zl[g, b:e, :]
    else:
        high = jnp.where(t == 0, zh[g, b:e, :], zh[g, sp.half + b : sp.half + e, :])
        low = jnp.where(t == 0, zl[g, b:e, :], zl[g, sp.half + b : sp.half + e, :])
    l = lanes(e - b)
    beside = jnp.where(((l + (64 - at)) & 63) < sp.h, high, low)
    beside = roll(beside, (sp.n + 128 - at) & 127, 1)
    q = l & 63
    return jnp.where(q < sp.n, own(x, a)[b:e], jnp.where((q < top) | (q >= bottom), beside, 0.0))


def ypack(sp, own, zl, zh, up_ref, dn_ref):
    h, half = sp.h, sp.half
    up0 = (half - h) // 8 * 8
    dn1 = min(half, -(-h // 8) * 8)
    top, bottom, _, _ = edge(sp, place())

    def pair(p):
        for a in range(sp.na):
            for ref, b, e, s, t, swap in ((up_ref, up0, half, half - h - up0, half - up0, False), (dn_ref, 0, dn1, 0, h, True)):
                even = merged(sp, own, zl, zh, 2 * p, a, b, e, top, bottom)
                odd = roll(merged(sp, own, zl, zh, 2 * p + 1, a, b, e, top, bottom), 64, 1)
                first, second = (odd, even) if swap else (even, odd)
                ref[p, a * h : (a + 1) * h, :] = jnp.where(upper(sp, e - b), first, second)[s:t]
        if sp.yrows > sp.na * h:
            pad = jnp.zeros((sp.yrows - sp.na * h, 128), F32)
            up_ref[p, sp.na * h :, :] = pad
            dn_ref[p, sp.na * h :, :] = pad

    loop(half, pair, UY)


def plane(sp, own, zl, zh, yl, yh, x, a, dst, xw, ends, spare):
    top, bottom, below, above = ends
    h, half = sp.h, sp.half
    m = merged(sp, own, zl, zh, x, a, 0, half, top, bottom)
    p = lax.div(x, 2)
    turn = 64 * (1 - lax.rem(x, 2))
    if sp.o == 8:
        low = roll(roll(yl[p], 8 - h - a * h, 0)[0:8], turn, 1) * below
        high = roll(roll(yh[p], -a * h, 0)[0:8], turn, 1) * above
        lower = jnp.concatenate([low, m], axis=0)
        higher = jnp.concatenate([m, high], axis=0)
        dst[xw] = jnp.where(upper(sp, sp.R), higher, lower)
    else:
        spare[0, 0:h, :] = roll(yl[p, a * h : (a + 1) * h, :], turn, 1) * below
        spare[0, h:, :] = m
        spare[1, 0:half, :] = m
        spare[1, half:, :] = roll(yh[p, a * h : (a + 1) * h, :], turn, 1) * above
        dst[xw] = jnp.where(upper(sp, sp.R), spare[1], spare[0])


def lane_z(sp, l):
    return jnp.where(l < sp.cut, l, jnp.where(l < sp.cut + 64, l - 64, l - 128))


def inside(sp, ids):
    _, gy, gz, ny, nz = ids
    n, h = sp.n, sp.h
    y = lax.broadcasted_iota(jnp.int32, (sp.R, 128), 0) - sp.o + jnp.where(upper(sp, sp.R), sp.R, 0)
    z = lane_z(sp, lanes(sp.R))
    ok = (y >= -h) & (y < n + h) & (z >= -h) & (z < n + h)
    y, z = y + gy * n, z + gz * n
    return ok & (y >= 0) & (y < ny * n) & (z >= 0) & (z < nz * n)


def paired(ref, x):
    c = ref[x + 1]
    R = c.shape[0]
    s = ref[x] + ref[x + 2]
    sub = lax.broadcasted_iota(jnp.int32, (8, 128), 0)
    seam = roll(jnp.where(sub == 0, c[0:8], c[R - 8 : R]), 64, 1)
    up, down = roll(c, R - 1, 0), roll(c, 1, 0)
    up = jnp.concatenate([up[: R - 8], jnp.where(sub == 7, roll(seam, 7, 0), up[R - 8 :])], axis=0)
    down = jnp.concatenate([jnp.where(sub == 0, roll(seam, 1, 0), down[0:8]), down[8:]], axis=0)
    s = s + (up + down)
    return s + (roll(c, 1, 1) + roll(c, 127, 1))


def domain(sp, n, h, r0, R, ids):
    row = lax.broadcasted_iota(jnp.int32, (R, 128), 0) - r0
    ln = lanes(R)
    z = jnp.where(ln < 64, ln, ln - 128)
    gy, gz, ny, nz = ids[1], ids[2], ids[3], ids[4]
    y_at, z_at = row + gy * n, z + gz * n
    ok = (row >= -h) & (row < n + h) & (z >= -h) & (z < n + h)
    return ok & (y_at >= 0) & (y_at < ny * n) & (z_at >= 0) & (z_at < nz * n)


def neighbours(ref, x):
    c = ref[x + 1]
    R = c.shape[0]
    s = ref[x] + ref[x + 2]
    s = s + (roll(c, 1, 0) + roll(c, R - 1, 0))
    return s + (roll(c, 1, 1) + roll(c, 127, 1))


def zero_ends(ref, n):
    ref[0] = jnp.zeros(ref.shape[1:], F32)
    ref[n + 1] = jnp.zeros(ref.shape[1:], F32)


def relax(src, dst, f, c, n, factor, u=9, near=None):
    near = near or neighbours

    def one(x):
        dst[x + 1] = (1.0 - W) * src[x + 1] + c[x] * (f[x] + factor * near(src, x))

    loop(n, one, u)


def lane_map(pick, value, cols=128):
    l = lax.broadcasted_iota(jnp.int32, (256, cols), 0) % 128
    m = lax.broadcasted_iota(jnp.int32, (256, cols), 1)
    return jnp.where(pick(l, m) == m, value, 0.0).astype(jnp.bfloat16)


def spread_map(pick):
    m = lax.broadcasted_iota(jnp.int32, (256, 128), 0) % 128
    l = lax.broadcasted_iota(jnp.int32, (256, 128), 1)
    return jnp.where(pick(l) == m, 1.0, 0.0).astype(jnp.bfloat16)


def floor_half(z):
    return lax.shift_right_arithmetic(z, 1)


def times(v, m):
    big = v.astype(jnp.bfloat16)
    rest = (v - big.astype(F32)).astype(jnp.bfloat16)
    return jnp.dot(jnp.concatenate([big, rest], axis=1), m, preferred_element_type=F32)


def coarsen_planes(pair, n, tmp, acc, rows, u=2):
    half = rows // 2

    def one(x):
        tmp[x, 0:rows, :] = pair(x)
        acc[x, 0:half, :] = tmp[x, pl.ds(0, half, stride=2), :] + tmp[x, pl.ds(1, half, stride=2), :]

    loop(n, one, u)


def flat(ref):
    n, rows, _ = ref.shape
    return ref[...].reshape(n * rows, 128)


def add_refined(wide, n, src, dst, u=3):
    R = dst.shape[1]

    def one(i):
        v = wide[i, 0 : R // 2, :]
        for k in range(2):
            dst[2 * i + 1, pl.ds(k, R // 2, stride=2), :] = v
        t = dst[2 * i + 1]
        dst[2 * i + 1] = src[2 * i + 1] + t
        dst[2 * i + 2] = src[2 * i + 2] + t

    loop(n, one, u)


def k_zpack0(x0, b, rea, hi, lo, own, raw, sems):
    def copy(a, ref, i):
        part = pl.ds(i * 8, 8)
        return pltpu.make_async_copy(ref.at[part], raw.at[a, part], sems.at[a, i])

    refs = (x0, b, rea)
    for i in range(6):
        for a, ref in enumerate(refs):
            copy(a, ref, i).start()

    def some(i):
        for a, ref in enumerate(refs):
            copy(a, ref, i).wait()
        for k in range(8):
            x = i * 8 + k
            for a in range(3):
                own[a, x, :, 0:48] = raw[a, x, 0:24, :]
                own[a, x, :, 64:112] = raw[a, x, 24:48, :]
        for k in range(2):
            ztile(L0, lambda x, a: own[a, x], hi, lo, i * 2 + k)

    loop(6, some)


def k_ypack0(own, zl, zh, up, dn):
    ypack(L0, lambda x, a: own[a, x], zl, zh, up, dn)


def xpack(sp, own, zl, zh, yl, yh, out, spare):
    ids = place()
    ends = edge(sp, ids)
    start = (1 - ids[0]) * (sp.n - sp.hx)

    def one(i):
        for a in range(sp.na):
            plane(sp, own, zl, zh, yl, yh, start + i, a, out.at[i], a, ends, None if spare is None else spare.at[a])

    loop(sp.hx, one, 2)


def k_xpack0(own, zl, zh, yl, yh, out):
    xpack(L0, lambda x, a: own[a, x], zl, zh, yl, yh, out, None)


def assemble(sp, ids, own, zl, zh, yl, yh, xr, dsts, spare, u):
    shift = ids[0] * sp.hx
    ends = edge(sp, ids)

    def some(i):
        for k in range(u):
            x = i * u + k
            for a, (dst, off) in enumerate(dsts):
                plane(sp, own, zl, zh, yl, yh, x, a, dst, x + shift + off, ends, None if spare is None else spare.at[k * sp.na + a])

    loop(sp.n // u, some)
    other = (1 - ids[0]) * sp.n

    def take(i):
        for a, (dst, off) in enumerate(dsts):
            dst[other + i + off] = xr[i, a]

    loop(sp.hx, take, 2)


def own_rows(sp, v):
    return jnp.where(upper(sp, sp.half), v[0 : sp.half], v[sp.o :])


def half_own(pair, tmp, acc, out, u):
    coarsen_planes(pair, 24, tmp, acc, 24, u)
    m = lane_map(lambda l, m: jnp.where(l < 64, l // 2, 32 + l // 2), 0.125)
    acc[...] = times(flat(acc), m).reshape(24, 16, 128)

    def keep(x):
        out[x] = acc[x, 0:12, :]

    loop(24, keep, 6)


def k_react(own, r1, tmp, acc):
    mine = lanes(24) % 64 < 48
    half_own(lambda x: jnp.where(mine, own[2, 2 * x] + own[2, 2 * x + 1], 0.0), tmp, acc, r1, 4)


def k_down0(own, r1, zl, zh, yl, yh, xr, f_out, c_out, d_out, e_out, f1, z1h, z1l, xw, bw, rw, ew, tmp, acc):
    ids = place()
    assemble(L0, ids, lambda x, a: own[a, x], zl, zh, yl, yh, xr, ((xw, 1), (bw, 0), (rw, 0)), None, UA)
    n = L0.nx
    ok = inside(L0, ids)
    zero_ends(xw, n)
    zero_ends(ew, n)
    zero_ends(e_out, n)

    def first(x):
        d = 6.0 + rw[x]
        c = jnp.where(ok, W / d, 0.0)
        f = bw[x] - d * xw[x + 1] + paired(xw, x)
        d_out[x] = d
        f_out[x] = f
        c_out[x] = c
        ew[x + 1] = c * f

    loop(n, first, UF)
    relax(ew, e_out, f_out, c_out, n, 1.0, UR, paired)
    shift = ids[0] * L0.hx

    def left(x):
        return own_rows(L0, f_out[x] - d_out[x] * e_out[x + 1] + paired(e_out, x))

    mine = lanes(24) % 64 < 48
    pair = lambda x: jnp.where(mine, left(2 * x + shift) + left(2 * x + shift + 1), 0.0)
    half_own(pair, tmp, acc, f1, UL)
    both = (f1, r1)
    loop(6, lambda g: ztile(L1, lambda x, a: both[a][x], z1h, z1l, g), 3)


def k_ypack1(f1, r1, zl, zh, up, dn):
    both = (f1, r1)
    ypack(L1, lambda x, a: both[a][x], zl, zh, up, dn)


def k_xpack1(f1, r1, zl, zh, yl, yh, out, spare):
    both = (f1, r1)
    xpack(L1, lambda x, a: both[a][x], zl, zh, yl, yh, out, spare)


def k_down1(f1, r1, zl, zh, yl, yh, xr, fw, cw, e_out, f2, c2, e2, out3, rw, ew, tmp, acc, r2, ew2, tmp2, t3, sq, spare):
    ids = place()
    both = (f1, r1)
    assemble(L1, ids, lambda x, a: both[a][x], zl, zh, yl, yh, xr, ((fw, 0), (rw, 0)), spare, 4)
    n = L1.nx
    ok = inside(L1, ids)
    zero_ends(ew, n)
    zero_ends(e_out, n)

    def first(x):
        c = jnp.where(ok, W / (1.5 + rw[x]), 0.0)
        cw[x] = c
        ew[x + 1] = c * fw[x]

    loop(n, first, 6)
    relax(ew, e_out, fw, cw, n, 0.25, UM, paired)

    def left(x):
        return fw[x] - (1.5 + rw[x]) * e_out[x + 1] + 0.25 * paired(e_out, x)

    def pick(l, m):
        z = lane_z(L1, l)
        up = (l >= L1.cut) & (l < L1.cut + 64)
        good = (z >= -12) & (z < 36) & (up == (m >= 128))
        return jnp.where(good, floor_half(z) + jnp.where(z < 0, 128, 0) + jnp.where(up, 128, 0), -1)

    m = lane_map(pick, 0.125, 256)
    for ref, pair in ((f2, lambda x: left(2 * x) + left(2 * x + 1)), (r2, lambda x: rw[2 * x] + rw[2 * x + 1])):
        coarsen_planes(pair, 18, tmp, acc.at[0], 24, 6)
        v = times(flat(acc.at[0]), m)
        acc[0] = v[:, 0:128].reshape(18, 16, 128)
        acc[1] = v[:, 128:256].reshape(18, 16, 128)

        def keep(x, ref=ref):
            ref[x] = jnp.zeros((32, 128), F32)
            ref[x, 2:14, :] = acc[0, x, 0:12, :]
            ref[x, 14:26, :] = acc[1, x, 0:12, :]

        loop(18, keep, 6)
    ok2 = domain(None, 12, 6, 8, 32, ids)
    zero_ends(ew2, 18)
    zero_ends(e2, 18)

    def second(x):
        c = jnp.where(ok2, W / (0.375 + r2[x]), 0.0)
        c2[x] = c
        ew2[x + 1] = c * f2[x]

    loop(18, second, 6)
    relax(ew2, e2, f2, c2, 18, 0.0625, 18)

    def left2(x):
        return f2[x] - (0.375 + r2[x]) * e2[x + 1] + 0.0625 * neighbours(e2, x)

    m = lane_map(lambda l, m: jnp.where(l < 64, l // 2, l // 2 + 64), 0.125)
    for a, pair in enumerate((lambda x: left2(2 * x) + left2(2 * x + 1), lambda x: r2[2 * x] + r2[2 * x + 1])):
        coarsen_planes(pair, 9, tmp2, t3.at[a], 32, 9)
        t3[a] = times(flat(t3.at[a]), m).reshape(9, 16, 128)
    shift = ids[0] * 3
    sq[...] = jnp.zeros((128, 128), F32)
    for a in range(2):
        for x in range(6):
            at = a * 36 + x * 6
            sq[at : at + 6, :] = t3[a, x + shift, 4:10, :]
    t = sq[...].T[0:8]
    ln = lanes(1)
    rows = []
    for u in range(2):
        for a in range(2):
            parts = [roll(t, 36 * (w - a), 1)[3 * u + w : 3 * u + w + 1] for w in range(3)]
            rows.append(jnp.where(ln < 36, parts[0], jnp.where(ln < 72, parts[1], parts[2])))
    tile = jnp.concatenate(rows + rows, axis=0)
    n8 = out3.shape[0] // 8
    out3[...] = jnp.broadcast_to(tile[None], (n8, 8, 128)).reshape(n8 * 8, 128)


def sum_all(v):
    s = jnp.sum(v, axis=0)
    return jnp.sum(jnp.sum(s, axis=1, keepdims=True), axis=0, keepdims=True)


def coarse_solve(g3, nx, ny, nz, e3, s3, f3, c3, r3, tmp, f4, r4, sq):
    R = f3.shape[1]
    for ref in (f3, r3):
        ref[...] = jnp.zeros(ref.shape, F32)
    kx, ky, kz = nx // 6, ny // 6, nz // 6
    for bx in range(kx):
        for by in range(ky):
            k = bx * ky + by
            if kz * 6 < 128:
                sq[k, kz * 6 :, :] = jnp.zeros((128 - kz * 6, 128), F32)
            got = [g3[pl.ds(k * kz * 4 + r, kz, stride=4), :] for r in range(4)]
            ln = lanes(kz)
            for u in range(2):
                for w in range(3):
                    f, r = roll(got[2 * u], -36 * w, 1), roll(got[2 * u + 1], 36 - 36 * w, 1)
                    sq[k, pl.ds(3 * u + w, kz, stride=6), :] = jnp.where(ln < 36, f, r)
            t = sq[k].T
            for x in range(6):
                f3[bx * 6 + x, by * 6 : by * 6 + 6, :] = t[x * 6 : x * 6 + 6]
                r3[bx * 6 + x, by * 6 : by * 6 + 6, :] = t[36 + x * 6 : 42 + x * 6]
    factor = 0.25**3
    ok = (lax.broadcasted_iota(jnp.int32, (R, 128), 0) < ny) & (lanes(R) < nz)
    for ref in (e3, s3):
        zero_ends(ref, nx)

    def first(x):
        c = jnp.where(ok, W / (6.0 * factor + r3[x]), 0.0)
        c3[x] = c
        s3[x + 1] = c * f3[x]

    loop(nx, first, 6)
    relax(s3, e3, f3, c3, nx, factor, 12)

    def left(x):
        v = f3[x] - (6.0 * factor + r3[x]) * e3[x + 1] + factor * neighbours(e3, x)
        return jnp.where(ok, v, 0.0)

    m = lane_map(lambda l, m: l // 2, 0.125)
    for ref, pair in ((f4, lambda x: left(2 * x) + left(2 * x + 1)), (r4, lambda x: r3[2 * x] + r3[2 * x + 1])):
        coarsen_planes(pair, nx // 2, tmp, ref, R, 6)
        ref[...] = times(flat(ref), m).reshape(ref.shape)
    f4k = 0.25**4
    H = R // 2
    row = lax.broadcasted_iota(jnp.int32, (nx // 2, H, 128), 1)
    lane = lax.broadcasted_iota(jnp.int32, (nx // 2, H, 128), 2)
    within = (row < ny // 2) & (lane < nz // 2)
    diag = 6.0 * f4k + r4[...]
    zero = jnp.zeros((1, H, 128), F32)

    def apply(p):
        s = jnp.concatenate([zero, p[:-1]], axis=0) + jnp.concatenate([p[1:], zero], axis=0)
        s = s + roll(p, 1, 1) + roll(p, H - 1, 1) + roll(p, 1, 2) + roll(p, 127, 2)
        return jnp.where(within, diag * p - f4k * s, 0.0)

    r = jnp.where(within, f4[...], 0.0)
    p = r
    e = jnp.zeros_like(r)
    rr = sum_all(r * r)
    for i in range(BOTTOM_ITERS):
        q = apply(p)
        a = rr / sum_all(p * q)
        e = e + a * p
        if i + 1 < BOTTOM_ITERS:
            r = r - a * q
            new = sum_all(r * r)
            p = r + (new / rr) * p
            rr = new
    f4[...] = times(e.reshape(nx // 2 * H, 128), spread_map(lambda l: l // 2)).reshape(e.shape)
    add_refined(f4, nx // 2, e3, s3, 6)
    relax(s3, e3, f3, c3, nx, factor, 12)
    relax(e3, s3, f3, c3, nx, factor, 12)


def k_up(g3, f2, c2, e2i, f1, c1, e1i, f0, c0, d0, e0i, z_out, az_out, sums,
         e3, s3, f3, c3, r3, tmp3, f4, r4, sq, w3, w2, na, nb, n1, e2, s2, e1, s1, e0, s0):
    gx, gy, gz, sy, sz = place()
    nx, ny, nz = f3.shape[0], sy * 6, sz * 6
    coarse_solve(g3, nx, ny, nz, e3, s3, f3, c3, r3, tmp3, f4, r4, sq)
    for ref, n in ((s2, 18), (s1, 36), (s0, 54), (e2, 18), (e1, 36), (e0, 54)):
        zero_ends(ref, n)
    R3 = s3.shape[1]
    pick = lax.broadcasted_iota(jnp.int32, (16, R3), 1) == lax.broadcasted_iota(jnp.int32, (16, R3), 0) + (gy * 6 - 4)
    pick = pick.astype(F32)
    for i in range(9):
        w3[i] = jnp.dot(pick, s3[i + 1 + gx * 3], precision=HI, preferred_element_type=F32)
    spread = spread_map(lambda l: gz * 6 + jnp.where(l < 64, l // 2, l // 2 - 64))
    w3[...] = times(flat(w3), spread).reshape(9, 16, 128)
    add_refined(w3, 9, e2i, e2, 9)
    relax(e2, s2, f2, c2, 18, 0.0625, 18)
    relax(s2, e2, f2, c2, 18, 0.0625, 18)

    def halves(i):
        na[i] = e2[i + 1, 2:18, :]
        nb[i] = e2[i + 1, 14:30, :]

    loop(18, halves, 6)

    def down(sp, l, want):
        z = lane_z(sp, l)
        up = (l >= sp.cut) & (l < sp.cut + 64)
        good = (z >= -sp.h) & (z < sp.n + sp.h)
        good = good & (up if want else jnp.logical_not(up))
        return jnp.where(good, floor_half(z) + jnp.where(z < 0, 128, 0), -1)

    w2[...] = (
        times(flat(na), spread_map(lambda l: down(L1, l, False))) + times(flat(nb), spread_map(lambda l: down(L1, l, True)))
    ).reshape(18, 16, 128)
    add_refined(w2, 18, e1i, e1, 6)
    relax(e1, s1, f1, c1, 36, 0.25, UM, paired)
    relax(s1, e1, f1, c1, 36, 0.25, UM, paired)

    def near(i):
        v = e1[i + 1 + gx * 9]
        n1[i] = jnp.where(upper(L1, 16), v[0:16], v[8:24])

    loop(27, near, 9)

    def both(l):
        lower, higher = down(L0, l, False), down(L0, l, True)
        return jnp.where(lower >= 0, lower, jnp.where(higher >= 0, (higher + 64) % 128, -1))

    n1[...] = times(flat(n1), spread_map(both)).reshape(27, 16, 128)
    add_refined(n1, 27, e0i, e0, 9)
    relax(e0, s0, f0, c0, 54, 1.0, UR, paired)
    relax(s0, e0, f0, c0, 54, 1.0, UR, paired)
    shift = gx * 6
    mine = lanes(24) % 64 < 48

    def last(x, carry):
        u, v = carry
        w = x + shift
        z = e0[w + 1]
        az = own_rows(L0, d0[w] * z - paired(e0, w))
        z = own_rows(L0, z)
        f = own_rows(L0, f0[w])
        z_out[x] = z
        az_out[x] = az
        return u + jnp.where(mine, f * z, 0.0), v + jnp.where(mine, z * az, 0.0)

    def some(i, carry):
        for k in range(UZ):
            carry = last(UZ * i + k, carry)
        return carry

    zero = jnp.zeros((24, 128), F32)
    u, v = lax.fori_loop(0, 48 // UZ, some, (zero, zero))

    def total(t):
        return jnp.sum(jnp.sum(t, axis=1, keepdims=True), axis=0, keepdims=True)

    ln = lanes(sums.shape[0])
    sums[...] = jnp.where(ln == 0, total(u), jnp.where(ln == 1, total(v), 0.0))


def k_last(sums, own, z, az, f, sol, res, sv, rv, sems):
    s = jnp.sum(sums[...], axis=0, keepdims=True)
    ln = lanes(1)
    over = jnp.sum(jnp.where(ln == 0, s, 0.0), axis=1, keepdims=True)
    under = jnp.sum(jnp.where(ln == 1, s, 0.0), axis=1, keepdims=True)
    step = over / under
    shift = lax.axis_index("gx") * 6
    pairs = ((0, sv, sol), (1, rv, res))

    def copy(a, src, dst, i):
        part = pl.ds(i * 8, 8)
        return pltpu.make_async_copy(src.at[part], dst.at[part], sems.at[a, i])

    def some(i):
        for k in range(8):
            x = i * 8 + k
            for ref, v in ((sv, own[0, x] + step * z[x]), (rv, own_rows(L0, f[x + shift]) - step * az[x])):
                ref[x, 0:24, :] = v[:, 0:48]
                ref[x, 24:48, :] = roll(v, 64, 1)[:, 0:48]
        for a, src, dst in pairs:
            copy(a, src, dst, i).start()

    loop(6, some)
    for i in range(6):
        for a, src, dst in pairs:
            copy(a, src, dst, i).wait()


def ring(up, dn, axis):
    n = lax.axis_size(axis)
    low = lax.ppermute(up, axis, [(i, (i + 1) % n) for i in range(n)])
    high = lax.ppermute(dn, axis, [(i, (i - 1) % n) for i in range(n)])
    return low, high


def swap(v):
    return lax.ppermute(v, "gx", [(0, 1), (1, 0)])


def body(b, x0, rea):
    ALL = ("gx", "gy", "gz")
    sizes = [lax.axis_size(a) for a in ALL]
    count = sizes[0] * sizes[1] * sizes[2]
    b, x0, rea = (pltpu.with_memory_space_constraint(v, pltpu.HBM) for v in (b, x0, rea))
    hi, lo, own = run(
        k_zpack0,
        (sds(*L0.zshape), sds(*L0.zshape), sds(3, 48, 24, 128)),
        (x0, b, rea),
        [(3, 48, 48, 48), pltpu.SemaphoreType.DMA((3, 6))],
        far_in=True,
    )
    zl, zh = ring(hi, lo, "gz")
    r1 = run(k_react, sds(24, 12, 128), (own,), [(24, 24, 128), (24, 16, 128)])
    up, dn = run(k_ypack0, (sds(*L0.yshape),) * 2, (own, zl, zh))
    yl, yh = ring(up, dn, "gy")
    xr = swap(run(k_xpack0, sds(*L0.xshape), (own, zl, zh, yl, yh)))
    p0, q0 = (54, 32, 128), (56, 32, 128)
    f0, c0, d0, e0, f1, z1h, z1l = run(
        k_down0,
        (sds(*p0), sds(*p0), sds(*p0), sds(*q0), sds(24, 12, 128), sds(*L1.zshape), sds(*L1.zshape)),
        (own, r1, zl, zh, yl, yh, xr),
        [q0, p0, p0, q0, (24, 24, 128), (24, 16, 128)],
        mib=M0,
    )
    zl, zh = ring(z1h, z1l, "gz")
    up, dn = run(k_ypack1, (sds(*L1.yshape),) * 2, (f1, r1, zl, zh))
    yl, yh = ring(up, dn, "gy")
    xr = swap(run(k_xpack1, sds(*L1.xshape), (f1, r1, zl, zh, yl, yh), [(2, 2, 24, 128)]))
    p1, q1, p2, q2 = (36, 24, 128), (38, 24, 128), (18, 32, 128), (20, 32, 128)
    f1w, c1w, e1w, f2w, c2w, e2w, g = run(
        k_down1,
        (sds(*p1), sds(*p1), sds(*q1), sds(*p2), sds(*p2), sds(*q2), sds(count * 4, 128)),
        (f1, r1, zl, zh, yl, yh, xr),
        [p1, q1, (18, 24, 128), (2, 18, 16, 128), p2, q2, (9, 32, 128), (2, 9, 16, 128), (128, 128), (8, 2, 24, 128)],
        mib=M1,
    )
    g = lax.all_to_all(g, ALL, 0, 0, tiled=True)
    n3 = [6 * s for s in sizes]
    R3 = (n3[1] + 8) // 8 * 8
    if R3 % 16:
        R3 += 8
    p3, q3, p4 = (n3[0], R3, 128), (n3[0] + 2, R3, 128), (n3[0] // 2, R3 // 2, 128)
    z, az, sums = run(
        k_up,
        (sds(48, 24, 128), sds(48, 24, 128), sds(count, 128)),
        (g, f2w, c2w, e2w, f1w, c1w, e1w, f0, c0, d0, e0),
        [q3, q3, p3, p3, p3, (n3[0] // 2, R3, 128), p4, p4, (sizes[0] * sizes[1], 128, 128), (9, 16, 128), (18, 16, 128),
         (18, 16, 128), (18, 16, 128), (27, 16, 128), q2, q2, q1, q1, q0, q0],
        mib=M2,
    )
    sums = lax.all_to_all(sums.reshape(count, 1, 128), ALL, 0, 0, tiled=True).reshape(count, 128)
    return run(
        k_last,
        (sds(48, 48, 48), sds(48, 48, 48)),
        (sums, own, z, az, f0),
        [(48, 48, 48), (48, 48, 48), pltpu.SemaphoreType.DMA((2, 6))],
        far_out=True,
    )


def solution(mesh):
    spec = P("gx", "gy", "gz")
    return jax.shard_map(body, mesh=mesh, in_specs=(spec, spec, spec), out_specs=(spec, spec), check_vma=False)
```

```python
import functools
import jax
import jax.numpy as jnp
from jax import lax
from jax.experimental import pallas as pl
from jax.experimental.pallas import tpu as pltpu
from jax.sharding import PartitionSpec as P

W = 6.0 / 7.0
BOTTOM_ITERS = 6
N0 = 48
F32 = jnp.float32
HI = lax.Precision.HIGHEST
M0, M1, M2 = 10, 8, 12
UA, UF, UR, UM, UZ, UY, UL = 8, 12, 18, 18, 12, 8, 6


class Spec:
    def __init__(self, n, h, na, R, o, hx, cut, kp, st):
        self.n, self.h, self.na, self.R, self.o, self.hx, self.cut, self.kp, self.st = n, h, na, R, o, hx, cut, kp, st
        self.half = n // 2
        self.zshape = (n // (kp * st), self.half * st, 128)
        self.yrows = -(-na * h // 8) * 8
        self.yshape = (self.half, self.yrows, 128)
        self.xshape = (hx, na, R, 128)
        self.nx = n + hx


L0 = Spec(48, 5, 3, 32, 8, 6, 56, 4, 1)
L1 = Spec(24, 12, 2, 24, 12, 12, 44, 2, 2)


def sds(*shape, dtype=F32):
    return jax.ShapeDtypeStruct(shape, dtype)


def run(kernel, outs, args, scratch=(), mib=12, far_in=False, far_out=False):
    vmem = pl.BlockSpec(memory_space=pltpu.VMEM)
    hbm = pl.BlockSpec(memory_space=pl.ANY)
    return pl.pallas_call(
        kernel,
        out_shape=outs,
        in_specs=[hbm if far_in else vmem] * len(args),
        out_specs=jax.tree.map(lambda _: hbm if far_out else vmem, outs),
        scratch_shapes=[pltpu.VMEM(s, F32) if isinstance(s, tuple) else s for s in scratch],
        compiler_params=pltpu.CompilerParams(vmem_limit_bytes=mib * 1024 * 1024),
    )(*args)


def place():
    return [lax.axis_index(a) for a in ("gx", "gy", "gz")] + [lax.axis_size(a) for a in ("gy", "gz")]


def lanes(rows):
    return lax.broadcasted_iota(jnp.int32, (rows, 128), 1)


def roll(v, shift, axis):
    if isinstance(shift, int):
        shift = shift % v.shape[axis]
        if shift == 0:
            return v
    return pltpu.roll(v, shift, axis)


def loop(n, f, u=1):
    u = max(d for d in range(1, u + 1) if n % d == 0)

    def some(i, c):
        for k in range(u):
            f(i * u + k)
        return c

    lax.fori_loop(0, n // u, some, 0)


def upper(sp, rows):
    l = lanes(rows)
    return (l >= sp.cut) & (l < sp.cut + 64)


def edge(sp, ids):
    _, gy, gz, ny, nz = ids
    high = jnp.where(gz < nz - 1, sp.n + sp.h, sp.n)
    low = jnp.where(gz > 0, 64 - sp.h, 64)
    return high, low, jnp.where(gy > 0, 1.0, 0.0), jnp.where(gy < ny - 1, 1.0, 0.0)


def ztile(sp, own, hi_ref, lo_ref, g):
    l = lanes(sp.half)
    for t in range(sp.st):
        hi = jnp.zeros((sp.half, 128), F32)
        lo = hi
        for k in range(sp.kp):
            for a in range(sp.na):
                v = own(t * (sp.n // sp.st) + g * sp.kp + k, a)
                at = sp.h * (k * sp.na + a)
                far = (at - sp.n - sp.h) % 64
                hi = jnp.where((l - far) % 64 < sp.h, roll(v, at - 2 * sp.n, 1), hi)
                lo = jnp.where((l - at) % 64 < sp.h, roll(v, at, 1), lo)
        hi_ref[g, t * sp.half : (t + 1) * sp.half, :] = hi
        lo_ref[g, t * sp.half : (t + 1) * sp.half, :] = lo


def merged(sp, own, zl, zh, x, a, b, e, top, bottom):
    per = sp.n // sp.st
    t, y = lax.div(x, per), lax.rem(x, per)
    g, k = lax.div(y, sp.kp), lax.rem(y, sp.kp)
    at = sp.h * (k * sp.na + a)
    if sp.st == 1:
        high, low = zh[g, b:e, :], zl[g, b:e, :]
    else:
        high = jnp.where(t == 0, zh[g, b:e, :], zh[g, sp.half + b : sp.half + e, :])
        low = jnp.where(t == 0, zl[g, b:e, :], zl[g, sp.half + b : sp.half + e, :])
    l = lanes(e - b)
    beside = jnp.where(((l + (64 - at)) & 63) < sp.h, high, low)
    beside = roll(beside, (sp.n + 128 - at) & 127, 1)
    q = l & 63
    return jnp.where(q < sp.n, own(x, a)[b:e], jnp.where((q < top) | (q >= bottom), beside, 0.0))


def ypack(sp, own, zl, zh, up_ref, dn_ref):
    h, half = sp.h, sp.half
    up0 = (half - h) // 8 * 8
    dn1 = min(half, -(-h // 8) * 8)
    top, bottom, _, _ = edge(sp, place())

    def pair(p):
        for a in range(sp.na):
            for ref, b, e, s, t, swap in ((up_ref, up0, half, half - h - up0, half - up0, False), (dn_ref, 0, dn1, 0, h, True)):
                even = merged(sp, own, zl, zh, 2 * p, a, b, e, top, bottom)
                odd = roll(merged(sp, own, zl, zh, 2 * p + 1, a, b, e, top, bottom), 64, 1)
                first, second = (odd, even) if swap else (even, odd)
                ref[p, a * h : (a + 1) * h, :] = jnp.where(upper(sp, e - b), first, second)[s:t]
        if sp.yrows > sp.na * h:
            pad = jnp.zeros((sp.yrows - sp.na * h, 128), F32)
            up_ref[p, sp.na * h :, :] = pad
            dn_ref[p, sp.na * h :, :] = pad

    loop(half, pair, UY)


def plane(sp, own, zl, zh, yl, yh, x, a, dst, xw, ends, spare):
    top, bottom, below, above = ends
    h, half = sp.h, sp.half
    m = merged(sp, own, zl, zh, x, a, 0, half, top, bottom)
    p = lax.div(x, 2)
    turn = 64 * (1 - lax.rem(x, 2))
    if sp.o == 8:
        low = roll(roll(yl[p], 8 - h - a * h, 0)[0:8], turn, 1) * below
        high = roll(roll(yh[p], -a * h, 0)[0:8], turn, 1) * above
        lower = jnp.concatenate([low, m], axis=0)
        higher = jnp.concatenate([m, high], axis=0)
        dst[xw] = jnp.where(upper(sp, sp.R), higher, lower)
    else:
        spare[0, 0:h, :] = roll(yl[p, a * h : (a + 1) * h, :], turn, 1) * below
        spare[0, h:, :] = m
        spare[1, 0:half, :] = m
        spare[1, half:, :] = roll(yh[p, a * h : (a + 1) * h, :], turn, 1) * above
        dst[xw] = jnp.where(upper(sp, sp.R), spare[1], spare[0])


def lane_z(sp, l):
    return jnp.where(l < sp.cut, l, jnp.where(l < sp.cut + 64, l - 64, l - 128))


def inside(sp, ids):
    _, gy, gz, ny, nz = ids
    n, h = sp.n, sp.h
    y = lax.broadcasted_iota(jnp.int32, (sp.R, 128), 0) - sp.o + jnp.where(upper(sp, sp.R), sp.R, 0)
    z = lane_z(sp, lanes(sp.R))
    ok = (y >= -h) & (y < n + h) & (z >= -h) & (z < n + h)
    y, z = y + gy * n, z + gz * n
    return ok & (y >= 0) & (y < ny * n) & (z >= 0) & (z < nz * n)


def paired(ref, x):
    c = ref[x + 1]
    R = c.shape[0]
    s = ref[x] + ref[x + 2]
    sub = lax.broadcasted_iota(jnp.int32, (8, 128), 0)
    seam = roll(jnp.where(sub == 0, c[0:8], c[R - 8 : R]), 64, 1)
    up, down = roll(c, R - 1, 0), roll(c, 1, 0)
    up = jnp.concatenate([up[: R - 8], jnp.where(sub == 7, roll(seam, 7, 0), up[R - 8 :])], axis=0)
    down = jnp.concatenate([jnp.where(sub == 0, roll(seam, 1, 0), down[0:8]), down[8:]], axis=0)
    s = s + (up + down)
    return s + (roll(c, 1, 1) + roll(c, 127, 1))


def domain(sp, n, h, r0, R, ids):
    row = lax.broadcasted_iota(jnp.int32, (R, 128), 0) - r0
    ln = lanes(R)
    z = jnp.where(ln < 64, ln, ln - 128)
    gy, gz, ny, nz = ids[1], ids[2], ids[3], ids[4]
    y_at, z_at = row + gy * n, z + gz * n
    ok = (row >= -h) & (row < n + h) & (z >= -h) & (z < n + h)
    return ok & (y_at >= 0) & (y_at < ny * n) & (z_at >= 0) & (z_at < nz * n)


def neighbours(ref, x):
    c = ref[x + 1]
    R = c.shape[0]
    s = ref[x] + ref[x + 2]
    s = s + (roll(c, 1, 0) + roll(c, R - 1, 0))
    return s + (roll(c, 1, 1) + roll(c, 127, 1))


def zero_ends(ref, n):
    ref[0] = jnp.zeros(ref.shape[1:], F32)
    ref[n + 1] = jnp.zeros(ref.shape[1:], F32)


def relax(src, dst, f, c, n, factor, u=9, near=None):
    near = near or neighbours

    def one(x):
        dst[x + 1] = (1.0 - W) * src[x + 1] + c[x] * (f[x] + factor * near(src, x))

    loop(n, one, u)


def lane_map(pick, value):
    l = lax.broadcasted_iota(jnp.int32, (256, 128), 0) & 127
    m = lax.broadcasted_iota(jnp.int32, (256, 128), 1)
    return jnp.where(pick(l) == m, value, 0.0).astype(jnp.bfloat16)


def spread_map(pick):
    m = lax.broadcasted_iota(jnp.int32, (256, 128), 0) & 127
    l = lax.broadcasted_iota(jnp.int32, (256, 128), 1)
    return jnp.where(pick(l) == m, 1.0, 0.0).astype(jnp.bfloat16)


def floor_half(z):
    return lax.shift_right_arithmetic(z, 1)


def coarse_lane(sp, l, want):
    z = lane_z(sp, l)
    up = (l >= sp.cut) & (l < sp.cut + 64)
    good = (z >= -sp.h) & (z < sp.n + sp.h)
    good = good & (up if want else jnp.logical_not(up))
    return jnp.where(good, floor_half(z) + jnp.where(z < 0, 128, 0), -1)


def both_lanes(l):
    lower, higher = coarse_lane(L0, l, False), coarse_lane(L0, l, True)
    return jnp.where(lower >= 0, lower, jnp.where(higher >= 0, (higher + 64) & 127, -1))


OWN, DOWN1A, DOWN1B, DOWN2, DOWN3, UP3, UP2, UP1A, UP1B, UP0 = range(10)


def all_maps(maps, gz):
    half = floor_half
    maps[OWN] = lane_map(lambda l: jnp.where(l < 64, half(l), 32 + half(l)), 0.125)
    maps[DOWN1A] = lane_map(lambda l: coarse_lane(L1, l, False), 0.125)
    maps[DOWN1B] = lane_map(lambda l: coarse_lane(L1, l, True), 0.125)
    maps[DOWN2] = lane_map(lambda l: jnp.where(l < 64, half(l), half(l) + 64), 0.125)
    maps[DOWN3] = lane_map(half, 0.125)
    maps[UP3] = spread_map(half)
    maps[UP2] = spread_map(lambda l: gz * 6 + jnp.where(l < 64, half(l), half(l) - 64))
    maps[UP1A] = spread_map(lambda l: coarse_lane(L1, l, False))
    maps[UP1B] = spread_map(lambda l: coarse_lane(L1, l, True))
    maps[UP0] = spread_map(both_lanes)


def times(v, m):
    big = v.astype(jnp.bfloat16)
    rest = (v - big.astype(F32)).astype(jnp.bfloat16)
    return jnp.dot(jnp.concatenate([big, rest], axis=1), m, preferred_element_type=F32)


def coarsen_planes(pair, n, tmp, acc, rows, u=2):
    half = rows // 2

    def one(x):
        tmp[x, 0:rows, :] = pair(x)
        acc[x, 0:half, :] = tmp[x, pl.ds(0, half, stride=2), :] + tmp[x, pl.ds(1, half, stride=2), :]

    loop(n, one, u)


def flat(ref):
    n, rows, _ = ref.shape
    return ref[...].reshape(n * rows, 128)


def add_refined(wide, n, src, dst, u=3):
    R = dst.shape[1]

    def one(i):
        v = wide[i, 0 : R // 2, :]
        for k in range(2):
            dst[2 * i + 1, pl.ds(k, R // 2, stride=2), :] = v
        t = dst[2 * i + 1]
        dst[2 * i + 1] = src[2 * i + 1] + t
        dst[2 * i + 2] = src[2 * i + 2] + t

    loop(n, one, u)


def k_zpack0(x0, b, rea, hi, lo, own, raw, sems):
    def copy(a, ref, i):
        part = pl.ds(i * 8, 8)
        return pltpu.make_async_copy(ref.at[part], raw.at[a, part], sems.at[a, i])

    refs = (x0, b, rea)
    for i in range(6):
        for a, ref in enumerate(refs):
            copy(a, ref, i).start()

    def some(i):
        for a, ref in enumerate(refs):
            copy(a, ref, i).wait()
        for k in range(8):
            x = i * 8 + k
            for a in range(3):
                own[a, x, :, 0:48] = raw[a, x, 0:24, :]
                own[a, x, :, 64:112] = raw[a, x, 24:48, :]
        for k in range(2):
            ztile(L0, lambda x, a: own[a, x], hi, lo, i * 2 + k)

    loop(6, some)


def k_ypack0(own, zl, zh, r1, up, dn):
    ypack(L0, lambda x, a: own[a, x], zl, zh, up, dn)


def xpack(sp, own, zl, zh, yl, yh, out, spare):
    ids = place()
    ends = edge(sp, ids)
    start = (1 - ids[0]) * (sp.n - sp.hx)

    def one(i):
        for a in range(sp.na):
            plane(sp, own, zl, zh, yl, yh, start + i, a, out.at[i], a, ends, None if spare is None else spare.at[a])

    loop(sp.hx, one, 2)


def k_xpack0(own, zl, zh, yl, yh, out):
    xpack(L0, lambda x, a: own[a, x], zl, zh, yl, yh, out, None)


def windows(sp, own, zl, zh, yl, yh, out, spare, u):
    ends = edge(sp, place())

    def some(i):
        for k in range(u):
            x = i * u + k
            for a in range(sp.na):
                plane(sp, own, zl, zh, yl, yh, x, a, out.at[a], x, ends, None if spare is None else spare.at[k * sp.na + a])

    loop(sp.n // u, some)


def own_rows(sp, v):
    return jnp.where(upper(sp, sp.half), v[0 : sp.half], v[sp.o :])


def half_own(pair, tmp, acc, out, u, m):
    coarsen_planes(pair, 24, tmp, acc, 24, u)
    acc[...] = times(flat(acc), m).reshape(24, 16, 128)

    def keep(x):
        out[x] = acc[x, 0:12, :]

    loop(24, keep, 6)


def k_early(own, r1, maps, tmp, acc):
    all_maps(maps, lax.axis_index("gz"))
    mine = lanes(24) % 64 < 48
    half_own(lambda x: jnp.where(mine, own[2, 2 * x] + own[2, 2 * x + 1], 0.0), tmp, acc, r1, 4, maps[OWN])


def k_windows0(own, zl, zh, yl, yh, out):
    windows(L0, lambda x, a: own[a, x], zl, zh, yl, yh, out, None, UA)


def k_down0(win, r1, maps, xr, f_out, c_out, d_out, e_out, f1, z1h, z1l, xw, ew, tmp, acc):
    ids = place()
    n = L0.nx
    shift = ids[0] * L0.hx
    other = (1 - ids[0]) * L0.n
    ok = inside(L0, ids)
    zero_ends(xw, n)
    zero_ends(ew, n)
    zero_ends(e_out, n)

    def put(x):
        xw[x + shift + 1] = win[0, x]

    def take(x):
        xw[x + other + 1] = xr[x, 0]

    loop(48, put, 12)
    loop(6, take, 6)

    def first(w, b, rea):
        d = 6.0 + rea
        c = jnp.where(ok, W / d, 0.0)
        f = b - d * xw[w + 1] + paired(xw, w)
        d_out[w] = d
        f_out[w] = f
        c_out[w] = c
        ew[w + 1] = c * f

    loop(48, lambda x: first(x + shift, win[1, x], win[2, x]), UF)
    loop(6, lambda x: first(x + other, xr[x, 1], xr[x, 2]), 6)
    relax(ew, e_out, f_out, c_out, n, 1.0, UR, paired)

    def left(x):
        return own_rows(L0, f_out[x] - d_out[x] * e_out[x + 1] + paired(e_out, x))

    mine = lanes(24) % 64 < 48
    pair = lambda x: jnp.where(mine, left(2 * x + shift) + left(2 * x + shift + 1), 0.0)
    half_own(pair, tmp, acc, f1, UL, maps[OWN])
    both = (f1, r1)
    loop(6, lambda g: ztile(L1, lambda x, a: both[a][x], z1h, z1l, g), 3)


def k_ypack1(f1, r1, zl, zh, up, dn):
    both = (f1, r1)
    ypack(L1, lambda x, a: both[a][x], zl, zh, up, dn)


def k_xpack1(f1, r1, zl, zh, yl, yh, out, spare):
    both = (f1, r1)
    xpack(L1, lambda x, a: both[a][x], zl, zh, yl, yh, out, spare)


def k_windows1(f1, r1, zl, zh, yl, yh, out, spare):
    both = (f1, r1)
    windows(L1, lambda x, a: both[a][x], zl, zh, yl, yh, out, spare, 4)


def k_down1(win, maps, xr, fw, cw, e_out, f2, c2, e2, out3, rw, ew, tmp, acc, r2, ew2, tmp2, t3, sq):
    ids = place()
    n = L1.nx
    shift = ids[0] * L1.hx
    other = (1 - ids[0]) * L1.n

    def put(x):
        fw[x + shift] = win[0, x]
        rw[x + shift] = win[1, x]

    def take(x):
        fw[x + other] = xr[x, 0]
        rw[x + other] = xr[x, 1]

    loop(24, put, 8)
    loop(12, take, 6)
    ok = inside(L1, ids)
    zero_ends(ew, n)
    zero_ends(e_out, n)

    def first(x):
        c = jnp.where(ok, W / (1.5 + rw[x]), 0.0)
        cw[x] = c
        ew[x + 1] = c * fw[x]

    loop(n, first, 6)
    relax(ew, e_out, fw, cw, n, 0.25, UM, paired)

    def left(x):
        return fw[x] - (1.5 + rw[x]) * e_out[x + 1] + 0.25 * paired(e_out, x)

    for ref, pair in ((f2, lambda x: left(2 * x) + left(2 * x + 1)), (r2, lambda x: rw[2 * x] + rw[2 * x + 1])):
        coarsen_planes(pair, 18, tmp, acc.at[0], 24, 9)
        v = flat(acc.at[0])
        acc[0] = times(v, maps[DOWN1A]).reshape(18, 16, 128)
        acc[1] = times(v, maps[DOWN1B]).reshape(18, 16, 128)

        def keep(x, ref=ref):
            ref[x] = jnp.zeros((32, 128), F32)
            ref[x, 2:14, :] = acc[0, x, 0:12, :]
            ref[x, 14:26, :] = acc[1, x, 0:12, :]

        loop(18, keep, 6)
    ok2 = domain(None, 12, 6, 8, 32, ids)
    zero_ends(ew2, 18)
    zero_ends(e2, 18)

    def second(x):
        c = jnp.where(ok2, W / (0.375 + r2[x]), 0.0)
        c2[x] = c
        ew2[x + 1] = c * f2[x]

    loop(18, second, 6)
    relax(ew2, e2, f2, c2, 18, 0.0625, 18)

    def left2(x):
        return f2[x] - (0.375 + r2[x]) * e2[x + 1] + 0.0625 * neighbours(e2, x)

    for a, pair in enumerate((lambda x: left2(2 * x) + left2(2 * x + 1), lambda x: r2[2 * x] + r2[2 * x + 1])):
        coarsen_planes(pair, 9, tmp2, t3.at[a], 32, 9)
        t3[a] = times(flat(t3.at[a]), maps[DOWN2]).reshape(9, 16, 128)
    shift = ids[0] * 3
    sq[...] = jnp.zeros((128, 128), F32)
    for a in range(2):
        for x in range(6):
            at = a * 36 + x * 6
            sq[at : at + 6, :] = t3[a, x + shift, 4:10, :]
    t = sq[...].T[0:8]
    ln = lanes(1)
    rows = []
    for u in range(2):
        for a in range(2):
            parts = [roll(t, 36 * (w - a), 1)[3 * u + w : 3 * u + w + 1] for w in range(3)]
            rows.append(jnp.where(ln < 36, parts[0], jnp.where(ln < 72, parts[1], parts[2])))
    tile = jnp.concatenate(rows + rows, axis=0)
    n8 = out3.shape[0] // 8
    out3[...] = jnp.broadcast_to(tile[None], (n8, 8, 128)).reshape(n8 * 8, 128)


def sum_all(v):
    s = jnp.sum(v, axis=0)
    return jnp.sum(jnp.sum(s, axis=1, keepdims=True), axis=0, keepdims=True)


def coarse_solve(g3, maps, nx, ny, nz, e3, s3, f3, c3, r3, tmp, f4, r4, sq):
    R = f3.shape[1]
    for ref in (f3, r3):
        ref[...] = jnp.zeros(ref.shape, F32)
    kx, ky, kz = nx // 6, ny // 6, nz // 6
    for bx in range(kx):
        for by in range(ky):
            k = bx * ky + by
            if kz * 6 < 128:
                sq[k, kz * 6 :, :] = jnp.zeros((128 - kz * 6, 128), F32)
            got = [g3[pl.ds(k * kz * 4 + r, kz, stride=4), :] for r in range(4)]
            ln = lanes(kz)
            for u in range(2):
                for w in range(3):
                    f, r = roll(got[2 * u], -36 * w, 1), roll(got[2 * u + 1], 36 - 36 * w, 1)
                    sq[k, pl.ds(3 * u + w, kz, stride=6), :] = jnp.where(ln < 36, f, r)
            t = sq[k].T
            for x in range(6):
                f3[bx * 6 + x, by * 6 : by * 6 + 6, :] = t[x * 6 : x * 6 + 6]
                r3[bx * 6 + x, by * 6 : by * 6 + 6, :] = t[36 + x * 6 : 42 + x * 6]
    factor = 0.25**3
    ok = (lax.broadcasted_iota(jnp.int32, (R, 128), 0) < ny) & (lanes(R) < nz)
    for ref in (e3, s3):
        zero_ends(ref, nx)

    def first(x):
        c = jnp.where(ok, W / (6.0 * factor + r3[x]), 0.0)
        c3[x] = c
        s3[x + 1] = c * f3[x]

    loop(nx, first, 6)
    relax(s3, e3, f3, c3, nx, factor, 12)

    def left(x):
        v = f3[x] - (6.0 * factor + r3[x]) * e3[x + 1] + factor * neighbours(e3, x)
        return jnp.where(ok, v, 0.0)

    for ref, pair in ((f4, lambda x: left(2 * x) + left(2 * x + 1)), (r4, lambda x: r3[2 * x] + r3[2 * x + 1])):
        coarsen_planes(pair, nx // 2, tmp, ref, R, 6)
        ref[...] = times(flat(ref), maps[DOWN3]).reshape(ref.shape)
    f4k = 0.25**4
    H = R // 2
    row = lax.broadcasted_iota(jnp.int32, (nx // 2, H, 128), 1)
    lane = lax.broadcasted_iota(jnp.int32, (nx // 2, H, 128), 2)
    within = (row < ny // 2) & (lane < nz // 2)
    diag = 6.0 * f4k + r4[...]
    zero = jnp.zeros((1, H, 128), F32)

    def apply(p):
        s = jnp.concatenate([zero, p[:-1]], axis=0) + jnp.concatenate([p[1:], zero], axis=0)
        s = s + roll(p, 1, 1) + roll(p, H - 1, 1) + roll(p, 1, 2) + roll(p, 127, 2)
        return jnp.where(within, diag * p - f4k * s, 0.0)

    r = jnp.where(within, f4[...], 0.0)
    p = r
    q = apply(r)
    rr = sum_all(r * r)
    a = rr / sum_all(r * q)
    e = a * p
    for i in range(1, BOTTOM_ITERS):
        r = r - a * q
        w = apply(r)
        new = sum_all(r * r)
        rw = sum_all(r * w)
        b = new / rr
        a = new / (rw - b * new / a)
        p = r + b * p
        q = w + b * q
        e = e + a * p
        rr = new
    f4[...] = times(e.reshape(nx // 2 * H, 128), maps[UP3]).reshape(e.shape)
    add_refined(f4, nx // 2, e3, s3, 6)
    relax(s3, e3, f3, c3, nx, factor, 12)
    relax(e3, s3, f3, c3, nx, factor, 12)


def k_up(g3, maps, f2, c2, e2i, f1, c1, e1i, f0, c0, d0, e0i, z_out, az_out, sums,
         e3, s3, f3, c3, r3, tmp3, f4, r4, sq, w3, w2, na, nb, n1, e2, s2, e1, s1, e0, s0):
    gx, gy, gz, sy, sz = place()
    nx, ny, nz = f3.shape[0], sy * 6, sz * 6
    coarse_solve(g3, maps, nx, ny, nz, e3, s3, f3, c3, r3, tmp3, f4, r4, sq)
    for ref, n in ((s2, 18), (s1, 36), (s0, 54), (e2, 18), (e1, 36), (e0, 54)):
        zero_ends(ref, n)
    R3 = s3.shape[1]
    pick = lax.broadcasted_iota(jnp.int32, (16, R3), 1) == lax.broadcasted_iota(jnp.int32, (16, R3), 0) + (gy * 6 - 4)
    pick = pick.astype(F32)
    for i in range(9):
        w3[i] = jnp.dot(pick, s3[i + 1 + gx * 3], precision=HI, preferred_element_type=F32)
    w3[...] = times(flat(w3), maps[UP2]).reshape(9, 16, 128)
    add_refined(w3, 9, e2i, e2, 9)
    relax(e2, s2, f2, c2, 18, 0.0625, 18)
    relax(s2, e2, f2, c2, 18, 0.0625, 18)

    def halves(i):
        na[i] = e2[i + 1, 2:18, :]
        nb[i] = e2[i + 1, 14:30, :]

    loop(18, halves, 6)

    w2[...] = (times(flat(na), maps[UP1A]) + times(flat(nb), maps[UP1B])).reshape(18, 16, 128)
    add_refined(w2, 18, e1i, e1, 6)
    relax(e1, s1, f1, c1, 36, 0.25, UM, paired)
    relax(s1, e1, f1, c1, 36, 0.25, UM, paired)

    def near(i):
        v = e1[i + 1 + gx * 9]
        n1[i] = jnp.where(upper(L1, 16), v[0:16], v[8:24])

    loop(27, near, 9)

    n1[...] = times(flat(n1), maps[UP0]).reshape(27, 16, 128)
    add_refined(n1, 27, e0i, e0, 9)
    relax(e0, s0, f0, c0, 54, 1.0, UR, paired)
    relax(s0, e0, f0, c0, 54, 1.0, UR, paired)
    shift = gx * 6
    mine = lanes(24) % 64 < 48

    def last(x, carry):
        u, v = carry
        w = x + shift
        z = e0[w + 1]
        az = own_rows(L0, d0[w] * z - paired(e0, w))
        z = own_rows(L0, z)
        f = own_rows(L0, f0[w])
        z_out[x] = z
        az_out[x] = az
        return u + jnp.where(mine, f * z, 0.0), v + jnp.where(mine, z * az, 0.0)

    def some(i, carry):
        for k in range(UZ):
            carry = last(UZ * i + k, carry)
        return carry

    zero = jnp.zeros((24, 128), F32)
    u, v = lax.fori_loop(0, 48 // UZ, some, (zero, zero))

    def total(t):
        return jnp.sum(jnp.sum(t, axis=1, keepdims=True), axis=0, keepdims=True)

    ln = lanes(sums.shape[0])
    sums[...] = jnp.where(ln == 0, total(u), jnp.where(ln == 1, total(v), 0.0))


def k_last(sums, own, z, az, f, sol, res, sv, rv, sems):
    s = jnp.sum(sums[...], axis=0, keepdims=True)
    ln = lanes(1)
    over = jnp.sum(jnp.where(ln == 0, s, 0.0), axis=1, keepdims=True)
    under = jnp.sum(jnp.where(ln == 1, s, 0.0), axis=1, keepdims=True)
    step = over / under
    shift = lax.axis_index("gx") * 6
    pairs = ((0, sv, sol), (1, rv, res))

    def copy(a, src, dst, i):
        part = pl.ds(i * 8, 8)
        return pltpu.make_async_copy(src.at[part], dst.at[part], sems.at[a, i])

    def some(i):
        for k in range(8):
            x = i * 8 + k
            for ref, v in ((sv, own[0, x] + step * z[x]), (rv, own_rows(L0, f[x + shift]) - step * az[x])):
                ref[x, 0:24, :] = v[:, 0:48]
                ref[x, 24:48, :] = roll(v, 64, 1)[:, 0:48]
        for a, src, dst in pairs:
            copy(a, src, dst, i).start()

    loop(6, some)
    for i in range(6):
        for a, src, dst in pairs:
            copy(a, src, dst, i).wait()


def ring(up, dn, axis):
    n = lax.axis_size(axis)
    low = lax.ppermute(up, axis, [(i, (i + 1) % n) for i in range(n)])
    high = lax.ppermute(dn, axis, [(i, (i - 1) % n) for i in range(n)])
    return low, high


def swap(v):
    return lax.ppermute(v, "gx", [(0, 1), (1, 0)])


def body(b, x0, rea):
    ALL = ("gx", "gy", "gz")
    sizes = [lax.axis_size(a) for a in ALL]
    count = sizes[0] * sizes[1] * sizes[2]
    b, x0, rea = (pltpu.with_memory_space_constraint(v, pltpu.HBM) for v in (b, x0, rea))
    hi, lo, own = run(
        k_zpack0,
        (sds(*L0.zshape), sds(*L0.zshape), sds(3, 48, 24, 128)),
        (x0, b, rea),
        [(3, 48, 48, 48), pltpu.SemaphoreType.DMA((3, 6))],
        far_in=True,
    )
    zl, zh = ring(hi, lo, "gz")
    r1, maps = run(
        k_early, (sds(24, 12, 128), sds(10, 256, 128, dtype=jnp.bfloat16)), (own,), [(24, 24, 128), (24, 16, 128)]
    )
    up, dn = run(k_ypack0, (sds(*L0.yshape),) * 2, (own, zl, zh, r1))
    yl, yh = ring(up, dn, "gy")
    xr = swap(run(k_xpack0, sds(*L0.xshape), (own, zl, zh, yl, yh)))
    win = run(k_windows0, sds(3, 48, 32, 128), (own, zl, zh, yl, yh))
    p0, q0 = (54, 32, 128), (56, 32, 128)
    f0, c0, d0, e0, f1, z1h, z1l = run(
        k_down0,
        (sds(*p0), sds(*p0), sds(*p0), sds(*q0), sds(24, 12, 128), sds(*L1.zshape), sds(*L1.zshape)),
        (win, r1, maps, xr),
        [q0, q0, (24, 24, 128), (24, 16, 128)],
        mib=M0,
    )
    zl, zh = ring(z1h, z1l, "gz")
    up, dn = run(k_ypack1, (sds(*L1.yshape),) * 2, (f1, r1, zl, zh))
    yl, yh = ring(up, dn, "gy")
    xr = swap(run(k_xpack1, sds(*L1.xshape), (f1, r1, zl, zh, yl, yh), [(2, 2, 24, 128)]))
    p1, q1, p2, q2 = (36, 24, 128), (38, 24, 128), (18, 32, 128), (20, 32, 128)
    win = run(k_windows1, sds(2, 24, 24, 128), (f1, r1, zl, zh, yl, yh), [(8, 2, 24, 128)])
    f1w, c1w, e1w, f2w, c2w, e2w, g = run(
        k_down1,
        (sds(*p1), sds(*p1), sds(*q1), sds(*p2), sds(*p2), sds(*q2), sds(count * 4, 128)),
        (win, maps, xr),
        [p1, q1, (18, 24, 128), (2, 18, 16, 128), p2, q2, (9, 32, 128), (2, 9, 16, 128), (128, 128)],
        mib=M1,
    )
    g = lax.all_to_all(g, ALL, 0, 0, tiled=True)
    n3 = [6 * s for s in sizes]
    R3 = (n3[1] + 8) // 8 * 8
    if R3 % 16:
        R3 += 8
    p3, q3, p4 = (n3[0], R3, 128), (n3[0] + 2, R3, 128), (n3[0] // 2, R3 // 2, 128)
    z, az, sums = run(
        k_up,
        (sds(48, 24, 128), sds(48, 24, 128), sds(count, 128)),
        (g, maps, f2w, c2w, e2w, f1w, c1w, e1w, f0, c0, d0, e0),
        [q3, q3, p3, p3, p3, (n3[0] // 2, R3, 128), p4, p4, (sizes[0] * sizes[1], 128, 128), (9, 16, 128), (18, 16, 128),
         (18, 16, 128), (18, 16, 128), (27, 16, 128), q2, q2, q1, q1, q0, q0],
        mib=M2,
    )
    sums = lax.all_to_all(sums.reshape(count, 1, 128), ALL, 0, 0, tiled=True).reshape(count, 128)
    return run(
        k_last,
        (sds(48, 48, 48), sds(48, 48, 48)),
        (sums, own, z, az, f0),
        [(48, 48, 48), (48, 48, 48), pltpu.SemaphoreType.DMA((2, 6))],
        far_out=True,
    )


def solution(mesh):
    spec = P("gx", "gy", "gz")
    return jax.shard_map(body, mesh=mesh, in_specs=(spec, spec, spec), out_specs=(spec, spec), check_vma=False)
```

```python
import functools
import jax
import jax.numpy as jnp
from jax import lax
from jax.experimental import pallas as pl
from jax.experimental.pallas import tpu as pltpu
from jax.sharding import PartitionSpec as P

W = 6.0 / 7.0
BOTTOM_ITERS = 6
N0 = 48
F32 = jnp.float32
HI = lax.Precision.HIGHEST
M0, M1, M2 = 10, 8, 12
UF, UR, UM, UZ, UL = 12, 27, 18, 12, 6


class Spec:
    def __init__(self, n, h, na, R, o, hx, cut, kp, st):
        self.n, self.h, self.na, self.R, self.o, self.hx, self.cut, self.kp, self.st = n, h, na, R, o, hx, cut, kp, st
        self.half = n // 2
        self.zshape = (n // (kp * st), self.half * st, 128)
        self.yshape = (self.half, na * h, 128)
        self.hs = (h,) * na
        self.xshape = (hx, na, R, 128)
        self.nx = n + hx

    def slot(self, x, a):
        if self.st == 1:
            h = self.hs[a]
            many = 64 // h
            return ZBASE[a] + lax.div(x, many), 0, h * lax.rem(x, many)
        per = self.n // self.st
        t, y = lax.div(x, per), lax.rem(x, per)
        return lax.div(y, self.kp), t, self.h * (lax.rem(y, self.kp) * self.na + a)


L0 = Spec(48, 5, 3, 32, 8, 6, 56, 4, 1)
L1 = Spec(24, 12, 2, 24, 12, 12, 44, 2, 2)
L0.hs = (5, 4, 4)
ZBASE = (0, 4, 7)
YBASE = (0, 40, 72)
L0.zshape = (10, 24, 128)
L0.yshape = (3, 104, 128)


def sds(*shape, dtype=F32):
    return jax.ShapeDtypeStruct(shape, dtype)


def run(kernel, outs, args, scratch=(), mib=12, far_in=False, far_out=False):
    vmem = pl.BlockSpec(memory_space=pltpu.VMEM)
    hbm = pl.BlockSpec(memory_space=pl.ANY)
    return pl.pallas_call(
        kernel,
        out_shape=outs,
        in_specs=[hbm if far_in else vmem] * len(args),
        out_specs=jax.tree.map(lambda _: hbm if far_out else vmem, outs),
        scratch_shapes=[pltpu.VMEM(s, F32) if isinstance(s, tuple) else s for s in scratch],
        compiler_params=pltpu.CompilerParams(vmem_limit_bytes=mib * 1024 * 1024),
    )(*args)


def place():
    return [lax.axis_index(a) for a in ("gx", "gy", "gz")] + [lax.axis_size(a) for a in ("gy", "gz")]


def lanes(rows):
    return lax.broadcasted_iota(jnp.int32, (rows, 128), 1)


def roll(v, shift, axis):
    if isinstance(shift, int):
        shift = shift % v.shape[axis]
        if shift == 0:
            return v
    return pltpu.roll(v, shift, axis)


def loop(n, f, u=1):
    u = max(d for d in range(1, u + 1) if n % d == 0)

    def some(i, c):
        for k in range(u):
            f(i * u + k)
        return c

    lax.fori_loop(0, n // u, some, 0)


def upper(sp, rows):
    l = lanes(rows)
    return (l >= sp.cut) & (l < sp.cut + 64)


def edge(sp, ids):
    _, gy, gz, ny, nz = ids
    high = jnp.where(gz < nz - 1, sp.n + sp.h, sp.n)
    low = jnp.where(gz > 0, 64 - sp.h, 64)
    return high, low, jnp.where(gy > 0, 1.0, 0.0), jnp.where(gy < ny - 1, 1.0, 0.0)


def zslot(sp, v, at, h, hi, lo):
    l = lanes(sp.half)
    hi = jnp.where((l - (at - sp.n - h)) % 64 < h, roll(v, at - 2 * sp.n, 1), hi)
    lo = jnp.where((l - at) % 64 < h, roll(v, at, 1), lo)
    return hi, lo


def ztile1(own, hi_ref, lo_ref, g):
    sp = L1
    for t in range(sp.st):
        hi = lo = jnp.zeros((sp.half, 128), F32)
        for k in range(sp.kp):
            for a in range(sp.na):
                v = own(t * (sp.n // sp.st) + g * sp.kp + k, a)
                hi, lo = zslot(sp, v, sp.h * (k * sp.na + a), sp.h, hi, lo)
        hi_ref[g, t * sp.half : (t + 1) * sp.half, :] = hi
        lo_ref[g, t * sp.half : (t + 1) * sp.half, :] = lo


def merged(sp, own, zl, zh, x, a, b, e, top, bottom):
    g, t, at = sp.slot(x, a)
    if sp.st == 1:
        high, low = zh[g, b:e, :], zl[g, b:e, :]
    else:
        high = jnp.where(t == 0, zh[g, b:e, :], zh[g, sp.half + b : sp.half + e, :])
        low = jnp.where(t == 0, zl[g, b:e, :], zl[g, sp.half + b : sp.half + e, :])
    l = lanes(e - b)
    beside = jnp.where(((l + (64 - at)) & 63) < sp.hs[a], high, low)
    beside = roll(beside, (sp.n + 128 - at) & 127, 1)
    q = l & 63
    return jnp.where(q < sp.n, own(x, a)[b:e], jnp.where((q < top) | (q >= bottom), beside, 0.0))


def ypack(sp, own, zl, zh, up_ref, dn_ref, u):
    half = sp.half
    top, bottom, _, _ = edge(sp, place())

    def some(i):
        for k in range(u):
            p = i * u + k
            for a in range(sp.na):
                h = sp.hs[a]
                up0 = (half - h) // 8 * 8
                dn1 = min(half, -(-h // 8) * 8)
                for ref, b, e, s, t, swap in ((up_ref, up0, half, half - h - up0, half - up0, False), (dn_ref, 0, dn1, 0, h, True)):
                    even = merged(sp, own, zl, zh, 2 * p, a, b, e, top, bottom)
                    odd = roll(merged(sp, own, zl, zh, 2 * p + 1, a, b, e, top, bottom), 64, 1)
                    first, second = (odd, even) if swap else (even, odd)
                    v = jnp.where(upper(sp, e - b), first, second)[s:t]
                    if sp is L0:
                        ref[i, pl.ds(YBASE[a] + k, h, stride=8), :] = v
                    else:
                        ref[p, a * h : (a + 1) * h, :] = v

    loop(half // u, some)


def y_tiles0(yl, yh, g, t, a):
    def rows(ref, start):
        return ref[g, pl.ds(start + t, 8, stride=8), :]

    if a == 0:
        return roll(rows(yl, 0), 3, 0), rows(yh, 0)
    return rows(yl, YBASE[a] - 32), rows(yh, 40) if a == 1 else roll(rows(yh, 40), 4, 0)


def plane0(own, zl, zh, tiles, x, a, dst, xw, ends, turn):
    top, bottom, below, above = ends
    sp = L0
    m = merged(sp, own, zl, zh, x, a, 0, sp.half, top, bottom)
    low, high = tiles
    lower = jnp.concatenate([roll(low, turn, 1) * below, m], axis=0)
    higher = jnp.concatenate([m, roll(high, turn, 1) * above], axis=0)
    dst[xw] = jnp.where(upper(sp, sp.R), higher, lower)


def plane1(own, zl, zh, yl, yh, x, a, dst, xw, ends, spare):
    top, bottom, below, above = ends
    sp = L1
    h, half = sp.h, sp.half
    m = merged(sp, own, zl, zh, x, a, 0, half, top, bottom)
    p = lax.div(x, 2)
    turn = 64 * (1 - lax.rem(x, 2))
    spare[0, 0:h, :] = roll(yl[p, a * h : (a + 1) * h, :], turn, 1) * below
    spare[0, h:, :] = m
    spare[1, 0:half, :] = m
    spare[1, half:, :] = roll(yh[p, a * h : (a + 1) * h, :], turn, 1) * above
    dst[xw] = jnp.where(upper(sp, sp.R), spare[1], spare[0])


def lane_z(sp, l):
    return jnp.where(l < sp.cut, l, jnp.where(l < sp.cut + 64, l - 64, l - 128))


def inside(sp, ids):
    _, gy, gz, ny, nz = ids
    n, h = sp.n, min(sp.hs)
    y = lax.broadcasted_iota(jnp.int32, (sp.R, 128), 0) - sp.o + jnp.where(upper(sp, sp.R), sp.R, 0)
    z = lane_z(sp, lanes(sp.R))
    ok = (y >= -h) & (y < n + h) & (z >= -h) & (z < n + h)
    y, z = y + gy * n, z + gz * n
    return ok & (y >= 0) & (y < ny * n) & (z >= 0) & (z < nz * n)


def paired(ref, x):
    c = ref[x + 1]
    R = c.shape[0]
    s = ref[x] + ref[x + 2]
    sub = lax.broadcasted_iota(jnp.int32, (8, 128), 0)
    seam = roll(jnp.where(sub == 0, c[0:8], c[R - 8 : R]), 64, 1)
    up, down = roll(c, R - 1, 0), roll(c, 1, 0)
    up = jnp.concatenate([up[: R - 8], jnp.where(sub == 7, roll(seam, 7, 0), up[R - 8 :])], axis=0)
    down = jnp.concatenate([jnp.where(sub == 0, roll(seam, 1, 0), down[0:8]), down[8:]], axis=0)
    s = s + (up + down)
    return s + (roll(c, 1, 1) + roll(c, 127, 1))


def domain(sp, n, h, r0, R, ids):
    row = lax.broadcasted_iota(jnp.int32, (R, 128), 0) - r0
    ln = lanes(R)
    z = jnp.where(ln < 64, ln, ln - 128)
    gy, gz, ny, nz = ids[1], ids[2], ids[3], ids[4]
    y_at, z_at = row + gy * n, z + gz * n
    ok = (row >= -h) & (row < n + h) & (z >= -h) & (z < n + h)
    return ok & (y_at >= 0) & (y_at < ny * n) & (z_at >= 0) & (z_at < nz * n)


def neighbours(ref, x):
    c = ref[x + 1]
    R = c.shape[0]
    s = ref[x] + ref[x + 2]
    s = s + (roll(c, 1, 0) + roll(c, R - 1, 0))
    return s + (roll(c, 1, 1) + roll(c, 127, 1))


def zero_ends(ref, n):
    ref[0] = jnp.zeros(ref.shape[1:], F32)
    ref[n + 1] = jnp.zeros(ref.shape[1:], F32)


def relax(src, dst, f, c, n, factor, u=9, near=None):
    near = near or neighbours

    def one(x):
        dst[x + 1] = (1.0 - W) * src[x + 1] + c[x] * (f[x] + factor * near(src, x))

    loop(n, one, u)


def lane_map(pick, value):
    l = lax.broadcasted_iota(jnp.int32, (256, 128), 0) & 127
    m = lax.broadcasted_iota(jnp.int32, (256, 128), 1)
    return jnp.where(pick(l) == m, value, 0.0).astype(jnp.bfloat16)


def spread_map(pick):
    m = lax.broadcasted_iota(jnp.int32, (256, 128), 0) & 127
    l = lax.broadcasted_iota(jnp.int32, (256, 128), 1)
    return jnp.where(pick(l) == m, 1.0, 0.0).astype(jnp.bfloat16)


def floor_half(z):
    return lax.shift_right_arithmetic(z, 1)


def coarse_lane(sp, l, want):
    z = lane_z(sp, l)
    up = (l >= sp.cut) & (l < sp.cut + 64)
    good = (z >= -sp.h) & (z < sp.n + sp.h)
    good = good & (up if want else jnp.logical_not(up))
    return jnp.where(good, floor_half(z) + jnp.where(z < 0, 128, 0), -1)


def both_lanes(l):
    lower, higher = coarse_lane(L0, l, False), coarse_lane(L0, l, True)
    return jnp.where(lower >= 0, lower, jnp.where(higher >= 0, (higher + 64) & 127, -1))


OWN, DOWN1A, DOWN1B, DOWN2, DOWN3, UP3, UP2, UP1A, UP1B, UP0 = range(10)


def all_maps(maps, gz):
    half = floor_half
    maps[OWN] = lane_map(lambda l: jnp.where(l < 64, half(l), 32 + half(l)), 0.125)
    maps[DOWN1A] = lane_map(lambda l: coarse_lane(L1, l, False), 0.125)
    maps[DOWN1B] = lane_map(lambda l: coarse_lane(L1, l, True), 0.125)
    maps[DOWN2] = lane_map(lambda l: jnp.where(l < 64, half(l), half(l) + 64), 0.125)
    maps[DOWN3] = lane_map(half, 0.125)
    maps[UP3] = spread_map(half)
    maps[UP2] = spread_map(lambda l: gz * 6 + jnp.where(l < 64, half(l), half(l) - 64))
    maps[UP1A] = spread_map(lambda l: coarse_lane(L1, l, False))
    maps[UP1B] = spread_map(lambda l: coarse_lane(L1, l, True))
    maps[UP0] = spread_map(both_lanes)


def times(v, m):
    big = v.astype(jnp.bfloat16)
    rest = (v - big.astype(F32)).astype(jnp.bfloat16)
    return jnp.dot(jnp.concatenate([big, rest], axis=1), m, preferred_element_type=F32)


def coarsen_planes(pair, n, tmp, acc, rows, u=2):
    half = rows // 2

    def one(x):
        tmp[x, 0:rows, :] = pair(x)
        acc[x, 0:half, :] = tmp[x, pl.ds(0, half, stride=2), :] + tmp[x, pl.ds(1, half, stride=2), :]

    loop(n, one, u)


def flat(ref):
    n, rows, _ = ref.shape
    return ref[...].reshape(n * rows, 128)


def add_refined(wide, n, src, dst, u=3):
    R = dst.shape[1]

    def one(i):
        v = wide[i, 0 : R // 2, :]
        for k in range(2):
            dst[2 * i + 1, pl.ds(k, R // 2, stride=2), :] = v
        t = dst[2 * i + 1]
        dst[2 * i + 1] = src[2 * i + 1] + t
        dst[2 * i + 2] = src[2 * i + 2] + t

    loop(n, one, u)


def k_zpack0(x0, b, rea, hi, lo, own, raw, sems):
    def copy(a, ref, i):
        many = 64 // L0.hs[a]
        part = pl.ds(i * many, many)
        return pltpu.make_async_copy(ref.at[part], raw.at[a, part], sems.at[a, i])

    refs = (x0, b, rea)
    parts = [48 * h // (64 // h * h) for h in L0.hs]
    for a, ref in enumerate(refs):
        for i in range(parts[a]):
            copy(a, ref, i).start()

    for a, ref in enumerate(refs):
        h = L0.hs[a]
        many = 64 // h

        def some(i, a=a, ref=ref, h=h, many=many):
            copy(a, ref, i).wait()
            hi_tile = lo_tile = jnp.zeros((24, 128), F32)
            for k in range(many):
                x = i * many + k
                own[a, x, :, 0:48] = raw[a, x, 0:24, :]
                own[a, x, :, 64:112] = raw[a, x, 24:48, :]
            for k in range(many):
                hi_tile, lo_tile = zslot(L0, own[a, i * many + k], h * k, h, hi_tile, lo_tile)
            hi[ZBASE[a] + i] = hi_tile
            lo[ZBASE[a] + i] = lo_tile

        loop(parts[a], some)


def k_ypack0(own, zl, zh, r1, up, dn):
    ypack(L0, lambda x, a: own[a, x], zl, zh, up, dn, 8)


def k_xpack0(own, zl, zh, yl, yh, out):
    ids = place()
    ends = edge(L0, ids)
    first = ids[0] == 0
    for i in range(6):
        x = jnp.where(first, 42, 0) + i
        for a in range(3):
            there, here = y_tiles0(yl, yh, 2, 5 + i // 2, a), y_tiles0(yl, yh, 0, i // 2, a)
            tiles = [jnp.where(first, v, w) for v, w in zip(there, here)]
            plane0(lambda x, a: own[a, x], zl, zh, tiles, x, a, out.at[i], a, ends, 64 * (1 - i % 2))


def k_xpack1(f1, r1, zl, zh, yl, yh, out, spare):
    both = (f1, r1)
    ids = place()
    ends = edge(L1, ids)

    def one(i):
        for a in range(2):
            plane1(lambda x, a: both[a][x], zl, zh, yl, yh, (1 - ids[0]) * 12 + i, a, out.at[i], a, ends, spare.at[a])

    loop(12, one, 2)


def k_windows0(own, zl, zh, yl, yh, out):
    ends = edge(L0, place())

    def some(i):
        for k in range(16):
            for a in range(3):
                tiles = y_tiles0(yl, yh, i, k // 2, a)
                plane0(lambda x, a: own[a, x], zl, zh, tiles, 16 * i + k, a, out.at[a], 16 * i + k, ends, 64 * (1 - k % 2))

    loop(3, some)


def own_rows(sp, v):
    return jnp.where(upper(sp, sp.half), v[0 : sp.half], v[sp.o :])


def half_own(pair, tmp, acc, out, u, m):
    coarsen_planes(pair, 24, tmp, acc, 24, u)
    acc[...] = times(flat(acc), m).reshape(24, 16, 128)

    def keep(x):
        out[x] = acc[x, 0:12, :]

    loop(24, keep, 6)


def k_early(own, r1, maps, tmp, acc):
    all_maps(maps, lax.axis_index("gz"))
    mine = lanes(24) % 64 < 48
    half_own(lambda x: jnp.where(mine, own[2, 2 * x] + own[2, 2 * x + 1], 0.0), tmp, acc, r1, 4, maps[OWN])


def k_down0(win, r1, maps, xr, f_out, c_out, d_out, e_out, f1, z1h, z1l, xw, ew, tmp, acc):
    ids = place()
    n = L0.nx
    shift = ids[0] * L0.hx
    other = (1 - ids[0]) * L0.n
    ok = inside(L0, ids)
    zero_ends(xw, n)
    zero_ends(ew, n)
    zero_ends(e_out, n)

    def put(x):
        xw[x + shift + 1] = win[0, x]

    def take(x):
        xw[x + other + 1] = xr[x, 0]

    loop(48, put, 12)
    loop(6, take, 6)

    def first(w, b, rea):
        d = 6.0 + rea
        c = jnp.where(ok, W / d, 0.0)
        f = b - d * xw[w + 1] + paired(xw, w)
        d_out[w] = d
        f_out[w] = f
        c_out[w] = c
        ew[w + 1] = c * f

    loop(48, lambda x: first(x + shift, win[1, x], win[2, x]), UF)
    loop(6, lambda x: first(x + other, xr[x, 1], xr[x, 2]), 6)
    relax(ew, e_out, f_out, c_out, n, 1.0, UR, paired)

    def left(x):
        return own_rows(L0, f_out[x] - d_out[x] * e_out[x + 1] + paired(e_out, x))

    mine = lanes(24) % 64 < 48
    pair = lambda x: jnp.where(mine, left(2 * x + shift) + left(2 * x + shift + 1), 0.0)
    half_own(pair, tmp, acc, f1, UL, maps[OWN])
    both = (f1, r1)
    loop(6, lambda g: ztile1(lambda x, a: both[a][x], z1h, z1l, g), 3)


def k_ypack1(f1, r1, zl, zh, up, dn):
    both = (f1, r1)
    ypack(L1, lambda x, a: both[a][x], zl, zh, up, dn, 6)


def k_windows1(f1, r1, zl, zh, yl, yh, out, spare):
    both = (f1, r1)
    ends = edge(L1, place())

    def some(i):
        for k in range(4):
            for a in range(2):
                plane1(lambda x, a: both[a][x], zl, zh, yl, yh, 4 * i + k, a, out.at[a], 4 * i + k, ends, spare.at[2 * k + a])

    loop(6, some)


def k_down1(win, maps, xr, fw, cw, e_out, f2, c2, e2, out3, rw, ew, tmp, acc, r2, ew2, tmp2, t3, sq):
    ids = place()
    n = L1.nx
    shift = ids[0] * L1.hx
    other = (1 - ids[0]) * L1.n

    def put(x):
        fw[x + shift] = win[0, x]
        rw[x + shift] = win[1, x]

    def take(x):
        fw[x + other] = xr[x, 0]
        rw[x + other] = xr[x, 1]

    loop(24, put, 8)
    loop(12, take, 6)
    ok = inside(L1, ids)
    zero_ends(ew, n)
    zero_ends(e_out, n)

    def first(x):
        c = jnp.where(ok, W / (1.5 + rw[x]), 0.0)
        cw[x] = c
        ew[x + 1] = c * fw[x]

    loop(n, first, 6)
    relax(ew, e_out, fw, cw, n, 0.25, UM, paired)

    def left(x):
        return fw[x] - (1.5 + rw[x]) * e_out[x + 1] + 0.25 * paired(e_out, x)

    for ref, pair in ((f2, lambda x: left(2 * x) + left(2 * x + 1)), (r2, lambda x: rw[2 * x] + rw[2 * x + 1])):
        coarsen_planes(pair, 18, tmp, acc.at[0], 24, 9)
        v = flat(acc.at[0])
        acc[0] = times(v, maps[DOWN1A]).reshape(18, 16, 128)
        acc[1] = times(v, maps[DOWN1B]).reshape(18, 16, 128)

        def keep(x, ref=ref):
            ref[x] = jnp.zeros((32, 128), F32)
            ref[x, 2:14, :] = acc[0, x, 0:12, :]
            ref[x, 14:26, :] = acc[1, x, 0:12, :]

        loop(18, keep, 6)
    ok2 = domain(None, 12, 6, 8, 32, ids)
    zero_ends(ew2, 18)
    zero_ends(e2, 18)

    def second(x):
        c = jnp.where(ok2, W / (0.375 + r2[x]), 0.0)
        c2[x] = c
        ew2[x + 1] = c * f2[x]

    loop(18, second, 6)
    relax(ew2, e2, f2, c2, 18, 0.0625, 18)

    def left2(x):
        return f2[x] - (0.375 + r2[x]) * e2[x + 1] + 0.0625 * neighbours(e2, x)

    for a, pair in enumerate((lambda x: left2(2 * x) + left2(2 * x + 1), lambda x: r2[2 * x] + r2[2 * x + 1])):
        coarsen_planes(pair, 9, tmp2, t3.at[a], 32, 9)
        t3[a] = times(flat(t3.at[a]), maps[DOWN2]).reshape(9, 16, 128)
    shift = ids[0] * 3
    sq[...] = jnp.zeros((128, 128), F32)
    for a in range(2):
        for x in range(6):
            at = a * 36 + x * 6
            sq[at : at + 6, :] = t3[a, x + shift, 4:10, :]
    t = sq[...].T[0:8]
    ln = lanes(1)
    rows = []
    for u in range(2):
        for a in range(2):
            parts = [roll(t, 36 * (w - a), 1)[3 * u + w : 3 * u + w + 1] for w in range(3)]
            rows.append(jnp.where(ln < 36, parts[0], jnp.where(ln < 72, parts[1], parts[2])))
    tile = jnp.concatenate(rows + rows, axis=0)
    n8 = out3.shape[0] // 8
    out3[...] = jnp.broadcast_to(tile[None], (n8, 8, 128)).reshape(n8 * 8, 128)


def sum_all(v):
    s = jnp.sum(v, axis=0)
    return jnp.sum(jnp.sum(s, axis=1, keepdims=True), axis=0, keepdims=True)


def coarse_solve(g3, maps, nx, ny, nz, e3, s3, f3, c3, r3, tmp, f4, r4, sq):
    R = f3.shape[1]
    for ref in (f3, r3):
        ref[...] = jnp.zeros(ref.shape, F32)
    kx, ky, kz = nx // 6, ny // 6, nz // 6
    for bx in range(kx):
        for by in range(ky):
            k = bx * ky + by
            if kz * 6 < 128:
                sq[k, kz * 6 :, :] = jnp.zeros((128 - kz * 6, 128), F32)
            got = [g3[pl.ds(k * kz * 4 + r, kz, stride=4), :] for r in range(4)]
            ln = lanes(kz)
            for u in range(2):
                for w in range(3):
                    f, r = roll(got[2 * u], -36 * w, 1), roll(got[2 * u + 1], 36 - 36 * w, 1)
                    sq[k, pl.ds(3 * u + w, kz, stride=6), :] = jnp.where(ln < 36, f, r)
            t = sq[k].T
            for x in range(6):
                f3[bx * 6 + x, by * 6 : by * 6 + 6, :] = t[x * 6 : x * 6 + 6]
                r3[bx * 6 + x, by * 6 : by * 6 + 6, :] = t[36 + x * 6 : 42 + x * 6]
    factor = 0.25**3
    ok = (lax.broadcasted_iota(jnp.int32, (R, 128), 0) < ny) & (lanes(R) < nz)
    for ref in (e3, s3):
        zero_ends(ref, nx)

    def first(x):
        c = jnp.where(ok, W / (6.0 * factor + r3[x]), 0.0)
        c3[x] = c
        s3[x + 1] = c * f3[x]

    loop(nx, first, 6)
    relax(s3, e3, f3, c3, nx, factor, 12)

    def left(x):
        v = f3[x] - (6.0 * factor + r3[x]) * e3[x + 1] + factor * neighbours(e3, x)
        return jnp.where(ok, v, 0.0)

    for ref, pair in ((f4, lambda x: left(2 * x) + left(2 * x + 1)), (r4, lambda x: r3[2 * x] + r3[2 * x + 1])):
        coarsen_planes(pair, nx // 2, tmp, ref, R, 6)
        ref[...] = times(flat(ref), maps[DOWN3]).reshape(ref.shape)
    f4k = 0.25**4
    H = R // 2
    row = lax.broadcasted_iota(jnp.int32, (nx // 2, H, 128), 1)
    lane = lax.broadcasted_iota(jnp.int32, (nx // 2, H, 128), 2)
    within = (row < ny // 2) & (lane < nz // 2)
    diag = 6.0 * f4k + r4[...]
    zero = jnp.zeros((1, H, 128), F32)

    def apply(p):
        s = jnp.concatenate([zero, p[:-1]], axis=0) + jnp.concatenate([p[1:], zero], axis=0)
        s = s + roll(p, 1, 1) + roll(p, H - 1, 1) + roll(p, 1, 2) + roll(p, 127, 2)
        return jnp.where(within, diag * p - f4k * s, 0.0)

    r = jnp.where(within, f4[...], 0.0)
    p = r
    q = apply(r)
    rr = sum_all(r * r)
    a = rr / sum_all(r * q)
    e = a * p
    for i in range(1, BOTTOM_ITERS):
        r = r - a * q
        w = apply(r)
        new = sum_all(r * r)
        rw = sum_all(r * w)
        b = new / rr
        a = new / (rw - b * new / a)
        p = r + b * p
        q = w + b * q
        e = e + a * p
        rr = new
    f4[...] = times(e.reshape(nx // 2 * H, 128), maps[UP3]).reshape(e.shape)
    add_refined(f4, nx // 2, e3, s3, 6)
    relax(s3, e3, f3, c3, nx, factor, 12)
    relax(e3, s3, f3, c3, nx, factor, 12)


def k_up(g3, maps, f2, c2, e2i, f1, c1, e1i, f0, c0, d0, e0i, z_out, az_out, sums,
         e3, s3, f3, c3, r3, tmp3, f4, r4, sq, w3, w2, na, nb, n1, e2, s2, e1, s1, e0, s0):
    gx, gy, gz, sy, sz = place()
    nx, ny, nz = f3.shape[0], sy * 6, sz * 6
    coarse_solve(g3, maps, nx, ny, nz, e3, s3, f3, c3, r3, tmp3, f4, r4, sq)
    for ref, n in ((s2, 18), (s1, 36), (s0, 54), (e2, 18), (e1, 36), (e0, 54)):
        zero_ends(ref, n)
    for i in range(9):
        e = s3[i + 1 + gx * 3]
        e = jnp.concatenate([jnp.zeros((8, 128), F32), e, jnp.zeros((8, 128), F32)], axis=0)
        v = e[4:20]
        for k in range(1, sy):
            v = jnp.where(gy == k, e[6 * k + 4 : 6 * k + 20], v)
        w3[i] = v
    w3[...] = times(flat(w3), maps[UP2]).reshape(9, 16, 128)
    add_refined(w3, 9, e2i, e2, 9)
    relax(e2, s2, f2, c2, 18, 0.0625, 18)
    relax(s2, e2, f2, c2, 18, 0.0625, 18)

    def halves(i):
        na[i] = e2[i + 1, 2:18, :]
        nb[i] = e2[i + 1, 14:30, :]

    loop(18, halves, 6)

    w2[...] = (times(flat(na), maps[UP1A]) + times(flat(nb), maps[UP1B])).reshape(18, 16, 128)
    add_refined(w2, 18, e1i, e1, 6)
    relax(e1, s1, f1, c1, 36, 0.25, UM, paired)
    relax(s1, e1, f1, c1, 36, 0.25, UM, paired)

    def near(i):
        v = e1[i + 1 + gx * 9]
        n1[i] = jnp.where(upper(L1, 16), v[0:16], v[8:24])

    loop(27, near, 9)

    n1[...] = times(flat(n1), maps[UP0]).reshape(27, 16, 128)
    add_refined(n1, 27, e0i, e0, 9)
    relax(e0, s0, f0, c0, 54, 1.0, UR, paired)
    relax(s0, e0, f0, c0, 54, 1.0, UR, paired)
    shift = gx * 6
    mine = lanes(24) % 64 < 48

    def last(x, carry):
        u, v = carry
        w = x + shift
        z = e0[w + 1]
        az = own_rows(L0, d0[w] * z - paired(e0, w))
        z = own_rows(L0, z)
        f = own_rows(L0, f0[w])
        z_out[x] = z
        az_out[x] = az
        return u + jnp.where(mine, f * z, 0.0), v + jnp.where(mine, z * az, 0.0)

    def some(i, carry):
        for k in range(UZ):
            carry = last(UZ * i + k, carry)
        return carry

    zero = jnp.zeros((24, 128), F32)
    u, v = lax.fori_loop(0, 48 // UZ, some, (zero, zero))

    def total(t):
        return jnp.sum(jnp.sum(t, axis=1, keepdims=True), axis=0, keepdims=True)

    ln = lanes(sums.shape[0])
    sums[...] = jnp.where(ln == 0, total(u), jnp.where(ln == 1, total(v), 0.0))


def k_last(sums, own, z, az, f, sol, res, sv, rv, sems):
    s = jnp.sum(sums[...], axis=0, keepdims=True)
    ln = lanes(1)
    over = jnp.sum(jnp.where(ln == 0, s, 0.0), axis=1, keepdims=True)
    under = jnp.sum(jnp.where(ln == 1, s, 0.0), axis=1, keepdims=True)
    step = over / under
    shift = lax.axis_index("gx") * 6
    pairs = ((0, sv, sol), (1, rv, res))

    def copy(a, src, dst, i):
        part = pl.ds(i * 8, 8)
        return pltpu.make_async_copy(src.at[part], dst.at[part], sems.at[a, i])

    def some(i):
        for k in range(8):
            x = i * 8 + k
            for ref, v in ((sv, own[0, x] + step * z[x]), (rv, own_rows(L0, f[x + shift]) - step * az[x])):
                ref[x, 0:24, :] = v[:, 0:48]
                ref[x, 24:48, :] = roll(v, 64, 1)[:, 0:48]
        for a, src, dst in pairs:
            copy(a, src, dst, i).start()

    loop(6, some)
    for i in range(6):
        for a, src, dst in pairs:
            copy(a, src, dst, i).wait()


def ring(up, dn, axis):
    n = lax.axis_size(axis)
    low = lax.ppermute(up, axis, [(i, (i + 1) % n) for i in range(n)])
    high = lax.ppermute(dn, axis, [(i, (i - 1) % n) for i in range(n)])
    return low, high


def swap(v):
    return lax.ppermute(v, "gx", [(0, 1), (1, 0)])


def body(b, x0, rea):
    ALL = ("gx", "gy", "gz")
    sizes = [lax.axis_size(a) for a in ALL]
    count = sizes[0] * sizes[1] * sizes[2]
    b, x0, rea = (pltpu.with_memory_space_constraint(v, pltpu.HBM) for v in (b, x0, rea))
    hi, lo, own = run(
        k_zpack0,
        (sds(*L0.zshape), sds(*L0.zshape), sds(3, 48, 24, 128)),
        (x0, b, rea),
        [(3, 48, 48, 48), pltpu.SemaphoreType.DMA((3, 4))],
        far_in=True,
    )
    zl, zh = ring(hi, lo, "gz")
    r1, maps = run(
        k_early, (sds(24, 12, 128), sds(10, 256, 128, dtype=jnp.bfloat16)), (own,), [(24, 24, 128), (24, 16, 128)]
    )
    up, dn = run(k_ypack0, (sds(*L0.yshape),) * 2, (own, zl, zh, r1))
    yl, yh = ring(up, dn, "gy")
    xr = swap(run(k_xpack0, sds(*L0.xshape), (own, zl, zh, yl, yh)))
    win = run(k_windows0, sds(3, 48, 32, 128), (own, zl, zh, yl, yh))
    p0, q0 = (54, 32, 128), (56, 32, 128)
    f0, c0, d0, e0, f1, z1h, z1l = run(
        k_down0,
        (sds(*p0), sds(*p0), sds(*p0), sds(*q0), sds(24, 12, 128), sds(*L1.zshape), sds(*L1.zshape)),
        (win, r1, maps, xr),
        [q0, q0, (24, 24, 128), (24, 16, 128)],
        mib=M0,
    )
    zl, zh = ring(z1h, z1l, "gz")
    up, dn = run(k_ypack1, (sds(*L1.yshape),) * 2, (f1, r1, zl, zh))
    yl, yh = ring(up, dn, "gy")
    xr = swap(run(k_xpack1, sds(*L1.xshape), (f1, r1, zl, zh, yl, yh), [(2, 2, 24, 128)]))
    p1, q1, p2, q2 = (36, 24, 128), (38, 24, 128), (18, 32, 128), (20, 32, 128)
    win = run(k_windows1, sds(2, 24, 24, 128), (f1, r1, zl, zh, yl, yh), [(8, 2, 24, 128)])
    f1w, c1w, e1w, f2w, c2w, e2w, g = run(
        k_down1,
        (sds(*p1), sds(*p1), sds(*q1), sds(*p2), sds(*p2), sds(*q2), sds(count * 4, 128)),
        (win, maps, xr),
        [p1, q1, (18, 24, 128), (2, 18, 16, 128), p2, q2, (9, 32, 128), (2, 9, 16, 128), (128, 128)],
        mib=M1,
    )
    g = lax.all_to_all(g, ALL, 0, 0, tiled=True)
    n3 = [6 * s for s in sizes]
    R3 = (n3[1] + 8) // 8 * 8
    if R3 % 16:
        R3 += 8
    p3, q3, p4 = (n3[0], R3, 128), (n3[0] + 2, R3, 128), (n3[0] // 2, R3 // 2, 128)
    z, az, sums = run(
        k_up,
        (sds(48, 24, 128), sds(48, 24, 128), sds(count, 128)),
        (g, maps, f2w, c2w, e2w, f1w, c1w, e1w, f0, c0, d0, e0),
        [q3, q3, p3, p3, p3, (n3[0] // 2, R3, 128), p4, p4, (sizes[0] * sizes[1], 128, 128), (9, 16, 128), (18, 16, 128),
         (18, 16, 128), (18, 16, 128), (27, 16, 128), q2, q2, q1, q1, q0, q0],
        mib=M2,
    )
    sums = lax.all_to_all(sums.reshape(count, 1, 128), ALL, 0, 0, tiled=True).reshape(count, 128)
    return run(
        k_last,
        (sds(48, 48, 48), sds(48, 48, 48)),
        (sums, own, z, az, f0),
        [(48, 48, 48), (48, 48, 48), pltpu.SemaphoreType.DMA((2, 6))],
        far_out=True,
    )


def solution(mesh):
    spec = P("gx", "gy", "gz")
    return jax.shard_map(body, mesh=mesh, in_specs=(spec, spec, spec), out_specs=(spec, spec), check_vma=False)
```

```python
import functools
import jax
import jax.numpy as jnp
from jax import lax
from jax.experimental import pallas as pl
from jax.experimental.pallas import tpu as pltpu
from jax.sharding import PartitionSpec as P

W = 6.0 / 7.0
BOTTOM_ITERS = 6
N0 = 48
F32 = jnp.float32
HI = lax.Precision.HIGHEST
M0, M1, M2 = 10, 8, 12
UF, UR, UM, UZ, UL = 12, 27, 18, 12, 6


class Spec:
    def __init__(self, n, h, na, R, o, hx, cut, kp, st):
        self.n, self.h, self.na, self.R, self.o, self.hx, self.cut, self.kp, self.st = n, h, na, R, o, hx, cut, kp, st
        self.half = n // 2
        self.zshape = (n // (kp * st), self.half * st, 128)
        self.yshape = (self.half, na * h, 128)
        self.hs = (h,) * na
        self.xshape = (hx, na, R, 128)
        self.nx = n + hx

    def slot(self, x, a):
        if self.st == 1:
            h = self.hs[a]
            many = 64 // h
            return ZBASE[a] + lax.div(x, many), 0, h * lax.rem(x, many)
        per = self.n // self.st
        t, y = lax.div(x, per), lax.rem(x, per)
        return lax.div(y, self.kp), t, self.h * (lax.rem(y, self.kp) * self.na + a)


L0 = Spec(48, 5, 3, 32, 8, 6, 56, 4, 1)
L1 = Spec(24, 12, 2, 24, 12, 12, 44, 2, 2)
L0.hs = (5, 4, 4)
ZBASE = (0, 4, 7)
YBASE = (0, 40, 72)
L0.zshape = (10, 24, 128)
L0.yshape = (3, 104, 128)


def sds(*shape, dtype=F32):
    return jax.ShapeDtypeStruct(shape, dtype)


def run(kernel, outs, args, scratch=(), mib=12, far_in=False, far_out=False):
    vmem = pl.BlockSpec(memory_space=pltpu.VMEM)
    hbm = pl.BlockSpec(memory_space=pl.ANY)
    return pl.pallas_call(
        kernel,
        out_shape=outs,
        in_specs=[hbm if far_in else vmem] * len(args),
        out_specs=jax.tree.map(lambda _: hbm if far_out else vmem, outs),
        scratch_shapes=[pltpu.VMEM(s, F32) if isinstance(s, tuple) else s for s in scratch],
        compiler_params=pltpu.CompilerParams(vmem_limit_bytes=mib * 1024 * 1024),
    )(*args)


def place():
    return [lax.axis_index(a) for a in ("gx", "gy", "gz")] + [lax.axis_size(a) for a in ("gy", "gz")]


def lanes(rows):
    return lax.broadcasted_iota(jnp.int32, (rows, 128), 1)


def roll(v, shift, axis):
    if isinstance(shift, int):
        shift = shift % v.shape[axis]
        if shift == 0:
            return v
    return pltpu.roll(v, shift, axis)


def loop(n, f, u=1):
    u = max(d for d in range(1, u + 1) if n % d == 0)

    def some(i, c):
        for k in range(u):
            f(i * u + k)
        return c

    lax.fori_loop(0, n // u, some, 0)


def upper(sp, rows):
    l = lanes(rows)
    return (l >= sp.cut) & (l < sp.cut + 64)


def edge(sp, ids):
    _, gy, gz, ny, nz = ids
    high = jnp.where(gz < nz - 1, sp.n + sp.h, sp.n)
    low = jnp.where(gz > 0, 64 - sp.h, 64)
    return high, low, jnp.where(gy > 0, 1.0, 0.0), jnp.where(gy < ny - 1, 1.0, 0.0)


def ztile(sp, items):
    l = lanes(sp.half)
    hi = [jnp.zeros((sp.half, 128), F32)] * 2
    lo = list(hi)
    for k, (v, at, h) in enumerate(items):
        r = roll(v, at, 1)
        hi[k % 2] = jnp.where(((l + (64 - (at + sp.n - h) % 64)) & 63) < h, r, hi[k % 2])
        lo[k % 2] = jnp.where(((l + (64 - at)) & 63) < h, r, lo[k % 2])
    return roll(hi[0] + hi[1], -2 * sp.n, 1), lo[0] + lo[1]


def ztile1(own, hi_ref, lo_ref, g):
    sp = L1
    for t in range(sp.st):
        items = [
            (own(t * (sp.n // sp.st) + g * sp.kp + k, a), sp.h * (k * sp.na + a), sp.h)
            for k in range(sp.kp)
            for a in range(sp.na)
        ]
        hi, lo = ztile(sp, items)
        hi_ref[g, t * sp.half : (t + 1) * sp.half, :] = hi
        lo_ref[g, t * sp.half : (t + 1) * sp.half, :] = lo


def merged(sp, own, zl, zh, x, a, b, e, top, bottom):
    g, t, at = sp.slot(x, a)
    if sp.st == 1:
        high, low = zh[g, b:e, :], zl[g, b:e, :]
    else:
        high = jnp.where(t == 0, zh[g, b:e, :], zh[g, sp.half + b : sp.half + e, :])
        low = jnp.where(t == 0, zl[g, b:e, :], zl[g, sp.half + b : sp.half + e, :])
    l = lanes(e - b)
    beside = jnp.where(((l + (64 - at)) & 63) < sp.hs[a], high, low)
    beside = roll(beside, (sp.n + 128 - at) & 127, 1)
    q = l & 63
    return jnp.where(q < sp.n, own(x, a)[b:e], jnp.where((q < top) | (q >= bottom), beside, 0.0))


def ypack0(own, turned, zl, zh, up_ref, dn_ref):
    top, bottom, _, _ = edge(L0, place())
    l = lanes(8)
    q = l & 63
    up = upper(L0, 8)

    def beside(x, a, b, turn):
        g, _, at = L0.slot(x, a)
        v = jnp.where(((l + (64 - at)) & 63) < L0.hs[a], zh[g, b : b + 8, :], zl[g, b : b + 8, :])
        v = roll(v, (L0.n + turn + 128 - at) & 127, 1)
        return jnp.where((q < top) | (q >= bottom), v, 0.0)

    def some(i):
        for k in range(8):
            p = 8 * i + k
            for a in range(3):
                h = L0.hs[a]
                for ref, b, s in ((up_ref, 16, 8 - h), (dn_ref, 0, 0)):
                    even = jnp.where(q < L0.n, own[a, 2 * p, b : b + 8, :], beside(2 * p, a, b, 0))
                    odd = jnp.where(q < L0.n, turned[a, p, b // 2 : b // 2 + 8, :], beside(2 * p + 1, a, b, 64))
                    v = jnp.where(up, even, odd) if b else jnp.where(up, odd, even)
                    ref[i, pl.ds(YBASE[a] + k, h, stride=8), :] = v[s : s + h]

    loop(3, some)


def ypack1(own, zl, zh, up_ref, dn_ref, u):
    sp = L1
    half = sp.half
    top, bottom, _, _ = edge(sp, place())

    def pair(p):
        for a in range(sp.na):
            even = merged(sp, own, zl, zh, 2 * p, a, 0, half, top, bottom)
            odd = roll(merged(sp, own, zl, zh, 2 * p + 1, a, 0, half, top, bottom), 64, 1)
            up = upper(sp, half)
            up_ref[p, a * half : (a + 1) * half, :] = jnp.where(up, even, odd)
            dn_ref[p, a * half : (a + 1) * half, :] = jnp.where(up, odd, even)

    loop(half, pair, u)


def y_tiles0(yl, yh, g, t, a):
    def rows(ref, start):
        return ref[g, pl.ds(start + t, 8, stride=8), :]

    if a == 0:
        return roll(rows(yl, 0), 3, 0), rows(yh, 0)
    return rows(yl, YBASE[a] - 32), rows(yh, 40) if a == 1 else roll(rows(yh, 40), 4, 0)


def plane0(own, zl, zh, tiles, x, a, dst, xw, ends, turn):
    top, bottom, below, above = ends
    sp = L0
    m = merged(sp, own, zl, zh, x, a, 0, sp.half, top, bottom)
    low, high = tiles
    lower = jnp.concatenate([roll(low, turn, 1) * below, m], axis=0)
    higher = jnp.concatenate([m, roll(high, turn, 1) * above], axis=0)
    dst[xw] = jnp.where(upper(sp, sp.R), higher, lower)


def plane1(own, zl, zh, yl, yh, x, a, dst, xw, ends, spare):
    top, bottom, below, above = ends
    sp = L1
    h, half = sp.h, sp.half
    m = merged(sp, own, zl, zh, x, a, 0, half, top, bottom)
    p = lax.div(x, 2)
    turn = 64 * (1 - lax.rem(x, 2))
    spare[0, 0:h, :] = roll(yl[p, a * h : (a + 1) * h, :], turn, 1) * below
    spare[0, h:, :] = m
    spare[1, 0:half, :] = m
    spare[1, half:, :] = roll(yh[p, a * h : (a + 1) * h, :], turn, 1) * above
    dst[xw] = jnp.where(upper(sp, sp.R), spare[1], spare[0])


def lane_z(sp, l):
    return jnp.where(l < sp.cut, l, jnp.where(l < sp.cut + 64, l - 64, l - 128))


def inside(sp, ids):
    _, gy, gz, ny, nz = ids
    n, h = sp.n, min(sp.hs)
    y = lax.broadcasted_iota(jnp.int32, (sp.R, 128), 0) - sp.o + jnp.where(upper(sp, sp.R), sp.R, 0)
    z = lane_z(sp, lanes(sp.R))
    ok = (y >= -h) & (y < n + h) & (z >= -h) & (z < n + h)
    y, z = y + gy * n, z + gz * n
    return ok & (y >= 0) & (y < ny * n) & (z >= 0) & (z < nz * n)


def paired(ref, x):
    c = ref[x + 1]
    R = c.shape[0]
    s = ref[x] + ref[x + 2]
    sub = lax.broadcasted_iota(jnp.int32, (8, 128), 0)
    seam = roll(jnp.where(sub == 0, c[0:8], c[R - 8 : R]), 64, 1)
    last = jnp.where(sub == 7, roll(seam, 7, 0), roll(c[R - 8 :], 7, 0))
    first = jnp.where(sub == 0, roll(seam, 1, 0), roll(c[0:8], 1, 0))
    up = jnp.concatenate([ref[x + 1, 1 : R - 7, :], last], axis=0)
    down = jnp.concatenate([first, ref[x + 1, 7 : R - 1, :]], axis=0)
    s = s + (up + down)
    return s + (roll(c, 1, 1) + roll(c, 127, 1))


def domain(sp, n, h, r0, R, ids):
    row = lax.broadcasted_iota(jnp.int32, (R, 128), 0) - r0
    ln = lanes(R)
    z = jnp.where(ln < 64, ln, ln - 128)
    gy, gz, ny, nz = ids[1], ids[2], ids[3], ids[4]
    y_at, z_at = row + gy * n, z + gz * n
    ok = (row >= -h) & (row < n + h) & (z >= -h) & (z < n + h)
    return ok & (y_at >= 0) & (y_at < ny * n) & (z_at >= 0) & (z_at < nz * n)


def neighbours(ref, x):
    c = ref[x + 1]
    R = c.shape[0]
    s = ref[x] + ref[x + 2]
    s = s + (roll(c, 1, 0) + roll(c, R - 1, 0))
    return s + (roll(c, 1, 1) + roll(c, 127, 1))


def zero_ends(ref, n):
    ref[0] = jnp.zeros(ref.shape[1:], F32)
    ref[n + 1] = jnp.zeros(ref.shape[1:], F32)


def relax(src, dst, f, c, n, factor, u=9, near=None):
    near = near or neighbours

    def one(x):
        dst[x + 1] = (1.0 - W) * src[x + 1] + c[x] * (f[x] + factor * near(src, x))

    loop(n, one, u)


def lane_map(pick, value):
    l = lax.broadcasted_iota(jnp.int32, (256, 128), 0) & 127
    m = lax.broadcasted_iota(jnp.int32, (256, 128), 1)
    return jnp.where(pick(l) == m, value, 0.0).astype(jnp.bfloat16)


def spread_map(pick):
    m = lax.broadcasted_iota(jnp.int32, (256, 128), 0) & 127
    l = lax.broadcasted_iota(jnp.int32, (256, 128), 1)
    return jnp.where(pick(l) == m, 1.0, 0.0).astype(jnp.bfloat16)


def floor_half(z):
    return lax.shift_right_arithmetic(z, 1)


def coarse_lane(sp, l, want):
    z = lane_z(sp, l)
    up = (l >= sp.cut) & (l < sp.cut + 64)
    good = (z >= -sp.h) & (z < sp.n + sp.h)
    good = good & (up if want else jnp.logical_not(up))
    return jnp.where(good, floor_half(z) + jnp.where(z < 0, 128, 0), -1)


def both_lanes(l):
    lower, higher = coarse_lane(L0, l, False), coarse_lane(L0, l, True)
    return jnp.where(lower >= 0, lower, jnp.where(higher >= 0, (higher + 64) & 127, -1))


OWN, DOWN1A, DOWN1B, DOWN2, DOWN3, UP3, UP2, UP1A, UP1B, UP0 = range(10)


def all_maps(maps, gz):
    half = floor_half
    maps[OWN] = lane_map(lambda l: jnp.where(l < 64, half(l), 32 + half(l)), 0.125)
    maps[DOWN1A] = lane_map(lambda l: coarse_lane(L1, l, False), 0.125)
    maps[DOWN1B] = lane_map(lambda l: coarse_lane(L1, l, True), 0.125)
    maps[DOWN2] = lane_map(lambda l: jnp.where(l < 64, half(l), half(l) + 64), 0.125)
    maps[DOWN3] = lane_map(half, 0.125)
    maps[UP3] = spread_map(half)
    maps[UP2] = spread_map(lambda l: gz * 6 + jnp.where(l < 64, half(l), half(l) - 64))
    maps[UP1A] = spread_map(lambda l: coarse_lane(L1, l, False))
    maps[UP1B] = spread_map(lambda l: coarse_lane(L1, l, True))
    maps[UP0] = spread_map(both_lanes)


def times(v, m):
    big = v.astype(jnp.bfloat16)
    rest = (v - big.astype(F32)).astype(jnp.bfloat16)
    return jnp.dot(jnp.concatenate([big, rest], axis=1), m, preferred_element_type=F32)


def coarsen_planes(pair, n, tmp, acc, rows, u=2):
    half = rows // 2

    def one(x):
        tmp[x, 0:rows, :] = pair(x)
        acc[x, 0:half, :] = tmp[x, pl.ds(0, half, stride=2), :] + tmp[x, pl.ds(1, half, stride=2), :]

    loop(n, one, u)


def flat(ref):
    n, rows, _ = ref.shape
    return ref[...].reshape(n * rows, 128)


def add_refined(wide, n, src, dst, u=3):
    R = dst.shape[1]

    def one(i):
        v = wide[i, 0 : R // 2, :]
        for k in range(2):
            dst[2 * i + 1, pl.ds(k, R // 2, stride=2), :] = v
        t = dst[2 * i + 1]
        dst[2 * i + 1] = src[2 * i + 1] + t
        dst[2 * i + 2] = src[2 * i + 2] + t

    loop(n, one, u)


def k_zpack0(x0, b, rea, hi, lo, own, raw, sems):
    def copy(a, ref, i):
        many = 64 // L0.hs[a]
        part = pl.ds(i * many, many)
        return pltpu.make_async_copy(ref.at[part], raw.at[a, part], sems.at[a, i])

    refs = (x0, b, rea)
    parts = [48 * h // (64 // h * h) for h in L0.hs]
    for a, ref in enumerate(refs):
        for i in range(parts[a]):
            copy(a, ref, i).start()

    def pack(a, i):
        h = L0.hs[a]
        many = 64 // h
        hi[ZBASE[a] + i], lo[ZBASE[a] + i] = ztile(L0, [(own[a, i * many + k], h * k, h) for k in range(many)])

    steps = [(a, ref, i) for a, ref in enumerate(refs) for i in range(parts[a])]
    for n, (a, ref, i) in enumerate(steps):
        copy(a, ref, i).wait()
        if n:
            pack(steps[n - 1][0], steps[n - 1][2])
        many = 64 // L0.hs[a]
        for x in range(i * many, i * many + many):
            own[a, x, :, 0:48] = raw[a, x, 0:24, :]
            own[a, x, :, 64:112] = raw[a, x, 24:48, :]
    pack(steps[-1][0], steps[-1][2])


def k_ypack0(own, turned, zl, zh, up, dn):
    ypack0(own, turned, zl, zh, up, dn)


def k_xpack0(own, zl, zh, yl, yh, out):
    ids = place()
    ends = edge(L0, ids)
    first = ids[0] == 0
    for i in range(6):
        x = jnp.where(first, 42, 0) + i
        for a in range(3):
            there, here = y_tiles0(yl, yh, 2, 5 + i // 2, a), y_tiles0(yl, yh, 0, i // 2, a)
            tiles = [jnp.where(first, v, w) for v, w in zip(there, here)]
            plane0(lambda x, a: own[a, x], zl, zh, tiles, x, a, out.at[i], a, ends, 64 * (1 - i % 2))


def k_xpack1(f1, r1, zl, zh, yl, yh, out, spare):
    both = (f1, r1)
    ids = place()
    ends = edge(L1, ids)

    def one(i):
        for a in range(2):
            plane1(lambda x, a: both[a][x], zl, zh, yl, yh, (1 - ids[0]) * 12 + i, a, out.at[i], a, ends, spare.at[a])

    loop(12, one, 2)


def k_windows0(own, zl, zh, yl, yh, out):
    ends = edge(L0, place())

    def some(i):
        for k in range(16):
            for a in range(3):
                tiles = y_tiles0(yl, yh, i, k // 2, a)
                plane0(lambda x, a: own[a, x], zl, zh, tiles, 16 * i + k, a, out.at[a], 16 * i + k, ends, 64 * (1 - k % 2))

    loop(3, some)


def own_rows(sp, v):
    return jnp.where(upper(sp, sp.half), v[0 : sp.half], v[sp.o :])


def half_own(pair, tmp, acc, out, u, m):
    coarsen_planes(pair, 24, tmp, acc, 24, u)
    acc[...] = times(flat(acc), m).reshape(24, 16, 128)

    def keep(x):
        out[x] = acc[x, 0:12, :]

    loop(24, keep, 6)


def k_early(own, turned, r1, maps, tmp, acc):
    def turn(p):
        for a in range(3):
            v = own[a, 2 * p + 1]
            turned[a, p, 0:8, :] = roll(v[0:8], 64, 1)
            turned[a, p, 8:16, :] = roll(v[16:24], 64, 1)

    loop(24, turn, 4)
    all_maps(maps, lax.axis_index("gz"))
    mine = lanes(24) % 64 < 48
    half_own(lambda x: jnp.where(mine, own[2, 2 * x] + own[2, 2 * x + 1], 0.0), tmp, acc, r1, 4, maps[OWN])


def k_down0(win, r1, maps, xr, f_out, c_out, d_out, e_out, f1, z1h, z1l, xw, ew, tmp, acc):
    ids = place()
    n = L0.nx
    shift = ids[0] * L0.hx
    other = (1 - ids[0]) * L0.n
    ok = inside(L0, ids)
    zero_ends(xw, n)
    zero_ends(ew, n)
    zero_ends(e_out, n)

    def put(x):
        xw[x + shift + 1] = win[0, x]

    def take(x):
        xw[x + other + 1] = xr[x, 0]

    loop(48, put, 12)
    loop(6, take, 6)

    def first(w, b, rea):
        d = 6.0 + rea
        c = jnp.where(ok, W / d, 0.0)
        f = b - d * xw[w + 1] + paired(xw, w)
        d_out[w] = d
        f_out[w] = f
        c_out[w] = c
        ew[w + 1] = c * f

    loop(48, lambda x: first(x + shift, win[1, x], win[2, x]), UF)
    loop(6, lambda x: first(x + other, xr[x, 1], xr[x, 2]), 6)
    relax(ew, e_out, f_out, c_out, n, 1.0, UR, paired)

    def left(x):
        return own_rows(L0, f_out[x] - d_out[x] * e_out[x + 1] + paired(e_out, x))

    mine = lanes(24) % 64 < 48
    pair = lambda x: jnp.where(mine, left(2 * x + shift) + left(2 * x + shift + 1), 0.0)
    half_own(pair, tmp, acc, f1, UL, maps[OWN])
    both = (f1, r1)
    loop(6, lambda g: ztile1(lambda x, a: both[a][x], z1h, z1l, g), 3)


def k_ypack1(f1, r1, zl, zh, up, dn):
    both = (f1, r1)
    ypack1(lambda x, a: both[a][x], zl, zh, up, dn, 6)


def k_windows1(f1, r1, zl, zh, yl, yh, out, spare):
    both = (f1, r1)
    ends = edge(L1, place())

    def some(i):
        for k in range(4):
            for a in range(2):
                plane1(lambda x, a: both[a][x], zl, zh, yl, yh, 4 * i + k, a, out.at[a], 4 * i + k, ends, spare.at[2 * k + a])

    loop(6, some)


def k_down1(win, maps, xr, fw, cw, e_out, f2, c2, e2, out3, rw, ew, tmp, acc, r2, ew2, tmp2, t3, sq):
    ids = place()
    n = L1.nx
    shift = ids[0] * L1.hx
    other = (1 - ids[0]) * L1.n

    def put(x):
        fw[x + shift] = win[0, x]
        rw[x + shift] = win[1, x]

    def take(x):
        fw[x + other] = xr[x, 0]
        rw[x + other] = xr[x, 1]

    loop(24, put, 8)
    loop(12, take, 6)
    ok = inside(L1, ids)
    zero_ends(ew, n)
    zero_ends(e_out, n)

    def first(x):
        c = jnp.where(ok, W / (1.5 + rw[x]), 0.0)
        cw[x] = c
        ew[x + 1] = c * fw[x]

    loop(n, first, 6)
    relax(ew, e_out, fw, cw, n, 0.25, UM, paired)

    def left(x):
        return fw[x] - (1.5 + rw[x]) * e_out[x + 1] + 0.25 * paired(e_out, x)

    for ref, pair in ((f2, lambda x: left(2 * x) + left(2 * x + 1)), (r2, lambda x: rw[2 * x] + rw[2 * x + 1])):
        coarsen_planes(pair, 18, tmp, acc.at[0], 24, 9)
        v = flat(acc.at[0])
        acc[0] = times(v, maps[DOWN1A]).reshape(18, 16, 128)
        acc[1] = times(v, maps[DOWN1B]).reshape(18, 16, 128)

        def keep(x, ref=ref):
            ref[x] = jnp.zeros((32, 128), F32)
            ref[x, 2:14, :] = acc[0, x, 0:12, :]
            ref[x, 14:26, :] = acc[1, x, 0:12, :]

        loop(18, keep, 6)
    ok2 = domain(None, 12, 6, 8, 32, ids)
    zero_ends(ew2, 18)
    zero_ends(e2, 18)

    def second(x):
        c = jnp.where(ok2, W / (0.375 + r2[x]), 0.0)
        c2[x] = c
        ew2[x + 1] = c * f2[x]

    loop(18, second, 6)
    relax(ew2, e2, f2, c2, 18, 0.0625, 18)

    def left2(x):
        return f2[x] - (0.375 + r2[x]) * e2[x + 1] + 0.0625 * neighbours(e2, x)

    for a, pair in enumerate((lambda x: left2(2 * x) + left2(2 * x + 1), lambda x: r2[2 * x] + r2[2 * x + 1])):
        coarsen_planes(pair, 9, tmp2, t3.at[a], 32, 9)
        t3[a] = times(flat(t3.at[a]), maps[DOWN2]).reshape(9, 16, 128)
    shift = ids[0] * 3
    sq[...] = jnp.zeros((128, 128), F32)
    for a in range(2):
        for x in range(6):
            at = a * 36 + x * 6
            sq[at : at + 6, :] = t3[a, x + shift, 4:10, :]
    t = sq[...].T[0:8]
    ln = lanes(1)
    rows = []
    for u in range(2):
        for a in range(2):
            parts = [roll(t, 36 * (w - a), 1)[3 * u + w : 3 * u + w + 1] for w in range(3)]
            rows.append(jnp.where(ln < 36, parts[0], jnp.where(ln < 72, parts[1], parts[2])))
    tile = jnp.concatenate(rows + rows, axis=0)
    n8 = out3.shape[0] // 8
    out3[...] = jnp.broadcast_to(tile[None], (n8, 8, 128)).reshape(n8 * 8, 128)


def sum_all(v):
    s = jnp.sum(v, axis=0)
    return jnp.sum(jnp.sum(s, axis=1, keepdims=True), axis=0, keepdims=True)


def coarse_solve(g3, maps, nx, ny, nz, e3, s3, f3, c3, r3, tmp, f4, r4, sq):
    R = f3.shape[1]
    for ref in (f3, r3):
        ref[...] = jnp.zeros(ref.shape, F32)
    kx, ky, kz = nx // 6, ny // 6, nz // 6
    for bx in range(kx):
        for by in range(ky):
            k = bx * ky + by
            if kz * 6 < 128:
                sq[k, kz * 6 :, :] = jnp.zeros((128 - kz * 6, 128), F32)
            got = [g3[pl.ds(k * kz * 4 + r, kz, stride=4), :] for r in range(4)]
            ln = lanes(kz)
            for u in range(2):
                for w in range(3):
                    f, r = roll(got[2 * u], -36 * w, 1), roll(got[2 * u + 1], 36 - 36 * w, 1)
                    sq[k, pl.ds(3 * u + w, kz, stride=6), :] = jnp.where(ln < 36, f, r)
            t = sq[k].T
            for x in range(6):
                f3[bx * 6 + x, by * 6 : by * 6 + 6, :] = t[x * 6 : x * 6 + 6]
                r3[bx * 6 + x, by * 6 : by * 6 + 6, :] = t[36 + x * 6 : 42 + x * 6]
    factor = 0.25**3
    ok = (lax.broadcasted_iota(jnp.int32, (R, 128), 0) < ny) & (lanes(R) < nz)
    for ref in (e3, s3):
        zero_ends(ref, nx)

    def first(x):
        c = jnp.where(ok, W / (6.0 * factor + r3[x]), 0.0)
        c3[x] = c
        s3[x + 1] = c * f3[x]

    loop(nx, first, 6)
    relax(s3, e3, f3, c3, nx, factor, 12)

    def left(x):
        v = f3[x] - (6.0 * factor + r3[x]) * e3[x + 1] + factor * neighbours(e3, x)
        return jnp.where(ok, v, 0.0)

    for ref, pair in ((f4, lambda x: left(2 * x) + left(2 * x + 1)), (r4, lambda x: r3[2 * x] + r3[2 * x + 1])):
        coarsen_planes(pair, nx // 2, tmp, ref, R, 6)
        ref[...] = times(flat(ref), maps[DOWN3]).reshape(ref.shape)
    f4k = 0.25**4
    H = R // 2
    row = lax.broadcasted_iota(jnp.int32, (nx // 2, H, 128), 1)
    lane = lax.broadcasted_iota(jnp.int32, (nx // 2, H, 128), 2)
    within = (row < ny // 2) & (lane < nz // 2)
    diag = 6.0 * f4k + r4[...]
    zero = jnp.zeros((1, H, 128), F32)

    def apply(p):
        s = jnp.concatenate([zero, p[:-1]], axis=0) + jnp.concatenate([p[1:], zero], axis=0)
        s = s + roll(p, 1, 1) + roll(p, H - 1, 1) + roll(p, 1, 2) + roll(p, 127, 2)
        return jnp.where(within, diag * p - f4k * s, 0.0)

    r = jnp.where(within, f4[...], 0.0)
    p = r
    q = apply(r)
    rr = sum_all(r * r)
    a = rr / sum_all(r * q)
    e = a * p
    for i in range(1, BOTTOM_ITERS):
        r = r - a * q
        w = apply(r)
        new = sum_all(r * r)
        rw = sum_all(r * w)
        b = new / rr
        a = new / (rw - b * new / a)
        p = r + b * p
        q = w + b * q
        e = e + a * p
        rr = new
    f4[...] = times(e.reshape(nx // 2 * H, 128), maps[UP3]).reshape(e.shape)
    add_refined(f4, nx // 2, e3, s3, 6)
    relax(s3, e3, f3, c3, nx, factor, 12)
    relax(e3, s3, f3, c3, nx, factor, 12)


def k_up(g3, maps, f2, c2, e2i, f1, c1, e1i, f0, c0, d0, e0i, z_out, az_out, sums,
         e3, s3, f3, c3, r3, tmp3, f4, r4, sq, w3, w2, na, nb, n1, e2, s2, e1, s1, e0, s0):
    gx, gy, gz, sy, sz = place()
    nx, ny, nz = f3.shape[0], sy * 6, sz * 6
    coarse_solve(g3, maps, nx, ny, nz, e3, s3, f3, c3, r3, tmp3, f4, r4, sq)
    for ref, n in ((s2, 18), (s1, 36), (s0, 54), (e2, 18), (e1, 36), (e0, 54)):
        zero_ends(ref, n)
    for i in range(9):
        e = s3[i + 1 + gx * 3]
        e = jnp.concatenate([jnp.zeros((8, 128), F32), e, jnp.zeros((8, 128), F32)], axis=0)
        v = e[4:20]
        for k in range(1, sy):
            v = jnp.where(gy == k, e[6 * k + 4 : 6 * k + 20], v)
        w3[i] = v
    w3[...] = times(flat(w3), maps[UP2]).reshape(9, 16, 128)
    add_refined(w3, 9, e2i, e2, 9)
    relax(e2, s2, f2, c2, 18, 0.0625, 18)
    relax(s2, e2, f2, c2, 18, 0.0625, 18)

    def halves(i):
        na[i] = e2[i + 1, 2:18, :]
        nb[i] = e2[i + 1, 14:30, :]

    loop(18, halves, 6)

    w2[...] = (times(flat(na), maps[UP1A]) + times(flat(nb), maps[UP1B])).reshape(18, 16, 128)
    add_refined(w2, 18, e1i, e1, 6)
    relax(e1, s1, f1, c1, 36, 0.25, UM, paired)
    relax(s1, e1, f1, c1, 36, 0.25, UM, paired)

    def near(i):
        v = e1[i + 1 + gx * 9]
        n1[i] = jnp.where(upper(L1, 16), v[0:16], v[8:24])

    loop(27, near, 9)

    n1[...] = times(flat(n1), maps[UP0]).reshape(27, 16, 128)
    add_refined(n1, 27, e0i, e0, 9)
    relax(e0, s0, f0, c0, 54, 1.0, UR, paired)
    relax(s0, e0, f0, c0, 54, 1.0, UR, paired)
    shift = gx * 6
    mine = lanes(24) % 64 < 48

    def last(x, carry):
        u, v = carry
        w = x + shift
        z = e0[w + 1]
        az = own_rows(L0, d0[w] * z - paired(e0, w))
        z = own_rows(L0, z)
        f = own_rows(L0, f0[w])
        z_out[x] = z
        az_out[x] = az
        return u + jnp.where(mine, f * z, 0.0), v + jnp.where(mine, z * az, 0.0)

    def some(i, carry):
        for k in range(UZ):
            carry = last(UZ * i + k, carry)
        return carry

    zero = jnp.zeros((24, 128), F32)
    u, v = lax.fori_loop(0, 48 // UZ, some, (zero, zero))

    def total(t):
        return jnp.sum(jnp.sum(t, axis=1, keepdims=True), axis=0, keepdims=True)

    ln = lanes(sums.shape[0])
    sums[...] = jnp.where(ln == 0, total(u), jnp.where(ln == 1, total(v), 0.0))


def k_last(sums, own, z, az, f, sol, res, sv, rv, sems):
    s = jnp.sum(sums[...], axis=0, keepdims=True)
    ln = lanes(1)
    over = jnp.sum(jnp.where(ln == 0, s, 0.0), axis=1, keepdims=True)
    under = jnp.sum(jnp.where(ln == 1, s, 0.0), axis=1, keepdims=True)
    step = over / under
    shift = lax.axis_index("gx") * 6
    pairs = ((0, sv, sol), (1, rv, res))

    def copy(a, src, dst, i):
        part = pl.ds(i * 8, 8)
        return pltpu.make_async_copy(src.at[part], dst.at[part], sems.at[a, i])

    def some(i):
        for k in range(8):
            x = i * 8 + k
            for ref, v in ((sv, own[0, x] + step * z[x]), (rv, own_rows(L0, f[x + shift]) - step * az[x])):
                ref[x, 0:24, :] = v[:, 0:48]
                ref[x, 24:48, :] = roll(v, 64, 1)[:, 0:48]
        for a, src, dst in pairs:
            copy(a, src, dst, i).start()

    loop(6, some)
    for i in range(6):
        for a, src, dst in pairs:
            copy(a, src, dst, i).wait()


def ring(up, dn, axis):
    n = lax.axis_size(axis)
    low = lax.ppermute(up, axis, [(i, (i + 1) % n) for i in range(n)])
    high = lax.ppermute(dn, axis, [(i, (i - 1) % n) for i in range(n)])
    return low, high


def swap(v):
    return lax.ppermute(v, "gx", [(0, 1), (1, 0)])


def body(b, x0, rea):
    ALL = ("gx", "gy", "gz")
    sizes = [lax.axis_size(a) for a in ALL]
    count = sizes[0] * sizes[1] * sizes[2]
    b, x0, rea = (pltpu.with_memory_space_constraint(v, pltpu.HBM) for v in (b, x0, rea))
    hi, lo, own = run(
        k_zpack0,
        (sds(*L0.zshape), sds(*L0.zshape), sds(3, 48, 24, 128)),
        (x0, b, rea),
        [(3, 48, 48, 48), pltpu.SemaphoreType.DMA((3, 4))],
        far_in=True,
    )
    zl, zh = ring(hi, lo, "gz")
    turned, r1, maps = run(
        k_early,
        (sds(3, 24, 16, 128), sds(24, 12, 128), sds(10, 256, 128, dtype=jnp.bfloat16)),
        (own,),
        [(24, 24, 128), (24, 16, 128)],
    )
    up, dn = run(k_ypack0, (sds(*L0.yshape),) * 2, (own, turned, zl, zh))
    yl, yh = ring(up, dn, "gy")
    xr = swap(run(k_xpack0, sds(*L0.xshape), (own, zl, zh, yl, yh)))
    win = run(k_windows0, sds(3, 48, 32, 128), (own, zl, zh, yl, yh))
    p0, q0 = (54, 32, 128), (56, 32, 128)
    f0, c0, d0, e0, f1, z1h, z1l = run(
        k_down0,
        (sds(*p0), sds(*p0), sds(*p0), sds(*q0), sds(24, 12, 128), sds(*L1.zshape), sds(*L1.zshape)),
        (win, r1, maps, xr),
        [q0, q0, (24, 24, 128), (24, 16, 128)],
        mib=M0,
    )
    zl, zh = ring(z1h, z1l, "gz")
    up, dn = run(k_ypack1, (sds(*L1.yshape),) * 2, (f1, r1, zl, zh))
    yl, yh = ring(up, dn, "gy")
    xr = swap(run(k_xpack1, sds(*L1.xshape), (f1, r1, zl, zh, yl, yh), [(2, 2, 24, 128)]))
    p1, q1, p2, q2 = (36, 24, 128), (38, 24, 128), (18, 32, 128), (20, 32, 128)
    win = run(k_windows1, sds(2, 24, 24, 128), (f1, r1, zl, zh, yl, yh), [(8, 2, 24, 128)])
    f1w, c1w, e1w, f2w, c2w, e2w, g = run(
        k_down1,
        (sds(*p1), sds(*p1), sds(*q1), sds(*p2), sds(*p2), sds(*q2), sds(count * 4, 128)),
        (win, maps, xr),
        [p1, q1, (18, 24, 128), (2, 18, 16, 128), p2, q2, (9, 32, 128), (2, 9, 16, 128), (128, 128)],
        mib=M1,
    )
    g = lax.all_to_all(g, ALL, 0, 0, tiled=True)
    n3 = [6 * s for s in sizes]
    R3 = (n3[1] + 8) // 8 * 8
    if R3 % 16:
        R3 += 8
    p3, q3, p4 = (n3[0], R3, 128), (n3[0] + 2, R3, 128), (n3[0] // 2, R3 // 2, 128)
    z, az, sums = run(
        k_up,
        (sds(48, 24, 128), sds(48, 24, 128), sds(count, 128)),
        (g, maps, f2w, c2w, e2w, f1w, c1w, e1w, f0, c0, d0, e0),
        [q3, q3, p3, p3, p3, (n3[0] // 2, R3, 128), p4, p4, (sizes[0] * sizes[1], 128, 128), (9, 16, 128), (18, 16, 128),
         (18, 16, 128), (18, 16, 128), (27, 16, 128), q2, q2, q1, q1, q0, q0],
        mib=M2,
    )
    sums = lax.all_to_all(sums.reshape(count, 1, 128), ALL, 0, 0, tiled=True).reshape(count, 128)
    return run(
        k_last,
        (sds(48, 48, 48), sds(48, 48, 48)),
        (sums, own, z, az, f0),
        [(48, 48, 48), (48, 48, 48), pltpu.SemaphoreType.DMA((2, 6))],
        far_out=True,
    )


def solution(mesh):
    spec = P("gx", "gy", "gz")
    return jax.shard_map(body, mesh=mesh, in_specs=(spec, spec, spec), out_specs=(spec, spec), check_vma=False)
```

```python
import functools
import jax
import jax.numpy as jnp
from jax import lax
from jax.experimental import pallas as pl
from jax.experimental.pallas import tpu as pltpu
from jax.sharding import PartitionSpec as P

W = 6.0 / 7.0
BOTTOM_ITERS = 6
N0 = 48
F32 = jnp.float32
HI = lax.Precision.HIGHEST
M0, M1, M2 = 10, 8, 12
UF, UR, UM, UZ, UL = 12, 27, 18, 12, 6


class Spec:
    def __init__(self, n, h, na, R, o, hx, cut, kp, st):
        self.n, self.h, self.na, self.R, self.o, self.hx, self.cut, self.kp, self.st = n, h, na, R, o, hx, cut, kp, st
        self.half = n // 2
        self.zshape = (n // (kp * st), self.half * st, 128)
        self.yshape = (self.half, na * h, 128)
        self.hs = (h,) * na
        self.xshape = (hx, na, R, 128)
        self.nx = n + hx

    def slot(self, x, a):
        if self.st == 1:
            h = self.hs[a]
            many = 64 // h
            return ZBASE[a] + lax.div(x, many), 0, h * lax.rem(x, many)
        per = self.n // self.st
        t, y = lax.div(x, per), lax.rem(x, per)
        return lax.div(y, self.kp), t, self.h * (lax.rem(y, self.kp) * self.na + a)


L0 = Spec(48, 5, 3, 32, 8, 6, 56, 4, 1)
L1 = Spec(24, 12, 2, 24, 12, 12, 44, 2, 2)
L0.hs = (5, 4, 4)
ZBASE = (0, 4, 7)
YBASE = (0, 40, 72)
L0.zshape = (10, 24, 128)
L0.yshape = (3, 104, 128)


def sds(*shape, dtype=F32):
    return jax.ShapeDtypeStruct(shape, dtype)


def run(kernel, outs, args, scratch=(), mib=12, far_in=False, far_out=False):
    vmem = pl.BlockSpec(memory_space=pltpu.VMEM)
    hbm = pl.BlockSpec(memory_space=pl.ANY)
    return pl.pallas_call(
        kernel,
        out_shape=outs,
        in_specs=[hbm if far_in else vmem] * len(args),
        out_specs=jax.tree.map(lambda _: hbm if far_out else vmem, outs),
        scratch_shapes=[pltpu.VMEM(s, F32) if isinstance(s, tuple) else s for s in scratch],
        compiler_params=pltpu.CompilerParams(vmem_limit_bytes=mib * 1024 * 1024),
    )(*args)


def place():
    return [lax.axis_index(a) for a in ("gx", "gy", "gz")] + [lax.axis_size(a) for a in ("gy", "gz")]


def lanes(rows):
    return lax.broadcasted_iota(jnp.int32, (rows, 128), 1)


def roll(v, shift, axis):
    if isinstance(shift, int):
        shift = shift % v.shape[axis]
        if shift == 0:
            return v
    return pltpu.roll(v, shift, axis)


def loop(n, f, u=1):
    u = max(d for d in range(1, u + 1) if n % d == 0)

    def some(i, c):
        for k in range(u):
            f(i * u + k)
        return c

    lax.fori_loop(0, n // u, some, 0)


def upper(sp, rows):
    l = lanes(rows)
    return (l >= sp.cut) & (l < sp.cut + 64)


def edge(sp, ids):
    _, gy, gz, ny, nz = ids
    high = jnp.where(gz < nz - 1, sp.n + sp.h, sp.n)
    low = jnp.where(gz > 0, 64 - sp.h, 64)
    return high, low, jnp.where(gy > 0, 1.0, 0.0), jnp.where(gy < ny - 1, 1.0, 0.0)


def ztile(sp, items):
    l = lanes(sp.half)
    hi = [jnp.zeros((sp.half, 128), F32)] * 2
    lo = list(hi)
    for k, (v, at, h) in enumerate(items):
        r = roll(v, at, 1)
        hi[k % 2] = jnp.where(((l + (64 - (at + sp.n - h) % 64)) & 63) < h, r, hi[k % 2])
        lo[k % 2] = jnp.where(((l + (64 - at)) & 63) < h, r, lo[k % 2])
    return roll(hi[0] + hi[1], -2 * sp.n, 1), lo[0] + lo[1]


def ztile1(own, hi_ref, lo_ref, g):
    sp = L1
    for t in range(sp.st):
        items = [
            (own(t * (sp.n // sp.st) + g * sp.kp + k, a), sp.h * (k * sp.na + a), sp.h)
            for k in range(sp.kp)
            for a in range(sp.na)
        ]
        hi, lo = ztile(sp, items)
        hi_ref[g, t * sp.half : (t + 1) * sp.half, :] = hi
        lo_ref[g, t * sp.half : (t + 1) * sp.half, :] = lo


def merged(sp, own, zl, zh, x, a, b, e, top, bottom):
    g, t, at = sp.slot(x, a)
    if sp.st == 1:
        high, low = zh[g, b:e, :], zl[g, b:e, :]
    else:
        high = jnp.where(t == 0, zh[g, b:e, :], zh[g, sp.half + b : sp.half + e, :])
        low = jnp.where(t == 0, zl[g, b:e, :], zl[g, sp.half + b : sp.half + e, :])
    l = lanes(e - b)
    beside = jnp.where(((l + (64 - at)) & 63) < sp.hs[a], high, low)
    beside = roll(beside, (sp.n + 128 - at) & 127, 1)
    q = l & 63
    return jnp.where(q < sp.n, own(x, a)[b:e], jnp.where((q < top) | (q >= bottom), beside, 0.0))


def ypack0(own, turned, zl, zh, up_ref, dn_ref):
    top, bottom, _, _ = edge(L0, place())
    l = lanes(8)
    q = l & 63
    up = upper(L0, 8)

    def beside(x, a, b, turn):
        g, _, at = L0.slot(x, a)
        v = jnp.where(((l + (64 - at)) & 63) < L0.hs[a], zh[g, b : b + 8, :], zl[g, b : b + 8, :])
        v = roll(v, (L0.n + turn + 128 - at) & 127, 1)
        return jnp.where((q < top) | (q >= bottom), v, 0.0)

    def some(i):
        for k in range(8):
            p = 8 * i + k
            for a in range(3):
                h = L0.hs[a]
                for ref, b, s in ((up_ref, 16, 8 - h), (dn_ref, 0, 0)):
                    even = jnp.where(q < L0.n, own[a, 2 * p, b : b + 8, :], beside(2 * p, a, b, 0))
                    odd = jnp.where(q < L0.n, turned[a, p, b // 2 : b // 2 + 8, :], beside(2 * p + 1, a, b, 64))
                    v = jnp.where(up, even, odd) if b else jnp.where(up, odd, even)
                    ref[i, pl.ds(YBASE[a] + k, h, stride=8), :] = v[s : s + h]

    loop(3, some)


def ypack1(own, zl, zh, up_ref, dn_ref, u):
    sp = L1
    half = sp.half
    top, bottom, _, _ = edge(sp, place())

    def pair(p):
        for a in range(sp.na):
            even = merged(sp, own, zl, zh, 2 * p, a, 0, half, top, bottom)
            odd = roll(merged(sp, own, zl, zh, 2 * p + 1, a, 0, half, top, bottom), 64, 1)
            up = upper(sp, half)
            up_ref[p, a * half : (a + 1) * half, :] = jnp.where(up, even, odd)
            dn_ref[p, a * half : (a + 1) * half, :] = jnp.where(up, odd, even)

    loop(half, pair, u)


def y_tiles0(yl, yh, g, t, a):
    def rows(ref, start):
        return ref[g, pl.ds(start + t, 8, stride=8), :]

    if a == 0:
        return roll(rows(yl, 0), 3, 0), rows(yh, 0)
    return rows(yl, YBASE[a] - 32), rows(yh, 40) if a == 1 else roll(rows(yh, 40), 4, 0)


def plane0(m, tiles, ends, turn):
    _, _, below, above = ends
    low, high = tiles
    lower = jnp.concatenate([roll(low, turn, 1) * below, m], axis=0)
    higher = jnp.concatenate([m, roll(high, turn, 1) * above], axis=0)
    return jnp.where(upper(L0, L0.R), higher, lower)


def plane1(own, zl, zh, yl, yh, x, a, dst, xw, ends, spare):
    top, bottom, below, above = ends
    sp = L1
    h, half = sp.h, sp.half
    m = merged(sp, own, zl, zh, x, a, 0, half, top, bottom)
    p = lax.div(x, 2)
    turn = 64 * (1 - lax.rem(x, 2))
    spare[0, 0:h, :] = roll(yl[p, a * h : (a + 1) * h, :], turn, 1) * below
    spare[0, h:, :] = m
    spare[1, 0:half, :] = m
    spare[1, half:, :] = roll(yh[p, a * h : (a + 1) * h, :], turn, 1) * above
    dst[xw] = jnp.where(upper(sp, sp.R), spare[1], spare[0])


def lane_z(sp, l):
    return jnp.where(l < sp.cut, l, jnp.where(l < sp.cut + 64, l - 64, l - 128))


def inside(sp, ids):
    _, gy, gz, ny, nz = ids
    n, h = sp.n, min(sp.hs)
    y = lax.broadcasted_iota(jnp.int32, (sp.R, 128), 0) - sp.o + jnp.where(upper(sp, sp.R), sp.R, 0)
    z = lane_z(sp, lanes(sp.R))
    ok = (y >= -h) & (y < n + h) & (z >= -h) & (z < n + h)
    y, z = y + gy * n, z + gz * n
    return ok & (y >= 0) & (y < ny * n) & (z >= 0) & (z < nz * n)


def paired(ref, x):
    c = ref[x + 1]
    R = c.shape[0]
    s = ref[x] + ref[x + 2]
    sub = lax.broadcasted_iota(jnp.int32, (8, 128), 0)
    seam = roll(jnp.where(sub == 0, c[0:8], c[R - 8 : R]), 64, 1)
    last = jnp.where(sub == 7, roll(seam, 7, 0), roll(c[R - 8 :], 7, 0))
    first = jnp.where(sub == 0, roll(seam, 1, 0), roll(c[0:8], 1, 0))
    up = jnp.concatenate([ref[x + 1, 1 : R - 7, :], last], axis=0)
    down = jnp.concatenate([first, ref[x + 1, 7 : R - 1, :]], axis=0)
    s = s + (up + down)
    return s + (roll(c, 1, 1) + roll(c, 127, 1))


def domain(sp, n, h, r0, R, ids):
    row = lax.broadcasted_iota(jnp.int32, (R, 128), 0) - r0
    ln = lanes(R)
    z = jnp.where(ln < 64, ln, ln - 128)
    gy, gz, ny, nz = ids[1], ids[2], ids[3], ids[4]
    y_at, z_at = row + gy * n, z + gz * n
    ok = (row >= -h) & (row < n + h) & (z >= -h) & (z < n + h)
    return ok & (y_at >= 0) & (y_at < ny * n) & (z_at >= 0) & (z_at < nz * n)


def neighbours(ref, x):
    c = ref[x + 1]
    R = c.shape[0]
    s = ref[x] + ref[x + 2]
    s = s + (roll(c, 1, 0) + roll(c, R - 1, 0))
    return s + (roll(c, 1, 1) + roll(c, 127, 1))


def zero_ends(ref, n):
    ref[0] = jnp.zeros(ref.shape[1:], F32)
    ref[n + 1] = jnp.zeros(ref.shape[1:], F32)


def relax(src, dst, f, c, n, factor, u=9, near=None):
    near = near or neighbours

    def one(x):
        dst[x + 1] = (1.0 - W) * src[x + 1] + c[x] * (f[x] + factor * near(src, x))

    loop(n, one, u)


def lane_map(pick, value):
    l = lax.broadcasted_iota(jnp.int32, (256, 128), 0) & 127
    m = lax.broadcasted_iota(jnp.int32, (256, 128), 1)
    return jnp.where(pick(l) == m, value, 0.0).astype(jnp.bfloat16)


def spread_map(pick):
    m = lax.broadcasted_iota(jnp.int32, (256, 128), 0) & 127
    l = lax.broadcasted_iota(jnp.int32, (256, 128), 1)
    return jnp.where(pick(l) == m, 1.0, 0.0).astype(jnp.bfloat16)


def floor_half(z):
    return lax.shift_right_arithmetic(z, 1)


def coarse_lane(sp, l, want):
    z = lane_z(sp, l)
    up = (l >= sp.cut) & (l < sp.cut + 64)
    good = (z >= -sp.h) & (z < sp.n + sp.h)
    good = good & (up if want else jnp.logical_not(up))
    return jnp.where(good, floor_half(z) + jnp.where(z < 0, 128, 0), -1)


def both_lanes(l):
    lower, higher = coarse_lane(L0, l, False), coarse_lane(L0, l, True)
    return jnp.where(lower >= 0, lower, jnp.where(higher >= 0, (higher + 64) & 127, -1))


OWN, DOWN1A, DOWN1B, DOWN2, DOWN3, UP3, UP2, UP1A, UP1B, UP0 = range(10)


def all_maps(maps, gz):
    half = floor_half
    maps[OWN] = lane_map(lambda l: jnp.where(l < 64, half(l), 32 + half(l)), 0.125)
    maps[DOWN1A] = lane_map(lambda l: coarse_lane(L1, l, False), 0.125)
    maps[DOWN1B] = lane_map(lambda l: coarse_lane(L1, l, True), 0.125)
    maps[DOWN2] = lane_map(lambda l: jnp.where(l < 64, half(l), half(l) + 64), 0.125)
    maps[DOWN3] = lane_map(half, 0.125)
    maps[UP3] = spread_map(half)
    maps[UP2] = spread_map(lambda l: gz * 6 + jnp.where(l < 64, half(l), half(l) - 64))
    maps[UP1A] = spread_map(lambda l: coarse_lane(L1, l, False))
    maps[UP1B] = spread_map(lambda l: coarse_lane(L1, l, True))
    maps[UP0] = spread_map(both_lanes)


def times(v, m):
    big = v.astype(jnp.bfloat16)
    rest = (v - big.astype(F32)).astype(jnp.bfloat16)
    return jnp.dot(jnp.concatenate([big, rest], axis=1), m, preferred_element_type=F32)


def coarsen_planes(pair, n, tmp, acc, rows, u=2):
    half = rows // 2

    def one(x):
        tmp[x, 0:rows, :] = pair(x)
        acc[x, 0:half, :] = tmp[x, pl.ds(0, half, stride=2), :] + tmp[x, pl.ds(1, half, stride=2), :]

    loop(n, one, u)


def flat(ref):
    n, rows, _ = ref.shape
    return ref[...].reshape(n * rows, 128)


def add_refined(wide, n, src, dst, u=3):
    R = dst.shape[1]

    def one(i):
        v = wide[i, 0 : R // 2, :]
        for k in range(2):
            dst[2 * i + 1, pl.ds(k, R // 2, stride=2), :] = v
        t = dst[2 * i + 1]
        dst[2 * i + 1] = src[2 * i + 1] + t
        dst[2 * i + 2] = src[2 * i + 2] + t

    loop(n, one, u)


def k_zpack0(x0, b, rea, hi, lo, own, raw, sems):
    def copy(a, ref, i):
        many = 64 // L0.hs[a]
        part = pl.ds(i * many, many)
        return pltpu.make_async_copy(ref.at[part], raw.at[a, part], sems.at[a, i])

    refs = (x0, b, rea)
    parts = [48 * h // (64 // h * h) for h in L0.hs]
    for a, ref in enumerate(refs):
        for i in range(parts[a]):
            copy(a, ref, i).start()

    def pack(a, i):
        h = L0.hs[a]
        many = 64 // h
        hi[ZBASE[a] + i], lo[ZBASE[a] + i] = ztile(L0, [(own[a, i * many + k], h * k, h) for k in range(many)])

    steps = [(a, ref, i) for a, ref in enumerate(refs) for i in range(parts[a])]
    for n, (a, ref, i) in enumerate(steps):
        copy(a, ref, i).wait()
        if n:
            pack(steps[n - 1][0], steps[n - 1][2])
        many = 64 // L0.hs[a]
        for x in range(i * many, i * many + many):
            own[a, x, :, 0:48] = raw[a, x, 0:24, :]
            own[a, x, :, 64:112] = raw[a, x, 24:48, :]
    pack(steps[-1][0], steps[-1][2])


def k_ypack0(own, turned, zl, zh, up, dn):
    ypack0(own, turned, zl, zh, up, dn)


def k_xpack0(mid, yl, yh, out):
    ids = place()
    ends = edge(L0, ids)
    first = ids[0] == 0
    for i in range(6):
        x = jnp.where(first, 42, 0) + i
        for a in range(3):
            there, here = y_tiles0(yl, yh, 2, 5 + i // 2, a), y_tiles0(yl, yh, 0, i // 2, a)
            tiles = [jnp.where(first, v, w) for v, w in zip(there, here)]
            out[i, a] = plane0(mid[a, x], tiles, ends, 64 * (1 - i % 2))


def k_xpack1(f1, r1, zl, zh, yl, yh, out, spare):
    both = (f1, r1)
    ids = place()
    ends = edge(L1, ids)

    def one(i):
        for a in range(2):
            plane1(lambda x, a: both[a][x], zl, zh, yl, yh, (1 - ids[0]) * 12 + i, a, out.at[i], a, ends, spare.at[a])

    loop(12, one, 2)


def beside0(c):
    R = L0.R
    sub = lax.broadcasted_iota(jnp.int32, (8, 128), 0)
    seam = roll(jnp.where(sub == 0, c[0:8], c[R - 8 : R]), 64, 1)
    up, down = roll(c, R - 1, 0), roll(c, 1, 0)
    up = jnp.concatenate([up[: R - 8], jnp.where(sub == 7, roll(seam, 7, 0), up[R - 8 :])], axis=0)
    down = jnp.concatenate([jnp.where(sub == 0, roll(seam, 1, 0), down[0:8]), down[8:]], axis=0)
    return (up + down) + (roll(c, 1, 1) + roll(c, 127, 1))


def k_windows0(mid, yl, yh, xw, part, d_out, c_out):
    ids = place()
    ends = edge(L0, ids)
    ok = inside(L0, ids)

    def some(i):
        for k in range(16):
            x = 16 * i + k
            v, b, rea = (plane0(mid[a, x], y_tiles0(yl, yh, i, k // 2, a), ends, 64 * (1 - k % 2)) for a in range(3))
            d = 6.0 + rea
            xw[x] = v
            part[x] = b - d * v + beside0(v)
            d_out[x] = d
            c_out[x] = jnp.where(ok, W / d, 0.0)

    loop(3, some)


def own_rows(sp, v):
    return jnp.where(upper(sp, sp.half), v[0 : sp.half], v[sp.o :])


def half_own(pair, tmp, acc, out, u, m):
    coarsen_planes(pair, 24, tmp, acc, 24, u)
    acc[...] = times(flat(acc), m).reshape(24, 16, 128)

    def keep(x):
        out[x] = acc[x, 0:12, :]

    loop(24, keep, 6)


def k_zmerge(own, zl, zh, up, out):
    top, bottom, _, _ = edge(L0, place())

    def one(x):
        for a in range(3):
            out[a, x] = merged(L0, lambda x, a: own[a, x], zl, zh, x, a, 0, 24, top, bottom)

    loop(48, one, 8)


def k_early(own, turned, r1, maps, tmp, acc):
    def turn(p):
        for a in range(3):
            v = own[a, 2 * p + 1]
            turned[a, p, 0:8, :] = roll(v[0:8], 64, 1)
            turned[a, p, 8:16, :] = roll(v[16:24], 64, 1)

    loop(24, turn, 4)
    all_maps(maps, lax.axis_index("gz"))
    mine = lanes(24) % 64 < 48
    half_own(lambda x: jnp.where(mine, own[2, 2 * x] + own[2, 2 * x + 1], 0.0), tmp, acc, r1, 4, maps[OWN])


def k_down0(xw, part, d, cw, r1, maps, xr, f_out, c_out, e_out, f1, z1h, z1l, xb, ew, tmp, acc):
    ids = place()
    n = L0.nx
    shift = ids[0] * L0.hx
    other = (1 - ids[0]) * L0.n
    low_side = ids[0] == 0
    ok = inside(L0, ids)
    zero_ends(ew, n)
    zero_ends(e_out, n)
    zero = jnp.zeros((L0.R, 128), F32)
    xb[0] = jnp.where(low_side, xw[47], zero)
    xb[7] = jnp.where(low_side, zero, xw[0])
    for i in range(6):
        xb[i + 1] = xr[i, 0]

    def put(w, f, c):
        f_out[w] = f
        c_out[w] = c
        ew[w + 1] = c * f

    def mine(x):
        put(x + shift, part[x] + (xw[x - 1] + xw[x + 1]), cw[x])

    loop(46, lambda i: mine(i + 1), 23)
    put(shift, part[0] + (jnp.where(low_side, zero, xr[5, 0]) + xw[1]), cw[0])
    put(47 + shift, part[47] + (xw[46] + jnp.where(low_side, xr[0, 0], zero)), cw[47])

    def theirs(i):
        v = xb[i + 1]
        dd = 6.0 + xr[i, 2]
        f = xr[i, 1] - dd * v + beside0(v) + (xb[i] + xb[i + 2])
        put(i + other, f, jnp.where(ok, W / dd, 0.0))

    loop(6, theirs, 6)
    relax(ew, e_out, f_out, c_out, n, 1.0, UR, paired)

    def left(x):
        return own_rows(L0, f_out[x + shift] - d[x] * e_out[x + shift + 1] + paired(e_out, x + shift))

    within = lanes(24) % 64 < 48
    pair = lambda x: jnp.where(within, left(2 * x) + left(2 * x + 1), 0.0)
    half_own(pair, tmp, acc, f1, UL, maps[OWN])
    both = (f1, r1)
    loop(6, lambda g: ztile1(lambda x, a: both[a][x], z1h, z1l, g), 3)


def k_ypack1(f1, r1, zl, zh, up, dn):
    both = (f1, r1)
    ypack1(lambda x, a: both[a][x], zl, zh, up, dn, 6)


def k_windows1(f1, r1, zl, zh, yl, yh, out, spare):
    both = (f1, r1)
    ends = edge(L1, place())

    def some(i):
        for k in range(4):
            for a in range(2):
                plane1(lambda x, a: both[a][x], zl, zh, yl, yh, 4 * i + k, a, out.at[a], 4 * i + k, ends, spare.at[2 * k + a])

    loop(6, some)


def k_down1(win, maps, xr, fw, cw, e_out, f2, c2, e2, out3, rw, ew, tmp, acc, r2, ew2, tmp2, t3, sq):
    ids = place()
    n = L1.nx
    shift = ids[0] * L1.hx
    other = (1 - ids[0]) * L1.n

    def put(x):
        fw[x + shift] = win[0, x]
        rw[x + shift] = win[1, x]

    def take(x):
        fw[x + other] = xr[x, 0]
        rw[x + other] = xr[x, 1]

    loop(24, put, 8)
    loop(12, take, 6)
    ok = inside(L1, ids)
    zero_ends(ew, n)
    zero_ends(e_out, n)

    def first(x):
        c = jnp.where(ok, W / (1.5 + rw[x]), 0.0)
        cw[x] = c
        ew[x + 1] = c * fw[x]

    loop(n, first, 6)
    relax(ew, e_out, fw, cw, n, 0.25, UM, paired)

    def left(x):
        return fw[x] - (1.5 + rw[x]) * e_out[x + 1] + 0.25 * paired(e_out, x)

    for ref, pair in ((f2, lambda x: left(2 * x) + left(2 * x + 1)), (r2, lambda x: rw[2 * x] + rw[2 * x + 1])):
        coarsen_planes(pair, 18, tmp, acc.at[0], 24, 9)
        v = flat(acc.at[0])
        acc[0] = times(v, maps[DOWN1A]).reshape(18, 16, 128)
        acc[1] = times(v, maps[DOWN1B]).reshape(18, 16, 128)

        def keep(x, ref=ref):
            ref[x] = jnp.zeros((32, 128), F32)
            ref[x, 2:14, :] = acc[0, x, 0:12, :]
            ref[x, 14:26, :] = acc[1, x, 0:12, :]

        loop(18, keep, 6)
    ok2 = domain(None, 12, 6, 8, 32, ids)
    zero_ends(ew2, 18)
    zero_ends(e2, 18)

    def second(x):
        c = jnp.where(ok2, W / (0.375 + r2[x]), 0.0)
        c2[x] = c
        ew2[x + 1] = c * f2[x]

    loop(18, second, 6)
    relax(ew2, e2, f2, c2, 18, 0.0625, 18)

    def left2(x):
        return f2[x] - (0.375 + r2[x]) * e2[x + 1] + 0.0625 * neighbours(e2, x)

    for a, pair in enumerate((lambda x: left2(2 * x) + left2(2 * x + 1), lambda x: r2[2 * x] + r2[2 * x + 1])):
        coarsen_planes(pair, 9, tmp2, t3.at[a], 32, 9)
        t3[a] = times(flat(t3.at[a]), maps[DOWN2]).reshape(9, 16, 128)
    shift = ids[0] * 3
    sq[...] = jnp.zeros((128, 128), F32)
    for a in range(2):
        for x in range(6):
            at = a * 36 + x * 6
            sq[at : at + 6, :] = t3[a, x + shift, 4:10, :]
    t = sq[...].T[0:8]
    ln = lanes(1)
    rows = []
    for u in range(2):
        for a in range(2):
            parts = [roll(t, 36 * (w - a), 1)[3 * u + w : 3 * u + w + 1] for w in range(3)]
            rows.append(jnp.where(ln < 36, parts[0], jnp.where(ln < 72, parts[1], parts[2])))
    tile = jnp.concatenate(rows + rows, axis=0)
    n8 = out3.shape[0] // 8
    out3[...] = jnp.broadcast_to(tile[None], (n8, 8, 128)).reshape(n8 * 8, 128)


def sum_all(v):
    s = jnp.sum(v, axis=0)
    s = sum(s[k : k + 8] for k in range(0, s.shape[0], 8))
    return jnp.sum(jnp.sum(s, axis=1, keepdims=True), axis=0, keepdims=True)


def coarse_solve(g3, maps, nx, ny, nz, e3, s3, f3, c3, r3, tmp, f4, r4, sq):
    R = f3.shape[1]
    for ref in (f3, r3):
        ref[...] = jnp.zeros(ref.shape, F32)
    kx, ky, kz = nx // 6, ny // 6, nz // 6
    for bx in range(kx):
        for by in range(ky):
            k = bx * ky + by
            if kz * 6 < 128:
                sq[k, kz * 6 :, :] = jnp.zeros((128 - kz * 6, 128), F32)
            got = [g3[pl.ds(k * kz * 4 + r, kz, stride=4), :] for r in range(4)]
            ln = lanes(kz)
            for u in range(2):
                for w in range(3):
                    f, r = roll(got[2 * u], -36 * w, 1), roll(got[2 * u + 1], 36 - 36 * w, 1)
                    sq[k, pl.ds(3 * u + w, kz, stride=6), :] = jnp.where(ln < 36, f, r)
            t = sq[k].T
            for x in range(6):
                f3[bx * 6 + x, by * 6 : by * 6 + 6, :] = t[x * 6 : x * 6 + 6]
                r3[bx * 6 + x, by * 6 : by * 6 + 6, :] = t[36 + x * 6 : 42 + x * 6]
    factor = 0.25**3
    ok = (lax.broadcasted_iota(jnp.int32, (R, 128), 0) < ny) & (lanes(R) < nz)
    for ref in (e3, s3):
        zero_ends(ref, nx)

    def first(x):
        c = jnp.where(ok, W / (6.0 * factor + r3[x]), 0.0)
        c3[x] = c
        s3[x + 1] = c * f3[x]

    loop(nx, first, 6)
    relax(s3, e3, f3, c3, nx, factor, 12)

    def left(x):
        v = f3[x] - (6.0 * factor + r3[x]) * e3[x + 1] + factor * neighbours(e3, x)
        return jnp.where(ok, v, 0.0)

    for ref, pair in ((f4, lambda x: left(2 * x) + left(2 * x + 1)), (r4, lambda x: r3[2 * x] + r3[2 * x + 1])):
        coarsen_planes(pair, nx // 2, tmp, ref, R, 6)
        ref[...] = times(flat(ref), maps[DOWN3]).reshape(ref.shape)
    f4k = 0.25**4
    H = R // 2
    row = lax.broadcasted_iota(jnp.int32, (nx // 2, H, 128), 1)
    lane = lax.broadcasted_iota(jnp.int32, (nx // 2, H, 128), 2)
    within = (row < ny // 2) & (lane < nz // 2)
    diag = 6.0 * f4k + r4[...]
    zero = jnp.zeros((1, H, 128), F32)

    def apply(p):
        s = jnp.concatenate([zero, p[:-1]], axis=0) + jnp.concatenate([p[1:], zero], axis=0)
        s = s + roll(p, 1, 1) + roll(p, H - 1, 1) + roll(p, 1, 2) + roll(p, 127, 2)
        return jnp.where(within, diag * p - f4k * s, 0.0)

    r = jnp.where(within, f4[...], 0.0)
    p = r
    q = apply(r)
    rr = sum_all(r * r)
    den = sum_all(r * q)
    a = rr / den
    one_over_rr, one_over_a = 1.0 / rr, den / rr
    e = a * p
    for i in range(1, BOTTOM_ITERS):
        r = r - a * q
        w = apply(r)
        new = sum_all(r * r)
        rw = sum_all(r * w)
        b = new * one_over_rr
        den = rw - b * new * one_over_a
        a = new / den
        one_over_rr, one_over_a = 1.0 / new, den / new
        p = r + b * p
        q = w + b * q
        e = e + a * p
    f4[...] = times(e.reshape(nx // 2 * H, 128), maps[UP3]).reshape(e.shape)
    add_refined(f4, nx // 2, e3, s3, 6)
    relax(s3, e3, f3, c3, nx, factor, 12)
    relax(e3, s3, f3, c3, nx, factor, 12)


def k_up(g3, maps, f2, c2, e2i, f1, c1, e1i, f0, c0, d0, e0i, z_out, az_out, sums,
         e3, s3, f3, c3, r3, tmp3, f4, r4, sq, w3, w2, na, nb, n1, e2, s2, e1, s1, e0, s0):
    gx, gy, gz, sy, sz = place()
    nx, ny, nz = f3.shape[0], sy * 6, sz * 6
    coarse_solve(g3, maps, nx, ny, nz, e3, s3, f3, c3, r3, tmp3, f4, r4, sq)
    for ref, n in ((s2, 18), (s1, 36), (s0, 54), (e2, 18), (e1, 36), (e0, 54)):
        zero_ends(ref, n)
    for i in range(9):
        e = s3[i + 1 + gx * 3]
        e = jnp.concatenate([jnp.zeros((8, 128), F32), e, jnp.zeros((8, 128), F32)], axis=0)
        v = e[4:20]
        for k in range(1, sy):
            v = jnp.where(gy == k, e[6 * k + 4 : 6 * k + 20], v)
        w3[i] = v
    w3[...] = times(flat(w3), maps[UP2]).reshape(9, 16, 128)
    add_refined(w3, 9, e2i, e2, 9)
    relax(e2, s2, f2, c2, 18, 0.0625, 18)
    relax(s2, e2, f2, c2, 18, 0.0625, 18)

    def halves(i):
        na[i] = e2[i + 1, 2:18, :]
        nb[i] = e2[i + 1, 14:30, :]

    loop(18, halves, 6)

    w2[...] = (times(flat(na), maps[UP1A]) + times(flat(nb), maps[UP1B])).reshape(18, 16, 128)
    add_refined(w2, 18, e1i, e1, 6)
    relax(e1, s1, f1, c1, 36, 0.25, UM, paired)
    relax(s1, e1, f1, c1, 36, 0.25, UM, paired)

    def near(i):
        v = e1[i + 1 + gx * 9]
        n1[i] = jnp.where(upper(L1, 16), v[0:16], v[8:24])

    loop(27, near, 9)

    n1[...] = times(flat(n1), maps[UP0]).reshape(27, 16, 128)
    add_refined(n1, 27, e0i, e0, 9)
    relax(e0, s0, f0, c0, 54, 1.0, UR, paired)
    relax(s0, e0, f0, c0, 54, 1.0, UR, paired)
    shift = gx * 6
    mine = lanes(24) % 64 < 48

    def last(x, carry):
        u, v = carry
        w = x + shift
        z = e0[w + 1]
        az = own_rows(L0, d0[x] * z - paired(e0, w))
        z = own_rows(L0, z)
        f = own_rows(L0, f0[w])
        z_out[x] = z
        az_out[x] = az
        return u + jnp.where(mine, f * z, 0.0), v + jnp.where(mine, z * az, 0.0)

    def some(i, carry):
        for k in range(UZ):
            carry = last(UZ * i + k, carry)
        return carry

    zero = jnp.zeros((24, 128), F32)
    u, v = lax.fori_loop(0, 48 // UZ, some, (zero, zero))

    def total(t):
        return jnp.sum(jnp.sum(t, axis=1, keepdims=True), axis=0, keepdims=True)

    ln = lanes(sums.shape[0])
    sums[...] = jnp.where(ln == 0, total(u), jnp.where(ln == 1, total(v), 0.0))


def k_last(sums, own, z, az, f, sol, res, sv, rv, sems):
    s = jnp.sum(sums[...], axis=0, keepdims=True)
    ln = lanes(1)
    over = jnp.sum(jnp.where(ln == 0, s, 0.0), axis=1, keepdims=True)
    under = jnp.sum(jnp.where(ln == 1, s, 0.0), axis=1, keepdims=True)
    step = over / under
    shift = lax.axis_index("gx") * 6
    pairs = ((0, sv, sol), (1, rv, res))

    def copy(a, src, dst, i):
        part = pl.ds(i * 8, 8)
        return pltpu.make_async_copy(src.at[part], dst.at[part], sems.at[a, i])

    def some(i):
        for k in range(8):
            x = i * 8 + k
            for ref, v in ((sv, own[0, x] + step * z[x]), (rv, own_rows(L0, f[x + shift]) - step * az[x])):
                ref[x, 0:24, :] = v[:, 0:48]
                ref[x, 24:48, :] = roll(v, 64, 1)[:, 0:48]
        for a, src, dst in pairs:
            copy(a, src, dst, i).start()

    loop(6, some)
    for i in range(6):
        for a, src, dst in pairs:
            copy(a, src, dst, i).wait()


def ring(up, dn, axis):
    n = lax.axis_size(axis)
    low = lax.ppermute(up, axis, [(i, (i + 1) % n) for i in range(n)])
    high = lax.ppermute(dn, axis, [(i, (i - 1) % n) for i in range(n)])
    return low, high


def swap(v):
    return lax.ppermute(v, "gx", [(0, 1), (1, 0)])


def body(b, x0, rea):
    ALL = ("gx", "gy", "gz")
    sizes = [lax.axis_size(a) for a in ALL]
    count = sizes[0] * sizes[1] * sizes[2]
    b, x0, rea = (pltpu.with_memory_space_constraint(v, pltpu.HBM) for v in (b, x0, rea))
    hi, lo, own = run(
        k_zpack0,
        (sds(*L0.zshape), sds(*L0.zshape), sds(3, 48, 24, 128)),
        (x0, b, rea),
        [(3, 48, 48, 48), pltpu.SemaphoreType.DMA((3, 4))],
        far_in=True,
    )
    zl, zh = ring(hi, lo, "gz")
    turned, r1, maps = run(
        k_early,
        (sds(3, 24, 16, 128), sds(24, 12, 128), sds(10, 256, 128, dtype=jnp.bfloat16)),
        (own,),
        [(24, 24, 128), (24, 16, 128)],
    )
    up, dn = run(k_ypack0, (sds(*L0.yshape),) * 2, (own, turned, zl, zh))
    yl, yh = ring(up, dn, "gy")
    mid = run(k_zmerge, sds(3, 48, 24, 128), (own, zl, zh, up))
    xr = swap(run(k_xpack0, sds(*L0.xshape), (mid, yl, yh)))
    p0, q0, o0 = (54, 32, 128), (56, 32, 128), (48, 32, 128)
    xw, part, d0, cw = run(k_windows0, (sds(*o0),) * 4, (mid, yl, yh))
    f0, c0, e0, f1, z1h, z1l = run(
        k_down0,
        (sds(*p0), sds(*p0), sds(*q0), sds(24, 12, 128), sds(*L1.zshape), sds(*L1.zshape)),
        (xw, part, d0, cw, r1, maps, xr),
        [(8, 32, 128), q0, (24, 24, 128), (24, 16, 128)],
        mib=M0,
    )
    zl, zh = ring(z1h, z1l, "gz")
    up, dn = run(k_ypack1, (sds(*L1.yshape),) * 2, (f1, r1, zl, zh))
    yl, yh = ring(up, dn, "gy")
    xr = swap(run(k_xpack1, sds(*L1.xshape), (f1, r1, zl, zh, yl, yh), [(2, 2, 24, 128)]))
    p1, q1, p2, q2 = (36, 24, 128), (38, 24, 128), (18, 32, 128), (20, 32, 128)
    win = run(k_windows1, sds(2, 24, 24, 128), (f1, r1, zl, zh, yl, yh), [(8, 2, 24, 128)])
    f1w, c1w, e1w, f2w, c2w, e2w, g = run(
        k_down1,
        (sds(*p1), sds(*p1), sds(*q1), sds(*p2), sds(*p2), sds(*q2), sds(count * 4, 128)),
        (win, maps, xr),
        [p1, q1, (18, 24, 128), (2, 18, 16, 128), p2, q2, (9, 32, 128), (2, 9, 16, 128), (128, 128)],
        mib=M1,
    )
    g = lax.all_to_all(g, ALL, 0, 0, tiled=True)
    n3 = [6 * s for s in sizes]
    R3 = (n3[1] + 8) // 8 * 8
    if R3 % 16:
        R3 += 8
    p3, q3, p4 = (n3[0], R3, 128), (n3[0] + 2, R3, 128), (n3[0] // 2, R3 // 2, 128)
    z, az, sums = run(
        k_up,
        (sds(48, 24, 128), sds(48, 24, 128), sds(count, 128)),
        (g, maps, f2w, c2w, e2w, f1w, c1w, e1w, f0, c0, d0, e0),
        [q3, q3, p3, p3, p3, (n3[0] // 2, R3, 128), p4, p4, (sizes[0] * sizes[1], 128, 128), (9, 16, 128), (18, 16, 128),
         (18, 16, 128), (18, 16, 128), (27, 16, 128), q2, q2, q1, q1, q0, q0],
        mib=M2,
    )
    sums = lax.all_to_all(sums.reshape(count, 1, 128), ALL, 0, 0, tiled=True).reshape(count, 128)
    return run(
        k_last,
        (sds(48, 48, 48), sds(48, 48, 48)),
        (sums, own, z, az, f0),
        [(48, 48, 48), (48, 48, 48), pltpu.SemaphoreType.DMA((2, 6))],
        far_out=True,
    )


def solution(mesh):
    spec = P("gx", "gy", "gz")
    return jax.shard_map(body, mesh=mesh, in_specs=(spec, spec, spec), out_specs=(spec, spec), check_vma=False)
```

```python
import functools
import jax
import jax.numpy as jnp
from jax import lax
from jax.experimental import pallas as pl
from jax.experimental.pallas import tpu as pltpu
from jax.sharding import PartitionSpec as P

W = 6.0 / 7.0
BOTTOM_ITERS = 6
N0 = 48
F32 = jnp.float32
HI = lax.Precision.HIGHEST
M0, M1, M2 = 10, 8, 12
UF, UR, UM, UZ, UL = 12, 27, 18, 12, 6


class Spec:
    def __init__(self, n, h, na, R, o, hx, cut, kp, st):
        self.n, self.h, self.na, self.R, self.o, self.hx, self.cut, self.kp, self.st = n, h, na, R, o, hx, cut, kp, st
        self.half = n // 2
        self.zshape = (n // (kp * st), self.half * st, 128)
        self.yshape = (self.half, na * h, 128)
        self.hs = (h,) * na
        self.xshape = (hx, na, R, 128)
        self.nx = n + hx

    def slot(self, x, a):
        if self.st == 1:
            h = self.hs[a]
            many = 64 // h
            return ZBASE[a] + lax.div(x, many), 0, h * lax.rem(x, many)
        per = self.n // self.st
        t, y = lax.div(x, per), lax.rem(x, per)
        return lax.div(y, self.kp), t, self.h * (lax.rem(y, self.kp) * self.na + a)


L0 = Spec(48, 5, 3, 32, 8, 6, 56, 4, 1)
L1 = Spec(24, 12, 2, 24, 12, 12, 44, 2, 2)
L0.hs = (5, 4, 4)
ZBASE = (0, 4, 7)
YBASE = (0, 40, 72)
L0.zshape = (10, 24, 128)
L0.yshape = (3, 104, 128)


def sds(*shape, dtype=F32):
    return jax.ShapeDtypeStruct(shape, dtype)


def run(kernel, outs, args, scratch=(), mib=12, far_in=False, far_out=False):
    vmem = pl.BlockSpec(memory_space=pltpu.VMEM)
    hbm = pl.BlockSpec(memory_space=pl.ANY)
    return pl.pallas_call(
        kernel,
        out_shape=outs,
        in_specs=[hbm if far_in else vmem] * len(args),
        out_specs=jax.tree.map(lambda _: hbm if far_out else vmem, outs),
        scratch_shapes=[pltpu.VMEM(s, F32) if isinstance(s, tuple) else s for s in scratch],
        compiler_params=pltpu.CompilerParams(vmem_limit_bytes=mib * 1024 * 1024),
    )(*args)


def place():
    return [lax.axis_index(a) for a in ("gx", "gy", "gz")] + [lax.axis_size(a) for a in ("gy", "gz")]


def lanes(rows):
    return lax.broadcasted_iota(jnp.int32, (rows, 128), 1)


def roll(v, shift, axis):
    if isinstance(shift, int):
        shift = shift % v.shape[axis]
        if shift == 0:
            return v
    return pltpu.roll(v, shift, axis)


def loop(n, f, u=1):
    u = max(d for d in range(1, u + 1) if n % d == 0)

    def some(i, c):
        for k in range(u):
            f(i * u + k)
        return c

    lax.fori_loop(0, n // u, some, 0)


def upper(sp, rows):
    l = lanes(rows)
    return (l >= sp.cut) & (l < sp.cut + 64)


def edge(sp, ids):
    _, gy, gz, ny, nz = ids
    high = jnp.where(gz < nz - 1, sp.n + sp.h, sp.n)
    low = jnp.where(gz > 0, 64 - sp.h, 64)
    return high, low, jnp.where(gy > 0, 1.0, 0.0), jnp.where(gy < ny - 1, 1.0, 0.0)


def ztile(sp, items):
    l = lanes(sp.half)
    hi = [jnp.zeros((sp.half, 128), F32)] * 2
    lo = list(hi)
    for k, (v, at, h) in enumerate(items):
        r = roll(v, at, 1)
        hi[k % 2] = jnp.where(((l + (64 - (at + sp.n - h) % 64)) & 63) < h, r, hi[k % 2])
        lo[k % 2] = jnp.where(((l + (64 - at)) & 63) < h, r, lo[k % 2])
    return roll(hi[0] + hi[1], -2 * sp.n, 1), lo[0] + lo[1]


def ztile1(own, hi_ref, lo_ref, g):
    sp = L1
    for t in range(sp.st):
        items = [
            (own(t * (sp.n // sp.st) + g * sp.kp + k, a), sp.h * (k * sp.na + a), sp.h)
            for k in range(sp.kp)
            for a in range(sp.na)
        ]
        hi, lo = ztile(sp, items)
        hi_ref[g, t * sp.half : (t + 1) * sp.half, :] = hi
        lo_ref[g, t * sp.half : (t + 1) * sp.half, :] = lo


def merged(sp, own, zl, zh, x, a, b, e, top, bottom):
    g, t, at = sp.slot(x, a)
    if sp.st == 1:
        high, low = zh[g, b:e, :], zl[g, b:e, :]
    else:
        high = jnp.where(t == 0, zh[g, b:e, :], zh[g, sp.half + b : sp.half + e, :])
        low = jnp.where(t == 0, zl[g, b:e, :], zl[g, sp.half + b : sp.half + e, :])
    l = lanes(e - b)
    beside = jnp.where(((l + (64 - at)) & 63) < sp.hs[a], high, low)
    beside = roll(beside, (sp.n + 128 - at) & 127, 1)
    q = l & 63
    return jnp.where(q < sp.n, own(x, a)[b:e], jnp.where((q < top) | (q >= bottom), beside, 0.0))


def ypack0(own, turned, zl, zh, up_ref, dn_ref):
    top, bottom, _, _ = edge(L0, place())
    l = lanes(8)
    q = l & 63
    up = upper(L0, 8)

    def beside(x, a, b, turn):
        g, _, at = L0.slot(x, a)
        v = jnp.where(((l + (64 - at)) & 63) < L0.hs[a], zh[g, b : b + 8, :], zl[g, b : b + 8, :])
        v = roll(v, (L0.n + turn + 128 - at) & 127, 1)
        return jnp.where((q < top) | (q >= bottom), v, 0.0)

    def some(i):
        for k in range(8):
            p = 8 * i + k
            for a in range(3):
                h = L0.hs[a]
                for ref, b, s in ((up_ref, 16, 8 - h), (dn_ref, 0, 0)):
                    even = jnp.where(q < L0.n, own[a, 2 * p, b : b + 8, :], beside(2 * p, a, b, 0))
                    odd = jnp.where(q < L0.n, turned[a, p, b // 2 : b // 2 + 8, :], beside(2 * p + 1, a, b, 64))
                    v = jnp.where(up, even, odd) if b else jnp.where(up, odd, even)
                    ref[i, pl.ds(YBASE[a] + k, h, stride=8), :] = v[s : s + h]

    loop(3, some)


def ypack1(own, zl, zh, up_ref, dn_ref, u):
    sp = L1
    half = sp.half
    top, bottom, _, _ = edge(sp, place())

    def pair(p):
        for a in range(sp.na):
            even = merged(sp, own, zl, zh, 2 * p, a, 0, half, top, bottom)
            odd = roll(merged(sp, own, zl, zh, 2 * p + 1, a, 0, half, top, bottom), 64, 1)
            up = upper(sp, half)
            up_ref[p, a * half : (a + 1) * half, :] = jnp.where(up, even, odd)
            dn_ref[p, a * half : (a + 1) * half, :] = jnp.where(up, odd, even)

    loop(half, pair, u)


def y_tiles0(yl, yh, g, t, a):
    def rows(ref, start):
        return ref[g, pl.ds(start + t, 8, stride=8), :]

    if a == 0:
        return roll(rows(yl, 0), 3, 0), rows(yh, 0)
    return rows(yl, YBASE[a] - 32), rows(yh, 40) if a == 1 else roll(rows(yh, 40), 4, 0)


def plane0(m, tiles, ends, turn):
    _, _, below, above = ends
    low, high = tiles
    lower = jnp.concatenate([roll(low, turn, 1) * below, m], axis=0)
    higher = jnp.concatenate([m, roll(high, turn, 1) * above], axis=0)
    return jnp.where(upper(L0, L0.R), higher, lower)


def plane1(own, zl, zh, yl, yh, x, a, dst, xw, ends, spare):
    top, bottom, below, above = ends
    sp = L1
    h, half = sp.h, sp.half
    m = merged(sp, own, zl, zh, x, a, 0, half, top, bottom)
    p = lax.div(x, 2)
    turn = 64 * (1 - lax.rem(x, 2))
    spare[0, 0:h, :] = roll(yl[p, a * h : (a + 1) * h, :], turn, 1) * below
    spare[0, h:, :] = m
    spare[1, 0:half, :] = m
    spare[1, half:, :] = roll(yh[p, a * h : (a + 1) * h, :], turn, 1) * above
    dst[xw] = jnp.where(upper(sp, sp.R), spare[1], spare[0])


def lane_z(sp, l):
    return jnp.where(l < sp.cut, l, jnp.where(l < sp.cut + 64, l - 64, l - 128))


def inside(sp, ids):
    _, gy, gz, ny, nz = ids
    n, h = sp.n, min(sp.hs)
    y = lax.broadcasted_iota(jnp.int32, (sp.R, 128), 0) - sp.o + jnp.where(upper(sp, sp.R), sp.R, 0)
    z = lane_z(sp, lanes(sp.R))
    ok = (y >= -h) & (y < n + h) & (z >= -h) & (z < n + h)
    y, z = y + gy * n, z + gz * n
    return ok & (y >= 0) & (y < ny * n) & (z >= 0) & (z < nz * n)


def paired(ref, x):
    c = ref[x + 1]
    R = c.shape[0]
    s = ref[x] + ref[x + 2]
    sub = lax.broadcasted_iota(jnp.int32, (8, 128), 0)
    seam = roll(jnp.where(sub == 0, c[0:8], c[R - 8 : R]), 64, 1)
    last = jnp.where(sub == 7, roll(seam, 7, 0), roll(c[R - 8 :], 7, 0))
    first = jnp.where(sub == 0, roll(seam, 1, 0), roll(c[0:8], 1, 0))
    up = jnp.concatenate([ref[x + 1, 1 : R - 7, :], last], axis=0)
    down = jnp.concatenate([first, ref[x + 1, 7 : R - 1, :]], axis=0)
    s = s + (up + down)
    return s + (roll(c, 1, 1) + roll(c, 127, 1))


def domain(sp, n, h, r0, R, ids):
    row = lax.broadcasted_iota(jnp.int32, (R, 128), 0) - r0
    ln = lanes(R)
    z = jnp.where(ln < 64, ln, ln - 128)
    gy, gz, ny, nz = ids[1], ids[2], ids[3], ids[4]
    y_at, z_at = row + gy * n, z + gz * n
    ok = (row >= -h) & (row < n + h) & (z >= -h) & (z < n + h)
    return ok & (y_at >= 0) & (y_at < ny * n) & (z_at >= 0) & (z_at < nz * n)


def neighbours(ref, x):
    c = ref[x + 1]
    R = c.shape[0]
    s = ref[x] + ref[x + 2]
    s = s + (roll(c, 1, 0) + roll(c, R - 1, 0))
    return s + (roll(c, 1, 1) + roll(c, 127, 1))


def zero_ends(ref, n):
    ref[0] = jnp.zeros(ref.shape[1:], F32)
    ref[n + 1] = jnp.zeros(ref.shape[1:], F32)


def relax(src, dst, f, c, n, factor, u=9, near=None):
    near = near or neighbours

    def one(x):
        dst[x + 1] = (1.0 - W) * src[x + 1] + c[x] * (f[x] + factor * near(src, x))

    loop(n, one, u)


def lane_map(pick, value):
    l = lax.broadcasted_iota(jnp.int32, (256, 128), 0) & 127
    m = lax.broadcasted_iota(jnp.int32, (256, 128), 1)
    return jnp.where(pick(l) == m, value, 0.0).astype(jnp.bfloat16)


def spread_map(pick):
    m = lax.broadcasted_iota(jnp.int32, (256, 128), 0) & 127
    l = lax.broadcasted_iota(jnp.int32, (256, 128), 1)
    return jnp.where(pick(l) == m, 1.0, 0.0).astype(jnp.bfloat16)


def floor_half(z):
    return lax.shift_right_arithmetic(z, 1)


def coarse_lane(sp, l, want):
    z = lane_z(sp, l)
    up = (l >= sp.cut) & (l < sp.cut + 64)
    good = (z >= -sp.h) & (z < sp.n + sp.h)
    good = good & (up if want else jnp.logical_not(up))
    return jnp.where(good, floor_half(z) + jnp.where(z < 0, 128, 0), -1)


def both_lanes(l):
    lower, higher = coarse_lane(L0, l, False), coarse_lane(L0, l, True)
    return jnp.where(lower >= 0, lower, jnp.where(higher >= 0, (higher + 64) & 127, -1))


OWN, DOWN1A, DOWN1B, DOWN2, DOWN3, UP3, UP2, UP1A, UP1B, UP0 = range(10)


def all_maps(maps, gz):
    half = floor_half
    maps[OWN] = lane_map(lambda l: jnp.where(l < 64, half(l), 32 + half(l)), 0.125)
    maps[DOWN1A] = lane_map(lambda l: coarse_lane(L1, l, False), 0.125)
    maps[DOWN1B] = lane_map(lambda l: coarse_lane(L1, l, True), 0.125)
    maps[DOWN2] = lane_map(lambda l: jnp.where(l < 64, half(l), half(l) + 64), 0.125)
    maps[DOWN3] = lane_map(half, 0.125)
    maps[UP3] = spread_map(half)
    maps[UP2] = spread_map(lambda l: gz * 6 + jnp.where(l < 64, half(l), half(l) - 64))
    maps[UP1A] = spread_map(lambda l: coarse_lane(L1, l, False))
    maps[UP1B] = spread_map(lambda l: coarse_lane(L1, l, True))
    maps[UP0] = spread_map(both_lanes)


def times(v, m):
    big = v.astype(jnp.bfloat16)
    rest = (v - big.astype(F32)).astype(jnp.bfloat16)
    return jnp.dot(jnp.concatenate([big, rest], axis=1), m, preferred_element_type=F32)


def coarsen_planes(pair, n, tmp, acc, rows, u=2):
    half = rows // 2

    def one(x):
        tmp[x, 0:rows, :] = pair(x)
        acc[x, 0:half, :] = tmp[x, pl.ds(0, half, stride=2), :] + tmp[x, pl.ds(1, half, stride=2), :]

    loop(n, one, u)


def flat(ref):
    n, rows, _ = ref.shape
    return ref[...].reshape(n * rows, 128)


def add_refined(wide, n, src, dst, u=3):
    R = dst.shape[1]

    def one(i):
        v = wide[i, 0 : R // 2, :]
        for k in range(2):
            dst[2 * i + 1, pl.ds(k, R // 2, stride=2), :] = v
        t = dst[2 * i + 1]
        dst[2 * i + 1] = src[2 * i + 1] + t
        dst[2 * i + 2] = src[2 * i + 2] + t

    loop(n, one, u)


def k_zpack0(x0, b, rea, hi, lo, own, raw, sems):
    def copy(a, ref, i):
        many = 64 // L0.hs[a]
        part = pl.ds(i * many, many)
        return pltpu.make_async_copy(ref.at[part], raw.at[a, part], sems.at[a, i])

    refs = (x0, b, rea)
    parts = [48 * h // (64 // h * h) for h in L0.hs]
    for a, ref in enumerate(refs):
        for i in range(parts[a]):
            copy(a, ref, i).start()

    def pack(a, i):
        h = L0.hs[a]
        many = 64 // h
        hi[ZBASE[a] + i], lo[ZBASE[a] + i] = ztile(L0, [(own[a, i * many + k], h * k, h) for k in range(many)])

    steps = [(a, ref, i) for a, ref in enumerate(refs) for i in range(parts[a])]
    for n, (a, ref, i) in enumerate(steps):
        copy(a, ref, i).wait()
        if n:
            pack(steps[n - 1][0], steps[n - 1][2])
        many = 64 // L0.hs[a]
        for x in range(i * many, i * many + many):
            own[a, x, :, 0:48] = raw[a, x, 0:24, :]
            own[a, x, :, 64:112] = raw[a, x, 24:48, :]
    pack(steps[-1][0], steps[-1][2])


def k_ypack0(own, turned, zl, zh, up, dn):
    ypack0(own, turned, zl, zh, up, dn)


def k_xpack0(mid, yl, yh, out):
    ids = place()
    ends = edge(L0, ids)
    first = ids[0] == 0
    for i in range(6):
        x = jnp.where(first, 42, 0) + i
        for a in range(3):
            there, here = y_tiles0(yl, yh, 2, 5 + i // 2, a), y_tiles0(yl, yh, 0, i // 2, a)
            tiles = [jnp.where(first, v, w) for v, w in zip(there, here)]
            out[i, a] = plane0(mid[a, x], tiles, ends, 64 * (1 - i % 2))


def k_xpack1(f1, r1, zl, zh, yl, yh, out, spare):
    both = (f1, r1)
    ids = place()
    ends = edge(L1, ids)

    def one(i):
        for a in range(2):
            plane1(lambda x, a: both[a][x], zl, zh, yl, yh, (1 - ids[0]) * 12 + i, a, out.at[i], a, ends, spare.at[a])

    loop(12, one, 2)


def beside0(c):
    R = L0.R
    sub = lax.broadcasted_iota(jnp.int32, (8, 128), 0)
    seam = roll(jnp.where(sub == 0, c[0:8], c[R - 8 : R]), 64, 1)
    up, down = roll(c, R - 1, 0), roll(c, 1, 0)
    up = jnp.concatenate([up[: R - 8], jnp.where(sub == 7, roll(seam, 7, 0), up[R - 8 :])], axis=0)
    down = jnp.concatenate([jnp.where(sub == 0, roll(seam, 1, 0), down[0:8]), down[8:]], axis=0)
    return (up + down) + (roll(c, 1, 1) + roll(c, 127, 1))


def k_windows0(mid, yl, yh, xw, part, d_out, c_out):
    ids = place()
    ends = edge(L0, ids)
    ok = inside(L0, ids)

    def some(i):
        for k in range(16):
            x = 16 * i + k
            v, b, rea = (plane0(mid[a, x], y_tiles0(yl, yh, i, k // 2, a), ends, 64 * (1 - k % 2)) for a in range(3))
            d = 6.0 + rea
            xw[x] = v
            part[x] = b - d * v + beside0(v)
            d_out[x] = d
            c_out[x] = jnp.where(ok, W / d, 0.0)

    loop(3, some)


def own_rows(sp, v):
    return jnp.where(upper(sp, sp.half), v[0 : sp.half], v[sp.o :])


def half_own(pair, tmp, acc, out, u, m):
    coarsen_planes(pair, 24, tmp, acc, 24, u)
    acc[...] = times(flat(acc), m).reshape(24, 16, 128)

    def keep(x):
        out[x] = acc[x, 0:12, :]

    loop(24, keep, 6)


def k_zmerge(own, zl, zh, dn, out):
    top, bottom, _, _ = edge(L0, place())

    def one(x):
        for a in range(3):
            out[a, x] = merged(L0, lambda x, a: own[a, x], zl, zh, x, a, 0, 24, top, bottom)

    loop(48, one, 8)


def k_early(own, turned, r1, maps, tmp, acc):
    def turn(p):
        for a in range(3):
            v = own[a, 2 * p + 1]
            turned[a, p, 0:8, :] = roll(v[0:8], 64, 1)
            turned[a, p, 8:16, :] = roll(v[16:24], 64, 1)

    loop(24, turn, 4)
    all_maps(maps, lax.axis_index("gz"))
    mine = lanes(24) % 64 < 48
    half_own(lambda x: jnp.where(mine, own[2, 2 * x] + own[2, 2 * x + 1], 0.0), tmp, acc, r1, 4, maps[OWN])


def k_down0(xw, part, d, cw, r1, maps, xr, f_out, c_out, e_out, f1, z1h, z1l, xb, ew, tmp, acc):
    ids = place()
    n = L0.nx
    shift = ids[0] * L0.hx
    other = (1 - ids[0]) * L0.n
    low_side = ids[0] == 0
    ok = inside(L0, ids)
    zero_ends(ew, n)
    zero_ends(e_out, n)
    zero = jnp.zeros((L0.R, 128), F32)
    xb[0] = jnp.where(low_side, xw[47], zero)
    xb[7] = jnp.where(low_side, zero, xw[0])
    for i in range(6):
        xb[i + 1] = xr[i, 0]

    def put(w, f, c):
        f_out[w] = f
        c_out[w] = c
        ew[w + 1] = c * f

    def mine(x):
        put(x + shift, part[x] + (xw[x - 1] + xw[x + 1]), cw[x])

    loop(46, lambda i: mine(i + 1), 23)
    put(shift, part[0] + (jnp.where(low_side, zero, xr[5, 0]) + xw[1]), cw[0])
    put(47 + shift, part[47] + (xw[46] + jnp.where(low_side, xr[0, 0], zero)), cw[47])

    def theirs(i):
        v = xb[i + 1]
        dd = 6.0 + xr[i, 2]
        f = xr[i, 1] - dd * v + beside0(v) + (xb[i] + xb[i + 2])
        put(i + other, f, jnp.where(ok, W / dd, 0.0))

    loop(6, theirs, 6)
    relax(ew, e_out, f_out, c_out, n, 1.0, UR, paired)

    def left(x):
        return own_rows(L0, f_out[x + shift] - d[x] * e_out[x + shift + 1] + paired(e_out, x + shift))

    within = lanes(24) % 64 < 48
    pair = lambda x: jnp.where(within, left(2 * x) + left(2 * x + 1), 0.0)
    half_own(pair, tmp, acc, f1, UL, maps[OWN])
    both = (f1, r1)
    loop(6, lambda g: ztile1(lambda x, a: both[a][x], z1h, z1l, g), 3)


def k_ypack1(f1, r1, zl, zh, up, dn):
    both = (f1, r1)
    ypack1(lambda x, a: both[a][x], zl, zh, up, dn, 6)


def k_windows1(f1, r1, zl, zh, yl, yh, out, spare):
    both = (f1, r1)
    ends = edge(L1, place())

    def some(i):
        for k in range(4):
            for a in range(2):
                plane1(lambda x, a: both[a][x], zl, zh, yl, yh, 4 * i + k, a, out.at[a], 4 * i + k, ends, spare.at[2 * k + a])

    loop(6, some)


def k_down1(win, maps, xr, fw, cw, e_out, f2, c2, e2, out3, rw, ew, tmp, acc, r2, ew2, tmp2, t3, sq):
    ids = place()
    n = L1.nx
    shift = ids[0] * L1.hx
    other = (1 - ids[0]) * L1.n

    def put(x):
        fw[x + shift] = win[0, x]
        rw[x + shift] = win[1, x]

    def take(x):
        fw[x + other] = xr[x, 0]
        rw[x + other] = xr[x, 1]

    loop(24, put, 8)
    loop(12, take, 6)
    ok = inside(L1, ids)
    zero_ends(ew, n)
    zero_ends(e_out, n)

    def first(x):
        c = jnp.where(ok, W / (1.5 + rw[x]), 0.0)
        cw[x] = c
        ew[x + 1] = c * fw[x]

    loop(n, first, 6)
    relax(ew, e_out, fw, cw, n, 0.25, UM, paired)

    def left(x):
        return fw[x] - (1.5 + rw[x]) * e_out[x + 1] + 0.25 * paired(e_out, x)

    for ref, pair in ((f2, lambda x: left(2 * x) + left(2 * x + 1)), (r2, lambda x: rw[2 * x] + rw[2 * x + 1])):
        coarsen_planes(pair, 18, tmp, acc.at[0], 24, 9)
        v = flat(acc.at[0])
        acc[0] = times(v, maps[DOWN1A]).reshape(18, 16, 128)
        acc[1] = times(v, maps[DOWN1B]).reshape(18, 16, 128)

        def keep(x, ref=ref):
            ref[x] = jnp.zeros((32, 128), F32)
            ref[x, 2:14, :] = acc[0, x, 0:12, :]
            ref[x, 14:26, :] = acc[1, x, 0:12, :]

        loop(18, keep, 6)
    ok2 = domain(None, 12, 6, 8, 32, ids)
    zero_ends(ew2, 18)
    zero_ends(e2, 18)

    def second(x):
        c = jnp.where(ok2, W / (0.375 + r2[x]), 0.0)
        c2[x] = c
        ew2[x + 1] = c * f2[x]

    loop(18, second, 6)
    relax(ew2, e2, f2, c2, 18, 0.0625, 18)

    def left2(x):
        return f2[x] - (0.375 + r2[x]) * e2[x + 1] + 0.0625 * neighbours(e2, x)

    for a, pair in enumerate((lambda x: left2(2 * x) + left2(2 * x + 1), lambda x: r2[2 * x] + r2[2 * x + 1])):
        coarsen_planes(pair, 9, tmp2, t3.at[a], 32, 9)
        t3[a] = times(flat(t3.at[a]), maps[DOWN2]).reshape(9, 16, 128)
    shift = ids[0] * 3
    sq[...] = jnp.zeros((128, 128), F32)
    for a in range(2):
        for x in range(6):
            at = a * 36 + x * 6
            sq[at : at + 6, :] = t3[a, x + shift, 4:10, :]
    t = sq[...].T[0:8]
    ln = lanes(1)
    rows = []
    for u in range(2):
        for a in range(2):
            parts = [roll(t, 36 * (w - a), 1)[3 * u + w : 3 * u + w + 1] for w in range(3)]
            rows.append(jnp.where(ln < 36, parts[0], jnp.where(ln < 72, parts[1], parts[2])))
    tile = jnp.concatenate(rows + rows, axis=0)
    n8 = out3.shape[0] // 8
    out3[...] = jnp.broadcast_to(tile[None], (n8, 8, 128)).reshape(n8 * 8, 128)


def sum_all(v):
    s = jnp.sum(v, axis=0)
    s = sum(s[k : k + 8] for k in range(0, s.shape[0], 8))
    return jnp.sum(jnp.sum(s, axis=1, keepdims=True), axis=0, keepdims=True)


def coarse_solve(g3, maps, nx, ny, nz, e3, s3, f3, c3, r3, tmp, f4, r4, sq):
    R = f3.shape[1]
    for ref in (f3, r3):
        ref[...] = jnp.zeros(ref.shape, F32)
    kx, ky, kz = nx // 6, ny // 6, nz // 6
    for bx in range(kx):
        for by in range(ky):
            k = bx * ky + by
            if kz * 6 < 128:
                sq[k, kz * 6 :, :] = jnp.zeros((128 - kz * 6, 128), F32)
            got = [g3[pl.ds(k * kz * 4 + r, kz, stride=4), :] for r in range(4)]
            ln = lanes(kz)
            for u in range(2):
                for w in range(3):
                    f, r = roll(got[2 * u], -36 * w, 1), roll(got[2 * u + 1], 36 - 36 * w, 1)
                    sq[k, pl.ds(3 * u + w, kz, stride=6), :] = jnp.where(ln < 36, f, r)
            t = sq[k].T
            for x in range(6):
                f3[bx * 6 + x, by * 6 : by * 6 + 6, :] = t[x * 6 : x * 6 + 6]
                r3[bx * 6 + x, by * 6 : by * 6 + 6, :] = t[36 + x * 6 : 42 + x * 6]
    factor = 0.25**3
    ok = (lax.broadcasted_iota(jnp.int32, (R, 128), 0) < ny) & (lanes(R) < nz)
    for ref in (e3, s3):
        zero_ends(ref, nx)

    def first(x):
        c = jnp.where(ok, W / (6.0 * factor + r3[x]), 0.0)
        c3[x] = c
        s3[x + 1] = c * f3[x]

    loop(nx, first, 6)
    relax(s3, e3, f3, c3, nx, factor, 12)

    def left(x):
        v = f3[x] - (6.0 * factor + r3[x]) * e3[x + 1] + factor * neighbours(e3, x)
        return jnp.where(ok, v, 0.0)

    for ref, pair in ((f4, lambda x: left(2 * x) + left(2 * x + 1)), (r4, lambda x: r3[2 * x] + r3[2 * x + 1])):
        coarsen_planes(pair, nx // 2, tmp, ref, R, 6)
        ref[...] = times(flat(ref), maps[DOWN3]).reshape(ref.shape)
    f4k = 0.25**4
    H = R // 2
    row = lax.broadcasted_iota(jnp.int32, (nx // 2, H, 128), 1)
    lane = lax.broadcasted_iota(jnp.int32, (nx // 2, H, 128), 2)
    within = (row < ny // 2) & (lane < nz // 2)
    diag = 6.0 * f4k + r4[...]
    zero = jnp.zeros((1, H, 128), F32)

    def apply(p):
        s = jnp.concatenate([zero, p[:-1]], axis=0) + jnp.concatenate([p[1:], zero], axis=0)
        s = s + roll(p, 1, 1) + roll(p, H - 1, 1) + roll(p, 1, 2) + roll(p, 127, 2)
        return jnp.where(within, diag * p - f4k * s, 0.0)

    r = jnp.where(within, f4[...], 0.0)
    p = r
    q = apply(r)
    rr = sum_all(r * r)
    den = sum_all(r * q)
    a = rr / den
    one_over_rr, one_over_a = 1.0 / rr, den / rr
    e = a * p
    for i in range(1, BOTTOM_ITERS):
        r = r - a * q
        w = apply(r)
        new = sum_all(r * r)
        rw = sum_all(r * w)
        b = new * one_over_rr
        den = rw - b * new * one_over_a
        a = new / den
        one_over_rr, one_over_a = 1.0 / new, den / new
        p = r + b * p
        q = w + b * q
        e = e + a * p
    f4[...] = times(e.reshape(nx // 2 * H, 128), maps[UP3]).reshape(e.shape)
    add_refined(f4, nx // 2, e3, s3, 6)
    relax(s3, e3, f3, c3, nx, factor, 12)
    relax(e3, s3, f3, c3, nx, factor, 12)


def k_up(g3, maps, f2, c2, e2i, f1, c1, e1i, f0, c0, d0, e0i, z_out, az_out, sums,
         e3, s3, f3, c3, r3, tmp3, f4, r4, sq, w3, w2, na, nb, n1, e2, s2, e1, s1, e0, s0):
    gx, gy, gz, sy, sz = place()
    nx, ny, nz = f3.shape[0], sy * 6, sz * 6
    coarse_solve(g3, maps, nx, ny, nz, e3, s3, f3, c3, r3, tmp3, f4, r4, sq)
    for ref, n in ((s2, 18), (s1, 36), (s0, 54), (e2, 18), (e1, 36), (e0, 54)):
        zero_ends(ref, n)
    for i in range(9):
        e = s3[i + 1 + gx * 3]
        e = jnp.concatenate([jnp.zeros((8, 128), F32), e, jnp.zeros((8, 128), F32)], axis=0)
        v = e[4:20]
        for k in range(1, sy):
            v = jnp.where(gy == k, e[6 * k + 4 : 6 * k + 20], v)
        w3[i] = v
    w3[...] = times(flat(w3), maps[UP2]).reshape(9, 16, 128)
    add_refined(w3, 9, e2i, e2, 9)
    relax(e2, s2, f2, c2, 18, 0.0625, 18)
    relax(s2, e2, f2, c2, 18, 0.0625, 18)

    def halves(i):
        na[i] = e2[i + 1, 2:18, :]
        nb[i] = e2[i + 1, 14:30, :]

    loop(18, halves, 6)

    w2[...] = (times(flat(na), maps[UP1A]) + times(flat(nb), maps[UP1B])).reshape(18, 16, 128)
    add_refined(w2, 18, e1i, e1, 6)
    relax(e1, s1, f1, c1, 36, 0.25, UM, paired)
    relax(s1, e1, f1, c1, 36, 0.25, UM, paired)

    def near(i):
        v = e1[i + 1 + gx * 9]
        n1[i] = jnp.where(upper(L1, 16), v[0:16], v[8:24])

    loop(27, near, 9)

    n1[...] = times(flat(n1), maps[UP0]).reshape(27, 16, 128)
    add_refined(n1, 27, e0i, e0, 9)
    relax(e0, s0, f0, c0, 54, 1.0, UR, paired)
    relax(s0, e0, f0, c0, 54, 1.0, UR, paired)
    shift = gx * 6
    mine = lanes(24) % 64 < 48

    def last(x, carry):
        u, v = carry
        w = x + shift
        z = e0[w + 1]
        az = own_rows(L0, d0[x] * z - paired(e0, w))
        z = own_rows(L0, z)
        f = own_rows(L0, f0[w])
        z_out[x] = z
        az_out[x] = az
        return u + jnp.where(mine, f * z, 0.0), v + jnp.where(mine, z * az, 0.0)

    def some(i, carry):
        for k in range(UZ):
            carry = last(UZ * i + k, carry)
        return carry

    zero = jnp.zeros((24, 128), F32)
    u, v = lax.fori_loop(0, 48 // UZ, some, (zero, zero))

    def total(t):
        return jnp.sum(jnp.sum(t, axis=1, keepdims=True), axis=0, keepdims=True)

    ln = lanes(sums.shape[0])
    sums[...] = jnp.where(ln == 0, total(u), jnp.where(ln == 1, total(v), 0.0))


def k_last(sums, own, z, az, f, sol, res, sv, rv, sems):
    s = jnp.sum(sums[...], axis=0, keepdims=True)
    ln = lanes(1)
    over = jnp.sum(jnp.where(ln == 0, s, 0.0), axis=1, keepdims=True)
    under = jnp.sum(jnp.where(ln == 1, s, 0.0), axis=1, keepdims=True)
    step = over / under
    shift = lax.axis_index("gx") * 6
    pairs = ((0, sv, sol), (1, rv, res))

    def copy(a, src, dst, i):
        part = pl.ds(i * 8, 8)
        return pltpu.make_async_copy(src.at[part], dst.at[part], sems.at[a, i])

    def some(i):
        for k in range(8):
            x = i * 8 + k
            for ref, v in ((sv, own[0, x] + step * z[x]), (rv, own_rows(L0, f[x + shift]) - step * az[x])):
                ref[x, 0:24, :] = v[:, 0:48]
                ref[x, 24:48, :] = roll(v, 64, 1)[:, 0:48]
        for a, src, dst in pairs:
            copy(a, src, dst, i).start()

    loop(6, some)
    for i in range(6):
        for a, src, dst in pairs:
            copy(a, src, dst, i).wait()


def ring(up, dn, axis, low_first=True):
    n = lax.axis_size(axis)
    rise = [(i, (i + 1) % n) for i in range(n)]
    fall = [(i, (i - 1) % n) for i in range(n)]
    if low_first:
        low = lax.ppermute(up, axis, rise)
        high = lax.ppermute(dn, axis, fall)
    else:
        high = lax.ppermute(dn, axis, fall)
        low = lax.ppermute(up, axis, rise)
    return low, high


def swap(v):
    return lax.ppermute(v, "gx", [(0, 1), (1, 0)])


def body(b, x0, rea):
    ALL = ("gx", "gy", "gz")
    sizes = [lax.axis_size(a) for a in ALL]
    count = sizes[0] * sizes[1] * sizes[2]
    b, x0, rea = (pltpu.with_memory_space_constraint(v, pltpu.HBM) for v in (b, x0, rea))
    hi, lo, own = run(
        k_zpack0,
        (sds(*L0.zshape), sds(*L0.zshape), sds(3, 48, 24, 128)),
        (x0, b, rea),
        [(3, 48, 48, 48), pltpu.SemaphoreType.DMA((3, 4))],
        far_in=True,
    )
    zl, zh = ring(hi, lo, "gz")
    turned, r1, maps = run(
        k_early,
        (sds(3, 24, 16, 128), sds(24, 12, 128), sds(10, 256, 128, dtype=jnp.bfloat16)),
        (own,),
        [(24, 24, 128), (24, 16, 128)],
    )
    up, dn = run(k_ypack0, (sds(*L0.yshape),) * 2, (own, turned, zl, zh))
    yl, yh = ring(up, dn, "gy")
    mid = run(k_zmerge, sds(3, 48, 24, 128), (own, zl, zh, dn))
    xr = swap(run(k_xpack0, sds(*L0.xshape), (mid, yl, yh)))
    p0, q0, o0 = (54, 32, 128), (56, 32, 128), (48, 32, 128)
    xw, part, d0, cw = run(k_windows0, (sds(*o0),) * 4, (mid, yl, yh))
    f0, c0, e0, f1, z1h, z1l = run(
        k_down0,
        (sds(*p0), sds(*p0), sds(*q0), sds(24, 12, 128), sds(*L1.zshape), sds(*L1.zshape)),
        (xw, part, d0, cw, r1, maps, xr),
        [(8, 32, 128), q0, (24, 24, 128), (24, 16, 128)],
        mib=M0,
    )
    zl, zh = ring(z1h, z1l, "gz")
    up, dn = run(k_ypack1, (sds(*L1.yshape),) * 2, (f1, r1, zl, zh))
    yl, yh = ring(up, dn, "gy")
    xr = swap(run(k_xpack1, sds(*L1.xshape), (f1, r1, zl, zh, yl, yh), [(2, 2, 24, 128)]))
    p1, q1, p2, q2 = (36, 24, 128), (38, 24, 128), (18, 32, 128), (20, 32, 128)
    win = run(k_windows1, sds(2, 24, 24, 128), (f1, r1, zl, zh, yl, yh), [(8, 2, 24, 128)])
    f1w, c1w, e1w, f2w, c2w, e2w, g = run(
        k_down1,
        (sds(*p1), sds(*p1), sds(*q1), sds(*p2), sds(*p2), sds(*q2), sds(count * 4, 128)),
        (win, maps, xr),
        [p1, q1, (18, 24, 128), (2, 18, 16, 128), p2, q2, (9, 32, 128), (2, 9, 16, 128), (128, 128)],
        mib=M1,
    )
    g = lax.all_to_all(g, ALL, 0, 0, tiled=True)
    n3 = [6 * s for s in sizes]
    R3 = (n3[1] + 8) // 8 * 8
    if R3 % 16:
        R3 += 8
    p3, q3, p4 = (n3[0], R3, 128), (n3[0] + 2, R3, 128), (n3[0] // 2, R3 // 2, 128)
    z, az, sums = run(
        k_up,
        (sds(48, 24, 128), sds(48, 24, 128), sds(count, 128)),
        (g, maps, f2w, c2w, e2w, f1w, c1w, e1w, f0, c0, d0, e0),
        [q3, q3, p3, p3, p3, (n3[0] // 2, R3, 128), p4, p4, (sizes[0] * sizes[1], 128, 128), (9, 16, 128), (18, 16, 128),
         (18, 16, 128), (18, 16, 128), (27, 16, 128), q2, q2, q1, q1, q0, q0],
        mib=M2,
    )
    sums = lax.all_to_all(sums.reshape(count, 1, 128), ALL, 0, 0, tiled=True).reshape(count, 128)
    return run(
        k_last,
        (sds(48, 48, 48), sds(48, 48, 48)),
        (sums, own, z, az, f0),
        [(48, 48, 48), (48, 48, 48), pltpu.SemaphoreType.DMA((2, 6))],
        far_out=True,
    )


def solution(mesh):
    spec = P("gx", "gy", "gz")
    return jax.shard_map(body, mesh=mesh, in_specs=(spec, spec, spec), out_specs=(spec, spec), check_vma=False)
```

```python
import functools
import jax
import jax.numpy as jnp
from jax import lax
from jax.experimental import pallas as pl
from jax.experimental.pallas import tpu as pltpu
from jax.sharding import PartitionSpec as P

W = 6.0 / 7.0
BOTTOM_ITERS = 6
N0 = 48
F32 = jnp.float32
HI = lax.Precision.HIGHEST
M0, M1, M2 = 10, 8, 12
UF, UR, UM, UZ, UL = 12, 54, 36, 24, 24


class Spec:
    def __init__(self, n, h, na, R, o, hx, cut, kp, st):
        self.n, self.h, self.na, self.R, self.o, self.hx, self.cut, self.kp, self.st = n, h, na, R, o, hx, cut, kp, st
        self.half = n // 2
        self.zshape = (n // (kp * st), self.half * st, 128)
        self.yshape = (self.half, na * h, 128)
        self.hs = (h,) * na
        self.xshape = (hx, na, R, 128)
        self.nx = n + hx

    def slot(self, x, a):
        if self.st == 1:
            h = self.hs[a]
            many = 64 // h
            return ZBASE[a] + lax.div(x, many), 0, h * lax.rem(x, many)
        per = self.n // self.st
        t, y = lax.div(x, per), lax.rem(x, per)
        return lax.div(y, self.kp), t, self.h * (lax.rem(y, self.kp) * self.na + a)


L0 = Spec(48, 5, 3, 32, 8, 6, 56, 4, 1)
L1 = Spec(24, 12, 2, 24, 12, 12, 44, 2, 2)
L0.hs = (5, 4, 4)
ZBASE = (0, 4, 7)
YBASE = (0, 40, 72)
L0.zshape = (10, 24, 128)
L0.yshape = (3, 104, 128)


def sds(*shape, dtype=F32):
    return jax.ShapeDtypeStruct(shape, dtype)


def run(kernel, outs, args, scratch=(), mib=12, far_in=False, far_out=False):
    vmem = pl.BlockSpec(memory_space=pltpu.VMEM)
    hbm = pl.BlockSpec(memory_space=pl.ANY)
    return pl.pallas_call(
        kernel,
        out_shape=outs,
        in_specs=[hbm if far_in else vmem] * len(args),
        out_specs=jax.tree.map(lambda _: hbm if far_out else vmem, outs),
        scratch_shapes=[pltpu.VMEM(s, F32) if isinstance(s, tuple) else s for s in scratch],
        compiler_params=pltpu.CompilerParams(vmem_limit_bytes=mib * 1024 * 1024),
    )(*args)


def place():
    return [lax.axis_index(a) for a in ("gx", "gy", "gz")] + [lax.axis_size(a) for a in ("gy", "gz")]


def lanes(rows):
    return lax.broadcasted_iota(jnp.int32, (rows, 128), 1)


def roll(v, shift, axis):
    if isinstance(shift, int):
        shift = shift % v.shape[axis]
        if shift == 0:
            return v
    return pltpu.roll(v, shift, axis)


def loop(n, f, u=1):
    u = max(d for d in range(1, u + 1) if n % d == 0)

    def some(i, c):
        for k in range(u):
            f(i * u + k)
        return c

    lax.fori_loop(0, n // u, some, 0)


def upper(sp, rows):
    l = lanes(rows)
    return (l >= sp.cut) & (l < sp.cut + 64)


def edge(sp, ids):
    _, gy, gz, ny, nz = ids
    high = jnp.where(gz < nz - 1, sp.n + sp.h, sp.n)
    low = jnp.where(gz > 0, 64 - sp.h, 64)
    return high, low, jnp.where(gy > 0, 1.0, 0.0), jnp.where(gy < ny - 1, 1.0, 0.0)


def ztile(sp, items):
    l = lanes(sp.half)
    hi = [jnp.zeros((sp.half, 128), F32)] * 2
    lo = list(hi)
    for k, (v, at, h) in enumerate(items):
        r = roll(v, at, 1)
        hi[k % 2] = jnp.where(((l + (64 - (at + sp.n - h) % 64)) & 63) < h, r, hi[k % 2])
        lo[k % 2] = jnp.where(((l + (64 - at)) & 63) < h, r, lo[k % 2])
    return roll(hi[0] + hi[1], -2 * sp.n, 1), lo[0] + lo[1]


def ztile1(own, hi_ref, lo_ref, g):
    sp = L1
    for t in range(sp.st):
        items = [
            (own(t * (sp.n // sp.st) + g * sp.kp + k, a), sp.h * (k * sp.na + a), sp.h)
            for k in range(sp.kp)
            for a in range(sp.na)
        ]
        hi, lo = ztile(sp, items)
        hi_ref[g, t * sp.half : (t + 1) * sp.half, :] = hi
        lo_ref[g, t * sp.half : (t + 1) * sp.half, :] = lo


def merged(sp, own, zl, zh, x, a, b, e, top, bottom):
    g, t, at = sp.slot(x, a)
    if sp.st == 1:
        high, low = zh[g, b:e, :], zl[g, b:e, :]
    else:
        high = jnp.where(t == 0, zh[g, b:e, :], zh[g, sp.half + b : sp.half + e, :])
        low = jnp.where(t == 0, zl[g, b:e, :], zl[g, sp.half + b : sp.half + e, :])
    l = lanes(e - b)
    beside = jnp.where(((l + (64 - at)) & 63) < sp.hs[a], high, low)
    beside = roll(beside, (sp.n + 128 - at) & 127, 1)
    q = l & 63
    return jnp.where(q < sp.n, own(x, a)[b:e], jnp.where((q < top) | (q >= bottom), beside, 0.0))


def ypack0(own, turned, zl, zh, up_ref, dn_ref):
    top, bottom, _, _ = edge(L0, place())
    l = lanes(8)
    q = l & 63
    up = upper(L0, 8)

    def beside(x, a, b, turn):
        g, _, at = L0.slot(x, a)
        v = jnp.where(((l + (64 - at)) & 63) < L0.hs[a], zh[g, b : b + 8, :], zl[g, b : b + 8, :])
        v = roll(v, (L0.n + turn + 128 - at) & 127, 1)
        return jnp.where((q < top) | (q >= bottom), v, 0.0)

    def some(i):
        for k in range(8):
            p = 8 * i + k
            for a in range(3):
                h = L0.hs[a]
                for ref, b, s in ((up_ref, 16, 8 - h), (dn_ref, 0, 0)):
                    even = jnp.where(q < L0.n, own[a, 2 * p, b : b + 8, :], beside(2 * p, a, b, 0))
                    odd = jnp.where(q < L0.n, turned[a, p, b // 2 : b // 2 + 8, :], beside(2 * p + 1, a, b, 64))
                    v = jnp.where(up, even, odd) if b else jnp.where(up, odd, even)
                    ref[i, pl.ds(YBASE[a] + k, h, stride=8), :] = v[s : s + h]

    loop(3, some)


def ypack1(own, zl, zh, up_ref, dn_ref, u):
    sp = L1
    half = sp.half
    top, bottom, _, _ = edge(sp, place())

    def pair(p):
        for a in range(sp.na):
            even = merged(sp, own, zl, zh, 2 * p, a, 0, half, top, bottom)
            odd = roll(merged(sp, own, zl, zh, 2 * p + 1, a, 0, half, top, bottom), 64, 1)
            up = upper(sp, half)
            up_ref[p, a * half : (a + 1) * half, :] = jnp.where(up, even, odd)
            dn_ref[p, a * half : (a + 1) * half, :] = jnp.where(up, odd, even)

    loop(half, pair, u)


def y_tiles0(yl, yh, g, t, a):
    def rows(ref, start):
        return ref[g, pl.ds(start + t, 8, stride=8), :]

    if a == 0:
        return roll(rows(yl, 0), 3, 0), rows(yh, 0)
    return rows(yl, YBASE[a] - 32), rows(yh, 40) if a == 1 else roll(rows(yh, 40), 4, 0)


def plane0(m, tiles, ends, turn):
    _, _, below, above = ends
    low, high = tiles
    lower = jnp.concatenate([roll(low, turn, 1) * below, m], axis=0)
    higher = jnp.concatenate([m, roll(high, turn, 1) * above], axis=0)
    return jnp.where(upper(L0, L0.R), higher, lower)


def plane1(own, zl, zh, yl, yh, x, a, dst, xw, ends, spare):
    top, bottom, below, above = ends
    sp = L1
    h, half = sp.h, sp.half
    m = merged(sp, own, zl, zh, x, a, 0, half, top, bottom)
    p = lax.div(x, 2)
    turn = 64 * (1 - lax.rem(x, 2))
    spare[0, 0:h, :] = roll(yl[p, a * h : (a + 1) * h, :], turn, 1) * below
    spare[0, h:, :] = m
    spare[1, 0:half, :] = m
    spare[1, half:, :] = roll(yh[p, a * h : (a + 1) * h, :], turn, 1) * above
    dst[xw] = jnp.where(upper(sp, sp.R), spare[1], spare[0])


def lane_z(sp, l):
    return jnp.where(l < sp.cut, l, jnp.where(l < sp.cut + 64, l - 64, l - 128))


def inside(sp, ids):
    _, gy, gz, ny, nz = ids
    n, h = sp.n, min(sp.hs)
    y = lax.broadcasted_iota(jnp.int32, (sp.R, 128), 0) - sp.o + jnp.where(upper(sp, sp.R), sp.R, 0)
    z = lane_z(sp, lanes(sp.R))
    ok = (y >= -h) & (y < n + h) & (z >= -h) & (z < n + h)
    y, z = y + gy * n, z + gz * n
    return ok & (y >= 0) & (y < ny * n) & (z >= 0) & (z < nz * n)


def paired(ref, x):
    c = ref[x + 1]
    R = c.shape[0]
    s = ref[x] + ref[x + 2]
    sub = lax.broadcasted_iota(jnp.int32, (8, 128), 0)
    seam = roll(jnp.where(sub == 0, c[0:8], c[R - 8 : R]), 64, 1)
    last = jnp.where(sub == 7, roll(seam, 7, 0), roll(c[R - 8 :], 7, 0))
    first = jnp.where(sub == 0, roll(seam, 1, 0), roll(c[0:8], 1, 0))
    up = jnp.concatenate([ref[x + 1, 1 : R - 7, :], last], axis=0)
    down = jnp.concatenate([first, ref[x + 1, 7 : R - 1, :]], axis=0)
    s = s + (up + down)
    return s + (roll(c, 1, 1) + roll(c, 127, 1))


def domain(sp, n, h, r0, R, ids):
    row = lax.broadcasted_iota(jnp.int32, (R, 128), 0) - r0
    ln = lanes(R)
    z = jnp.where(ln < 64, ln, ln - 128)
    gy, gz, ny, nz = ids[1], ids[2], ids[3], ids[4]
    y_at, z_at = row + gy * n, z + gz * n
    ok = (row >= -h) & (row < n + h) & (z >= -h) & (z < n + h)
    return ok & (y_at >= 0) & (y_at < ny * n) & (z_at >= 0) & (z_at < nz * n)


def neighbours(ref, x):
    c = ref[x + 1]
    R = c.shape[0]
    s = ref[x] + ref[x + 2]
    s = s + (roll(c, 1, 0) + roll(c, R - 1, 0))
    return s + (roll(c, 1, 1) + roll(c, 127, 1))


def zero_ends(ref, n):
    ref[0] = jnp.zeros(ref.shape[1:], F32)
    ref[n + 1] = jnp.zeros(ref.shape[1:], F32)


def relax(src, dst, f, c, n, factor, u=9, near=None):
    near = near or neighbours

    def one(x):
        dst[x + 1] = (1.0 - W) * src[x + 1] + c[x] * (f[x] + factor * near(src, x))

    loop(n, one, u)


def lane_map(pick, value):
    l = lax.broadcasted_iota(jnp.int32, (256, 128), 0) & 127
    m = lax.broadcasted_iota(jnp.int32, (256, 128), 1)
    return jnp.where(pick(l) == m, value, 0.0).astype(jnp.bfloat16)


def spread_map(pick):
    m = lax.broadcasted_iota(jnp.int32, (256, 128), 0) & 127
    l = lax.broadcasted_iota(jnp.int32, (256, 128), 1)
    return jnp.where(pick(l) == m, 1.0, 0.0).astype(jnp.bfloat16)


def floor_half(z):
    return lax.shift_right_arithmetic(z, 1)


def coarse_lane(sp, l, want):
    z = lane_z(sp, l)
    up = (l >= sp.cut) & (l < sp.cut + 64)
    good = (z >= -sp.h) & (z < sp.n + sp.h)
    good = good & (up if want else jnp.logical_not(up))
    return jnp.where(good, floor_half(z) + jnp.where(z < 0, 128, 0), -1)


def both_lanes(l):
    lower, higher = coarse_lane(L0, l, False), coarse_lane(L0, l, True)
    return jnp.where(lower >= 0, lower, jnp.where(higher >= 0, (higher + 64) & 127, -1))


OWN, DOWN1A, DOWN1B, DOWN2, DOWN3, UP3, UP2, UP1A, UP1B, UP0 = range(10)


def all_maps(maps, gz):
    half = floor_half
    maps[OWN] = lane_map(lambda l: jnp.where(l < 64, half(l), 32 + half(l)), 0.125)
    maps[DOWN1A] = lane_map(lambda l: coarse_lane(L1, l, False), 0.125)
    maps[DOWN1B] = lane_map(lambda l: coarse_lane(L1, l, True), 0.125)
    maps[DOWN2] = lane_map(lambda l: jnp.where(l < 64, half(l), half(l) + 64), 0.125)
    maps[DOWN3] = lane_map(half, 0.125)
    maps[UP3] = spread_map(half)
    maps[UP2] = spread_map(lambda l: gz * 6 + jnp.where(l < 64, half(l), half(l) - 64))
    maps[UP1A] = spread_map(lambda l: coarse_lane(L1, l, False))
    maps[UP1B] = spread_map(lambda l: coarse_lane(L1, l, True))
    maps[UP0] = spread_map(both_lanes)


def times(v, m):
    big = v.astype(jnp.bfloat16)
    rest = (v - big.astype(F32)).astype(jnp.bfloat16)
    return jnp.dot(jnp.concatenate([big, rest], axis=1), m, preferred_element_type=F32)


def coarsen_planes(pair, n, tmp, acc, rows, u=2):
    half = rows // 2

    def one(x):
        tmp[x, 0:rows, :] = pair(x)
        acc[x, 0:half, :] = tmp[x, pl.ds(0, half, stride=2), :] + tmp[x, pl.ds(1, half, stride=2), :]

    loop(n, one, u)


def flat(ref):
    n, rows, _ = ref.shape
    return ref[...].reshape(n * rows, 128)


def add_refined(wide, n, src, dst, u=3):
    R = dst.shape[1]

    def one(i):
        v = wide[i, 0 : R // 2, :]
        for k in range(2):
            dst[2 * i + 1, pl.ds(k, R // 2, stride=2), :] = v
        t = dst[2 * i + 1]
        dst[2 * i + 1] = src[2 * i + 1] + t
        dst[2 * i + 2] = src[2 * i + 2] + t

    loop(n, one, u)


def k_zpack0(x0, b, rea, hi, lo, own, raw, sems):
    def copy(a, ref, i):
        many = 64 // L0.hs[a]
        part = pl.ds(i * many, many)
        return pltpu.make_async_copy(ref.at[part], raw.at[a, part], sems.at[a, i])

    refs = (x0, b, rea)
    parts = [48 * h // (64 // h * h) for h in L0.hs]
    for a, ref in enumerate(refs):
        for i in range(parts[a]):
            copy(a, ref, i).start()

    def pack(a, i):
        h = L0.hs[a]
        many = 64 // h
        hi[ZBASE[a] + i], lo[ZBASE[a] + i] = ztile(L0, [(own[a, i * many + k], h * k, h) for k in range(many)])

    steps = [(a, ref, i) for a, ref in enumerate(refs) for i in range(parts[a])]
    for n, (a, ref, i) in enumerate(steps):
        copy(a, ref, i).wait()
        if n:
            pack(steps[n - 1][0], steps[n - 1][2])
        many = 64 // L0.hs[a]
        for x in range(i * many, i * many + many):
            own[a, x, :, 0:48] = raw[a, x, 0:24, :]
            own[a, x, :, 64:112] = raw[a, x, 24:48, :]
    pack(steps[-1][0], steps[-1][2])


def k_ypack0(own, turned, zl, zh, up, dn):
    ypack0(own, turned, zl, zh, up, dn)


def k_xpack0(mid, yl, yh, out):
    ids = place()
    ends = edge(L0, ids)
    first = ids[0] == 0
    for i in range(6):
        x = jnp.where(first, 42, 0) + i
        for a in range(3):
            there, here = y_tiles0(yl, yh, 2, 5 + i // 2, a), y_tiles0(yl, yh, 0, i // 2, a)
            tiles = [jnp.where(first, v, w) for v, w in zip(there, here)]
            out[i, a] = plane0(mid[a, x], tiles, ends, 64 * (1 - i % 2))


def k_xpack1(f1, r1, zl, zh, yl, yh, out, spare):
    both = (f1, r1)
    ids = place()
    ends = edge(L1, ids)

    def one(i):
        for a in range(2):
            plane1(lambda x, a: both[a][x], zl, zh, yl, yh, (1 - ids[0]) * 12 + i, a, out.at[i], a, ends, spare.at[a])

    loop(12, one, 2)


def beside0(c):
    R = L0.R
    sub = lax.broadcasted_iota(jnp.int32, (8, 128), 0)
    seam = roll(jnp.where(sub == 0, c[0:8], c[R - 8 : R]), 64, 1)
    up, down = roll(c, R - 1, 0), roll(c, 1, 0)
    up = jnp.concatenate([up[: R - 8], jnp.where(sub == 7, roll(seam, 7, 0), up[R - 8 :])], axis=0)
    down = jnp.concatenate([jnp.where(sub == 0, roll(seam, 1, 0), down[0:8]), down[8:]], axis=0)
    return (up + down) + (roll(c, 1, 1) + roll(c, 127, 1))


def k_windows0(mid, yl, yh, xw, part, d_out, c_out):
    ids = place()
    ends = edge(L0, ids)
    ok = inside(L0, ids)

    def some(i):
        for k in range(16):
            x = 16 * i + k
            v, b, rea = (plane0(mid[a, x], y_tiles0(yl, yh, i, k // 2, a), ends, 64 * (1 - k % 2)) for a in range(3))
            d = 6.0 + rea
            xw[x] = v
            part[x] = b - d * v + beside0(v)
            d_out[x] = d
            c_out[x] = jnp.where(ok, W / d, 0.0)

    loop(3, some)


def own_rows(sp, v):
    return jnp.where(upper(sp, sp.half), v[0 : sp.half], v[sp.o :])


def half_own(pair, tmp, acc, out, u, m):
    coarsen_planes(pair, 24, tmp, acc, 24, u)
    acc[...] = times(flat(acc), m).reshape(24, 16, 128)

    def keep(x):
        out[x] = acc[x, 0:12, :]

    loop(24, keep, 6)


def k_zmerge(own, zl, zh, dn, out):
    top, bottom, _, _ = edge(L0, place())

    def one(x):
        for a in range(3):
            out[a, x] = merged(L0, lambda x, a: own[a, x], zl, zh, x, a, 0, 24, top, bottom)

    loop(48, one, 8)


def k_early(own, turned, r1, maps, tmp, acc):
    def turn(p):
        for a in range(3):
            v = own[a, 2 * p + 1]
            turned[a, p, 0:8, :] = roll(v[0:8], 64, 1)
            turned[a, p, 8:16, :] = roll(v[16:24], 64, 1)

    loop(24, turn, 4)
    all_maps(maps, lax.axis_index("gz"))
    mine = lanes(24) % 64 < 48
    half_own(lambda x: jnp.where(mine, own[2, 2 * x] + own[2, 2 * x + 1], 0.0), tmp, acc, r1, 4, maps[OWN])


def k_down0(xw, part, d, cw, r1, maps, xr, f_out, c_out, e_out, f1, z1h, z1l, xb, ew, tmp, acc):
    ids = place()
    n = L0.nx
    shift = ids[0] * L0.hx
    other = (1 - ids[0]) * L0.n
    low_side = ids[0] == 0
    ok = inside(L0, ids)
    zero_ends(ew, n)
    zero_ends(e_out, n)
    zero = jnp.zeros((L0.R, 128), F32)
    xb[0] = jnp.where(low_side, xw[47], zero)
    xb[7] = jnp.where(low_side, zero, xw[0])
    for i in range(6):
        xb[i + 1] = xr[i, 0]

    def put(w, f, c):
        f_out[w] = f
        c_out[w] = c
        ew[w + 1] = c * f

    def mine(x):
        put(x + shift, part[x] + (xw[x - 1] + xw[x + 1]), cw[x])

    loop(46, lambda i: mine(i + 1), 23)
    put(shift, part[0] + (jnp.where(low_side, zero, xr[5, 0]) + xw[1]), cw[0])
    put(47 + shift, part[47] + (xw[46] + jnp.where(low_side, xr[0, 0], zero)), cw[47])

    def theirs(i):
        v = xb[i + 1]
        dd = 6.0 + xr[i, 2]
        f = xr[i, 1] - dd * v + beside0(v) + (xb[i] + xb[i + 2])
        put(i + other, f, jnp.where(ok, W / dd, 0.0))

    loop(6, theirs, 6)
    relax(ew, e_out, f_out, c_out, n, 1.0, UR, paired)

    def left(x):
        return own_rows(L0, f_out[x + shift] - d[x] * e_out[x + shift + 1] + paired(e_out, x + shift))

    within = lanes(24) % 64 < 48
    pair = lambda x: jnp.where(within, left(2 * x) + left(2 * x + 1), 0.0)
    half_own(pair, tmp, acc, f1, UL, maps[OWN])
    both = (f1, r1)
    loop(6, lambda g: ztile1(lambda x, a: both[a][x], z1h, z1l, g), 3)


def k_ypack1(f1, r1, zl, zh, up, dn):
    both = (f1, r1)
    ypack1(lambda x, a: both[a][x], zl, zh, up, dn, 6)


def k_windows1(f1, r1, zl, zh, yl, yh, out, spare):
    both = (f1, r1)
    ends = edge(L1, place())

    def some(i):
        for k in range(4):
            for a in range(2):
                plane1(lambda x, a: both[a][x], zl, zh, yl, yh, 4 * i + k, a, out.at[a], 4 * i + k, ends, spare.at[2 * k + a])

    loop(6, some)


def k_down1(win, maps, xr, fw, cw, e_out, f2, c2, e2, out3, rw, ew, tmp, acc, r2, ew2, tmp2, t3, sq):
    ids = place()
    n = L1.nx
    shift = ids[0] * L1.hx
    other = (1 - ids[0]) * L1.n

    def put(x):
        fw[x + shift] = win[0, x]
        rw[x + shift] = win[1, x]

    def take(x):
        fw[x + other] = xr[x, 0]
        rw[x + other] = xr[x, 1]

    loop(24, put, 8)
    loop(12, take, 6)
    ok = inside(L1, ids)
    zero_ends(ew, n)
    zero_ends(e_out, n)

    def first(x):
        c = jnp.where(ok, W / (1.5 + rw[x]), 0.0)
        cw[x] = c
        ew[x + 1] = c * fw[x]

    loop(n, first, 6)
    relax(ew, e_out, fw, cw, n, 0.25, UM, paired)

    def left(x):
        return fw[x] - (1.5 + rw[x]) * e_out[x + 1] + 0.25 * paired(e_out, x)

    for ref, pair in ((f2, lambda x: left(2 * x) + left(2 * x + 1)), (r2, lambda x: rw[2 * x] + rw[2 * x + 1])):
        coarsen_planes(pair, 18, tmp, acc.at[0], 24, 18)
        v = flat(acc.at[0])
        acc[0] = times(v, maps[DOWN1A]).reshape(18, 16, 128)
        acc[1] = times(v, maps[DOWN1B]).reshape(18, 16, 128)

        def keep(x, ref=ref):
            ref[x] = jnp.zeros((32, 128), F32)
            ref[x, 2:14, :] = acc[0, x, 0:12, :]
            ref[x, 14:26, :] = acc[1, x, 0:12, :]

        loop(18, keep, 6)
    ok2 = domain(None, 12, 6, 8, 32, ids)
    zero_ends(ew2, 18)
    zero_ends(e2, 18)

    def second(x):
        c = jnp.where(ok2, W / (0.375 + r2[x]), 0.0)
        c2[x] = c
        ew2[x + 1] = c * f2[x]

    loop(18, second, 6)
    relax(ew2, e2, f2, c2, 18, 0.0625, 18)

    def left2(x):
        return f2[x] - (0.375 + r2[x]) * e2[x + 1] + 0.0625 * neighbours(e2, x)

    for a, pair in enumerate((lambda x: left2(2 * x) + left2(2 * x + 1), lambda x: r2[2 * x] + r2[2 * x + 1])):
        coarsen_planes(pair, 9, tmp2, t3.at[a], 32, 9)
        t3[a] = times(flat(t3.at[a]), maps[DOWN2]).reshape(9, 16, 128)
    shift = ids[0] * 3
    sq[...] = jnp.zeros((128, 128), F32)
    for a in range(2):
        for x in range(6):
            at = a * 36 + x * 6
            sq[at : at + 6, :] = t3[a, x + shift, 4:10, :]
    t = sq[...].T[0:8]
    ln = lanes(1)
    rows = []
    for u in range(2):
        for a in range(2):
            parts = [roll(t, 36 * (w - a), 1)[3 * u + w : 3 * u + w + 1] for w in range(3)]
            rows.append(jnp.where(ln < 36, parts[0], jnp.where(ln < 72, parts[1], parts[2])))
    tile = jnp.concatenate(rows + rows, axis=0)
    n8 = out3.shape[0] // 8
    out3[...] = jnp.broadcast_to(tile[None], (n8, 8, 128)).reshape(n8 * 8, 128)


def sum_all(v):
    s = jnp.sum(v, axis=0)
    s = sum(s[k : k + 8] for k in range(0, s.shape[0], 8))
    return jnp.sum(jnp.sum(s, axis=1, keepdims=True), axis=0, keepdims=True)


def coarse_solve(g3, maps, nx, ny, nz, e3, s3, f3, c3, r3, tmp, f4, r4, sq):
    R = f3.shape[1]
    for ref in (f3, r3):
        ref[...] = jnp.zeros(ref.shape, F32)
    kx, ky, kz = nx // 6, ny // 6, nz // 6
    for bx in range(kx):
        for by in range(ky):
            k = bx * ky + by
            if kz * 6 < 128:
                sq[k, kz * 6 :, :] = jnp.zeros((128 - kz * 6, 128), F32)
            got = [g3[pl.ds(k * kz * 4 + r, kz, stride=4), :] for r in range(4)]
            ln = lanes(kz)
            for u in range(2):
                for w in range(3):
                    f, r = roll(got[2 * u], -36 * w, 1), roll(got[2 * u + 1], 36 - 36 * w, 1)
                    sq[k, pl.ds(3 * u + w, kz, stride=6), :] = jnp.where(ln < 36, f, r)
            t = sq[k].T
            for x in range(6):
                f3[bx * 6 + x, by * 6 : by * 6 + 6, :] = t[x * 6 : x * 6 + 6]
                r3[bx * 6 + x, by * 6 : by * 6 + 6, :] = t[36 + x * 6 : 42 + x * 6]
    factor = 0.25**3
    ok = (lax.broadcasted_iota(jnp.int32, (R, 128), 0) < ny) & (lanes(R) < nz)
    for ref in (e3, s3):
        zero_ends(ref, nx)

    def first(x):
        c = jnp.where(ok, W / (6.0 * factor + r3[x]), 0.0)
        c3[x] = c
        s3[x + 1] = c * f3[x]

    loop(nx, first, 6)
    relax(s3, e3, f3, c3, nx, factor, 12)

    def left(x):
        v = f3[x] - (6.0 * factor + r3[x]) * e3[x + 1] + factor * neighbours(e3, x)
        return jnp.where(ok, v, 0.0)

    for ref, pair in ((f4, lambda x: left(2 * x) + left(2 * x + 1)), (r4, lambda x: r3[2 * x] + r3[2 * x + 1])):
        coarsen_planes(pair, nx // 2, tmp, ref, R, 6)
        ref[...] = times(flat(ref), maps[DOWN3]).reshape(ref.shape)
    f4k = 0.25**4
    H = R // 2
    row = lax.broadcasted_iota(jnp.int32, (nx // 2, H, 128), 1)
    lane = lax.broadcasted_iota(jnp.int32, (nx // 2, H, 128), 2)
    within = (row < ny // 2) & (lane < nz // 2)
    diag = 6.0 * f4k + r4[...]
    zero = jnp.zeros((1, H, 128), F32)

    def apply(p):
        s = jnp.concatenate([zero, p[:-1]], axis=0) + jnp.concatenate([p[1:], zero], axis=0)
        s = s + roll(p, 1, 1) + roll(p, H - 1, 1) + roll(p, 1, 2) + roll(p, 127, 2)
        return jnp.where(within, diag * p - f4k * s, 0.0)

    r = jnp.where(within, f4[...], 0.0)
    p = r
    q = apply(r)
    rr = sum_all(r * r)
    den = sum_all(r * q)
    a = rr / den
    one_over_rr, one_over_a = 1.0 / rr, den / rr
    e = a * p
    for i in range(1, BOTTOM_ITERS):
        r = r - a * q
        w = apply(r)
        new = sum_all(r * r)
        rw = sum_all(r * w)
        b = new * one_over_rr
        den = rw - b * new * one_over_a
        a = new / den
        one_over_rr, one_over_a = 1.0 / new, den / new
        p = r + b * p
        q = w + b * q
        e = e + a * p
    f4[...] = times(e.reshape(nx // 2 * H, 128), maps[UP3]).reshape(e.shape)
    add_refined(f4, nx // 2, e3, s3, 6)
    relax(s3, e3, f3, c3, nx, factor, 12)
    relax(e3, s3, f3, c3, nx, factor, 12)


def k_up(g3, maps, f2, c2, e2i, f1, c1, e1i, f0, c0, d0, e0i, z_out, az_out, sums,
         e3, s3, f3, c3, r3, tmp3, f4, r4, sq, w3, w2, na, nb, n1, e2, s2, e1, s1, e0, s0):
    gx, gy, gz, sy, sz = place()
    nx, ny, nz = f3.shape[0], sy * 6, sz * 6
    coarse_solve(g3, maps, nx, ny, nz, e3, s3, f3, c3, r3, tmp3, f4, r4, sq)
    for ref, n in ((s2, 18), (s1, 36), (s0, 54), (e2, 18), (e1, 36), (e0, 54)):
        zero_ends(ref, n)
    for i in range(9):
        e = s3[i + 1 + gx * 3]
        e = jnp.concatenate([jnp.zeros((8, 128), F32), e, jnp.zeros((8, 128), F32)], axis=0)
        v = e[4:20]
        for k in range(1, sy):
            v = jnp.where(gy == k, e[6 * k + 4 : 6 * k + 20], v)
        w3[i] = v
    w3[...] = times(flat(w3), maps[UP2]).reshape(9, 16, 128)
    add_refined(w3, 9, e2i, e2, 9)
    relax(e2, s2, f2, c2, 18, 0.0625, 18)
    relax(s2, e2, f2, c2, 18, 0.0625, 18)

    def halves(i):
        na[i] = e2[i + 1, 2:18, :]
        nb[i] = e2[i + 1, 14:30, :]

    loop(18, halves, 6)

    w2[...] = (times(flat(na), maps[UP1A]) + times(flat(nb), maps[UP1B])).reshape(18, 16, 128)
    add_refined(w2, 18, e1i, e1, 6)
    relax(e1, s1, f1, c1, 36, 0.25, UM, paired)
    relax(s1, e1, f1, c1, 36, 0.25, UM, paired)

    def near(i):
        v = e1[i + 1 + gx * 9]
        n1[i] = jnp.where(upper(L1, 16), v[0:16], v[8:24])

    loop(27, near, 9)

    n1[...] = times(flat(n1), maps[UP0]).reshape(27, 16, 128)
    add_refined(n1, 27, e0i, e0, 9)
    relax(e0, s0, f0, c0, 54, 1.0, UR, paired)
    relax(s0, e0, f0, c0, 54, 1.0, UR, paired)
    shift = gx * 6
    mine = lanes(24) % 64 < 48

    def last(x, carry):
        u, v = carry
        w = x + shift
        z = e0[w + 1]
        az = own_rows(L0, d0[x] * z - paired(e0, w))
        z = own_rows(L0, z)
        f = own_rows(L0, f0[w])
        z_out[x] = z
        az_out[x] = az
        return u + jnp.where(mine, f * z, 0.0), v + jnp.where(mine, z * az, 0.0)

    def some(i, carry):
        for k in range(UZ):
            carry = last(UZ * i + k, carry)
        return carry

    zero = jnp.zeros((24, 128), F32)
    u, v = lax.fori_loop(0, 48 // UZ, some, (zero, zero))

    def total(t):
        return jnp.sum(jnp.sum(t, axis=1, keepdims=True), axis=0, keepdims=True)

    ln = lanes(sums.shape[0])
    sums[...] = jnp.where(ln == 0, total(u), jnp.where(ln == 1, total(v), 0.0))


def k_last(sums, own, z, az, f, sol, res, sv, rv, sems):
    s = jnp.sum(sums[...], axis=0, keepdims=True)
    ln = lanes(1)
    over = jnp.sum(jnp.where(ln == 0, s, 0.0), axis=1, keepdims=True)
    under = jnp.sum(jnp.where(ln == 1, s, 0.0), axis=1, keepdims=True)
    step = over / under
    shift = lax.axis_index("gx") * 6
    pairs = ((0, sv, sol), (1, rv, res))

    def copy(a, src, dst, i):
        part = pl.ds(i * 8, 8)
        return pltpu.make_async_copy(src.at[part], dst.at[part], sems.at[a, i])

    def some(i):
        for k in range(8):
            x = i * 8 + k
            for ref, v in ((sv, own[0, x] + step * z[x]), (rv, own_rows(L0, f[x + shift]) - step * az[x])):
                ref[x, 0:24, :] = v[:, 0:48]
                ref[x, 24:48, :] = roll(v, 64, 1)[:, 0:48]
        for a, src, dst in pairs:
            copy(a, src, dst, i).start()

    loop(6, some)
    for i in range(6):
        for a, src, dst in pairs:
            copy(a, src, dst, i).wait()


def ring(up, dn, axis, low_first=True):
    n = lax.axis_size(axis)
    rise = [(i, (i + 1) % n) for i in range(n)]
    fall = [(i, (i - 1) % n) for i in range(n)]
    if low_first:
        low = lax.ppermute(up, axis, rise)
        high = lax.ppermute(dn, axis, fall)
    else:
        high = lax.ppermute(dn, axis, fall)
        low = lax.ppermute(up, axis, rise)
    return low, high


def swap(v):
    return lax.ppermute(v, "gx", [(0, 1), (1, 0)])


def body(b, x0, rea):
    ALL = ("gx", "gy", "gz")
    sizes = [lax.axis_size(a) for a in ALL]
    count = sizes[0] * sizes[1] * sizes[2]
    b, x0, rea = (pltpu.with_memory_space_constraint(v, pltpu.HBM) for v in (b, x0, rea))
    hi, lo, own = run(
        k_zpack0,
        (sds(*L0.zshape), sds(*L0.zshape), sds(3, 48, 24, 128)),
        (x0, b, rea),
        [(3, 48, 48, 48), pltpu.SemaphoreType.DMA((3, 4))],
        far_in=True,
    )
    zl, zh = ring(hi, lo, "gz")
    turned, r1, maps = run(
        k_early,
        (sds(3, 24, 16, 128), sds(24, 12, 128), sds(10, 256, 128, dtype=jnp.bfloat16)),
        (own,),
        [(24, 24, 128), (24, 16, 128)],
    )
    up, dn = run(k_ypack0, (sds(*L0.yshape),) * 2, (own, turned, zl, zh))
    yl, yh = ring(up, dn, "gy")
    mid = run(k_zmerge, sds(3, 48, 24, 128), (own, zl, zh, dn))
    xr = swap(run(k_xpack0, sds(*L0.xshape), (mid, yl, yh)))
    p0, q0, o0 = (54, 32, 128), (56, 32, 128), (48, 32, 128)
    xw, part, d0, cw = run(k_windows0, (sds(*o0),) * 4, (mid, yl, yh))
    f0, c0, e0, f1, z1h, z1l = run(
        k_down0,
        (sds(*p0), sds(*p0), sds(*q0), sds(24, 12, 128), sds(*L1.zshape), sds(*L1.zshape)),
        (xw, part, d0, cw, r1, maps, xr),
        [(8, 32, 128), q0, (24, 24, 128), (24, 16, 128)],
        mib=M0,
    )
    zl, zh = ring(z1h, z1l, "gz")
    up, dn = run(k_ypack1, (sds(*L1.yshape),) * 2, (f1, r1, zl, zh))
    yl, yh = ring(up, dn, "gy")
    xr = swap(run(k_xpack1, sds(*L1.xshape), (f1, r1, zl, zh, yl, yh), [(2, 2, 24, 128)]))
    p1, q1, p2, q2 = (36, 24, 128), (38, 24, 128), (18, 32, 128), (20, 32, 128)
    win = run(k_windows1, sds(2, 24, 24, 128), (f1, r1, zl, zh, yl, yh), [(8, 2, 24, 128)])
    f1w, c1w, e1w, f2w, c2w, e2w, g = run(
        k_down1,
        (sds(*p1), sds(*p1), sds(*q1), sds(*p2), sds(*p2), sds(*q2), sds(count * 4, 128)),
        (win, maps, xr),
        [p1, q1, (18, 24, 128), (2, 18, 16, 128), p2, q2, (9, 32, 128), (2, 9, 16, 128), (128, 128)],
        mib=M1,
    )
    g = lax.all_to_all(g, ALL, 0, 0, tiled=True)
    n3 = [6 * s for s in sizes]
    R3 = (n3[1] + 8) // 8 * 8
    if R3 % 16:
        R3 += 8
    p3, q3, p4 = (n3[0], R3, 128), (n3[0] + 2, R3, 128), (n3[0] // 2, R3 // 2, 128)
    z, az, sums = run(
        k_up,
        (sds(48, 24, 128), sds(48, 24, 128), sds(count, 128)),
        (g, maps, f2w, c2w, e2w, f1w, c1w, e1w, f0, c0, d0, e0),
        [q3, q3, p3, p3, p3, (n3[0] // 2, R3, 128), p4, p4, (sizes[0] * sizes[1], 128, 128), (9, 16, 128), (18, 16, 128),
         (18, 16, 128), (18, 16, 128), (27, 16, 128), q2, q2, q1, q1, q0, q0],
        mib=M2,
    )
    sums = lax.all_to_all(sums.reshape(count, 1, 128), ALL, 0, 0, tiled=True).reshape(count, 128)
    return run(
        k_last,
        (sds(48, 48, 48), sds(48, 48, 48)),
        (sums, own, z, az, f0),
        [(48, 48, 48), (48, 48, 48), pltpu.SemaphoreType.DMA((2, 6))],
        far_out=True,
    )


def solution(mesh):
    spec = P("gx", "gy", "gz")
    return jax.shard_map(body, mesh=mesh, in_specs=(spec, spec, spec), out_specs=(spec, spec), check_vma=False)
```

```python
import functools
import jax
import jax.numpy as jnp
from jax import lax
from jax.experimental import pallas as pl
from jax.experimental.pallas import tpu as pltpu
from jax.sharding import PartitionSpec as P

W = 6.0 / 7.0
BOTTOM_ITERS = 6
N0 = 48
F32 = jnp.float32
HI = lax.Precision.HIGHEST
M0, M1, M2 = 10, 8, 12
UF, UR, UM, UZ, UL = 12, 54, 36, 24, 24


class Spec:
    def __init__(self, n, h, na, R, o, hx, cut, kp, st):
        self.n, self.h, self.na, self.R, self.o, self.hx, self.cut, self.kp, self.st = n, h, na, R, o, hx, cut, kp, st
        self.half = n // 2
        self.zshape = (n // (kp * st), self.half * st, 128)
        self.yshape = (self.half, na * h, 128)
        self.hs = (h,) * na
        self.xshape = (hx, na, R, 128)
        self.nx = n + hx

    def slot(self, x, a):
        if self.st == 1:
            h = self.hs[a]
            many = 64 // h
            return ZBASE[a] + lax.div(x, many), 0, h * lax.rem(x, many)
        per = self.n // self.st
        t, y = lax.div(x, per), lax.rem(x, per)
        return lax.div(y, self.kp), t, self.h * (lax.rem(y, self.kp) * self.na + a)


L0 = Spec(48, 5, 3, 32, 8, 6, 56, 4, 1)
L1 = Spec(24, 12, 2, 24, 12, 12, 44, 2, 2)
L0.hs = (5, 4, 4)
ZBASE = (0, 4, 7)
YBASE = (0, 40, 72)
L0.zshape = (10, 24, 128)
L0.yshape = (3, 104, 128)


def sds(*shape, dtype=F32):
    return jax.ShapeDtypeStruct(shape, dtype)


def run(kernel, outs, args, scratch=(), mib=12, far_in=False, far_out=False):
    vmem = pl.BlockSpec(memory_space=pltpu.VMEM)
    hbm = pl.BlockSpec(memory_space=pl.ANY)
    return pl.pallas_call(
        kernel,
        out_shape=outs,
        in_specs=[hbm if far_in else vmem] * len(args),
        out_specs=jax.tree.map(lambda _: hbm if far_out else vmem, outs),
        scratch_shapes=[pltpu.VMEM(s, F32) if isinstance(s, tuple) else s for s in scratch],
        compiler_params=pltpu.CompilerParams(vmem_limit_bytes=mib * 1024 * 1024),
    )(*args)


def place():
    return [lax.axis_index(a) for a in ("gx", "gy", "gz")] + [lax.axis_size(a) for a in ("gy", "gz")]


def lanes(rows):
    return lax.broadcasted_iota(jnp.int32, (rows, 128), 1)


def roll(v, shift, axis):
    if isinstance(shift, int):
        shift = shift % v.shape[axis]
        if shift == 0:
            return v
    return pltpu.roll(v, shift, axis)


def loop(n, f, u=1):
    u = max(d for d in range(1, u + 1) if n % d == 0)

    def some(i, c):
        for k in range(u):
            f(i * u + k)
        return c

    lax.fori_loop(0, n // u, some, 0)


def upper(sp, rows):
    l = lanes(rows)
    return (l >= sp.cut) & (l < sp.cut + 64)


def edge(sp, ids):
    _, gy, gz, ny, nz = ids
    high = jnp.where(gz < nz - 1, sp.n + sp.h, sp.n)
    low = jnp.where(gz > 0, 64 - sp.h, 64)
    return high, low, jnp.where(gy > 0, 1.0, 0.0), jnp.where(gy < ny - 1, 1.0, 0.0)


def ztile(sp, items):
    l = lanes(sp.half)
    hi = [jnp.zeros((sp.half, 128), F32)] * 2
    lo = list(hi)
    for k, (v, at, h) in enumerate(items):
        r = roll(v, at, 1)
        hi[k % 2] = jnp.where(((l + (64 - (at + sp.n - h) % 64)) & 63) < h, r, hi[k % 2])
        lo[k % 2] = jnp.where(((l + (64 - at)) & 63) < h, r, lo[k % 2])
    return roll(hi[0] + hi[1], -2 * sp.n, 1), lo[0] + lo[1]


def ztile1(own, hi_ref, lo_ref, g):
    sp = L1
    for t in range(sp.st):
        items = [
            (own(t * (sp.n // sp.st) + g * sp.kp + k, a), sp.h * (k * sp.na + a), sp.h)
            for k in range(sp.kp)
            for a in range(sp.na)
        ]
        hi, lo = ztile(sp, items)
        hi_ref[g, t * sp.half : (t + 1) * sp.half, :] = hi
        lo_ref[g, t * sp.half : (t + 1) * sp.half, :] = lo


def merged(sp, own, zl, zh, x, a, b, e, top, bottom):
    g, t, at = sp.slot(x, a)
    if sp.st == 1:
        high, low = zh[g, b:e, :], zl[g, b:e, :]
    else:
        high = jnp.where(t == 0, zh[g, b:e, :], zh[g, sp.half + b : sp.half + e, :])
        low = jnp.where(t == 0, zl[g, b:e, :], zl[g, sp.half + b : sp.half + e, :])
    l = lanes(e - b)
    beside = jnp.where(((l + (64 - at)) & 63) < sp.hs[a], high, low)
    beside = roll(beside, (sp.n + 128 - at) & 127, 1)
    q = l & 63
    return jnp.where(q < sp.n, own(x, a)[b:e], jnp.where((q < top) | (q >= bottom), beside, 0.0))


def ypack0(own, turned, zl, zh, up_ref, dn_ref):
    top, bottom, _, _ = edge(L0, place())
    l = lanes(8)
    q = l & 63
    up = upper(L0, 8)

    def beside(x, a, b, turn):
        g, _, at = L0.slot(x, a)
        v = jnp.where(((l + (64 - at)) & 63) < L0.hs[a], zh[g, b : b + 8, :], zl[g, b : b + 8, :])
        v = roll(v, (L0.n + turn + 128 - at) & 127, 1)
        return jnp.where((q < top) | (q >= bottom), v, 0.0)

    def some(i):
        for k in range(8):
            p = 8 * i + k
            for a in range(3):
                h = L0.hs[a]
                for ref, b, s in ((up_ref, 16, 8 - h), (dn_ref, 0, 0)):
                    even = jnp.where(q < L0.n, own[a, 2 * p, b : b + 8, :], beside(2 * p, a, b, 0))
                    odd = jnp.where(q < L0.n, turned[a, p, b // 2 : b // 2 + 8, :], beside(2 * p + 1, a, b, 64))
                    v = jnp.where(up, even, odd) if b else jnp.where(up, odd, even)
                    ref[i, pl.ds(YBASE[a] + k, h, stride=8), :] = v[s : s + h]

    loop(3, some, 3)


def ypack1(own, zl, zh, up_ref, dn_ref, u):
    sp = L1
    half = sp.half
    top, bottom, _, _ = edge(sp, place())

    def pair(p):
        for a in range(sp.na):
            even = merged(sp, own, zl, zh, 2 * p, a, 0, half, top, bottom)
            odd = roll(merged(sp, own, zl, zh, 2 * p + 1, a, 0, half, top, bottom), 64, 1)
            up = upper(sp, half)
            up_ref[p, a * half : (a + 1) * half, :] = jnp.where(up, even, odd)
            dn_ref[p, a * half : (a + 1) * half, :] = jnp.where(up, odd, even)

    loop(half, pair, u)


def y_tiles0(yl, yh, g, t, a):
    def rows(ref, start):
        return ref[g, pl.ds(start + t, 8, stride=8), :]

    if a == 0:
        return roll(rows(yl, 0), 3, 0), rows(yh, 0)
    return rows(yl, YBASE[a] - 32), rows(yh, 40) if a == 1 else roll(rows(yh, 40), 4, 0)


def plane0(m, tiles, ends, turn):
    _, _, below, above = ends
    low, high = tiles
    lower = jnp.concatenate([roll(low, turn, 1) * below, m], axis=0)
    higher = jnp.concatenate([m, roll(high, turn, 1) * above], axis=0)
    return jnp.where(upper(L0, L0.R), higher, lower)


def plane1(own, zl, zh, yl, yh, x, a, dst, xw, ends, spare):
    top, bottom, below, above = ends
    sp = L1
    h, half = sp.h, sp.half
    m = merged(sp, own, zl, zh, x, a, 0, half, top, bottom)
    p = lax.div(x, 2)
    turn = 64 * (1 - lax.rem(x, 2))
    spare[0, 0:h, :] = roll(yl[p, a * h : (a + 1) * h, :], turn, 1) * below
    spare[0, h:, :] = m
    spare[1, 0:half, :] = m
    spare[1, half:, :] = roll(yh[p, a * h : (a + 1) * h, :], turn, 1) * above
    dst[xw] = jnp.where(upper(sp, sp.R), spare[1], spare[0])


def lane_z(sp, l):
    return jnp.where(l < sp.cut, l, jnp.where(l < sp.cut + 64, l - 64, l - 128))


def inside(sp, ids):
    _, gy, gz, ny, nz = ids
    n, h = sp.n, min(sp.hs)
    y = lax.broadcasted_iota(jnp.int32, (sp.R, 128), 0) - sp.o + jnp.where(upper(sp, sp.R), sp.R, 0)
    z = lane_z(sp, lanes(sp.R))
    ok = (y >= -h) & (y < n + h) & (z >= -h) & (z < n + h)
    y, z = y + gy * n, z + gz * n
    return ok & (y >= 0) & (y < ny * n) & (z >= 0) & (z < nz * n)


def paired(ref, x):
    c = ref[x + 1]
    R = c.shape[0]
    s = ref[x] + ref[x + 2]
    sub = lax.broadcasted_iota(jnp.int32, (8, 128), 0)
    seam = roll(jnp.where(sub == 0, c[0:8], c[R - 8 : R]), 64, 1)
    last = jnp.where(sub == 7, roll(seam, 7, 0), roll(c[R - 8 :], 7, 0))
    first = jnp.where(sub == 0, roll(seam, 1, 0), roll(c[0:8], 1, 0))
    up = jnp.concatenate([ref[x + 1, 1 : R - 7, :], last], axis=0)
    down = jnp.concatenate([first, ref[x + 1, 7 : R - 1, :]], axis=0)
    s = s + (up + down)
    return s + (roll(c, 1, 1) + roll(c, 127, 1))


def domain(sp, n, h, r0, R, ids):
    row = lax.broadcasted_iota(jnp.int32, (R, 128), 0) - r0
    ln = lanes(R)
    z = jnp.where(ln < 64, ln, ln - 128)
    gy, gz, ny, nz = ids[1], ids[2], ids[3], ids[4]
    y_at, z_at = row + gy * n, z + gz * n
    ok = (row >= -h) & (row < n + h) & (z >= -h) & (z < n + h)
    return ok & (y_at >= 0) & (y_at < ny * n) & (z_at >= 0) & (z_at < nz * n)


def neighbours(ref, x):
    c = ref[x + 1]
    R = c.shape[0]
    s = ref[x] + ref[x + 2]
    s = s + (roll(c, 1, 0) + roll(c, R - 1, 0))
    return s + (roll(c, 1, 1) + roll(c, 127, 1))


def zero_ends(ref, n):
    ref[0] = jnp.zeros(ref.shape[1:], F32)
    ref[n + 1] = jnp.zeros(ref.shape[1:], F32)


def relax(src, dst, f, c, n, factor, u=9, near=None):
    near = near or neighbours

    def one(x):
        dst[x + 1] = (1.0 - W) * src[x + 1] + c[x] * (f[x] + factor * near(src, x))

    loop(n, one, u)


def lane_map(pick, value):
    l = lax.broadcasted_iota(jnp.int32, (256, 128), 0) & 127
    m = lax.broadcasted_iota(jnp.int32, (256, 128), 1)
    return jnp.where(pick(l) == m, value, 0.0).astype(jnp.bfloat16)


def spread_map(pick):
    m = lax.broadcasted_iota(jnp.int32, (256, 128), 0) & 127
    l = lax.broadcasted_iota(jnp.int32, (256, 128), 1)
    return jnp.where(pick(l) == m, 1.0, 0.0).astype(jnp.bfloat16)


def floor_half(z):
    return lax.shift_right_arithmetic(z, 1)


def coarse_lane(sp, l, want):
    z = lane_z(sp, l)
    up = (l >= sp.cut) & (l < sp.cut + 64)
    good = (z >= -sp.h) & (z < sp.n + sp.h)
    good = good & (up if want else jnp.logical_not(up))
    return jnp.where(good, floor_half(z) + jnp.where(z < 0, 128, 0), -1)


def both_lanes(l):
    lower, higher = coarse_lane(L0, l, False), coarse_lane(L0, l, True)
    return jnp.where(lower >= 0, lower, jnp.where(higher >= 0, (higher + 64) & 127, -1))


OWN, DOWN1A, DOWN1B, DOWN2, DOWN3, UP3, UP2, UP1A, UP1B, UP0 = range(10)


def all_maps(maps, gz):
    half = floor_half
    maps[OWN] = lane_map(lambda l: jnp.where(l < 64, half(l), 32 + half(l)), 0.125)
    maps[DOWN1A] = lane_map(lambda l: coarse_lane(L1, l, False), 0.125)
    maps[DOWN1B] = lane_map(lambda l: coarse_lane(L1, l, True), 0.125)
    maps[DOWN2] = lane_map(lambda l: jnp.where(l < 64, half(l), half(l) + 64), 0.125)
    maps[DOWN3] = lane_map(half, 0.125)
    maps[UP3] = spread_map(half)
    maps[UP2] = spread_map(lambda l: gz * 6 + jnp.where(l < 64, half(l), half(l) - 64))
    maps[UP1A] = spread_map(lambda l: coarse_lane(L1, l, False))
    maps[UP1B] = spread_map(lambda l: coarse_lane(L1, l, True))
    maps[UP0] = spread_map(both_lanes)


def times(v, m):
    big = v.astype(jnp.bfloat16)
    rest = (v - big.astype(F32)).astype(jnp.bfloat16)
    return jnp.dot(jnp.concatenate([big, rest], axis=1), m, preferred_element_type=F32)


def coarsen_planes(pair, n, tmp, acc, rows, u=2):
    half = rows // 2

    def one(x):
        tmp[x, 0:rows, :] = pair(x)
        acc[x, 0:half, :] = tmp[x, pl.ds(0, half, stride=2), :] + tmp[x, pl.ds(1, half, stride=2), :]

    loop(n, one, u)


def flat(ref):
    n, rows, _ = ref.shape
    return ref[...].reshape(n * rows, 128)


def add_refined(wide, n, src, dst, u=3):
    R = dst.shape[1]

    def one(i):
        v = wide[i, 0 : R // 2, :]
        for k in range(2):
            dst[2 * i + 1, pl.ds(k, R // 2, stride=2), :] = v
        t = dst[2 * i + 1]
        dst[2 * i + 1] = src[2 * i + 1] + t
        dst[2 * i + 2] = src[2 * i + 2] + t

    loop(n, one, u)


def k_zpack0(x0, b, rea, hi, lo, own, raw, sems):
    def copy(a, ref, i):
        many = 64 // L0.hs[a]
        part = pl.ds(i * many, many)
        return pltpu.make_async_copy(ref.at[part], raw.at[a, part], sems.at[a, i])

    refs = (x0, b, rea)
    parts = [48 * h // (64 // h * h) for h in L0.hs]
    for a, ref in enumerate(refs):
        for i in range(parts[a]):
            copy(a, ref, i).start()

    def pack(a, i):
        h = L0.hs[a]
        many = 64 // h
        hi[ZBASE[a] + i], lo[ZBASE[a] + i] = ztile(L0, [(own[a, i * many + k], h * k, h) for k in range(many)])

    steps = [(a, ref, i) for a, ref in enumerate(refs) for i in range(parts[a])]
    for n, (a, ref, i) in enumerate(steps):
        copy(a, ref, i).wait()
        if n:
            pack(steps[n - 1][0], steps[n - 1][2])
        many = 64 // L0.hs[a]
        for x in range(i * many, i * many + many):
            own[a, x, :, 0:48] = raw[a, x, 0:24, :]
            own[a, x, :, 64:112] = raw[a, x, 24:48, :]
    pack(steps[-1][0], steps[-1][2])


def k_ypack0(own, turned, zl, zh, up, dn):
    ypack0(own, turned, zl, zh, up, dn)


def k_xpack0(mid, yl, yh, out):
    ids = place()
    ends = edge(L0, ids)
    first = ids[0] == 0
    for i in range(6):
        x = jnp.where(first, 42, 0) + i
        for a in range(3):
            there, here = y_tiles0(yl, yh, 2, 5 + i // 2, a), y_tiles0(yl, yh, 0, i // 2, a)
            tiles = [jnp.where(first, v, w) for v, w in zip(there, here)]
            out[i, a] = plane0(mid[a, x], tiles, ends, 64 * (1 - i % 2))


def k_xpack1(f1, r1, zl, zh, yl, yh, out, spare):
    both = (f1, r1)
    ids = place()
    ends = edge(L1, ids)

    def one(i):
        for a in range(2):
            plane1(lambda x, a: both[a][x], zl, zh, yl, yh, (1 - ids[0]) * 12 + i, a, out.at[i], a, ends, spare.at[i, a])

    loop(12, one, 12)


def beside0(c):
    R = L0.R
    sub = lax.broadcasted_iota(jnp.int32, (8, 128), 0)
    seam = roll(jnp.where(sub == 0, c[0:8], c[R - 8 : R]), 64, 1)
    up, down = roll(c, R - 1, 0), roll(c, 1, 0)
    up = jnp.concatenate([up[: R - 8], jnp.where(sub == 7, roll(seam, 7, 0), up[R - 8 :])], axis=0)
    down = jnp.concatenate([jnp.where(sub == 0, roll(seam, 1, 0), down[0:8]), down[8:]], axis=0)
    return (up + down) + (roll(c, 1, 1) + roll(c, 127, 1))


def k_windows0(mid, yl, yh, xw, part, d_out, c_out):
    ids = place()
    ends = edge(L0, ids)
    ok = inside(L0, ids)

    def some(i):
        for k in range(16):
            x = 16 * i + k
            v, b, rea = (plane0(mid[a, x], y_tiles0(yl, yh, i, k // 2, a), ends, 64 * (1 - k % 2)) for a in range(3))
            d = 6.0 + rea
            xw[x] = v
            part[x] = b - d * v + beside0(v)
            d_out[x] = d
            c_out[x] = jnp.where(ok, W / d, 0.0)

    loop(3, some)


def own_rows(sp, v):
    return jnp.where(upper(sp, sp.half), v[0 : sp.half], v[sp.o :])


def half_own(pair, tmp, acc, out, u, m):
    coarsen_planes(pair, 24, tmp, acc, 24, u)
    acc[...] = times(flat(acc), m).reshape(24, 16, 128)

    def keep(x):
        out[x] = acc[x, 0:12, :]

    loop(24, keep, 6)


def k_zmerge(own, zl, zh, dn, out):
    top, bottom, _, _ = edge(L0, place())

    def one(x):
        for a in range(3):
            out[a, x] = merged(L0, lambda x, a: own[a, x], zl, zh, x, a, 0, 24, top, bottom)

    loop(48, one, 8)


def k_early(own, turned, r1, maps, tmp, acc):
    def turn(p):
        for a in range(3):
            v = own[a, 2 * p + 1]
            turned[a, p, 0:8, :] = roll(v[0:8], 64, 1)
            turned[a, p, 8:16, :] = roll(v[16:24], 64, 1)

    loop(24, turn, 4)
    all_maps(maps, lax.axis_index("gz"))
    mine = lanes(24) % 64 < 48
    half_own(lambda x: jnp.where(mine, own[2, 2 * x] + own[2, 2 * x + 1], 0.0), tmp, acc, r1, 4, maps[OWN])


def k_down0(xw, part, d, cw, r1, maps, xr, f_out, c_out, e_out, f1, z1h, z1l, xb, ew, tmp, acc):
    ids = place()
    n = L0.nx
    shift = ids[0] * L0.hx
    other = (1 - ids[0]) * L0.n
    low_side = ids[0] == 0
    ok = inside(L0, ids)
    zero_ends(ew, n)
    zero_ends(e_out, n)
    zero = jnp.zeros((L0.R, 128), F32)
    xb[0] = jnp.where(low_side, xw[47], zero)
    xb[7] = jnp.where(low_side, zero, xw[0])
    for i in range(6):
        xb[i + 1] = xr[i, 0]

    def put(w, f, c):
        f_out[w] = f
        c_out[w] = c
        ew[w + 1] = c * f

    def mine(x):
        put(x + shift, part[x] + (xw[x - 1] + xw[x + 1]), cw[x])

    loop(46, lambda i: mine(i + 1), 23)
    put(shift, part[0] + (jnp.where(low_side, zero, xr[5, 0]) + xw[1]), cw[0])
    put(47 + shift, part[47] + (xw[46] + jnp.where(low_side, xr[0, 0], zero)), cw[47])

    def theirs(i):
        v = xb[i + 1]
        dd = 6.0 + xr[i, 2]
        f = xr[i, 1] - dd * v + beside0(v) + (xb[i] + xb[i + 2])
        put(i + other, f, jnp.where(ok, W / dd, 0.0))

    loop(6, theirs, 6)
    relax(ew, e_out, f_out, c_out, n, 1.0, UR, paired)

    def left(x):
        return own_rows(L0, f_out[x + shift] - d[x] * e_out[x + shift + 1] + paired(e_out, x + shift))

    within = lanes(24) % 64 < 48
    pair = lambda x: jnp.where(within, left(2 * x) + left(2 * x + 1), 0.0)
    half_own(pair, tmp, acc, f1, UL, maps[OWN])
    both = (f1, r1)
    loop(6, lambda g: ztile1(lambda x, a: both[a][x], z1h, z1l, g), 3)


def k_ypack1(f1, r1, zl, zh, up, dn):
    both = (f1, r1)
    ypack1(lambda x, a: both[a][x], zl, zh, up, dn, 12)


def k_windows1(f1, r1, zl, zh, yl, yh, out, spare):
    both = (f1, r1)
    ends = edge(L1, place())

    def some(i):
        for k in range(4):
            for a in range(2):
                plane1(lambda x, a: both[a][x], zl, zh, yl, yh, 4 * i + k, a, out.at[a], 4 * i + k, ends, spare.at[2 * k + a])

    loop(6, some)


def k_down1(win, maps, xr, fw, cw, e_out, f2, c2, e2, out3, rw, ew, tmp, acc, r2, ew2, tmp2, t3, sq):
    ids = place()
    n = L1.nx
    shift = ids[0] * L1.hx
    other = (1 - ids[0]) * L1.n

    def put(x):
        fw[x + shift] = win[0, x]
        rw[x + shift] = win[1, x]

    def take(x):
        fw[x + other] = xr[x, 0]
        rw[x + other] = xr[x, 1]

    loop(24, put, 8)
    loop(12, take, 6)
    ok = inside(L1, ids)
    zero_ends(ew, n)
    zero_ends(e_out, n)

    def first(x):
        c = jnp.where(ok, W / (1.5 + rw[x]), 0.0)
        cw[x] = c
        ew[x + 1] = c * fw[x]

    loop(n, first, 6)
    relax(ew, e_out, fw, cw, n, 0.25, UM, paired)

    def left(x):
        return fw[x] - (1.5 + rw[x]) * e_out[x + 1] + 0.25 * paired(e_out, x)

    for ref, pair in ((f2, lambda x: left(2 * x) + left(2 * x + 1)), (r2, lambda x: rw[2 * x] + rw[2 * x + 1])):
        coarsen_planes(pair, 18, tmp, acc.at[0], 24, 18)
        v = flat(acc.at[0])
        acc[0] = times(v, maps[DOWN1A]).reshape(18, 16, 128)
        acc[1] = times(v, maps[DOWN1B]).reshape(18, 16, 128)

        def keep(x, ref=ref):
            ref[x] = jnp.zeros((32, 128), F32)
            ref[x, 2:14, :] = acc[0, x, 0:12, :]
            ref[x, 14:26, :] = acc[1, x, 0:12, :]

        loop(18, keep, 6)
    ok2 = domain(None, 12, 6, 8, 32, ids)
    zero_ends(ew2, 18)
    zero_ends(e2, 18)

    def second(x):
        c = jnp.where(ok2, W / (0.375 + r2[x]), 0.0)
        c2[x] = c
        ew2[x + 1] = c * f2[x]

    loop(18, second, 6)
    relax(ew2, e2, f2, c2, 18, 0.0625, 18)

    def left2(x):
        return f2[x] - (0.375 + r2[x]) * e2[x + 1] + 0.0625 * neighbours(e2, x)

    for a, pair in enumerate((lambda x: left2(2 * x) + left2(2 * x + 1), lambda x: r2[2 * x] + r2[2 * x + 1])):
        coarsen_planes(pair, 9, tmp2, t3.at[a], 32, 9)
        t3[a] = times(flat(t3.at[a]), maps[DOWN2]).reshape(9, 16, 128)
    shift = ids[0] * 3
    sq[...] = jnp.zeros((128, 128), F32)
    for a in range(2):
        for x in range(6):
            at = a * 36 + x * 6
            sq[at : at + 6, :] = t3[a, x + shift, 4:10, :]
    t = sq[...].T[0:8]
    ln = lanes(1)
    rows = []
    for u in range(2):
        for a in range(2):
            parts = [roll(t, 36 * (w - a), 1)[3 * u + w : 3 * u + w + 1] for w in range(3)]
            rows.append(jnp.where(ln < 36, parts[0], jnp.where(ln < 72, parts[1], parts[2])))
    tile = jnp.concatenate(rows + rows, axis=0)
    n8 = out3.shape[0] // 8
    out3[...] = jnp.broadcast_to(tile[None], (n8, 8, 128)).reshape(n8 * 8, 128)


def sum_all(v):
    s = jnp.sum(v, axis=0)
    s = sum(s[k : k + 8] for k in range(0, s.shape[0], 8))
    return jnp.sum(jnp.sum(s, axis=1, keepdims=True), axis=0, keepdims=True)


def coarse_solve(g3, maps, nx, ny, nz, e3, s3, f3, c3, r3, tmp, f4, r4, sq):
    R = f3.shape[1]
    for ref in (f3, r3):
        ref[...] = jnp.zeros(ref.shape, F32)
    kx, ky, kz = nx // 6, ny // 6, nz // 6
    for bx in range(kx):
        for by in range(ky):
            k = bx * ky + by
            if kz * 6 < 128:
                sq[k, kz * 6 :, :] = jnp.zeros((128 - kz * 6, 128), F32)
            got = [g3[pl.ds(k * kz * 4 + r, kz, stride=4), :] for r in range(4)]
            ln = lanes(kz)
            for u in range(2):
                for w in range(3):
                    f, r = roll(got[2 * u], -36 * w, 1), roll(got[2 * u + 1], 36 - 36 * w, 1)
                    sq[k, pl.ds(3 * u + w, kz, stride=6), :] = jnp.where(ln < 36, f, r)
            t = sq[k].T
            for x in range(6):
                f3[bx * 6 + x, by * 6 : by * 6 + 6, :] = t[x * 6 : x * 6 + 6]
                r3[bx * 6 + x, by * 6 : by * 6 + 6, :] = t[36 + x * 6 : 42 + x * 6]
    factor = 0.25**3
    ok = (lax.broadcasted_iota(jnp.int32, (R, 128), 0) < ny) & (lanes(R) < nz)
    for ref in (e3, s3):
        zero_ends(ref, nx)

    def first(x):
        c = jnp.where(ok, W / (6.0 * factor + r3[x]), 0.0)
        c3[x] = c
        s3[x + 1] = c * f3[x]

    loop(nx, first, 6)
    relax(s3, e3, f3, c3, nx, factor, 12)

    def left(x):
        v = f3[x] - (6.0 * factor + r3[x]) * e3[x + 1] + factor * neighbours(e3, x)
        return jnp.where(ok, v, 0.0)

    for ref, pair in ((f4, lambda x: left(2 * x) + left(2 * x + 1)), (r4, lambda x: r3[2 * x] + r3[2 * x + 1])):
        coarsen_planes(pair, nx // 2, tmp, ref, R, 6)
        ref[...] = times(flat(ref), maps[DOWN3]).reshape(ref.shape)
    f4k = 0.25**4
    H = R // 2
    row = lax.broadcasted_iota(jnp.int32, (nx // 2, H, 128), 1)
    lane = lax.broadcasted_iota(jnp.int32, (nx // 2, H, 128), 2)
    within = (row < ny // 2) & (lane < nz // 2)
    diag = 6.0 * f4k + r4[...]
    zero = jnp.zeros((1, H, 128), F32)

    def apply(p):
        s = jnp.concatenate([zero, p[:-1]], axis=0) + jnp.concatenate([p[1:], zero], axis=0)
        s = s + roll(p, 1, 1) + roll(p, H - 1, 1) + roll(p, 1, 2) + roll(p, 127, 2)
        return jnp.where(within, diag * p - f4k * s, 0.0)

    r = jnp.where(within, f4[...], 0.0)
    p = r
    q = apply(r)
    rr = sum_all(r * r)
    den = sum_all(r * q)
    a = rr / den
    one_over_rr, one_over_a = 1.0 / rr, den / rr
    e = a * p
    for i in range(1, BOTTOM_ITERS):
        r = r - a * q
        w = apply(r)
        new = sum_all(r * r)
        rw = sum_all(r * w)
        b = new * one_over_rr
        den = rw - b * new * one_over_a
        a = new / den
        one_over_rr, one_over_a = 1.0 / new, den / new
        p = r + b * p
        q = w + b * q
        e = e + a * p
    f4[...] = times(e.reshape(nx // 2 * H, 128), maps[UP3]).reshape(e.shape)
    add_refined(f4, nx // 2, e3, s3, 6)
    relax(s3, e3, f3, c3, nx, factor, 12)
    relax(e3, s3, f3, c3, nx, factor, 12)


def k_up(g3, maps, f2, c2, e2i, f1, c1, e1i, f0, c0, d0, e0i, z_out, az_out, sums,
         e3, s3, f3, c3, r3, tmp3, f4, r4, sq, w3, w2, na, nb, n1, e2, s2, e1, s1, e0, s0):
    gx, gy, gz, sy, sz = place()
    nx, ny, nz = f3.shape[0], sy * 6, sz * 6
    coarse_solve(g3, maps, nx, ny, nz, e3, s3, f3, c3, r3, tmp3, f4, r4, sq)
    for ref, n in ((s2, 18), (s1, 36), (s0, 54), (e2, 18), (e1, 36), (e0, 54)):
        zero_ends(ref, n)
    for i in range(9):
        e = s3[i + 1 + gx * 3]
        e = jnp.concatenate([jnp.zeros((8, 128), F32), e, jnp.zeros((8, 128), F32)], axis=0)
        v = e[4:20]
        for k in range(1, sy):
            v = jnp.where(gy == k, e[6 * k + 4 : 6 * k + 20], v)
        w3[i] = v
    w3[...] = times(flat(w3), maps[UP2]).reshape(9, 16, 128)
    add_refined(w3, 9, e2i, e2, 9)
    relax(e2, s2, f2, c2, 18, 0.0625, 18)
    relax(s2, e2, f2, c2, 18, 0.0625, 18)

    def halves(i):
        na[i] = e2[i + 1, 2:18, :]
        nb[i] = e2[i + 1, 14:30, :]

    loop(18, halves, 6)

    w2[...] = (times(flat(na), maps[UP1A]) + times(flat(nb), maps[UP1B])).reshape(18, 16, 128)
    add_refined(w2, 18, e1i, e1, 6)
    relax(e1, s1, f1, c1, 36, 0.25, UM, paired)
    relax(s1, e1, f1, c1, 36, 0.25, UM, paired)

    def near(i):
        v = e1[i + 1 + gx * 9]
        n1[i] = jnp.where(upper(L1, 16), v[0:16], v[8:24])

    loop(27, near, 9)

    n1[...] = times(flat(n1), maps[UP0]).reshape(27, 16, 128)
    add_refined(n1, 27, e0i, e0, 9)
    relax(e0, s0, f0, c0, 54, 1.0, UR, paired)
    relax(s0, e0, f0, c0, 54, 1.0, UR, paired)
    shift = gx * 6
    mine = lanes(24) % 64 < 48

    def last(x, carry):
        u, v = carry
        w = x + shift
        z = e0[w + 1]
        az = own_rows(L0, d0[x] * z - paired(e0, w))
        z = own_rows(L0, z)
        f = own_rows(L0, f0[w])
        z_out[x] = z
        az_out[x] = az
        return u + jnp.where(mine, f * z, 0.0), v + jnp.where(mine, z * az, 0.0)

    def some(i, carry):
        for k in range(UZ):
            carry = last(UZ * i + k, carry)
        return carry

    zero = jnp.zeros((24, 128), F32)
    u, v = lax.fori_loop(0, 48 // UZ, some, (zero, zero))

    def total(t):
        return jnp.sum(jnp.sum(t, axis=1, keepdims=True), axis=0, keepdims=True)

    ln = lanes(sums.shape[0])
    sums[...] = jnp.where(ln == 0, total(u), jnp.where(ln == 1, total(v), 0.0))


def k_last(sums, own, z, az, f, sol, res, sv, rv, sems):
    s = jnp.sum(sums[...], axis=0, keepdims=True)
    ln = lanes(1)
    over = jnp.sum(jnp.where(ln == 0, s, 0.0), axis=1, keepdims=True)
    under = jnp.sum(jnp.where(ln == 1, s, 0.0), axis=1, keepdims=True)
    step = over / under
    shift = lax.axis_index("gx") * 6
    pairs = ((0, sv, sol), (1, rv, res))

    def copy(a, src, dst, i):
        part = pl.ds(i * 8, 8)
        return pltpu.make_async_copy(src.at[part], dst.at[part], sems.at[a, i])

    def some(i):
        for k in range(8):
            x = i * 8 + k
            for ref, v in ((sv, own[0, x] + step * z[x]), (rv, own_rows(L0, f[x + shift]) - step * az[x])):
                ref[x, 0:24, :] = v[:, 0:48]
                ref[x, 24:48, :] = roll(v, 64, 1)[:, 0:48]
        for a, src, dst in pairs:
            copy(a, src, dst, i).start()

    loop(6, some)
    for i in range(6):
        for a, src, dst in pairs:
            copy(a, src, dst, i).wait()


def ring(up, dn, axis, low_first=True):
    n = lax.axis_size(axis)
    rise = [(i, (i + 1) % n) for i in range(n)]
    fall = [(i, (i - 1) % n) for i in range(n)]
    if low_first:
        low = lax.ppermute(up, axis, rise)
        high = lax.ppermute(dn, axis, fall)
    else:
        high = lax.ppermute(dn, axis, fall)
        low = lax.ppermute(up, axis, rise)
    return low, high


def swap(v):
    return lax.ppermute(v, "gx", [(0, 1), (1, 0)])


def body(b, x0, rea):
    ALL = ("gx", "gy", "gz")
    sizes = [lax.axis_size(a) for a in ALL]
    count = sizes[0] * sizes[1] * sizes[2]
    b, x0, rea = (pltpu.with_memory_space_constraint(v, pltpu.HBM) for v in (b, x0, rea))
    hi, lo, own = run(
        k_zpack0,
        (sds(*L0.zshape), sds(*L0.zshape), sds(3, 48, 24, 128)),
        (x0, b, rea),
        [(3, 48, 48, 48), pltpu.SemaphoreType.DMA((3, 4))],
        far_in=True,
    )
    zl, zh = ring(hi, lo, "gz")
    turned, r1, maps = run(
        k_early,
        (sds(3, 24, 16, 128), sds(24, 12, 128), sds(10, 256, 128, dtype=jnp.bfloat16)),
        (own,),
        [(24, 24, 128), (24, 16, 128)],
    )
    up, dn = run(k_ypack0, (sds(*L0.yshape),) * 2, (own, turned, zl, zh))
    yl, yh = ring(up, dn, "gy")
    mid = run(k_zmerge, sds(3, 48, 24, 128), (own, zl, zh, dn))
    xr = swap(run(k_xpack0, sds(*L0.xshape), (mid, yl, yh)))
    p0, q0, o0 = (54, 32, 128), (56, 32, 128), (48, 32, 128)
    xw, part, d0, cw = run(k_windows0, (sds(*o0),) * 4, (mid, yl, yh))
    f0, c0, e0, f1, z1h, z1l = run(
        k_down0,
        (sds(*p0), sds(*p0), sds(*q0), sds(24, 12, 128), sds(*L1.zshape), sds(*L1.zshape)),
        (xw, part, d0, cw, r1, maps, xr),
        [(8, 32, 128), q0, (24, 24, 128), (24, 16, 128)],
        mib=M0,
    )
    zl, zh = ring(z1h, z1l, "gz")
    up, dn = run(k_ypack1, (sds(*L1.yshape),) * 2, (f1, r1, zl, zh))
    yl, yh = ring(up, dn, "gy")
    xr = swap(run(k_xpack1, sds(*L1.xshape), (f1, r1, zl, zh, yl, yh), [(12, 2, 2, 24, 128)]))
    p1, q1, p2, q2 = (36, 24, 128), (38, 24, 128), (18, 32, 128), (20, 32, 128)
    win = run(k_windows1, sds(2, 24, 24, 128), (f1, r1, zl, zh, yl, yh), [(8, 2, 24, 128)])
    f1w, c1w, e1w, f2w, c2w, e2w, g = run(
        k_down1,
        (sds(*p1), sds(*p1), sds(*q1), sds(*p2), sds(*p2), sds(*q2), sds(count * 4, 128)),
        (win, maps, xr),
        [p1, q1, (18, 24, 128), (2, 18, 16, 128), p2, q2, (9, 32, 128), (2, 9, 16, 128), (128, 128)],
        mib=M1,
    )
    g = lax.all_to_all(g, ALL, 0, 0, tiled=True)
    n3 = [6 * s for s in sizes]
    R3 = (n3[1] + 8) // 8 * 8
    if R3 % 16:
        R3 += 8
    p3, q3, p4 = (n3[0], R3, 128), (n3[0] + 2, R3, 128), (n3[0] // 2, R3 // 2, 128)
    z, az, sums = run(
        k_up,
        (sds(48, 24, 128), sds(48, 24, 128), sds(count, 128)),
        (g, maps, f2w, c2w, e2w, f1w, c1w, e1w, f0, c0, d0, e0),
        [q3, q3, p3, p3, p3, (n3[0] // 2, R3, 128), p4, p4, (sizes[0] * sizes[1], 128, 128), (9, 16, 128), (18, 16, 128),
         (18, 16, 128), (18, 16, 128), (27, 16, 128), q2, q2, q1, q1, q0, q0],
        mib=M2,
    )
    sums = lax.all_to_all(sums.reshape(count, 1, 128), ALL, 0, 0, tiled=True).reshape(count, 128)
    return run(
        k_last,
        (sds(48, 48, 48), sds(48, 48, 48)),
        (sums, own, z, az, f0),
        [(48, 48, 48), (48, 48, 48), pltpu.SemaphoreType.DMA((2, 6))],
        far_out=True,
    )


def solution(mesh):
    spec = P("gx", "gy", "gz")
    return jax.shard_map(body, mesh=mesh, in_specs=(spec, spec, spec), out_specs=(spec, spec), check_vma=False)
```

```python
import functools
import jax
import jax.numpy as jnp
from jax import lax
from jax.experimental import pallas as pl
from jax.experimental.pallas import tpu as pltpu
from jax.sharding import PartitionSpec as P

W = 6.0 / 7.0
BOTTOM_ITERS = 6
N0 = 48
F32 = jnp.float32
HI = lax.Precision.HIGHEST
M0, M1, M2 = 10, 8, 12
UF, UR, UM, UZ, UL = 12, 54, 36, 24, 24


class Spec:
    def __init__(self, n, h, na, R, o, hx, cut, kp, st):
        self.n, self.h, self.na, self.R, self.o, self.hx, self.cut, self.kp, self.st = n, h, na, R, o, hx, cut, kp, st
        self.half = n // 2
        self.zshape = (n // (kp * st), self.half * st, 128)
        self.yshape = (self.half, na * h, 128)
        self.hs = (h,) * na
        self.xshape = (hx, na, R, 128)
        self.nx = n + hx

    def slot(self, x, a):
        if self.st == 1:
            h = self.hs[a]
            many = 64 // h
            return ZBASE[a] + lax.div(x, many), 0, h * lax.rem(x, many)
        per = self.n // self.st
        t, y = lax.div(x, per), lax.rem(x, per)
        return lax.div(y, self.kp), t, self.h * (lax.rem(y, self.kp) * self.na + a)


L0 = Spec(48, 5, 3, 32, 8, 6, 56, 4, 1)
L1 = Spec(24, 12, 2, 24, 12, 12, 44, 2, 2)
L0.hs = (5, 4, 4)
ZBASE = (0, 4, 7)
YBASE = (0, 40, 72)
L0.zshape = (10, 24, 128)
L0.yshape = (3, 104, 128)


def sds(*shape, dtype=F32):
    return jax.ShapeDtypeStruct(shape, dtype)


def run(kernel, outs, args, scratch=(), mib=12, far_in=False, far_out=False):
    vmem = pl.BlockSpec(memory_space=pltpu.VMEM)
    hbm = pl.BlockSpec(memory_space=pl.ANY)
    return pl.pallas_call(
        kernel,
        out_shape=outs,
        in_specs=[hbm if far_in else vmem] * len(args),
        out_specs=jax.tree.map(lambda _: hbm if far_out else vmem, outs),
        scratch_shapes=[pltpu.VMEM(s, F32) if isinstance(s, tuple) else s for s in scratch],
        compiler_params=pltpu.CompilerParams(vmem_limit_bytes=mib * 1024 * 1024),
    )(*args)


def place():
    return [lax.axis_index(a) for a in ("gx", "gy", "gz")] + [lax.axis_size(a) for a in ("gy", "gz")]


def lanes(rows):
    return lax.broadcasted_iota(jnp.int32, (rows, 128), 1)


def roll(v, shift, axis):
    if isinstance(shift, int):
        shift = shift % v.shape[axis]
        if shift == 0:
            return v
    return pltpu.roll(v, shift, axis)


def loop(n, f, u=1):
    u = max(d for d in range(1, u + 1) if n % d == 0)

    def some(i, c):
        for k in range(u):
            f(i * u + k)
        return c

    lax.fori_loop(0, n // u, some, 0)


def upper(sp, rows):
    l = lanes(rows)
    return (l >= sp.cut) & (l < sp.cut + 64)


def edge(sp, ids):
    _, gy, gz, ny, nz = ids
    high = jnp.where(gz < nz - 1, sp.n + sp.h, sp.n)
    low = jnp.where(gz > 0, 64 - sp.h, 64)
    return high, low, jnp.where(gy > 0, 1.0, 0.0), jnp.where(gy < ny - 1, 1.0, 0.0)


def ztile(sp, items):
    l = lanes(sp.half)
    hi = [jnp.zeros((sp.half, 128), F32)] * 2
    lo = list(hi)
    for k, (v, at, h) in enumerate(items):
        r = roll(v, at, 1)
        hi[k % 2] = jnp.where(((l + (64 - (at + sp.n - h) % 64)) & 63) < h, r, hi[k % 2])
        lo[k % 2] = jnp.where(((l + (64 - at)) & 63) < h, r, lo[k % 2])
    return roll(hi[0] + hi[1], -2 * sp.n, 1), lo[0] + lo[1]


def ztile1(own, hi_ref, lo_ref, g):
    sp = L1
    for t in range(sp.st):
        items = [
            (own(t * (sp.n // sp.st) + g * sp.kp + k, a), sp.h * (k * sp.na + a), sp.h)
            for k in range(sp.kp)
            for a in range(sp.na)
        ]
        hi, lo = ztile(sp, items)
        hi_ref[g, t * sp.half : (t + 1) * sp.half, :] = hi
        lo_ref[g, t * sp.half : (t + 1) * sp.half, :] = lo


def merged(sp, own, zl, zh, x, a, b, e, top, bottom):
    g, t, at = sp.slot(x, a)
    if sp.st == 1:
        high, low = zh[g, b:e, :], zl[g, b:e, :]
    else:
        high = jnp.where(t == 0, zh[g, b:e, :], zh[g, sp.half + b : sp.half + e, :])
        low = jnp.where(t == 0, zl[g, b:e, :], zl[g, sp.half + b : sp.half + e, :])
    l = lanes(e - b)
    beside = jnp.where(((l + (64 - at)) & 63) < sp.hs[a], high, low)
    beside = roll(beside, (sp.n + 128 - at) & 127, 1)
    q = l & 63
    return jnp.where(q < sp.n, own(x, a)[b:e], jnp.where((q < top) | (q >= bottom), beside, 0.0))


def ypack0(own, turned, zl, zh, up_ref, dn_ref):
    top, bottom, _, _ = edge(L0, place())
    l = lanes(8)
    q = l & 63
    up = upper(L0, 8)

    def beside(x, a, b, turn):
        g, _, at = L0.slot(x, a)
        v = jnp.where(((l + (64 - at)) & 63) < L0.hs[a], zh[g, b : b + 8, :], zl[g, b : b + 8, :])
        v = roll(v, (L0.n + turn + 128 - at) & 127, 1)
        return jnp.where((q < top) | (q >= bottom), v, 0.0)

    def some(i):
        for k in range(8):
            p = 8 * i + k
            for a in range(3):
                h = L0.hs[a]
                for ref, b, s in ((up_ref, 16, 8 - h), (dn_ref, 0, 0)):
                    even = jnp.where(q < L0.n, own[a, 2 * p, b : b + 8, :], beside(2 * p, a, b, 0))
                    odd = jnp.where(q < L0.n, turned[a, p, b // 2 : b // 2 + 8, :], beside(2 * p + 1, a, b, 64))
                    v = jnp.where(up, even, odd) if b else jnp.where(up, odd, even)
                    ref[i, pl.ds(YBASE[a] + k, h, stride=8), :] = v[s : s + h]

    loop(3, some, 3)


def ypack1(own, zl, zh, up_ref, dn_ref, u):
    sp = L1
    half = sp.half
    top, bottom, _, _ = edge(sp, place())

    def pair(p):
        for a in range(sp.na):
            even = merged(sp, own, zl, zh, 2 * p, a, 0, half, top, bottom)
            odd = roll(merged(sp, own, zl, zh, 2 * p + 1, a, 0, half, top, bottom), 64, 1)
            up = upper(sp, half)
            up_ref[p, a * half : (a + 1) * half, :] = jnp.where(up, even, odd)
            dn_ref[p, a * half : (a + 1) * half, :] = jnp.where(up, odd, even)

    loop(half, pair, u)


def y_tiles0(yl, yh, g, t, a):
    def rows(ref, start):
        return ref[g, pl.ds(start + t, 8, stride=8), :]

    if a == 0:
        return roll(rows(yl, 0), 3, 0), rows(yh, 0)
    return rows(yl, YBASE[a] - 32), rows(yh, 40) if a == 1 else roll(rows(yh, 40), 4, 0)


def plane0(m, tiles, ends, turn):
    _, _, below, above = ends
    low, high = tiles
    lower = jnp.concatenate([roll(low, turn, 1) * below, m], axis=0)
    higher = jnp.concatenate([m, roll(high, turn, 1) * above], axis=0)
    return jnp.where(upper(L0, L0.R), higher, lower)


def plane1(own, zl, zh, yl, yh, x, a, dst, xw, ends, spare):
    top, bottom, below, above = ends
    sp = L1
    h, half = sp.h, sp.half
    m = merged(sp, own, zl, zh, x, a, 0, half, top, bottom)
    p = lax.div(x, 2)
    turn = 64 * (1 - lax.rem(x, 2))
    spare[0, 0:h, :] = roll(yl[p, a * h : (a + 1) * h, :], turn, 1) * below
    spare[0, h:, :] = m
    spare[1, 0:half, :] = m
    spare[1, half:, :] = roll(yh[p, a * h : (a + 1) * h, :], turn, 1) * above
    dst[xw] = jnp.where(upper(sp, sp.R), spare[1], spare[0])


def lane_z(sp, l):
    return jnp.where(l < sp.cut, l, jnp.where(l < sp.cut + 64, l - 64, l - 128))


def inside(sp, ids):
    _, gy, gz, ny, nz = ids
    n, h = sp.n, min(sp.hs)
    y = lax.broadcasted_iota(jnp.int32, (sp.R, 128), 0) - sp.o + jnp.where(upper(sp, sp.R), sp.R, 0)
    z = lane_z(sp, lanes(sp.R))
    ok = (y >= -h) & (y < n + h) & (z >= -h) & (z < n + h)
    y, z = y + gy * n, z + gz * n
    return ok & (y >= 0) & (y < ny * n) & (z >= 0) & (z < nz * n)


def paired(ref, x):
    c = ref[x + 1]
    R = c.shape[0]
    s = ref[x] + ref[x + 2]
    sub = lax.broadcasted_iota(jnp.int32, (8, 128), 0)
    seam = roll(jnp.where(sub == 0, c[0:8], c[R - 8 : R]), 64, 1)
    last = jnp.where(sub == 7, roll(seam, 7, 0), roll(c[R - 8 :], 7, 0))
    first = jnp.where(sub == 0, roll(seam, 1, 0), roll(c[0:8], 1, 0))
    up = jnp.concatenate([ref[x + 1, 1 : R - 7, :], last], axis=0)
    down = jnp.concatenate([first, ref[x + 1, 7 : R - 1, :]], axis=0)
    s = s + (up + down)
    return s + (roll(c, 1, 1) + roll(c, 127, 1))


def domain(sp, n, h, r0, R, ids):
    row = lax.broadcasted_iota(jnp.int32, (R, 128), 0) - r0
    ln = lanes(R)
    z = jnp.where(ln < 64, ln, ln - 128)
    gy, gz, ny, nz = ids[1], ids[2], ids[3], ids[4]
    y_at, z_at = row + gy * n, z + gz * n
    ok = (row >= -h) & (row < n + h) & (z >= -h) & (z < n + h)
    return ok & (y_at >= 0) & (y_at < ny * n) & (z_at >= 0) & (z_at < nz * n)


def neighbours(ref, x):
    c = ref[x + 1]
    R = c.shape[0]
    s = ref[x] + ref[x + 2]
    s = s + (roll(c, 1, 0) + roll(c, R - 1, 0))
    return s + (roll(c, 1, 1) + roll(c, 127, 1))


def zero_ends(ref, n):
    ref[0] = jnp.zeros(ref.shape[1:], F32)
    ref[n + 1] = jnp.zeros(ref.shape[1:], F32)


def relax(src, dst, f, c, n, factor, u=9, near=None):
    near = near or neighbours

    def one(x):
        dst[x + 1] = (1.0 - W) * src[x + 1] + c[x] * (f[x] + factor * near(src, x))

    loop(n, one, u)


def lane_map(pick, value):
    l = lax.broadcasted_iota(jnp.int32, (256, 128), 0) & 127
    m = lax.broadcasted_iota(jnp.int32, (256, 128), 1)
    return jnp.where(pick(l) == m, value, 0.0).astype(jnp.bfloat16)


def spread_map(pick):
    m = lax.broadcasted_iota(jnp.int32, (256, 128), 0) & 127
    l = lax.broadcasted_iota(jnp.int32, (256, 128), 1)
    return jnp.where(pick(l) == m, 1.0, 0.0).astype(jnp.bfloat16)


def floor_half(z):
    return lax.shift_right_arithmetic(z, 1)


def coarse_lane(sp, l, want):
    z = lane_z(sp, l)
    up = (l >= sp.cut) & (l < sp.cut + 64)
    good = (z >= -sp.h) & (z < sp.n + sp.h)
    good = good & (up if want else jnp.logical_not(up))
    return jnp.where(good, floor_half(z) + jnp.where(z < 0, 128, 0), -1)


def both_lanes(l):
    lower, higher = coarse_lane(L0, l, False), coarse_lane(L0, l, True)
    return jnp.where(lower >= 0, lower, jnp.where(higher >= 0, (higher + 64) & 127, -1))


OWN, DOWN1A, DOWN1B, DOWN2, DOWN3, UP3, UP2, UP1A, UP1B, UP0 = range(10)


def all_maps(maps, gz):
    half = floor_half
    maps[OWN] = lane_map(lambda l: jnp.where(l < 64, half(l), 32 + half(l)), 0.125)
    maps[DOWN1A] = lane_map(lambda l: coarse_lane(L1, l, False), 0.125)
    maps[DOWN1B] = lane_map(lambda l: coarse_lane(L1, l, True), 0.125)
    maps[DOWN2] = lane_map(lambda l: jnp.where(l < 64, half(l), half(l) + 64), 0.125)
    maps[DOWN3] = lane_map(half, 0.125)
    maps[UP3] = spread_map(half)
    maps[UP2] = spread_map(lambda l: gz * 6 + jnp.where(l < 64, half(l), half(l) - 64))
    maps[UP1A] = spread_map(lambda l: coarse_lane(L1, l, False))
    maps[UP1B] = spread_map(lambda l: coarse_lane(L1, l, True))
    maps[UP0] = spread_map(both_lanes)


def times(v, m):
    big = v.astype(jnp.bfloat16)
    rest = (v - big.astype(F32)).astype(jnp.bfloat16)
    return jnp.dot(jnp.concatenate([big, rest], axis=1), m, preferred_element_type=F32)


def coarsen_planes(pair, n, tmp, acc, rows, u=2):
    half = rows // 2

    def one(x):
        tmp[x, 0:rows, :] = pair(x)
        acc[x, 0:half, :] = tmp[x, pl.ds(0, half, stride=2), :] + tmp[x, pl.ds(1, half, stride=2), :]

    loop(n, one, u)


def flat(ref):
    n, rows, _ = ref.shape
    return ref[...].reshape(n * rows, 128)


def add_refined(wide, n, src, dst, u=3):
    R = dst.shape[1]

    def one(i):
        v = wide[i, 0 : R // 2, :]
        for k in range(2):
            dst[2 * i + 1, pl.ds(k, R // 2, stride=2), :] = v
        t = dst[2 * i + 1]
        dst[2 * i + 1] = src[2 * i + 1] + t
        dst[2 * i + 2] = src[2 * i + 2] + t

    loop(n, one, u)


def k_zpack0(x0, b, rea, hi, lo, own, raw, sems):
    def copy(a, ref, i):
        many = 64 // L0.hs[a]
        part = pl.ds(i * many, many)
        return pltpu.make_async_copy(ref.at[part], raw.at[a, part], sems.at[a, i])

    refs = (x0, b, rea)
    parts = [48 * h // (64 // h * h) for h in L0.hs]
    for a, ref in enumerate(refs):
        for i in range(parts[a]):
            copy(a, ref, i).start()

    def pack(a, i):
        h = L0.hs[a]
        many = 64 // h
        hi[ZBASE[a] + i], lo[ZBASE[a] + i] = ztile(L0, [(own[a, i * many + k], h * k, h) for k in range(many)])

    steps = [(a, ref, i) for a, ref in enumerate(refs) for i in range(parts[a])]
    for n, (a, ref, i) in enumerate(steps):
        copy(a, ref, i).wait()
        if n:
            pack(steps[n - 1][0], steps[n - 1][2])
        many = 64 // L0.hs[a]
        for x in range(i * many, i * many + many):
            own[a, x, :, 0:48] = raw[a, x, 0:24, :]
            own[a, x, :, 64:112] = raw[a, x, 24:48, :]
    pack(steps[-1][0], steps[-1][2])


def k_ypack0(own, turned, zl, zh, up, dn):
    ypack0(own, turned, zl, zh, up, dn)


def k_xpack0(mid, yl, yh, out):
    ids = place()
    ends = edge(L0, ids)
    first = ids[0] == 0
    for i in range(6):
        x = jnp.where(first, 42, 0) + i
        for a in range(3):
            there, here = y_tiles0(yl, yh, 2, 5 + i // 2, a), y_tiles0(yl, yh, 0, i // 2, a)
            tiles = [jnp.where(first, v, w) for v, w in zip(there, here)]
            out[i, a] = plane0(mid[a, x], tiles, ends, 64 * (1 - i % 2))


def k_xpack1(f1, r1, zl, zh, yl, yh, out, spare):
    both = (f1, r1)
    ids = place()
    ends = edge(L1, ids)

    def one(i):
        for a in range(2):
            plane1(lambda x, a: both[a][x], zl, zh, yl, yh, (1 - ids[0]) * 12 + i, a, out.at[i], a, ends, spare.at[i, a])

    loop(12, one, 12)


def beside0(c):
    R = L0.R
    sub = lax.broadcasted_iota(jnp.int32, (8, 128), 0)
    seam = roll(jnp.where(sub == 0, c[0:8], c[R - 8 : R]), 64, 1)
    up, down = roll(c, R - 1, 0), roll(c, 1, 0)
    up = jnp.concatenate([up[: R - 8], jnp.where(sub == 7, roll(seam, 7, 0), up[R - 8 :])], axis=0)
    down = jnp.concatenate([jnp.where(sub == 0, roll(seam, 1, 0), down[0:8]), down[8:]], axis=0)
    return (up + down) + (roll(c, 1, 1) + roll(c, 127, 1))


def k_windows0(mid, yl, yh, xw, part, d_out, c_out):
    ids = place()
    ends = edge(L0, ids)
    ok = inside(L0, ids)

    def some(i):
        for k in range(16):
            x = 16 * i + k
            v, b, rea = (plane0(mid[a, x], y_tiles0(yl, yh, i, k // 2, a), ends, 64 * (1 - k % 2)) for a in range(3))
            d = 6.0 + rea
            xw[x] = v
            part[x] = b - d * v + beside0(v)
            d_out[x] = d
            c_out[x] = jnp.where(ok, W / d, 0.0)

    loop(3, some, 3)


def own_rows(sp, v):
    return jnp.where(upper(sp, sp.half), v[0 : sp.half], v[sp.o :])


def half_own(pair, tmp, acc, out, u, m):
    coarsen_planes(pair, 24, tmp, acc, 24, u)
    acc[...] = times(flat(acc), m).reshape(24, 16, 128)

    def keep(x):
        out[x] = acc[x, 0:12, :]

    loop(24, keep, 6)


def k_zmerge(own, zl, zh, dn, out):
    top, bottom, _, _ = edge(L0, place())

    def one(x):
        for a in range(3):
            out[a, x] = merged(L0, lambda x, a: own[a, x], zl, zh, x, a, 0, 24, top, bottom)

    loop(48, one, 8)


def k_early(own, turned, r1, maps, tmp, acc):
    def turn(p):
        for a in range(3):
            v = own[a, 2 * p + 1]
            turned[a, p, 0:8, :] = roll(v[0:8], 64, 1)
            turned[a, p, 8:16, :] = roll(v[16:24], 64, 1)

    loop(24, turn, 4)
    all_maps(maps, lax.axis_index("gz"))
    mine = lanes(24) % 64 < 48
    half_own(lambda x: jnp.where(mine, own[2, 2 * x] + own[2, 2 * x + 1], 0.0), tmp, acc, r1, 4, maps[OWN])


def k_down0(xw, part, d, cw, r1, maps, xr, f_out, c_out, e_out, f1, z1h, z1l, xb, ew, tmp, acc):
    ids = place()
    n = L0.nx
    shift = ids[0] * L0.hx
    other = (1 - ids[0]) * L0.n
    low_side = ids[0] == 0
    ok = inside(L0, ids)
    zero_ends(ew, n)
    zero_ends(e_out, n)
    zero = jnp.zeros((L0.R, 128), F32)
    xb[0] = jnp.where(low_side, xw[47], zero)
    xb[7] = jnp.where(low_side, zero, xw[0])
    for i in range(6):
        xb[i + 1] = xr[i, 0]

    def put(w, f, c):
        f_out[w] = f
        c_out[w] = c
        ew[w + 1] = c * f

    def mine(x):
        put(x + shift, part[x] + (xw[x - 1] + xw[x + 1]), cw[x])

    loop(46, lambda i: mine(i + 1), 46)
    put(shift, part[0] + (jnp.where(low_side, zero, xr[5, 0]) + xw[1]), cw[0])
    put(47 + shift, part[47] + (xw[46] + jnp.where(low_side, xr[0, 0], zero)), cw[47])

    def theirs(i):
        v = xb[i + 1]
        dd = 6.0 + xr[i, 2]
        f = xr[i, 1] - dd * v + beside0(v) + (xb[i] + xb[i + 2])
        put(i + other, f, jnp.where(ok, W / dd, 0.0))

    loop(6, theirs, 6)
    relax(ew, e_out, f_out, c_out, n, 1.0, UR, paired)

    def left(x):
        return own_rows(L0, f_out[x + shift] - d[x] * e_out[x + shift + 1] + paired(e_out, x + shift))

    within = lanes(24) % 64 < 48
    pair = lambda x: jnp.where(within, left(2 * x) + left(2 * x + 1), 0.0)
    half_own(pair, tmp, acc, f1, UL, maps[OWN])
    both = (f1, r1)
    loop(6, lambda g: ztile1(lambda x, a: both[a][x], z1h, z1l, g), 3)


def k_ypack1(f1, r1, zl, zh, up, dn):
    both = (f1, r1)
    ypack1(lambda x, a: both[a][x], zl, zh, up, dn, 12)


def k_windows1(f1, r1, zl, zh, yl, yh, out, spare):
    both = (f1, r1)
    ends = edge(L1, place())

    def some(i):
        for k in range(4):
            for a in range(2):
                plane1(lambda x, a: both[a][x], zl, zh, yl, yh, 4 * i + k, a, out.at[a], 4 * i + k, ends, spare.at[8 * i + 2 * k + a])

    loop(6, some, 6)


def k_down1(win, maps, xr, fw, cw, e_out, f2, c2, e2, out3, rw, ew, tmp, acc, r2, ew2, tmp2, t3, sq):
    ids = place()
    n = L1.nx
    shift = ids[0] * L1.hx
    other = (1 - ids[0]) * L1.n

    def put(x):
        fw[x + shift] = win[0, x]
        rw[x + shift] = win[1, x]

    def take(x):
        fw[x + other] = xr[x, 0]
        rw[x + other] = xr[x, 1]

    loop(24, put, 8)
    loop(12, take, 6)
    ok = inside(L1, ids)
    zero_ends(ew, n)
    zero_ends(e_out, n)

    def first(x):
        c = jnp.where(ok, W / (1.5 + rw[x]), 0.0)
        cw[x] = c
        ew[x + 1] = c * fw[x]

    loop(n, first, 6)
    relax(ew, e_out, fw, cw, n, 0.25, UM, paired)

    def left(x):
        return fw[x] - (1.5 + rw[x]) * e_out[x + 1] + 0.25 * paired(e_out, x)

    for ref, pair in ((f2, lambda x: left(2 * x) + left(2 * x + 1)), (r2, lambda x: rw[2 * x] + rw[2 * x + 1])):
        coarsen_planes(pair, 18, tmp, acc.at[0], 24, 18)
        v = flat(acc.at[0])
        acc[0] = times(v, maps[DOWN1A]).reshape(18, 16, 128)
        acc[1] = times(v, maps[DOWN1B]).reshape(18, 16, 128)

        def keep(x, ref=ref):
            ref[x] = jnp.zeros((32, 128), F32)
            ref[x, 2:14, :] = acc[0, x, 0:12, :]
            ref[x, 14:26, :] = acc[1, x, 0:12, :]

        loop(18, keep, 6)
    ok2 = domain(None, 12, 6, 8, 32, ids)
    zero_ends(ew2, 18)
    zero_ends(e2, 18)

    def second(x):
        c = jnp.where(ok2, W / (0.375 + r2[x]), 0.0)
        c2[x] = c
        ew2[x + 1] = c * f2[x]

    loop(18, second, 6)
    relax(ew2, e2, f2, c2, 18, 0.0625, 18)

    def left2(x):
        return f2[x] - (0.375 + r2[x]) * e2[x + 1] + 0.0625 * neighbours(e2, x)

    for a, pair in enumerate((lambda x: left2(2 * x) + left2(2 * x + 1), lambda x: r2[2 * x] + r2[2 * x + 1])):
        coarsen_planes(pair, 9, tmp2, t3.at[a], 32, 9)
        t3[a] = times(flat(t3.at[a]), maps[DOWN2]).reshape(9, 16, 128)
    shift = ids[0] * 3
    sq[...] = jnp.zeros((128, 128), F32)
    for a in range(2):
        for x in range(6):
            at = a * 36 + x * 6
            sq[at : at + 6, :] = t3[a, x + shift, 4:10, :]
    t = sq[...].T[0:8]
    ln = lanes(1)
    rows = []
    for u in range(2):
        for a in range(2):
            parts = [roll(t, 36 * (w - a), 1)[3 * u + w : 3 * u + w + 1] for w in range(3)]
            rows.append(jnp.where(ln < 36, parts[0], jnp.where(ln < 72, parts[1], parts[2])))
    tile = jnp.concatenate(rows + rows, axis=0)
    n8 = out3.shape[0] // 8
    out3[...] = jnp.broadcast_to(tile[None], (n8, 8, 128)).reshape(n8 * 8, 128)


def sum_all(v):
    s = jnp.sum(v, axis=0)
    s = sum(s[k : k + 8] for k in range(0, s.shape[0], 8))
    return jnp.sum(jnp.sum(s, axis=1, keepdims=True), axis=0, keepdims=True)


def coarse_solve(g3, maps, nx, ny, nz, e3, s3, f3, c3, r3, tmp, f4, r4, sq):
    R = f3.shape[1]
    for ref in (f3, r3):
        ref[...] = jnp.zeros(ref.shape, F32)
    kx, ky, kz = nx // 6, ny // 6, nz // 6
    for bx in range(kx):
        for by in range(ky):
            k = bx * ky + by
            if kz * 6 < 128:
                sq[k, kz * 6 :, :] = jnp.zeros((128 - kz * 6, 128), F32)
            got = [g3[pl.ds(k * kz * 4 + r, kz, stride=4), :] for r in range(4)]
            ln = lanes(kz)
            for u in range(2):
                for w in range(3):
                    f, r = roll(got[2 * u], -36 * w, 1), roll(got[2 * u + 1], 36 - 36 * w, 1)
                    sq[k, pl.ds(3 * u + w, kz, stride=6), :] = jnp.where(ln < 36, f, r)
            t = sq[k].T
            for x in range(6):
                f3[bx * 6 + x, by * 6 : by * 6 + 6, :] = t[x * 6 : x * 6 + 6]
                r3[bx * 6 + x, by * 6 : by * 6 + 6, :] = t[36 + x * 6 : 42 + x * 6]
    factor = 0.25**3
    ok = (lax.broadcasted_iota(jnp.int32, (R, 128), 0) < ny) & (lanes(R) < nz)
    for ref in (e3, s3):
        zero_ends(ref, nx)

    def first(x):
        c = jnp.where(ok, W / (6.0 * factor + r3[x]), 0.0)
        c3[x] = c
        s3[x + 1] = c * f3[x]

    loop(nx, first, 6)
    relax(s3, e3, f3, c3, nx, factor, 12)

    def left(x):
        v = f3[x] - (6.0 * factor + r3[x]) * e3[x + 1] + factor * neighbours(e3, x)
        return jnp.where(ok, v, 0.0)

    for ref, pair in ((f4, lambda x: left(2 * x) + left(2 * x + 1)), (r4, lambda x: r3[2 * x] + r3[2 * x + 1])):
        coarsen_planes(pair, nx // 2, tmp, ref, R, 6)
        ref[...] = times(flat(ref), maps[DOWN3]).reshape(ref.shape)
    f4k = 0.25**4
    H = R // 2
    row = lax.broadcasted_iota(jnp.int32, (nx // 2, H, 128), 1)
    lane = lax.broadcasted_iota(jnp.int32, (nx // 2, H, 128), 2)
    within = (row < ny // 2) & (lane < nz // 2)
    diag = 6.0 * f4k + r4[...]
    zero = jnp.zeros((1, H, 128), F32)

    def apply(p):
        s = jnp.concatenate([zero, p[:-1]], axis=0) + jnp.concatenate([p[1:], zero], axis=0)
        s = s + roll(p, 1, 1) + roll(p, H - 1, 1) + roll(p, 1, 2) + roll(p, 127, 2)
        return jnp.where(within, diag * p - f4k * s, 0.0)

    r = jnp.where(within, f4[...], 0.0)
    p = r
    q = apply(r)
    rr = sum_all(r * r)
    den = sum_all(r * q)
    a = rr / den
    one_over_rr, one_over_a = 1.0 / rr, den / rr
    e = a * p
    for i in range(1, BOTTOM_ITERS):
        r = r - a * q
        w = apply(r)
        new = sum_all(r * r)
        rw = sum_all(r * w)
        b = new * one_over_rr
        den = rw - b * new * one_over_a
        a = new / den
        one_over_rr, one_over_a = 1.0 / new, den / new
        p = r + b * p
        q = w + b * q
        e = e + a * p
    f4[...] = times(e.reshape(nx // 2 * H, 128), maps[UP3]).reshape(e.shape)
    add_refined(f4, nx // 2, e3, s3, 6)
    relax(s3, e3, f3, c3, nx, factor, 12)
    relax(e3, s3, f3, c3, nx, factor, 12)


def k_up(g3, maps, f2, c2, e2i, f1, c1, e1i, f0, c0, d0, e0i, z_out, az_out, sums,
         e3, s3, f3, c3, r3, tmp3, f4, r4, sq, w3, w2, na, nb, n1, e2, s2, e1, s1, e0, s0):
    gx, gy, gz, sy, sz = place()
    nx, ny, nz = f3.shape[0], sy * 6, sz * 6
    coarse_solve(g3, maps, nx, ny, nz, e3, s3, f3, c3, r3, tmp3, f4, r4, sq)
    for ref, n in ((s2, 18), (s1, 36), (s0, 54), (e2, 18), (e1, 36), (e0, 54)):
        zero_ends(ref, n)
    for i in range(9):
        e = s3[i + 1 + gx * 3]
        e = jnp.concatenate([jnp.zeros((8, 128), F32), e, jnp.zeros((8, 128), F32)], axis=0)
        v = e[4:20]
        for k in range(1, sy):
            v = jnp.where(gy == k, e[6 * k + 4 : 6 * k + 20], v)
        w3[i] = v
    w3[...] = times(flat(w3), maps[UP2]).reshape(9, 16, 128)
    add_refined(w3, 9, e2i, e2, 9)
    relax(e2, s2, f2, c2, 18, 0.0625, 18)
    relax(s2, e2, f2, c2, 18, 0.0625, 18)

    def halves(i):
        na[i] = e2[i + 1, 2:18, :]
        nb[i] = e2[i + 1, 14:30, :]

    loop(18, halves, 6)

    w2[...] = (times(flat(na), maps[UP1A]) + times(flat(nb), maps[UP1B])).reshape(18, 16, 128)
    add_refined(w2, 18, e1i, e1, 6)
    relax(e1, s1, f1, c1, 36, 0.25, UM, paired)
    relax(s1, e1, f1, c1, 36, 0.25, UM, paired)

    def near(i):
        v = e1[i + 1 + gx * 9]
        n1[i] = jnp.where(upper(L1, 16), v[0:16], v[8:24])

    loop(27, near, 9)

    n1[...] = times(flat(n1), maps[UP0]).reshape(27, 16, 128)
    add_refined(n1, 27, e0i, e0, 9)
    relax(e0, s0, f0, c0, 54, 1.0, UR, paired)
    relax(s0, e0, f0, c0, 54, 1.0, UR, paired)
    shift = gx * 6
    mine = lanes(24) % 64 < 48

    def last(x, carry):
        u, v = carry
        w = x + shift
        z = e0[w + 1]
        az = own_rows(L0, d0[x] * z - paired(e0, w))
        z = own_rows(L0, z)
        f = own_rows(L0, f0[w])
        z_out[x] = z
        az_out[x] = az
        return u + jnp.where(mine, f * z, 0.0), v + jnp.where(mine, z * az, 0.0)

    def some(i, carry):
        for k in range(UZ):
            carry = last(UZ * i + k, carry)
        return carry

    zero = jnp.zeros((24, 128), F32)
    u, v = lax.fori_loop(0, 48 // UZ, some, (zero, zero))

    def total(t):
        return jnp.sum(jnp.sum(t, axis=1, keepdims=True), axis=0, keepdims=True)

    ln = lanes(sums.shape[0])
    sums[...] = jnp.where(ln == 0, total(u), jnp.where(ln == 1, total(v), 0.0))


def k_last(sums, own, z, az, f, sol, res, sv, rv, sems):
    s = jnp.sum(sums[...], axis=0, keepdims=True)
    ln = lanes(1)
    over = jnp.sum(jnp.where(ln == 0, s, 0.0), axis=1, keepdims=True)
    under = jnp.sum(jnp.where(ln == 1, s, 0.0), axis=1, keepdims=True)
    step = over / under
    shift = lax.axis_index("gx") * 6
    pairs = ((0, sv, sol), (1, rv, res))

    def copy(a, src, dst, i):
        part = pl.ds(i * 8, 8)
        return pltpu.make_async_copy(src.at[part], dst.at[part], sems.at[a, i])

    def some(i):
        for k in range(8):
            x = i * 8 + k
            for ref, v in ((sv, own[0, x] + step * z[x]), (rv, own_rows(L0, f[x + shift]) - step * az[x])):
                ref[x, 0:24, :] = v[:, 0:48]
                ref[x, 24:48, :] = roll(v, 64, 1)[:, 0:48]
        for a, src, dst in pairs:
            copy(a, src, dst, i).start()

    loop(6, some)
    for i in range(6):
        for a, src, dst in pairs:
            copy(a, src, dst, i).wait()


def ring(up, dn, axis, low_first=True):
    n = lax.axis_size(axis)
    rise = [(i, (i + 1) % n) for i in range(n)]
    fall = [(i, (i - 1) % n) for i in range(n)]
    if low_first:
        low = lax.ppermute(up, axis, rise)
        high = lax.ppermute(dn, axis, fall)
    else:
        high = lax.ppermute(dn, axis, fall)
        low = lax.ppermute(up, axis, rise)
    return low, high


def swap(v):
    return lax.ppermute(v, "gx", [(0, 1), (1, 0)])


def body(b, x0, rea):
    ALL = ("gx", "gy", "gz")
    sizes = [lax.axis_size(a) for a in ALL]
    count = sizes[0] * sizes[1] * sizes[2]
    b, x0, rea = (pltpu.with_memory_space_constraint(v, pltpu.HBM) for v in (b, x0, rea))
    hi, lo, own = run(
        k_zpack0,
        (sds(*L0.zshape), sds(*L0.zshape), sds(3, 48, 24, 128)),
        (x0, b, rea),
        [(3, 48, 48, 48), pltpu.SemaphoreType.DMA((3, 4))],
        far_in=True,
    )
    zl, zh = ring(hi, lo, "gz")
    turned, r1, maps = run(
        k_early,
        (sds(3, 24, 16, 128), sds(24, 12, 128), sds(10, 256, 128, dtype=jnp.bfloat16)),
        (own,),
        [(24, 24, 128), (24, 16, 128)],
    )
    up, dn = run(k_ypack0, (sds(*L0.yshape),) * 2, (own, turned, zl, zh))
    yl, yh = ring(up, dn, "gy")
    mid = run(k_zmerge, sds(3, 48, 24, 128), (own, zl, zh, dn))
    xr = swap(run(k_xpack0, sds(*L0.xshape), (mid, yl, yh)))
    p0, q0, o0 = (54, 32, 128), (56, 32, 128), (48, 32, 128)
    xw, part, d0, cw = run(k_windows0, (sds(*o0),) * 4, (mid, yl, yh))
    f0, c0, e0, f1, z1h, z1l = run(
        k_down0,
        (sds(*p0), sds(*p0), sds(*q0), sds(24, 12, 128), sds(*L1.zshape), sds(*L1.zshape)),
        (xw, part, d0, cw, r1, maps, xr),
        [(8, 32, 128), q0, (24, 24, 128), (24, 16, 128)],
        mib=M0,
    )
    zl, zh = ring(z1h, z1l, "gz")
    up, dn = run(k_ypack1, (sds(*L1.yshape),) * 2, (f1, r1, zl, zh))
    yl, yh = ring(up, dn, "gy")
    xr = swap(run(k_xpack1, sds(*L1.xshape), (f1, r1, zl, zh, yl, yh), [(12, 2, 2, 24, 128)]))
    p1, q1, p2, q2 = (36, 24, 128), (38, 24, 128), (18, 32, 128), (20, 32, 128)
    win = run(k_windows1, sds(2, 24, 24, 128), (f1, r1, zl, zh, yl, yh), [(48, 2, 24, 128)])
    f1w, c1w, e1w, f2w, c2w, e2w, g = run(
        k_down1,
        (sds(*p1), sds(*p1), sds(*q1), sds(*p2), sds(*p2), sds(*q2), sds(count * 4, 128)),
        (win, maps, xr),
        [p1, q1, (18, 24, 128), (2, 18, 16, 128), p2, q2, (9, 32, 128), (2, 9, 16, 128), (128, 128)],
        mib=M1,
    )
    g = lax.all_to_all(g, ALL, 0, 0, tiled=True)
    n3 = [6 * s for s in sizes]
    R3 = (n3[1] + 8) // 8 * 8
    if R3 % 16:
        R3 += 8
    p3, q3, p4 = (n3[0], R3, 128), (n3[0] + 2, R3, 128), (n3[0] // 2, R3 // 2, 128)
    z, az, sums = run(
        k_up,
        (sds(48, 24, 128), sds(48, 24, 128), sds(count, 128)),
        (g, maps, f2w, c2w, e2w, f1w, c1w, e1w, f0, c0, d0, e0),
        [q3, q3, p3, p3, p3, (n3[0] // 2, R3, 128), p4, p4, (sizes[0] * sizes[1], 128, 128), (9, 16, 128), (18, 16, 128),
         (18, 16, 128), (18, 16, 128), (27, 16, 128), q2, q2, q1, q1, q0, q0],
        mib=M2,
    )
    sums = lax.all_to_all(sums.reshape(count, 1, 128), ALL, 0, 0, tiled=True).reshape(count, 128)
    return run(
        k_last,
        (sds(48, 48, 48), sds(48, 48, 48)),
        (sums, own, z, az, f0),
        [(48, 48, 48), (48, 48, 48), pltpu.SemaphoreType.DMA((2, 6))],
        far_out=True,
    )


def solution(mesh):
    spec = P("gx", "gy", "gz")
    return jax.shard_map(body, mesh=mesh, in_specs=(spec, spec, spec), out_specs=(spec, spec), check_vma=False)
```

```python
import functools
import jax
import jax.numpy as jnp
from jax import lax
from jax.experimental import pallas as pl
from jax.experimental.pallas import tpu as pltpu
from jax.sharding import PartitionSpec as P

W = 6.0 / 7.0
BOTTOM_ITERS = 6
N0 = 48
F32 = jnp.float32
HI = lax.Precision.HIGHEST
M0, M1, M2 = 10, 8, 12
UF, UR, UM, UZ, UL = 12, 54, 36, 24, 24


class Spec:
    def __init__(self, n, h, na, R, o, hx, cut, kp, st):
        self.n, self.h, self.na, self.R, self.o, self.hx, self.cut, self.kp, self.st = n, h, na, R, o, hx, cut, kp, st
        self.half = n // 2
        self.zshape = (n // (kp * st), self.half * st, 128)
        self.yshape = (self.half, na * h, 128)
        self.hs = (h,) * na
        self.xshape = (hx, na, R, 128)
        self.nx = n + hx

    def slot(self, x, a):
        if self.st == 1:
            h = self.hs[a]
            many = 64 // h
            return ZBASE[a] + lax.div(x, many), 0, h * lax.rem(x, many)
        per = self.n // self.st
        t, y = lax.div(x, per), lax.rem(x, per)
        return lax.div(y, self.kp), t, self.h * (lax.rem(y, self.kp) * self.na + a)


L0 = Spec(48, 5, 3, 32, 8, 6, 56, 4, 1)
L1 = Spec(24, 12, 2, 24, 12, 12, 44, 2, 2)
L0.hs = (5, 4, 4)
ZBASE = (0, 4, 7)
YBASE = (0, 40, 72)
L0.zshape = (10, 24, 128)
L0.yshape = (3, 104, 128)


def sds(*shape, dtype=F32):
    return jax.ShapeDtypeStruct(shape, dtype)


def run(kernel, outs, args, scratch=(), mib=12, far_in=False, far_out=False):
    vmem = pl.BlockSpec(memory_space=pltpu.VMEM)
    hbm = pl.BlockSpec(memory_space=pl.ANY)
    return pl.pallas_call(
        kernel,
        out_shape=outs,
        in_specs=[hbm if far_in else vmem] * len(args),
        out_specs=jax.tree.map(lambda _: hbm if far_out else vmem, outs),
        scratch_shapes=[pltpu.VMEM(s, F32) if isinstance(s, tuple) else s for s in scratch],
        compiler_params=pltpu.CompilerParams(vmem_limit_bytes=mib * 1024 * 1024),
    )(*args)


def place():
    return [lax.axis_index(a) for a in ("gx", "gy", "gz")] + [lax.axis_size(a) for a in ("gy", "gz")]


def lanes(rows):
    return lax.broadcasted_iota(jnp.int32, (rows, 128), 1)


def roll(v, shift, axis):
    if isinstance(shift, int):
        shift = shift % v.shape[axis]
        if shift == 0:
            return v
    return pltpu.roll(v, shift, axis)


def loop(n, f, u=1):
    u = max(d for d in range(1, u + 1) if n % d == 0)

    def some(i, c):
        for k in range(u):
            f(i * u + k)
        return c

    lax.fori_loop(0, n // u, some, 0)


def upper(sp, rows):
    l = lanes(rows)
    return (l >= sp.cut) & (l < sp.cut + 64)


def edge(sp, ids):
    _, gy, gz, ny, nz = ids
    high = jnp.where(gz < nz - 1, sp.n + sp.h, sp.n)
    low = jnp.where(gz > 0, 64 - sp.h, 64)
    return high, low, jnp.where(gy > 0, 1.0, 0.0), jnp.where(gy < ny - 1, 1.0, 0.0)


def ztile(sp, items):
    l = lanes(sp.half)
    hi = [jnp.zeros((sp.half, 128), F32)] * 2
    lo = list(hi)
    for k, (v, at, h) in enumerate(items):
        r = roll(v, at, 1)
        hi[k % 2] = jnp.where(((l + (64 - (at + sp.n - h) % 64)) & 63) < h, r, hi[k % 2])
        lo[k % 2] = jnp.where(((l + (64 - at)) & 63) < h, r, lo[k % 2])
    return roll(hi[0] + hi[1], -2 * sp.n, 1), lo[0] + lo[1]


def ztile1(own, hi_ref, lo_ref, g):
    sp = L1
    for t in range(sp.st):
        items = [
            (own(t * (sp.n // sp.st) + g * sp.kp + k, a), sp.h * (k * sp.na + a), sp.h)
            for k in range(sp.kp)
            for a in range(sp.na)
        ]
        hi, lo = ztile(sp, items)
        hi_ref[g, t * sp.half : (t + 1) * sp.half, :] = hi
        lo_ref[g, t * sp.half : (t + 1) * sp.half, :] = lo


def merged(sp, own, zl, zh, x, a, b, e, top, bottom):
    g, t, at = sp.slot(x, a)
    if sp.st == 1:
        high, low = zh[g, b:e, :], zl[g, b:e, :]
    else:
        high = jnp.where(t == 0, zh[g, b:e, :], zh[g, sp.half + b : sp.half + e, :])
        low = jnp.where(t == 0, zl[g, b:e, :], zl[g, sp.half + b : sp.half + e, :])
    l = lanes(e - b)
    beside = jnp.where(((l + (64 - at)) & 63) < sp.hs[a], high, low)
    beside = roll(beside, (sp.n + 128 - at) & 127, 1)
    q = l & 63
    return jnp.where(q < sp.n, own(x, a)[b:e], jnp.where((q < top) | (q >= bottom), beside, 0.0))


def ypack0(own, turned, zl, zh, up_ref, dn_ref):
    top, bottom, _, _ = edge(L0, place())
    l = lanes(8)
    q = l & 63
    up = upper(L0, 8)

    def beside(x, a, b, turn):
        g, _, at = L0.slot(x, a)
        v = jnp.where(((l + (64 - at)) & 63) < L0.hs[a], zh[g, b : b + 8, :], zl[g, b : b + 8, :])
        v = roll(v, (L0.n + turn + 128 - at) & 127, 1)
        return jnp.where((q < top) | (q >= bottom), v, 0.0)

    def some(i):
        for k in range(8):
            p = 8 * i + k
            for a in range(3):
                h = L0.hs[a]
                for ref, b, s in ((up_ref, 16, 8 - h), (dn_ref, 0, 0)):
                    even = jnp.where(q < L0.n, own[a, 2 * p, b : b + 8, :], beside(2 * p, a, b, 0))
                    odd = jnp.where(q < L0.n, turned[a, p, b // 2 : b // 2 + 8, :], beside(2 * p + 1, a, b, 64))
                    v = jnp.where(up, even, odd) if b else jnp.where(up, odd, even)
                    ref[i, pl.ds(YBASE[a] + k, h, stride=8), :] = v[s : s + h]

    loop(3, some, 3)


def ypack1(own, zl, zh, up_ref, dn_ref, u):
    sp = L1
    half = sp.half
    top, bottom, _, _ = edge(sp, place())

    def pair(p):
        for a in range(sp.na):
            even = merged(sp, own, zl, zh, 2 * p, a, 0, half, top, bottom)
            odd = roll(merged(sp, own, zl, zh, 2 * p + 1, a, 0, half, top, bottom), 64, 1)
            up = upper(sp, half)
            up_ref[p, a * half : (a + 1) * half, :] = jnp.where(up, even, odd)
            dn_ref[p, a * half : (a + 1) * half, :] = jnp.where(up, odd, even)

    loop(half, pair, u)


def y_tiles0(yl, yh, g, t, a):
    def rows(ref, start):
        return ref[g, pl.ds(start + t, 8, stride=8), :]

    if a == 0:
        return roll(rows(yl, 0), 3, 0), rows(yh, 0)
    return rows(yl, YBASE[a] - 32), rows(yh, 40) if a == 1 else roll(rows(yh, 40), 4, 0)


def plane0(m, tiles, ends, turn):
    _, _, below, above = ends
    low, high = tiles
    lower = jnp.concatenate([roll(low, turn, 1) * below, m], axis=0)
    higher = jnp.concatenate([m, roll(high, turn, 1) * above], axis=0)
    return jnp.where(upper(L0, L0.R), higher, lower)


def plane1(own, zl, zh, yl, yh, x, a, dst, xw, ends, spare):
    top, bottom, below, above = ends
    sp = L1
    h, half = sp.h, sp.half
    m = merged(sp, own, zl, zh, x, a, 0, half, top, bottom)
    p = lax.div(x, 2)
    turn = 64 * (1 - lax.rem(x, 2))
    spare[0, 0:h, :] = roll(yl[p, a * h : (a + 1) * h, :], turn, 1) * below
    spare[0, h:, :] = m
    spare[1, 0:half, :] = m
    spare[1, half:, :] = roll(yh[p, a * h : (a + 1) * h, :], turn, 1) * above
    dst[xw] = jnp.where(upper(sp, sp.R), spare[1], spare[0])


def lane_z(sp, l):
    return jnp.where(l < sp.cut, l, jnp.where(l < sp.cut + 64, l - 64, l - 128))


def inside(sp, ids):
    _, gy, gz, ny, nz = ids
    n, h = sp.n, min(sp.hs)
    y = lax.broadcasted_iota(jnp.int32, (sp.R, 128), 0) - sp.o + jnp.where(upper(sp, sp.R), sp.R, 0)
    z = lane_z(sp, lanes(sp.R))
    ok = (y >= -h) & (y < n + h) & (z >= -h) & (z < n + h)
    y, z = y + gy * n, z + gz * n
    return ok & (y >= 0) & (y < ny * n) & (z >= 0) & (z < nz * n)


def paired(ref, x):
    c = ref[x + 1]
    R = c.shape[0]
    s = ref[x] + ref[x + 2]
    sub = lax.broadcasted_iota(jnp.int32, (8, 128), 0)
    seam = roll(jnp.where(sub == 0, c[0:8], c[R - 8 : R]), 64, 1)
    last = jnp.where(sub == 7, roll(seam, 7, 0), roll(c[R - 8 :], 7, 0))
    first = jnp.where(sub == 0, roll(seam, 1, 0), roll(c[0:8], 1, 0))
    up = jnp.concatenate([ref[x + 1, 1 : R - 7, :], last], axis=0)
    down = jnp.concatenate([first, ref[x + 1, 7 : R - 1, :]], axis=0)
    s = s + (up + down)
    return s + (roll(c, 1, 1) + roll(c, 127, 1))


def domain(sp, n, h, r0, R, ids):
    row = lax.broadcasted_iota(jnp.int32, (R, 128), 0) - r0
    ln = lanes(R)
    z = jnp.where(ln < 64, ln, ln - 128)
    gy, gz, ny, nz = ids[1], ids[2], ids[3], ids[4]
    y_at, z_at = row + gy * n, z + gz * n
    ok = (row >= -h) & (row < n + h) & (z >= -h) & (z < n + h)
    return ok & (y_at >= 0) & (y_at < ny * n) & (z_at >= 0) & (z_at < nz * n)


def neighbours(ref, x):
    c = ref[x + 1]
    R = c.shape[0]
    s = ref[x] + ref[x + 2]
    s = s + (roll(c, 1, 0) + roll(c, R - 1, 0))
    return s + (roll(c, 1, 1) + roll(c, 127, 1))


def zero_ends(ref, n):
    ref[0] = jnp.zeros(ref.shape[1:], F32)
    ref[n + 1] = jnp.zeros(ref.shape[1:], F32)


def relax(src, dst, f, c, n, factor, u=9, near=None):
    near = near or neighbours

    def one(x):
        dst[x + 1] = (1.0 - W) * src[x + 1] + c[x] * (f[x] + factor * near(src, x))

    loop(n, one, u)


def lane_map(pick, value):
    l = lax.broadcasted_iota(jnp.int32, (256, 128), 0) & 127
    m = lax.broadcasted_iota(jnp.int32, (256, 128), 1)
    return jnp.where(pick(l) == m, value, 0.0).astype(jnp.bfloat16)


def spread_map(pick):
    m = lax.broadcasted_iota(jnp.int32, (256, 128), 0) & 127
    l = lax.broadcasted_iota(jnp.int32, (256, 128), 1)
    return jnp.where(pick(l) == m, 1.0, 0.0).astype(jnp.bfloat16)


def floor_half(z):
    return lax.shift_right_arithmetic(z, 1)


def coarse_lane(sp, l, want):
    z = lane_z(sp, l)
    up = (l >= sp.cut) & (l < sp.cut + 64)
    good = (z >= -sp.h) & (z < sp.n + sp.h)
    good = good & (up if want else jnp.logical_not(up))
    return jnp.where(good, floor_half(z) + jnp.where(z < 0, 128, 0), -1)


def both_lanes(l):
    lower, higher = coarse_lane(L0, l, False), coarse_lane(L0, l, True)
    return jnp.where(lower >= 0, lower, jnp.where(higher >= 0, (higher + 64) & 127, -1))


OWN, DOWN1A, DOWN1B, DOWN2, DOWN3, UP3, UP2, UP1A, UP1B, UP0 = range(10)


def all_maps(maps, gz):
    half = floor_half
    maps[OWN] = lane_map(lambda l: jnp.where(l < 64, half(l), 32 + half(l)), 0.125)
    maps[DOWN1A] = lane_map(lambda l: coarse_lane(L1, l, False), 0.125)
    maps[DOWN1B] = lane_map(lambda l: coarse_lane(L1, l, True), 0.125)
    maps[DOWN2] = lane_map(lambda l: jnp.where(l < 64, half(l), half(l) + 64), 0.125)
    maps[DOWN3] = lane_map(half, 0.125)
    maps[UP3] = spread_map(half)
    maps[UP2] = spread_map(lambda l: gz * 6 + jnp.where(l < 64, half(l), half(l) - 64))
    maps[UP1A] = spread_map(lambda l: coarse_lane(L1, l, False))
    maps[UP1B] = spread_map(lambda l: coarse_lane(L1, l, True))
    maps[UP0] = spread_map(both_lanes)


def times(v, m):
    big = v.astype(jnp.bfloat16)
    rest = (v - big.astype(F32)).astype(jnp.bfloat16)
    return jnp.dot(jnp.concatenate([big, rest], axis=1), m, preferred_element_type=F32)


def coarsen_planes(pair, n, tmp, acc, rows, u=2):
    half = rows // 2

    def one(x):
        tmp[x, 0:rows, :] = pair(x)
        acc[x, 0:half, :] = tmp[x, pl.ds(0, half, stride=2), :] + tmp[x, pl.ds(1, half, stride=2), :]

    loop(n, one, u)


def flat(ref):
    n, rows, _ = ref.shape
    return ref[...].reshape(n * rows, 128)


def add_refined(wide, n, src, dst, u=3):
    R = dst.shape[1]

    def one(i):
        v = wide[i, 0 : R // 2, :]
        for k in range(2):
            dst[2 * i + 1, pl.ds(k, R // 2, stride=2), :] = v
        t = dst[2 * i + 1]
        dst[2 * i + 1] = src[2 * i + 1] + t
        dst[2 * i + 2] = src[2 * i + 2] + t

    loop(n, one, u)


def k_zpack0(x0, b, rea, hi, lo, own, raw, sems):
    def copy(a, ref, i):
        many = 64 // L0.hs[a]
        part = pl.ds(i * many, many)
        return pltpu.make_async_copy(ref.at[part], raw.at[a, part], sems.at[a, i])

    refs = (x0, b, rea)
    parts = [48 * h // (64 // h * h) for h in L0.hs]
    for a, ref in enumerate(refs):
        for i in range(parts[a]):
            copy(a, ref, i).start()

    def pack(a, i):
        h = L0.hs[a]
        many = 64 // h
        hi[ZBASE[a] + i], lo[ZBASE[a] + i] = ztile(L0, [(own[a, i * many + k], h * k, h) for k in range(many)])

    steps = [(a, ref, i) for a, ref in enumerate(refs) for i in range(parts[a])]
    for n, (a, ref, i) in enumerate(steps):
        copy(a, ref, i).wait()
        if n:
            pack(steps[n - 1][0], steps[n - 1][2])
        many = 64 // L0.hs[a]
        for x in range(i * many, i * many + many):
            own[a, x, :, 0:48] = raw[a, x, 0:24, :]
            own[a, x, :, 64:112] = raw[a, x, 24:48, :]
    pack(steps[-1][0], steps[-1][2])


def k_ypack0(own, turned, zl, zh, up, dn):
    ypack0(own, turned, zl, zh, up, dn)


def k_xpack0(mid, yl, yh, out):
    ids = place()
    ends = edge(L0, ids)
    first = ids[0] == 0
    for i in range(6):
        x = jnp.where(first, 42, 0) + i
        for a in range(3):
            there, here = y_tiles0(yl, yh, 2, 5 + i // 2, a), y_tiles0(yl, yh, 0, i // 2, a)
            tiles = [jnp.where(first, v, w) for v, w in zip(there, here)]
            out[i, a] = plane0(mid[a, x], tiles, ends, 64 * (1 - i % 2))


def k_xpack1(f1, r1, zl, zh, yl, yh, out, spare):
    both = (f1, r1)
    ids = place()
    ends = edge(L1, ids)

    def one(i):
        for a in range(2):
            plane1(lambda x, a: both[a][x], zl, zh, yl, yh, (1 - ids[0]) * 12 + i, a, out.at[i], a, ends, spare.at[i, a])

    loop(12, one, 12)


def beside0(c):
    R = L0.R
    sub = lax.broadcasted_iota(jnp.int32, (8, 128), 0)
    seam = roll(jnp.where(sub == 0, c[0:8], c[R - 8 : R]), 64, 1)
    up, down = roll(c, R - 1, 0), roll(c, 1, 0)
    up = jnp.concatenate([up[: R - 8], jnp.where(sub == 7, roll(seam, 7, 0), up[R - 8 :])], axis=0)
    down = jnp.concatenate([jnp.where(sub == 0, roll(seam, 1, 0), down[0:8]), down[8:]], axis=0)
    return (up + down) + (roll(c, 1, 1) + roll(c, 127, 1))


def k_windows0(mid, yl, yh, xw, part, d_out, c_out):
    ids = place()
    ends = edge(L0, ids)
    ok = inside(L0, ids)

    def some(i):
        for k in range(16):
            x = 16 * i + k
            v, b, rea = (plane0(mid[a, x], y_tiles0(yl, yh, i, k // 2, a), ends, 64 * (1 - k % 2)) for a in range(3))
            d = 6.0 + rea
            xw[x] = v
            part[x] = b - d * v + beside0(v)
            d_out[x] = d
            c_out[x] = jnp.where(ok, W / d, 0.0)

    loop(3, some)


def own_rows(sp, v):
    return jnp.where(upper(sp, sp.half), v[0 : sp.half], v[sp.o :])


def half_own(pair, tmp, acc, out, u, m):
    coarsen_planes(pair, 24, tmp, acc, 24, u)
    acc[...] = times(flat(acc), m).reshape(24, 16, 128)

    def keep(x):
        out[x] = acc[x, 0:12, :]

    loop(24, keep, 6)


def k_zmerge(own, zl, zh, dn, out):
    top, bottom, _, _ = edge(L0, place())

    def one(x):
        for a in range(3):
            out[a, x] = merged(L0, lambda x, a: own[a, x], zl, zh, x, a, 0, 24, top, bottom)

    loop(48, one, 8)


def k_early(own, turned, r1, maps, tmp, acc):
    def turn(p):
        for a in range(3):
            v = own[a, 2 * p + 1]
            turned[a, p, 0:8, :] = roll(v[0:8], 64, 1)
            turned[a, p, 8:16, :] = roll(v[16:24], 64, 1)

    loop(24, turn, 4)
    all_maps(maps, lax.axis_index("gz"))
    mine = lanes(24) % 64 < 48
    half_own(lambda x: jnp.where(mine, own[2, 2 * x] + own[2, 2 * x + 1], 0.0), tmp, acc, r1, 4, maps[OWN])


def k_down0(xw, part, d, cw, r1, maps, xr, f_out, c_out, e_out, f1, z1h, z1l, xb, ew, tmp, acc):
    ids = place()
    n = L0.nx
    shift = ids[0] * L0.hx
    other = (1 - ids[0]) * L0.n
    low_side = ids[0] == 0
    ok = inside(L0, ids)
    zero_ends(ew, n)
    zero_ends(e_out, n)
    zero = jnp.zeros((L0.R, 128), F32)
    xb[0] = jnp.where(low_side, xw[47], zero)
    xb[7] = jnp.where(low_side, zero, xw[0])
    for i in range(6):
        xb[i + 1] = xr[i, 0]

    def put(w, f, c):
        f_out[w] = f
        c_out[w] = c
        ew[w + 1] = c * f

    def mine(x):
        put(x + shift, part[x] + (xw[x - 1] + xw[x + 1]), cw[x])

    loop(46, lambda i: mine(i + 1), 46)
    put(shift, part[0] + (jnp.where(low_side, zero, xr[5, 0]) + xw[1]), cw[0])
    put(47 + shift, part[47] + (xw[46] + jnp.where(low_side, xr[0, 0], zero)), cw[47])

    def theirs(i):
        v = xb[i + 1]
        dd = 6.0 + xr[i, 2]
        f = xr[i, 1] - dd * v + beside0(v) + (xb[i] + xb[i + 2])
        put(i + other, f, jnp.where(ok, W / dd, 0.0))

    loop(6, theirs, 6)
    relax(ew, e_out, f_out, c_out, n, 1.0, UR, paired)

    def left(x):
        return own_rows(L0, f_out[x + shift] - d[x] * e_out[x + shift + 1] + paired(e_out, x + shift))

    within = lanes(24) % 64 < 48
    pair = lambda x: jnp.where(within, left(2 * x) + left(2 * x + 1), 0.0)
    half_own(pair, tmp, acc, f1, UL, maps[OWN])
    both = (f1, r1)
    loop(6, lambda g: ztile1(lambda x, a: both[a][x], z1h, z1l, g), 3)


def k_ypack1(f1, r1, zl, zh, up, dn):
    both = (f1, r1)
    ypack1(lambda x, a: both[a][x], zl, zh, up, dn, 12)


def k_windows1(f1, r1, zl, zh, yl, yh, out, spare):
    both = (f1, r1)
    ends = edge(L1, place())

    def some(i):
        for k in range(4):
            for a in range(2):
                plane1(lambda x, a: both[a][x], zl, zh, yl, yh, 4 * i + k, a, out.at[a], 4 * i + k, ends, spare.at[2 * k + a])

    loop(6, some)


def k_down1(win, maps, xr, fw, cw, e_out, f2, c2, e2, out3, rw, ew, tmp, acc, r2, ew2, tmp2, t3, sq):
    ids = place()
    n = L1.nx
    shift = ids[0] * L1.hx
    other = (1 - ids[0]) * L1.n

    def put(x):
        fw[x + shift] = win[0, x]
        rw[x + shift] = win[1, x]

    def take(x):
        fw[x + other] = xr[x, 0]
        rw[x + other] = xr[x, 1]

    loop(24, put, 8)
    loop(12, take, 6)
    ok = inside(L1, ids)
    zero_ends(ew, n)
    zero_ends(e_out, n)

    def first(x):
        c = jnp.where(ok, W / (1.5 + rw[x]), 0.0)
        cw[x] = c
        ew[x + 1] = c * fw[x]

    loop(n, first, 6)
    relax(ew, e_out, fw, cw, n, 0.25, UM, paired)

    def left(x):
        return fw[x] - (1.5 + rw[x]) * e_out[x + 1] + 0.25 * paired(e_out, x)

    for ref, pair in ((f2, lambda x: left(2 * x) + left(2 * x + 1)), (r2, lambda x: rw[2 * x] + rw[2 * x + 1])):
        coarsen_planes(pair, 18, tmp, acc.at[0], 24, 18)
        v = flat(acc.at[0])
        acc[0] = times(v, maps[DOWN1A]).reshape(18, 16, 128)
        acc[1] = times(v, maps[DOWN1B]).reshape(18, 16, 128)

        def keep(x, ref=ref):
            ref[x] = jnp.zeros((32, 128), F32)
            ref[x, 2:14, :] = acc[0, x, 0:12, :]
            ref[x, 14:26, :] = acc[1, x, 0:12, :]

        loop(18, keep, 6)
    ok2 = domain(None, 12, 6, 8, 32, ids)
    zero_ends(ew2, 18)
    zero_ends(e2, 18)

    def second(x):
        c = jnp.where(ok2, W / (0.375 + r2[x]), 0.0)
        c2[x] = c
        ew2[x + 1] = c * f2[x]

    loop(18, second, 6)
    relax(ew2, e2, f2, c2, 18, 0.0625, 18)

    def left2(x):
        return f2[x] - (0.375 + r2[x]) * e2[x + 1] + 0.0625 * neighbours(e2, x)

    for a, pair in enumerate((lambda x: left2(2 * x) + left2(2 * x + 1), lambda x: r2[2 * x] + r2[2 * x + 1])):
        coarsen_planes(pair, 9, tmp2, t3.at[a], 32, 9)
        t3[a] = times(flat(t3.at[a]), maps[DOWN2]).reshape(9, 16, 128)
    shift = ids[0] * 3
    sq[...] = jnp.zeros((128, 128), F32)
    for a in range(2):
        for x in range(6):
            at = a * 36 + x * 6
            sq[at : at + 6, :] = t3[a, x + shift, 4:10, :]
    t = sq[...].T[0:8]
    ln = lanes(1)
    rows = []
    for u in range(2):
        for a in range(2):
            parts = [roll(t, 36 * (w - a), 1)[3 * u + w : 3 * u + w + 1] for w in range(3)]
            rows.append(jnp.where(ln < 36, parts[0], jnp.where(ln < 72, parts[1], parts[2])))
    tile = jnp.concatenate(rows + rows, axis=0)
    n8 = out3.shape[0] // 8
    out3[...] = jnp.broadcast_to(tile[None], (n8, 8, 128)).reshape(n8 * 8, 128)


def sum_all(v):
    s = jnp.sum(v, axis=0)
    s = sum(s[k : k + 8] for k in range(0, s.shape[0], 8))
    return jnp.sum(jnp.sum(s, axis=1, keepdims=True), axis=0, keepdims=True)


def coarse_solve(g3, maps, nx, ny, nz, e3, s3, f3, c3, r3, tmp, f4, r4, sq):
    R = f3.shape[1]
    for ref in (f3, r3):
        ref[...] = jnp.zeros(ref.shape, F32)
    kx, ky, kz = nx // 6, ny // 6, nz // 6
    for bx in range(kx):
        for by in range(ky):
            k = bx * ky + by
            if kz * 6 < 128:
                sq[k, kz * 6 :, :] = jnp.zeros((128 - kz * 6, 128), F32)
            got = [g3[pl.ds(k * kz * 4 + r, kz, stride=4), :] for r in range(4)]
            ln = lanes(kz)
            for u in range(2):
                for w in range(3):
                    f, r = roll(got[2 * u], -36 * w, 1), roll(got[2 * u + 1], 36 - 36 * w, 1)
                    sq[k, pl.ds(3 * u + w, kz, stride=6), :] = jnp.where(ln < 36, f, r)
            t = sq[k].T
            for x in range(6):
                f3[bx * 6 + x, by * 6 : by * 6 + 6, :] = t[x * 6 : x * 6 + 6]
                r3[bx * 6 + x, by * 6 : by * 6 + 6, :] = t[36 + x * 6 : 42 + x * 6]
    factor = 0.25**3
    ok = (lax.broadcasted_iota(jnp.int32, (R, 128), 0) < ny) & (lanes(R) < nz)
    for ref in (e3, s3):
        zero_ends(ref, nx)

    def first(x):
        c = jnp.where(ok, W / (6.0 * factor + r3[x]), 0.0)
        c3[x] = c
        s3[x + 1] = c * f3[x]

    loop(nx, first, 6)
    relax(s3, e3, f3, c3, nx, factor, 12)

    def left(x):
        v = f3[x] - (6.0 * factor + r3[x]) * e3[x + 1] + factor * neighbours(e3, x)
        return jnp.where(ok, v, 0.0)

    for ref, pair in ((f4, lambda x: left(2 * x) + left(2 * x + 1)), (r4, lambda x: r3[2 * x] + r3[2 * x + 1])):
        coarsen_planes(pair, nx // 2, tmp, ref, R, 6)
        ref[...] = times(flat(ref), maps[DOWN3]).reshape(ref.shape)
    f4k = 0.25**4
    H = R // 2
    row = lax.broadcasted_iota(jnp.int32, (nx // 2, H, 128), 1)
    lane = lax.broadcasted_iota(jnp.int32, (nx // 2, H, 128), 2)
    within = (row < ny // 2) & (lane < nz // 2)
    diag = 6.0 * f4k + r4[...]
    zero = jnp.zeros((1, H, 128), F32)

    def apply(p):
        s = jnp.concatenate([zero, p[:-1]], axis=0) + jnp.concatenate([p[1:], zero], axis=0)
        s = s + roll(p, 1, 1) + roll(p, H - 1, 1) + roll(p, 1, 2) + roll(p, 127, 2)
        return jnp.where(within, diag * p - f4k * s, 0.0)

    r = jnp.where(within, f4[...], 0.0)
    p = r
    q = apply(r)
    rr = sum_all(r * r)
    den = sum_all(r * q)
    a = rr / den
    one_over_rr, one_over_a = 1.0 / rr, den / rr
    e = a * p
    for i in range(1, BOTTOM_ITERS):
        r = r - a * q
        w = apply(r)
        new = sum_all(r * r)
        rw = sum_all(r * w)
        b = new * one_over_rr
        den = rw - b * new * one_over_a
        a = new / den
        one_over_rr, one_over_a = 1.0 / new, den / new
        p = r + b * p
        q = w + b * q
        e = e + a * p
    f4[...] = times(e.reshape(nx // 2 * H, 128), maps[UP3]).reshape(e.shape)
    add_refined(f4, nx // 2, e3, s3, 6)
    relax(s3, e3, f3, c3, nx, factor, 12)
    relax(e3, s3, f3, c3, nx, factor, 12)


def k_up(g3, maps, f2, c2, e2i, f1, c1, e1i, f0, c0, d0, e0i, z_out, az_out, sums,
         e3, s3, f3, c3, r3, tmp3, f4, r4, sq, w3, w2, na, nb, n1, e2, s2, e1, s1, e0, s0):
    gx, gy, gz, sy, sz = place()
    nx, ny, nz = f3.shape[0], sy * 6, sz * 6
    coarse_solve(g3, maps, nx, ny, nz, e3, s3, f3, c3, r3, tmp3, f4, r4, sq)
    for ref, n in ((s2, 18), (s1, 36), (s0, 54), (e2, 18), (e1, 36), (e0, 54)):
        zero_ends(ref, n)
    for i in range(9):
        e = s3[i + 1 + gx * 3]
        e = jnp.concatenate([jnp.zeros((8, 128), F32), e, jnp.zeros((8, 128), F32)], axis=0)
        v = e[4:20]
        for k in range(1, sy):
            v = jnp.where(gy == k, e[6 * k + 4 : 6 * k + 20], v)
        w3[i] = v
    w3[...] = times(flat(w3), maps[UP2]).reshape(9, 16, 128)
    add_refined(w3, 9, e2i, e2, 9)
    relax(e2, s2, f2, c2, 18, 0.0625, 18)
    relax(s2, e2, f2, c2, 18, 0.0625, 18)

    def halves(i):
        na[i] = e2[i + 1, 2:18, :]
        nb[i] = e2[i + 1, 14:30, :]

    loop(18, halves, 6)

    w2[...] = (times(flat(na), maps[UP1A]) + times(flat(nb), maps[UP1B])).reshape(18, 16, 128)
    add_refined(w2, 18, e1i, e1, 6)
    relax(e1, s1, f1, c1, 36, 0.25, UM, paired)
    relax(s1, e1, f1, c1, 36, 0.25, UM, paired)

    def near(i):
        v = e1[i + 1 + gx * 9]
        n1[i] = jnp.where(upper(L1, 16), v[0:16], v[8:24])

    loop(27, near, 9)

    n1[...] = times(flat(n1), maps[UP0]).reshape(27, 16, 128)
    add_refined(n1, 27, e0i, e0, 9)
    relax(e0, s0, f0, c0, 54, 1.0, UR, paired)
    relax(s0, e0, f0, c0, 54, 1.0, UR, paired)
    shift = gx * 6
    mine = lanes(24) % 64 < 48

    def last(x, carry):
        u, v = carry
        w = x + shift
        z = e0[w + 1]
        az = own_rows(L0, d0[x] * z - paired(e0, w))
        z = own_rows(L0, z)
        f = own_rows(L0, f0[w])
        z_out[x] = z
        az_out[x] = az
        return u + jnp.where(mine, f * z, 0.0), v + jnp.where(mine, z * az, 0.0)

    def some(i, carry):
        for k in range(UZ):
            carry = last(UZ * i + k, carry)
        return carry

    zero = jnp.zeros((24, 128), F32)
    u, v = lax.fori_loop(0, 48 // UZ, some, (zero, zero))

    def total(t):
        return jnp.sum(jnp.sum(t, axis=1, keepdims=True), axis=0, keepdims=True)

    ln = lanes(sums.shape[0])
    sums[...] = jnp.where(ln == 0, total(u), jnp.where(ln == 1, total(v), 0.0))


def k_last(sums, own, z, az, f, sol, res, sv, rv, sems):
    s = jnp.sum(sums[...], axis=0, keepdims=True)
    ln = lanes(1)
    over = jnp.sum(jnp.where(ln == 0, s, 0.0), axis=1, keepdims=True)
    under = jnp.sum(jnp.where(ln == 1, s, 0.0), axis=1, keepdims=True)
    step = over / under
    shift = lax.axis_index("gx") * 6
    pairs = ((0, sv, sol), (1, rv, res))

    def copy(a, src, dst, i):
        part = pl.ds(i * 8, 8)
        return pltpu.make_async_copy(src.at[part], dst.at[part], sems.at[a, i])

    def some(i):
        for k in range(8):
            x = i * 8 + k
            for ref, v in ((sv, own[0, x] + step * z[x]), (rv, own_rows(L0, f[x + shift]) - step * az[x])):
                ref[x, 0:24, :] = v[:, 0:48]
                ref[x, 24:48, :] = roll(v, 64, 1)[:, 0:48]
        for a, src, dst in pairs:
            copy(a, src, dst, i).start()

    loop(6, some)
    for i in range(6):
        for a, src, dst in pairs:
            copy(a, src, dst, i).wait()


def ring(up, dn, axis, low_first=True):
    n = lax.axis_size(axis)
    rise = [(i, (i + 1) % n) for i in range(n)]
    fall = [(i, (i - 1) % n) for i in range(n)]
    if low_first:
        low = lax.ppermute(up, axis, rise)
        high = lax.ppermute(dn, axis, fall)
    else:
        high = lax.ppermute(dn, axis, fall)
        low = lax.ppermute(up, axis, rise)
    return low, high


def swap(v):
    return lax.ppermute(v, "gx", [(0, 1), (1, 0)])


def body(b, x0, rea):
    ALL = ("gx", "gy", "gz")
    sizes = [lax.axis_size(a) for a in ALL]
    count = sizes[0] * sizes[1] * sizes[2]
    b, x0, rea = (pltpu.with_memory_space_constraint(v, pltpu.HBM) for v in (b, x0, rea))
    hi, lo, own = run(
        k_zpack0,
        (sds(*L0.zshape), sds(*L0.zshape), sds(3, 48, 24, 128)),
        (x0, b, rea),
        [(3, 48, 48, 48), pltpu.SemaphoreType.DMA((3, 4))],
        far_in=True,
    )
    zl, zh = ring(hi, lo, "gz")
    turned, r1, maps = run(
        k_early,
        (sds(3, 24, 16, 128), sds(24, 12, 128), sds(10, 256, 128, dtype=jnp.bfloat16)),
        (own,),
        [(24, 24, 128), (24, 16, 128)],
    )
    up, dn = run(k_ypack0, (sds(*L0.yshape),) * 2, (own, turned, zl, zh))
    yl, yh = ring(up, dn, "gy")
    mid = run(k_zmerge, sds(3, 48, 24, 128), (own, zl, zh, dn))
    xr = swap(run(k_xpack0, sds(*L0.xshape), (mid, yl, yh)))
    p0, q0, o0 = (54, 32, 128), (56, 32, 128), (48, 32, 128)
    xw, part, d0, cw = run(k_windows0, (sds(*o0),) * 4, (mid, yl, yh))
    f0, c0, e0, f1, z1h, z1l = run(
        k_down0,
        (sds(*p0), sds(*p0), sds(*q0), sds(24, 12, 128), sds(*L1.zshape), sds(*L1.zshape)),
        (xw, part, d0, cw, r1, maps, xr),
        [(8, 32, 128), q0, (24, 24, 128), (24, 16, 128)],
        mib=M0,
    )
    zl, zh = ring(z1h, z1l, "gz")
    up, dn = run(k_ypack1, (sds(*L1.yshape),) * 2, (f1, r1, zl, zh))
    yl, yh = ring(up, dn, "gy")
    xr = swap(run(k_xpack1, sds(*L1.xshape), (f1, r1, zl, zh, yl, yh), [(12, 2, 2, 24, 128)]))
    p1, q1, p2, q2 = (36, 24, 128), (38, 24, 128), (18, 32, 128), (20, 32, 128)
    win = run(k_windows1, sds(2, 24, 24, 128), (f1, r1, zl, zh, yl, yh), [(8, 2, 24, 128)])
    f1w, c1w, e1w, f2w, c2w, e2w, g = run(
        k_down1,
        (sds(*p1), sds(*p1), sds(*q1), sds(*p2), sds(*p2), sds(*q2), sds(count * 4, 128)),
        (win, maps, xr),
        [p1, q1, (18, 24, 128), (2, 18, 16, 128), p2, q2, (9, 32, 128), (2, 9, 16, 128), (128, 128)],
        mib=M1,
    )
    g = lax.all_to_all(g, ALL, 0, 0, tiled=True)
    n3 = [6 * s for s in sizes]
    R3 = (n3[1] + 8) // 8 * 8
    if R3 % 16:
        R3 += 8
    p3, q3, p4 = (n3[0], R3, 128), (n3[0] + 2, R3, 128), (n3[0] // 2, R3 // 2, 128)
    z, az, sums = run(
        k_up,
        (sds(48, 24, 128), sds(48, 24, 128), sds(count, 128)),
        (g, maps, f2w, c2w, e2w, f1w, c1w, e1w, f0, c0, d0, e0),
        [q3, q3, p3, p3, p3, (n3[0] // 2, R3, 128), p4, p4, (sizes[0] * sizes[1], 128, 128), (9, 16, 128), (18, 16, 128),
         (18, 16, 128), (18, 16, 128), (27, 16, 128), q2, q2, q1, q1, q0, q0],
        mib=M2,
    )
    sums = lax.all_to_all(sums.reshape(count, 1, 128), ALL, 0, 0, tiled=True).reshape(count, 128)
    return run(
        k_last,
        (sds(48, 48, 48), sds(48, 48, 48)),
        (sums, own, z, az, f0),
        [(48, 48, 48), (48, 48, 48), pltpu.SemaphoreType.DMA((2, 6))],
        far_out=True,
    )


def solution(mesh):
    spec = P("gx", "gy", "gz")
    return jax.shard_map(body, mesh=mesh, in_specs=(spec, spec, spec), out_specs=(spec, spec), check_vma=False)
```
